32 devices in a mesh: dp: 2 (over x), tp: 4 (over z), sp: 4 (over y, core).
Axes of the slice: x: 2, y: 2, z: 4, core: 2. Of those that a mesh axis runs over, the one named last changes fastest.
Arguments:
- hidden: bfloat16 [32768, 2048], P(('dp', 'sp')), parts along dimension 0
- w_query: bfloat16 [2048, 2048], P(None, 'tp')
- w_key: bfloat16 [2048, 2048], P(None, 'tp')
- w_value: bfloat16 [2048, 2048], P(None, 'tp')
- w_out: bfloat16 [2048, 2048], P('tp')
- branch_bias: float32 [4, 8], replicated
Outputs:
- output: bfloat16 [32768, 2048], P(('dp', 'sp'), 'tp'), parts along dimension 0
There are 2 independent parts. The reference program is written for one: setup_inputs(seed, part) draws one part's arguments, and reference() takes and returns one part's arrays. A program takes and returns all parts, laid end to end along the dimension named above; an argument that names none is the same for every part.
All inputs are finite; a program needn't handle non-finite values.
Results may differ from the reference program's by a relative error of at most 0.00343.
Values are sent between devices in bfloat16 or wider.
A program may use at most 1 GiB of HBM per device.

```python
import jax
import jax.numpy as jnp
from jax import lax

MODEL_DIM = 2048
NUM_HEADS = 8
NUM_BRANCHES = 4
SEQ_LEN = 16384
SEG_BASE = 2048

HEAD_DIM = MODEL_DIM // NUM_HEADS
LOGIT_SCALE = HEAD_DIM ** -0.5


def setup_inputs(seed: int = 0, part: int = 0) -> dict:
    root_key = jax.random.key(seed)
    hidden_key = jax.random.fold_in(jax.random.fold_in(root_key, 1), part)
    key_list = jax.random.split(jax.random.fold_in(root_key, 2), 5)
    fan_scale = MODEL_DIM ** -0.5

    def weight(key_w, gain_factor):
        drawn = jax.random.normal(key_w, (MODEL_DIM, MODEL_DIM), jnp.float32)
        return (drawn * (gain_factor * fan_scale)).astype(jnp.bfloat16)

    hidden = jax.random.normal(hidden_key, (SEQ_LEN, MODEL_DIM), jnp.float32)
    branch_bias = jax.random.normal(key_list[4], (NUM_BRANCHES, NUM_HEADS), jnp.float32)
    return {'hidden': hidden.astype(jnp.bfloat16), 'w_query': weight(key_list[0], 1.5), 'w_key': weight(key_list[1], 1.5), 'w_value': weight(key_list[2], 1.0), 'w_out': weight(key_list[3], 2.0), 'branch_bias': branch_bias}


def attend_block(blocks):
    q_blk, k_blk, v_blk = blocks
    logits = jnp.dot(q_blk, k_blk.T, preferred_element_type=jnp.float32) * LOGIT_SCALE
    row_max = jnp.max(logits, axis=-1, keepdims=True)
    weights = jnp.exp(logits - row_max)
    row_sum = jnp.sum(weights, axis=-1, keepdims=True)
    numer_sum = jnp.dot(weights.astype(jnp.bfloat16), v_blk, preferred_element_type=jnp.float32)
    return numer_sum / row_sum, (row_max + jnp.log(row_sum))[:, 0]


def branch_attention(q_all, k_all, v_all, branch):
    dil_rate = 2 ** branch
    num_segs = SEQ_LEN // (SEG_BASE * dil_rate)
    phase_ok = jnp.arange(NUM_HEADS)[:, None] % dil_rate == jnp.arange(dil_rate)[None, :]
    phase_f = phase_ok.astype(jnp.float32)

    def pick_rows(source):
        split_rows = source.astype(jnp.float32).reshape(num_segs, SEG_BASE, dil_rate, NUM_HEADS, HEAD_DIM)
        chosen = jnp.einsum('asihd,hi->ahsd', split_rows, phase_f).astype(jnp.bfloat16)
        return chosen.reshape(num_segs * NUM_HEADS, SEG_BASE, HEAD_DIM)

    attn_out, log_norm = lax.map(attend_block, (pick_rows(q_all), pick_rows(k_all), pick_rows(v_all)))
    attn_out = attn_out.reshape(num_segs, NUM_HEADS, SEG_BASE, HEAD_DIM)
    log_norm = log_norm.reshape(num_segs, NUM_HEADS, SEG_BASE)
    out_full = jnp.einsum('ahsd,hi->asihd', attn_out, phase_f).reshape(SEQ_LEN, NUM_HEADS, HEAD_DIM)
    lse_full = jnp.einsum('ahs,hi->asih', log_norm, phase_f).reshape(SEQ_LEN, NUM_HEADS)
    mask_full = jnp.broadcast_to(phase_ok.T[None, None], (num_segs, SEG_BASE, dil_rate, NUM_HEADS)).reshape(SEQ_LEN, NUM_HEADS)
    return out_full, lse_full, mask_full


def reference(hidden, w_query, w_key, w_value, w_out, branch_bias):
    def project(weight):
        return jnp.dot(hidden, weight, preferred_element_type=jnp.float32).astype(jnp.bfloat16).reshape(SEQ_LEN, NUM_HEADS, HEAD_DIM)

    q_all = project(w_query)
    k_all = project(w_key)
    v_all = project(w_value)
    for branch in range(NUM_BRANCHES):
        out_full, lse_full, mask_full = branch_attention(q_all, k_all, v_all, branch)
        branch_score = jnp.where(mask_full, lse_full + branch_bias[branch][None, :], -jnp.inf)
        if branch == 0:
            run_num = out_full
            run_max = branch_score
            run_den = jnp.ones_like(branch_score)
        else:
            new_max = jnp.maximum(run_max, branch_score)
            keep_old = jnp.exp(run_max - new_max)
            take_new = jnp.exp(branch_score - new_max)
            run_num = run_num * keep_old[..., None] + out_full * take_new[..., None]
            run_den = run_den * keep_old + take_new
            run_max = new_max
    combined = (run_num / run_den[..., None]).astype(jnp.bfloat16).reshape(SEQ_LEN, MODEL_DIM)
    return jnp.dot(combined, w_out, preferred_element_type=jnp.float32).astype(jnp.bfloat16)
```

```python
import functools
import math

import jax
import jax.numpy as jnp
from jax import lax
from jax.experimental import pallas as pl
from jax.experimental.pallas import tpu as pltpu
from jax.sharding import PartitionSpec as P

MESH = pl.DeviceIdType.MESH
BF = jnp.bfloat16
F32 = jnp.float32
D = 256
REL = (0, 4, 2, 6, 1, 5, 3, 7)
PAIR = (0, 2, 1, 3)
KAPPA = math.log2(math.e) / 16.0
VMEM = 66_000_000


def nn(a, b):
    return lax.dot_general(a, b, (((1,), (0,)), ((), ())), preferred_element_type=F32)


def nt(a, b):
    return lax.dot_general(a, b, (((1,), (1,)), ((), ())), preferred_element_type=F32)


def params(**kw):
    return pltpu.CompilerParams(vmem_limit_bytes=VMEM, **kw)


def phase_matrix(transposed):
    r = lax.broadcasted_iota(jnp.int32, (256, 256), 1 if transposed else 0)
    p = lax.broadcasted_iota(jnp.int32, (256, 256), 0 if transposed else 1)
    k = r // 32
    return (p == (r % 32) * 8 + k // 2 + 4 * (k % 2)).astype(F32).astype(BF)


def permute_kernel(x_ref, o_ref, pm_ref):
    @pl.when(pl.program_id(0) + pl.program_id(1) == 0)
    def _():
        pm_ref[...] = phase_matrix(False)

    o_ref[...] = nn(pm_ref[...], x_ref[...]).astype(BF).reshape(o_ref.shape)


def permute(x):
    n, d = x.shape
    return pl.pallas_call(
        permute_kernel,
        grid=(n // 2048, 8),
        in_specs=[pl.BlockSpec((256, d), lambda s, j: (s * 8 + j, 0))],
        out_specs=pl.BlockSpec((None, 8, 32, d), lambda s, j: (s, 0, j, 0)),
        out_shape=jax.ShapeDtypeStruct((n // 2048, 8, 256, d), BF),
        scratch_shapes=[pltpu.VMEM((256, 256), BF)],
        compiler_params=params(),
        cost_estimate=pl.CostEstimate(flops=2 * n * d * 256, bytes_accessed=4 * n * d, transcendentals=0),
        name='permute',
    )(x)


def unpermute_kernel(y_ref, o_ref, pm_ref):
    @pl.when(pl.program_id(0) + pl.program_id(1) == 0)
    def _():
        pm_ref[...] = phase_matrix(True)

    for j in range(y_ref.shape[1] // 32):
        y = y_ref[:, j * 32:(j + 1) * 32, :].reshape(256, y_ref.shape[2])
        o_ref[j * 256:(j + 1) * 256, :] = nn(pm_ref[...], y).astype(BF)


def unpermute(y):
    s, _, _, c = y.shape
    return pl.pallas_call(
        unpermute_kernel,
        grid=(s, 2),
        in_specs=[pl.BlockSpec((None, 8, 128, c), lambda s, j: (s, 0, j, 0))],
        out_specs=pl.BlockSpec((1024, c), lambda s, j: (s * 2 + j, 0)),
        out_shape=jax.ShapeDtypeStruct((s * 2048, c), BF),
        scratch_shapes=[pltpu.VMEM((256, 256), BF)],
        compiler_params=params(),
        name='unpermute',
    )(y)


def project_kernel(ids_ref, x_ref, wq_ref, wk_ref, wv_ref, q_ref, kv_ref, *k3_ref, pair0):
    hh = pl.program_id(0)
    pair = pl.program_id(2) + pair0
    rel = jnp.where(pair == 1, 2, jnp.where(pair == 2, 1, pair))
    swap = ((ids_ref[0] + hh + rel) & 7) >> 2
    x = x_ref[...].reshape(512, x_ref.shape[-1])
    q = nn(x, wq_ref[...]).astype(BF)
    k = nn(x, wk_ref[...]).astype(BF)
    v = nn(x, wv_ref[...])
    for j in range(2):
        rank = j ^ swap
        rows = slice(j * 256, (j + 1) * 256)
        vt = v[rows].T.astype(BF)
        q_ref[rank] = q[rows]
        kv_ref[rank, 0] = k[rows]
        kv_ref[rank, 1] = vt
        if k3_ref:
            @pl.when(rank == 0)
            def _(rows=rows, vt=vt):
                k3_ref[0][0] = k[rows]
                k3_ref[0][1] = vt


def project(ids, xp, wq, wk, wv, pair0, pairs, heads):
    segs, d = xp.shape[0], xp.shape[3]

    def x_map(h, s, p, ids):
        pair = p + pair0
        rel = jnp.where(pair == 1, 2, jnp.where(pair == 2, 1, pair))
        return (s, (ids[0] + h + rel) & 3, 0, 0)

    w_spec = pl.BlockSpec((d, D), lambda h, s, p, ids: (0, h))
    out_specs = [
        pl.BlockSpec((None, None, 2, 256, D), lambda h, s, p, ids: (h, s, p, 0, 0)),
        pl.BlockSpec((None, None, 2, 2, 256, D), lambda h, s, p, ids: (h, s, p, 0, 0, 0)),
    ]
    out_shape = [
        jax.ShapeDtypeStruct((heads, segs, 2 * pairs, 256, D), BF),
        jax.ShapeDtypeStruct((heads, segs, 2 * pairs, 2, 256, D), BF),
    ]
    if pair0 == 0:
        out_specs.append(pl.BlockSpec((None, None, 2, 256, D), lambda h, s, p, ids: (h, s, 0, 0, 0)))
        out_shape.append(jax.ShapeDtypeStruct((heads, segs, 2, 256, D), BF))
    rows = segs * pairs * 512
    return pl.pallas_call(
        functools.partial(project_kernel, pair0=pair0),
        grid_spec=pltpu.PrefetchScalarGridSpec(
            num_scalar_prefetch=1,
            grid=(heads, segs, pairs),
            in_specs=[pl.BlockSpec((None, 2, 256, d), x_map), w_spec, w_spec, w_spec],
            out_specs=out_specs,
        ),
        out_shape=out_shape,
        compiler_params=params(),
        cost_estimate=pl.CostEstimate(flops=heads * rows * d * D * 6, bytes_accessed=heads * rows * d * 2 + 6 * heads * d * D, transcendentals=0),
        name='project',
    )(ids, xp, wq, wk, wv)


def attend(kind, a, w, beta, hh, q, kv_s, kvp_s, kvr_s, s_scr, sr_scr):
    o = 1 - w

    def local(seg, r, n):
        return (lambda: kv_s[hh, seg, r:r + n, 0].reshape(n * 256, D), lambda: [kv_s[hh, seg, r + i, 1] for i in range(n)], n)

    def pair(seg, r):
        return (lambda: kvp_s[hh, seg, r, 0], lambda: [kvp_s[hh, seg, r, 1]], 1)

    def remote(i):
        return (lambda: kvr_s[hh, i:i + 2, 0].reshape(512, D), lambda: [kvr_s[hh, i, 1], kvr_s[hh, i + 1, 1]], 2)

    b0, b01, b1, b012, b12, b2, b0123, b123, b23, b3 = [beta(i) for i in range(10)]
    lane = lax.broadcasted_iota(jnp.int32, (1, 512), 1)

    def mix(x0, x1):
        return jnp.where(lane < 256, x0, x1)

    extra = []
    if kind == 2:
        parts = [(local(w, r, 2), None) for r in range(0, 8, 2)]
    elif kind == 1:
        parts = [(local(w, 0, 2), b01), (local(w, 2, 2), b01), (local(w, 4, 2), b0), (local(w, 6, 2), b0), (local(o, 0, 2), b1), (local(o, 2, 2), b1)]
    else:
        parts = [(local(w, 2, 2), b01), (local(w, 4, 2), b0), (local(w, 6, 2), b0), (local(o, 2, 2), b1),
                 (local(w, 0, 1), mix(b0123, b012)), (local(w, 1, 1), b012), (local(o, 0, 1), mix(b123, b12)), (local(o, 1, 1), b12)]
        for seg in range(2):
            parts += [(pair(seg, 0), mix(b23, b2)), (pair(seg, 1), b2)]
        extra = [(remote(0), b3), (remote(2), b3)]

    top = None
    off = 0
    for (k, _, n), b in parts:
        s = nt(k(), q)
        s_scr[off:off + n * 256, :] = s
        t = jnp.max(s, axis=0, keepdims=True) * KAPPA
        if b is not None:
            t = t + b
        top = t if top is None else jnp.maximum(top, t)
        off += n * 256
    if extra:
        topx = top[:, :256]
        off = 0
        for (k, _, n), b in extra:
            s = nt(k(), q[:256])
            sr_scr[off:off + n * 256, :] = s
            topx = jnp.maximum(topx, jnp.max(s, axis=0, keepdims=True) * KAPPA + b)
            off += n * 256
        top = jnp.concatenate([topx, top[:, 256:]], axis=1)

    acc = den = None
    off = 0
    for (_, v, n), b in parts:
        shift = top if b is None else top - b
        e = jnp.exp2(s_scr[off:off + n * 256, :] * KAPPA - shift)
        l = jnp.sum(e, axis=0, keepdims=True)
        vt = v()
        o_part = nn(vt[0] if n == 1 else jnp.concatenate(vt, axis=1), e.astype(BF))
        acc = o_part if acc is None else acc + o_part
        den = l if den is None else den + l
        off += n * 256
    if extra:
        accx, denx = None, den[:, :256]
        off = 0
        for (_, v, n), b in extra:
            e = jnp.exp2(sr_scr[off:off + n * 256, :] * KAPPA - (top[:, :256] - b))
            denx = denx + jnp.sum(e, axis=0, keepdims=True)
            o_part = nn(jnp.concatenate(v(), axis=1), e.astype(BF))
            accx = o_part if accx is None else accx + o_part
            off += n * 256
        acc = jnp.concatenate([acc[:, :256] + accx, acc[:, 256:]], axis=1)
        den = jnp.concatenate([denx, den[:, 256:]], axis=1)
    return acc / den


def mix_kernel(beta_ref, q0_ref, q1_ref, kv0_ref, kv1_ref, kvp_ref, kva_ref, kvb_ref, wown_ref, wlo_ref, whi_ref, out_ref,
               q_s, kv_s, kvp_s, kvr_s, wo_s, o_s, r_s, s_scr, sr_scr, in_sem, w_sem, o_send, r_sem, y_send, y_recv, *, axes, steps):
    t = pl.program_id(0)
    tp = lax.axis_index('tp')
    side = tp // 2
    inner = (tp == 1) | (tp == 2)
    idx = lax.axis_index('dp') * 4 + lax.axis_index('sp')
    a0 = 2 * tp
    n_attn = 16

    def loads():
        out = []
        for i, (src, dst) in enumerate(((q0_ref, lambda: q_s.at[:, :, pl.ds(0, 2)]), (q1_ref, lambda: q_s.at[:, :, pl.ds(2, 6)]),
                                        (kv0_ref, lambda: kv_s.at[:, :, pl.ds(0, 2)]), (kv1_ref, lambda: kv_s.at[:, :, pl.ds(2, 6)]),
                                        (kvp_ref, lambda: kvp_s), (kva_ref, lambda: kvr_s.at[:, pl.ds(0, 2)]), (kvb_ref, lambda: kvr_s.at[:, pl.ds(2, 2)]))):
            out.append(pltpu.make_async_copy(src, dst(), in_sem.at[i]))
        return out

    def w_loads():
        out = []
        for c in range(4):
            v = c ^ tp
            out.append(pltpu.make_async_copy(wown_ref.at[:, pl.ds(c * 512, 512)], wo_s.at[0, :, pl.ds(pl.multiple_of(v * 512, 512), 512)], w_sem.at[c]))
        for g, ref in ((0, wlo_ref), (1, whi_ref)):
            for j, m in enumerate((0, 4, 2, 6)):
                col = idx ^ (m + g)
                v = (col // 2) ^ tp
                dst = pl.multiple_of(v * 512 + (col & 1) * 256, 256)
                for b in range(3):
                    out.append(pltpu.make_async_copy(ref.at[j, b], wo_s.at[1 + b, :, pl.ds(dst, 256)], w_sem.at[4 + g * 12 + j * 3 + b]))
        return out

    def o_copy(c, seg, src_v, dst_tp):
        return pltpu.make_async_remote_copy(
            src_ref=o_s.at[seg, pl.ds(2 * c, 2)], dst_ref=r_s.at[src_v, pl.ds(2 * c, 2)],
            send_sem=o_send.at[seg, c], recv_sem=r_sem.at[src_v, c], device_id={'tp': dst_tp}, device_id_type=MESH)

    def y_src(k, v):
        return o_s.at[side, k] if v == 0 else r_s.at[v - 1, k]

    def y_copy(k, v, seg):
        return pltpu.make_async_remote_copy(
            src_ref=y_src(k, v), dst_ref=out_ref.at[seg, k], send_sem=y_send.at[k, v], recv_sem=y_recv.at[seg, k],
            device_id={'tp': tp ^ v}, device_id_type=MESH)

    def y_local(k):
        return pltpu.make_async_copy(y_src(k, 0), out_ref.at[side, k], y_send.at[k, 0])

    @pl.when(t == 0)
    def _():
        for c in loads():
            c.start()
        for c in w_loads():
            c.start()
        barrier = pltpu.get_barrier_semaphore()
        for v in (1, 2, 3):
            pl.semaphore_signal(barrier, inc=1, device_id={'tp': tp ^ v}, device_id_type=MESH)
        pl.semaphore_wait(barrier, 3)
        for c in loads():
            c.wait()

    p_steps = [i for i, s in enumerate(steps) if s == 'P']
    is_p = functools.reduce(jnp.logical_or, [t == i for i in p_steps])
    p_done = sum(jnp.where(t > i, 1, 0) for i in p_steps)
    u = t - p_done
    c = u // 4
    seg = jnp.where((u & 3) < 2, 1 - side, side)
    hh = u & 1
    a = a0 + hh
    rel = (c - a) & 3
    w = seg
    projector = 1 + seg

    def run(kind):
        rank_pair = {0: 0, 1: 1}.get(kind)
        if rank_pair is None:
            rank_pair = jnp.where(rel == 1, 2, 3)
        q = q_s[hh, w, pl.ds(2 * rank_pair, 2)].reshape(512, D)
        ot = attend(kind, a, w, lambda i: beta_ref[i, hh], hh, q, kv_s, kvp_s, kvr_s, s_scr, sr_scr)
        swap = ((a + rel) & 7) >> 2
        for j in range(2):
            o_s[w, 2 * c + (j ^ swap), :, pl.ds(pl.multiple_of(hh * D, D), D)] = ot[:, j * 256:(j + 1) * 256].T.astype(BF)

    @pl.when(jnp.logical_not(is_p))
    def _():
        pl.when(rel == 0)(lambda: run(0))
        pl.when(rel == 2)(lambda: run(1))
        pl.when((rel & 1) == 1)(lambda: run(2))

        @pl.when((hh == 1) & (tp != projector))
        def _():
            v = tp ^ projector
            o_copy(c, seg, v - 1, projector).start()

    @pl.when(t == p_steps[0])
    def _():
        for cp in w_loads():
            cp.wait()

    @pl.when(is_p & inner)
    def _():
        k = p_done
        cc = k // 2

        @pl.when(k % 2 == 0)
        def _():
            for v in (1, 2, 3):
                o_copy(cc, side, v - 1, tp).wait_recv()

        y = nn(o_s[side, k], wo_s[0])
        for v in (1, 2, 3):
            y = y + nn(r_s[v - 1, k], wo_s[v])
        y = y.astype(BF)
        o_s[side, k] = y[:, 0:512]
        for v in (1, 2, 3):
            r_s[v - 1, k] = y[:, v * 512:(v + 1) * 512]
        y_local(k).start()
        for v in (1, 2, 3):
            y_copy(k, v, side).start()

    @pl.when(t == len(steps) - 1)
    def _():
        for sg in range(2):
            @pl.when(tp != 1 + sg)
            def _():
                for cc in range(4):
                    o_copy(cc, sg, (tp ^ (1 + sg)) - 1, 1 + sg).wait_send()
                for k in range(8):
                    y_copy(k, 1, sg).wait_recv()

        @pl.when(inner)
        def _():
            for k in range(8):
                y_local(k).wait()
                for v in (1, 2, 3):
                    y_copy(k, v, side).wait_send()


STEPS = ('A',) * 12 + ('P', 'P') + ('A',) * 4 + ('P',) * 6


def mix_and_project(axes, beta, q0, q1, kv0, kv1, kvp, kva, kvb, w_out, wlo, whi):
    anyspec = pl.BlockSpec(memory_space=pl.ANY)
    return pl.pallas_call(
        functools.partial(mix_kernel, axes=axes, steps=STEPS),
        grid=(len(STEPS),),
        in_specs=[pl.BlockSpec(memory_space=pltpu.SMEM)] + [anyspec] * 10,
        out_specs=anyspec,
        out_shape=jax.ShapeDtypeStruct((2, 8, 256, 512), BF),
        scratch_shapes=[
            pltpu.VMEM((2, 2, 8, 256, D), BF),
            pltpu.VMEM((2, 2, 8, 2, 256, D), BF),
            pltpu.VMEM((2, 2, 2, 2, 256, D), BF),
            pltpu.VMEM((2, 4, 2, 256, D), BF),
            pltpu.VMEM((4, 512, 2048), BF),
            pltpu.VMEM((2, 8, 256, 512), BF),
            pltpu.VMEM((3, 8, 256, 512), BF),
            pltpu.VMEM((4096, 512), F32),
            pltpu.VMEM((1024, 256), F32),
            pltpu.SemaphoreType.DMA((7,)),
            pltpu.SemaphoreType.DMA((28,)),
            pltpu.SemaphoreType.DMA((2, 4)),
            pltpu.SemaphoreType.DMA((3, 4)),
            pltpu.SemaphoreType.DMA((8, 4)),
            pltpu.SemaphoreType.DMA((2, 8)),
        ],
        compiler_params=params(collective_id=0, has_side_effects=True),
        cost_estimate=pl.CostEstimate(flops=100_000_000_000, bytes_accessed=40_000_000, transcendentals=0),
        name='mix',
    )(beta, q0, q1, kv0, kv1, kvp, kva, kvb, w_out, wlo, whi)


def solution(mesh):
    axes = tuple(mesh.axis_names)
    sp_size = mesh.shape['sp']
    tp_size = mesh.shape['tp']
    dp_size = mesh.shape['dp']

    def xor_perm(x, axis, m, only=None):
        n = mesh.shape[axis]
        pairs = [(i, i ^ m) for i in range(n) if only is None or (i ^ m) in only]
        return lax.ppermute(x, axis, pairs)

    def plane_gather(x):
        x = x[None]
        x = jnp.concatenate([x, xor_perm(x, 'dp', 1) if dp_size > 1 else x])
        x = jnp.concatenate([x, xor_perm(x, 'sp', 2)])
        return x, xor_perm(x, 'sp', 1)

    def device_fn(hidden, w_query, w_key, w_value, w_out, branch_bias):
        tp = lax.axis_index('tp')
        idx = lax.axis_index('dp') * sp_size + lax.axis_index('sp')
        heads = branch_bias.shape[1] // tp_size

        w_sl = lax.dynamic_slice_in_dim(w_out, idx * 256, 256, axis=1)
        w_sl = jnp.stack([xor_perm(w_sl, 'tp', v, (1, 2)) for v in (1, 2, 3)])
        wlo, whi = plane_gather(w_sl)

        b = lax.dynamic_slice_in_dim(branch_bias, tp * heads, heads, axis=1)
        sets = ((0,), (0, 1), (1,), (0, 1, 2), (1, 2), (2,), (0, 1, 2, 3), (1, 2, 3), (2, 3), (3,))
        beta = []
        for st in sets:
            rows = b[jnp.array(st)]
            m = jnp.max(rows, axis=0)
            beta.append((m + jnp.log(jnp.sum(jnp.exp(rows - m), axis=0))) * math.log2(math.e))
        beta = jnp.stack(beta)

        ids = jnp.stack([2 * tp]).astype(jnp.int32)
        xp = permute(hidden)
        q0, kv0, kv3 = project(ids, xp, w_query, w_key, w_value, 0, 1, heads)
        kvp = xor_perm(kv0, 'sp', 1)
        kva = xor_perm(kv3, 'sp', 2)
        q1, kv1 = project(ids, xp, w_query, w_key, w_value, 1, 3, heads)
        kvb = xor_perm(kva, 'sp', 1)
        y = mix_and_project(axes, beta, q0, q1, kv0, kv1, kvp, kva, kvb, w_out, wlo, whi)
        return unpermute(y)

    return jax.shard_map(device_fn, mesh=mesh, in_specs=(P(('dp', 'sp'), None), P(None, 'tp'), P(None, 'tp'), P(None, 'tp'), P('tp', None), P(None, None)), out_specs=P(('dp', 'sp'), 'tp'), check_vma=False)
```

```python
import functools
import math

import jax
import jax.numpy as jnp
from jax import lax
from jax.experimental import pallas as pl
from jax.experimental.pallas import tpu as pltpu
from jax.sharding import PartitionSpec as P

MESH = pl.DeviceIdType.MESH
BF = jnp.bfloat16
F32 = jnp.float32
D = 256
KAPPA = math.log2(math.e) / 16.0
VMEM = 66_900_000
SLOT = (0, 4, 2, 6, 1, 5, 3, 7)


def nn(a, b):
    return lax.dot_general(a, b, (((1,), (0,)), ((), ())), preferred_element_type=F32)


def nt(a, b):
    return lax.dot_general(a, b, (((1,), (1,)), ((), ())), preferred_element_type=F32)


def params(**kw):
    return pltpu.CompilerParams(vmem_limit_bytes=VMEM, **kw)


def aligned(x, m):
    return pl.multiple_of(x, m)


def phase_matrix(transposed):
    r = lax.broadcasted_iota(jnp.int32, (256, 256), 1 if transposed else 0)
    p = lax.broadcasted_iota(jnp.int32, (256, 256), 0 if transposed else 1)
    k = r // 32
    return (p == (r % 32) * 8 + k // 2 + 4 * (k % 2)).astype(F32).astype(BF)


def unpermute_kernel(y_ref, o_ref, pm_ref):
    @pl.when(pl.program_id(0) + pl.program_id(1) == 0)
    def _():
        pm_ref[...] = phase_matrix(True)

    for j in range(y_ref.shape[1] // 32):
        y = y_ref[:, j * 32:(j + 1) * 32, :].reshape(256, y_ref.shape[2])
        o_ref[j * 256:(j + 1) * 256, :] = nn(pm_ref[...], y).astype(BF)


def unpermute(y):
    s, _, _, c = y.shape
    return pl.pallas_call(
        unpermute_kernel,
        grid=(s, 2),
        in_specs=[pl.BlockSpec((None, 8, 128, c), lambda s, j: (s, 0, j, 0))],
        out_specs=pl.BlockSpec((1024, c), lambda s, j: (s * 2 + j, 0)),
        out_shape=jax.ShapeDtypeStruct((s * 2048, c), BF),
        scratch_shapes=[pltpu.VMEM((256, 256), BF)],
        compiler_params=params(),
        name='unpermute',
    )(y)


def softmax_mix(q, parts, s_at):
    top = None
    for i, (k, _, n, b) in enumerate(parts):
        s = nt(k(), q)
        s_at(i)[...] = s
        t = jnp.max(s, axis=0, keepdims=True) * KAPPA
        if b is not None:
            t = t + b
        top = t if top is None else jnp.maximum(top, t)
    acc = den = None
    for i, (_, v, n, b) in enumerate(parts):
        shift = top if b is None else top - b
        e = jnp.exp2(s_at(i)[...] * KAPPA - shift)
        l = jnp.sum(e, axis=0, keepdims=True)
        o = nn(v(), e.astype(BF))
        acc = o if acc is None else acc + o
        den = l if den is None else den + l
    return acc / den


def main_kernel(beta_ref, x_ref, wk_ref, wv_ref, wq_ref, wout_ref, out_ref, lq_ref, lo_ref,
                xb, pm, xp, ws, q_s, kv_s, kvp_s, kvr_s, s_scr,
                x_sem, w_sem, wo_sem, lq_send, lq_recv, lo_zsend, lo_zrecv, lo_send, lo_recv,
                kvp_send, kvp_recv, kvr_send, kvr_recv, kvf_send, kvf_recv, o_send, o_recv, y_send, y_recv, ready, *, steps):
    dp, tp, sp = lax.axis_index('dp'), lax.axis_index('tp'), lax.axis_index('sp')
    idx = dp * 4 + sp
    side = tp // 2
    inner = (tp == 1) | (tp == 2)
    outer = jnp.logical_not(inner)
    W = (wk_ref, wv_ref, wq_ref)
    peer_x, peer_y, peer_c = {'dp': dp ^ 1}, {'sp': sp ^ 2}, {'sp': sp ^ 1}

    def remote(src, dst, ss, rs, dev):
        return pltpu.make_async_remote_copy(src_ref=src, dst_ref=dst, send_sem=ss, recv_sem=rs, device_id=dev, device_id_type=MESH)

    def lq_copy(t, src, dst, dev):
        return remote(lq_ref.at[src, t], lq_ref.at[dst, t], lq_send.at[t, dst], lq_recv.at[t, dst], dev)

    def lq_z(t):
        return remote(W[t].at[pl.ds(aligned(idx * 256, 256), 256), :], lq_ref.at[0, t], lq_send.at[t, 0], lq_recv.at[t, 0], {'tp': tp ^ 2})

    def lo_copy(u, src, dst, dev):
        return remote(lo_ref.at[src, u], lo_ref.at[dst, u], lo_send.at[u, dst], lo_recv.at[u, dst], dev)

    def lo_z(u, dst):
        v = tp ^ dst
        b = jnp.where(v == 2, 0, jnp.where(v == 1, 1, 2))
        far = 1 - dst // 2 if u == 0 else dst // 2
        return remote(wout_ref.at[:, pl.ds(aligned(far * 1024 + idx * 128, 128), 128)], lo_ref.at[0, u, b], lo_zsend.at[dst - 1, u], lo_zrecv.at[u, b], {'tp': dst})

    def ev_z(copy, p, wait):
        wait()
        copy(p, 0, 2, peer_y).start()
        copy(p, 0, 1, peer_x).start()
        copy(p, 0, 4, peer_c).start()

    def ev_xy(copy, p):
        copy(p, 0, 2, peer_y).wait_recv()
        copy(p, 2, 3, peer_x).start()
        copy(p, 2, 6, peer_c).start()
        copy(p, 0, 1, peer_x).wait_recv()
        copy(p, 1, 5, peer_c).start()

    def ev_x2(copy, p):
        copy(p, 2, 3, peer_x).wait_recv()
        copy(p, 3, 7, peer_c).start()

    def ev_done(copy, p):
        for s in range(4):
            copy(p, s, 4 + s, peer_c).wait_recv()

    def sends_done(copy, p):
        for src, dst, dev in ((0, 2, peer_y), (0, 1, peer_x), (0, 4, peer_c), (2, 3, peer_x), (2, 6, peer_c), (1, 5, peer_c), (3, 7, peer_c)):
            copy(p, src, dst, dev).wait_send()

    def lo_wait_z(u):
        def wait():
            for b in range(3):
                remote(lo_ref.at[0, u, b], lo_ref.at[0, u, b], lo_zsend.at[0, u], lo_zrecv.at[u, b], {'tp': tp}).wait_recv()
        return wait

    def w_load(t):
        return [pltpu.make_async_copy(lq_ref.at[s, t], ws.at[t, pl.ds(aligned((idx ^ m) * 256, 256), 256), :], w_sem.at[t, s]) for s, m in enumerate(SLOT)]

    def own_load(t):
        return pltpu.make_async_copy(W[t], ws.at[t], w_sem.at[t, 0])

    def wo_pos(col):
        return ((col // 512) ^ tp ^ 2) * 512 + col % 512

    def wo_own():
        out = []
        for r in range(2):
            for c in range(4):
                out.append(pltpu.make_async_copy(wout_ref.at[pl.ds(r * 256, 256), pl.ds(c * 512, 512)],
                                                 xp.at[0, r, :, pl.ds(aligned((c ^ tp ^ 2) * 512, 512), 512)], wo_sem.at[2, r * 4 + c, 0, 0]))
        return out

    def wo_load(u):
        out = []
        base = 1024 * (1 - side) if u == 0 else 1024 * side
        for s, m in enumerate(SLOT):
            pos = aligned(wo_pos(base + (idx ^ m) * 128), 128)
            for b in range(3):
                for r in range(2):
                    out.append(pltpu.make_async_copy(lo_ref.at[s, u, b, pl.ds(r * 256, 256)], xp.at[0, 2 + 2 * b + r, :, pl.ds(pos, 128)], wo_sem.at[u, s, b, r]))
        return out

    def kvp_copy(h):
        return remote(kv_s.at[h, pl.ds(0, 4)], kvp_s.at[h], kvp_send.at[h], kvp_recv.at[h], peer_c)

    def kvr_copy(h, s):
        return remote(kv_s.at[h, 2 * s], kvr_s.at[h, s], kvr_send.at[h, s], kvr_recv.at[h, s], peer_y)

    def kvf_copy(h, s):
        return remote(kvr_s.at[h, s], kvr_s.at[h, 2 + s], kvf_send.at[h, s], kvf_recv.at[h, s], peer_c)

    def kv_forward(hs):
        for h in hs:
            for s in range(2):
                kvr_copy(h, s).wait_recv()
                kvf_copy(h, s).start()

    def order(k):
        return 2 * (k % 4) + ((k // 4) ^ side)

    def o_copy(k):
        return remote(xp.at[1, k, :, pl.ds(0, 1024)], xp.at[1, k, :, pl.ds(1024, 1024)], o_send.at[k], o_recv.at[k], {'tp': tp ^ 1})

    def y_src(k, v):
        if v == 0:
            return xp.at[1, k, :, pl.ds(0, 512)]
        return ws.at[{2: 0, 3: 1, 1: 2}[v], pl.ds(aligned(k * 256, 256), 256), :]

    def y_copy(k, v, seg):
        return remote(y_src(k, v), out_ref.at[seg, k], y_send.at[k, v], y_recv.at[seg, k], {'tp': tp ^ v})

    def y_local(k):
        return pltpu.make_async_copy(y_src(k, 0), out_ref.at[side, k], y_send.at[k, 0])

    def x_copy(j):
        return pltpu.make_async_copy(x_ref.at[pl.ds(aligned(j * 256, 256), 256), :], xb.at[lax.rem(j, 4)], x_sem.at[lax.rem(j, 4)])

    for j in range(4):
        x_copy(j).start()
    for t in range(3):
        own_load(t).start()
    barrier = pltpu.get_barrier_semaphore()
    peers = [{'tp': tp ^ 1}, {'tp': tp ^ 2}, {'tp': tp ^ 3}, peer_x, peer_y, peer_c]
    for dev in peers:
        pl.semaphore_signal(barrier, inc=1, device_id=dev, device_id_type=MESH)
    pl.semaphore_wait(barrier, len(peers))
    for t in range(3):
        lq_z(t).start()
    for u in range(2):
        for dst in (1, 2):
            pl.when(tp != dst)(lambda u=u, dst=dst: lo_z(u, dst).start())

    pm[...] = phase_matrix(False)

    def permute_body(j, _):
        x_copy(j).wait()
        y = nn(pm[...], xb[lax.rem(j, 4)]).astype(BF).reshape(8, 32, 2048)
        xp[j // 8, :, pl.ds(aligned(lax.rem(j, 8) * 32, 32), 32), :] = y
        pl.when(j < 12)(lambda: x_copy(j + 4).start())
        return None

    lax.fori_loop(0, 16, permute_body, None)

    def rows_of(a, g):
        sigma = jnp.where(g < 4, g & 1, 0)
        pair = jnp.where(g < 4, g // 2, g - 2)
        rel = jnp.where(pair == 1, 2, jnp.where(pair == 2, 1, pair))
        x = xp[side ^ sigma, pl.ds(2 * ((a + rel) & 3), 2)].reshape(512, 2048)
        return x, ((a + rel) & 7) >> 2, pair, sigma

    def wcols(t, hh):
        return ws[t, :, pl.ds(aligned(hh * 256, 256), 256)]

    def put_k(h, g, swap, k):
        k = k.astype(BF)
        for j in range(2):
            kv_s[h, 2 * g + (j ^ swap), 0] = k[j * 256:(j + 1) * 256]

    def put_v(h, g, swap, v):
        for j in range(2):
            kv_s[h, 2 * g + (j ^ swap), 1] = v[j * 256:(j + 1) * 256].T.astype(BF)

    def put_q(h, pair, swap, q):
        q = q.astype(BF)
        for j in range(2):
            q_s[h, 2 * pair + (j ^ swap)] = q[j * 256:(j + 1) * 256]

    for t in range(3):
        own_load(t).wait()

    def own_body(i, _):
        hh, g = i & 1, i // 2
        x, swap, pair, sigma = rows_of(2 * tp + hh, g)
        put_k(hh, g, swap, nn(x, wcols(0, hh)))
        put_v(hh, g, swap, nn(x, wcols(1, hh)))
        pl.when(sigma == 0)(lambda: put_q(hh, pair, swap, nn(x, wcols(2, hh))))

        @pl.when(i == 3)
        def _():
            for h in range(2):
                kvp_copy(h).start()
            ev_z(lq_copy, 0, lambda: lq_z(0).wait_recv())

        @pl.when(i == 6)
        def _():
            ev_xy(lq_copy, 0)

        @pl.when(i == 8)
        def _():
            ev_z(lq_copy, 1, lambda: lq_z(1).wait_recv())
            for s in range(2):
                kvr_copy(0, s).start()

        @pl.when(i == 10)
        def _():
            ev_x2(lq_copy, 0)
        return None

    lax.fori_loop(0, 12, own_body, None)
    ev_done(lq_copy, 0)
    for c in w_load(0):
        c.start()
    for c in w_load(0):
        c.wait()

    a_par = 2 * (tp ^ 2)

    def k_body(i, _):
        hh, g = i & 1, i // 2
        x, swap, pair, sigma = rows_of(a_par + hh, g)
        put_k(2 + hh, g, swap, nn(x, wcols(0, hh)))

        @pl.when(i == 1)
        def _():
            ev_xy(lq_copy, 1)

        @pl.when(i == 6)
        def _():
            ev_z(lq_copy, 2, lambda: lq_z(2).wait_recv())
            for s in range(2):
                kvr_copy(1, s).start()
        return None

    lax.fori_loop(0, 12, k_body, None)
    ev_x2(lq_copy, 1)
    ev_done(lq_copy, 1)
    for c in w_load(1):
        c.start()
    for c in w_load(1):
        c.wait()

    def v_body(i, _):
        hh, g = i & 1, i // 2
        x, swap, pair, sigma = rows_of(a_par + hh, g)
        put_v(2 + hh, g, swap, nn(x, wcols(1, hh)))

        @pl.when(i == 3)
        def _():
            for h in range(2, 4):
                kvp_copy(h).start()

        @pl.when(i == 6)
        def _():
            ev_xy(lq_copy, 2)

        @pl.when((i == 8) & inner)
        def _():
            ev_z(lo_copy, 0, lo_wait_z(0))
        return None

    lax.fori_loop(0, 12, v_body, None)
    for h in range(2, 4):
        for s in range(2):
            kvr_copy(h, s).start()
    ev_x2(lq_copy, 2)
    ev_done(lq_copy, 2)
    for c in w_load(2):
        c.start()
    for c in w_load(2):
        c.wait()

    def q_body(i, _):
        hh, pair = i & 1, i // 2
        g = jnp.where(pair == 3, 5, 2 * pair)
        x, swap, pair, sigma = rows_of(a_par + hh, g)
        put_q(2 + hh, pair, swap, nn(x, wcols(2, hh)))

        @pl.when((i == 3) & inner)
        def _():
            ev_xy(lo_copy, 0)
        return None

    lax.fori_loop(0, 8, q_body, None)

    pl.when(inner)(lambda: pl.semaphore_signal(ready, inc=1, device_id={'tp': tp ^ 1}, device_id_type=MESH))
    pl.when(outer)(lambda: pl.semaphore_wait(ready, 1))
    for c in wo_own():
        c.start()
    kv_forward((0, 1))
    for h in range(4):
        kvp_copy(h).wait_recv()
    for h in range(2):
        for s in range(2):
            kvf_copy(h, s).wait_recv()

    n_steps = len(steps)
    n_tiles = sum(s == 'A' for s in steps)

    def count_before(t, kind):
        return sum(jnp.where(t > i, 1, 0) for i, s in enumerate(steps) if s == kind)

    def is_kind(t, kind):
        return functools.reduce(jnp.logical_or, [t == i for i, s in enumerate(steps) if s == kind])

    def attn_tile(e):
        late = e >= 16
        h = jnp.where(late, e - 14, e & 3)
        a = (2 * jnp.where(h < 2, tp, tp ^ 2) + (h & 1))
        c = jnp.where(late, a & 3, e // 4)
        rel = (c - a) & 3
        b0, b01, b1, b012, b12, b2, b0123, b123, b23, b3 = [beta_ref[i, h] for i in range(10)]

        def loc(i, n, b):
            if n == 1:
                return (lambda: kv_s[h, i, 0], lambda: kv_s[h, i, 1], 256, b)
            return (lambda: kv_s[h, i:i + 2, 0].reshape(512, D), lambda: jnp.concatenate([kv_s[h, i, 1], kv_s[h, i + 1, 1]], axis=1), 512, b)

        def par(ref, i, n, b):
            if n == 1:
                return (lambda: ref[h, i, 0], lambda: ref[h, i, 1], 256, b)
            return (lambda: ref[h, i:i + 2, 0].reshape(512, D), lambda: jnp.concatenate([ref[h, i, 1], ref[h, i + 1, 1]], axis=1), 512, b)

        def wide(i):
            return s_scr.at[pl.ds(i * 512, 512), :]

        def narrow(parts):
            at = []
            off = 0
            for p in parts:
                lane, row = (0, off) if off < 3072 else (256, off - 3072)
                at.append((row, p[2], lane))
                off += p[2]
            return lambda i: s_scr.at[pl.ds(at[i][0], at[i][1]), pl.ds(at[i][2], 256)]

        def put(k, ot):
            xp[1, k, :, pl.ds(aligned(h * D, D), D)] = ot.T.astype(BF)

        def both(ot):
            swap = ((a + rel) & 7) >> 2
            for j in range(2):
                put(2 * c + (j ^ swap), ot[:, j * 256:(j + 1) * 256])

        @pl.when((rel & 1) == 1)
        def _():
            q = q_s[h, pl.ds(jnp.where(rel == 1, 4, 6), 2)].reshape(512, D)
            both(softmax_mix(q, [loc(i, 2, None) for i in (0, 4, 8, 10)], wide))

        @pl.when(rel == 2)
        def _():
            q = q_s[h, 2:4].reshape(512, D)
            both(softmax_mix(q, [loc(0, 2, b01), loc(4, 2, b01), loc(8, 2, b0), loc(10, 2, b0), loc(2, 2, b1), loc(6, 2, b1)], wide))

        @pl.when((rel == 0) & jnp.logical_not(late))
        def _():
            parts = [loc(0, 2, b012), loc(4, 2, b01), loc(8, 2, b0), loc(10, 2, b0), loc(2, 2, b12), loc(6, 2, b1), par(kvp_s, 0, 2, b2), par(kvp_s, 2, 2, b2)]
            put(2 * c + ((a >> 2) ^ 1), softmax_mix(q_s[h, 1], parts, narrow(parts)))

        @pl.when((rel == 0) & (late | (h < 2)))
        def _():
            parts = [loc(0, 1, b0123), loc(1, 1, b012), loc(4, 2, b01), loc(8, 2, b0), loc(10, 2, b0), loc(2, 1, b123), loc(3, 1, b12), loc(6, 2, b1),
                     par(kvp_s, 0, 1, b23), par(kvp_s, 1, 1, b2), par(kvp_s, 2, 1, b23), par(kvp_s, 3, 1, b2), par(kvr_s, 0, 2, b3), par(kvr_s, 2, 2, b3)]
            put(2 * c + (a >> 2), softmax_mix(q_s[h, 0], parts, narrow(parts)))

        @pl.when(outer)
        def _():
            for j in range(4):
                pl.when(e == 4 * j + 3)(lambda j=j: o_copy(order(j)).start())

            @pl.when(e == n_tiles - 1)
            def _():
                for j in range(4, 8):
                    o_copy(order(j)).start()

    def step_body(t, _):
        @pl.when(is_kind(t, 'A'))
        def _():
            attn_tile(count_before(t, 'A'))

        for i, s in enumerate(steps):
            if s == 'W0':
                @pl.when((t == i) & inner)
                def _():
                    ev_x2(lo_copy, 0)
                    ev_done(lo_copy, 0)
                    for c in wo_load(0):
                        c.start()
                    ev_z(lo_copy, 1, lo_wait_z(1))
                    for c in wo_load(0):
                        c.wait()
                @pl.when(t == i)
                def _():
                    for c in wo_own():
                        c.wait()
            elif s == 'W1':
                @pl.when((t == i) & inner)
                def _():
                    ev_xy(lo_copy, 1)
            elif s == 'W2':
                @pl.when((t == i) & inner)
                def _():
                    ev_x2(lo_copy, 1)
                    ev_done(lo_copy, 1)
                    for c in wo_load(1):
                        c.start()
                    for c in wo_load(1):
                        c.wait()
            elif s == 'F':
                pl.when(t == i)(lambda: kv_forward((2, 3)))
            elif s == 'G':
                @pl.when(t == i)
                def _():
                    for h in (2, 3):
                        for z in range(2):
                            kvf_copy(h, z).wait_recv()

        @pl.when(is_kind(t, 'R') & inner)
        def _():
            k = order(count_before(t, 'R'))
            o_copy(k).wait_recv()
            y = nn(xp[1, k], xp[0, :, :, 0:1024].reshape(2048, 1024)).astype(BF)
            for v in (2, 3):
                ws[v - 2, pl.ds(aligned(k * 256, 256), 256), :] = y[:, (v - 2) * 512:(v - 1) * 512]
                y_copy(k, v, side).start()

        @pl.when(is_kind(t, 'L') & inner)
        def _():
            k = order(count_before(t, 'L'))
            y = nn(xp[1, k], xp[0, :, :, 1024:2048].reshape(2048, 1024)).astype(BF)
            ws[2, pl.ds(aligned(k * 256, 256), 256), :] = y[:, 512:1024]
            y_copy(k, 1, side).start()
            xp[1, k, :, 0:512] = y[:, 0:512]
            y_local(k).start()
        return None

    lax.fori_loop(0, n_steps, step_body, None)

    for t in range(3):
        lq_z(t).wait_send()
        sends_done(lq_copy, t)
    for u in range(2):
        for dst in (1, 2):
            pl.when(tp != dst)(lambda u=u, dst=dst: lo_z(u, dst).wait_send())
        pl.when(inner)(lambda u=u: sends_done(lo_copy, u))
    for h in range(4):
        kvp_copy(h).wait_send()
        for s in range(2):
            kvr_copy(h, s).wait_send()
            kvf_copy(h, s).wait_send()

    @pl.when(outer)
    def _():
        for k in range(8):
            o_copy(k).wait_send()

    @pl.when(inner)
    def _():
        for k in range(8):
            for v in (1, 2, 3):
                y_copy(k, v, side).wait_send()
            y_local(k).wait()

    for seg in range(2):
        @pl.when(tp != 1 + seg)
        def _():
            for k in range(8):
                y_copy(k, 1, seg).wait_recv()


STEPS = ('A',) * 8 + ('W0', 'A', 'A', 'R', 'W1', 'A', 'A', 'A', 'A', 'R', 'F', 'A', 'A', 'W2', 'L', 'G', 'A', 'A', 'R', 'L', 'R', 'L', 'R', 'L', 'R', 'L', 'R', 'L', 'R', 'L', 'L')


def main(beta, x, wk, wv, wq, w_out):
    assert sum(s == 'A' for s in STEPS) == 18 and sum(s == 'R' for s in STEPS) == 8 and sum(s == 'L' for s in STEPS) == 8
    anyspec = pl.BlockSpec(memory_space=pl.ANY)
    dma = pltpu.SemaphoreType.DMA
    return pl.pallas_call(
        functools.partial(main_kernel, steps=STEPS),
        in_specs=[pl.BlockSpec(memory_space=pltpu.SMEM)] + [anyspec] * 5,
        out_specs=[anyspec] * 3,
        out_shape=[jax.ShapeDtypeStruct((2, 8, 256, 512), BF), jax.ShapeDtypeStruct((8, 3, 256, 512), BF), jax.ShapeDtypeStruct((8, 2, 3, 512, 128), BF)],
        scratch_shapes=[
            pltpu.VMEM((4, 256, 2048), BF),
            pltpu.VMEM((256, 256), BF),
            pltpu.VMEM((2, 8, 256, 2048), BF),
            pltpu.VMEM((3, 2048, 512), BF),
            pltpu.VMEM((4, 8, 256, D), BF),
            pltpu.VMEM((4, 12, 2, 256, D), BF),
            pltpu.VMEM((4, 4, 2, 256, D), BF),
            pltpu.VMEM((4, 4, 2, 256, D), BF),
            pltpu.VMEM((3072, 512), F32),
            dma((4,)), dma((3, 8)), dma((3, 8, 3, 2)), dma((3, 8)), dma((3, 8)), dma((2, 2)), dma((2, 3)), dma((2, 8)), dma((2, 8)),
            dma((4,)), dma((4,)), dma((4, 2)), dma((4, 2)), dma((4, 2)), dma((4, 2)), dma((8,)), dma((8,)), dma((8, 4)), dma((2, 8)),
            pltpu.SemaphoreType.REGULAR,
        ],
        compiler_params=params(collective_id=0, has_side_effects=True),
        cost_estimate=pl.CostEstimate(flops=100_000_000_000, bytes_accessed=40_000_000, transcendentals=0),
        name='main',
    )(beta, x, wk, wv, wq, w_out)[0]


def solution(mesh):
    tp_size = mesh.shape['tp']

    def device_fn(hidden, w_query, w_key, w_value, w_out, branch_bias):
        tp = lax.axis_index('tp')
        heads = branch_bias.shape[1] // tp_size
        b = jnp.concatenate([lax.dynamic_slice_in_dim(branch_bias, t * heads, heads, axis=1) for t in (tp, tp ^ 2)], axis=1)
        sets = ((0,), (0, 1), (1,), (0, 1, 2), (1, 2), (2,), (0, 1, 2, 3), (1, 2, 3), (2, 3), (3,))
        beta = []
        for st in sets:
            rows = [b[i:i + 1] for i in st]
            m = functools.reduce(jnp.maximum, rows)
            beta.append((m + jnp.log(sum(jnp.exp(r - m) for r in rows))) * math.log2(math.e))
        beta = jnp.concatenate(beta)
        return unpermute(main(beta, hidden, w_key, w_value, w_query, w_out))

    return jax.shard_map(device_fn, mesh=mesh, in_specs=(P(('dp', 'sp'), None), P(None, 'tp'), P(None, 'tp'), P(None, 'tp'), P('tp', None), P(None, None)), out_specs=P(('dp', 'sp'), 'tp'), check_vma=False)
```

```python
import functools
import math

import jax
import jax.numpy as jnp
from jax import lax
from jax.experimental import pallas as pl
from jax.experimental.pallas import tpu as pltpu
from jax.sharding import PartitionSpec as P

MESH = pl.DeviceIdType.MESH
BF = jnp.bfloat16
F32 = jnp.float32
B, H, M = 256, 512, 2048
KAPPA = math.log2(math.e) / 16
VMEM = 66_900_000
SLOT = (0, 4, 2, 6, 1, 5, 3, 7)
KEY, VAL, QUE = range(3)
HEADS = range(4)
TWO = range(2)
ROWS = range(8)


def nn(a, b):
    return lax.dot_general(a, b, (((1,), (0,)), ((), ())), preferred_element_type=F32)


def nt(a, b):
    return lax.dot_general(a, b, (((1,), (1,)), ((), ())), preferred_element_type=F32)


def params(**kw):
    return pltpu.CompilerParams(vmem_limit_bytes=VMEM, **kw)


def ds(start, size):
    return pl.ds(pl.multiple_of(start, 128), size)


def part(i, size):
    return slice(i * size, i * size + size)


def phase_matrix(transposed):
    r = lax.broadcasted_iota(jnp.int32, (B, B), int(transposed))
    p = lax.broadcasted_iota(jnp.int32, (B, B), int(not transposed))
    k = r // 32
    return (p == (r % 32) * 8 + k // 2 + 4 * (k % 2)).astype(F32).astype(BF)


def unpermute_kernel(y_ref, o_ref, pm_ref):
    @pl.when(pl.program_id(0) + pl.program_id(1) == 0)
    def _():
        pm_ref[...] = phase_matrix(True)

    for j in range(y_ref.shape[1] // 32):
        y = y_ref[:, part(j, 32), :].reshape(B, y_ref.shape[-1])
        o_ref[part(j, B), :] = nn(pm_ref[...], y).astype(BF)


def unpermute(y):
    s, k, i, c = y.shape
    return pl.pallas_call(
        unpermute_kernel,
        grid=(s, 2),
        in_specs=[pl.BlockSpec((None, k, i // 2, c), lambda s, j: (s, 0, j, 0))],
        out_specs=pl.BlockSpec((k * i // 2, c), lambda s, j: (s * 2 + j, 0)),
        out_shape=jax.ShapeDtypeStruct((s * k * i, c), BF),
        scratch_shapes=[pltpu.VMEM((B, B), BF)],
        compiler_params=params(),
        name='unpermute',
    )(y)


def tile_steps(q, groups, s_at, done):
    st = {}
    logits, sums = [], []
    off = 0
    for keys, parts in groups:
        def qk(keys=keys, parts=parts, off=off):
            s = nt(keys(), q())
            o = 0
            for _, n, b in parts:
                piece = s[o:o + n]
                s_at(off + o, n)[...] = piece
                t = jnp.max(piece, axis=0, keepdims=True) * KAPPA
                if b is not None:
                    t = t + b
                st['top'] = jnp.maximum(st['top'], t) if 'top' in st else t
                o += n
        logits.append(qk)
        for v, n, b in parts:
            def sv(v=v, n=n, b=b, off=off):
                e = jnp.exp2(s_at(off, n)[...] * KAPPA - (st['top'] if b is None else st['top'] - b))
                l = jnp.sum(e, axis=0, keepdims=True)
                o = nn(v(), e.astype(BF))
                st['o'] = st['o'] + o if 'o' in st else o
                st['l'] = st['l'] + l if 'l' in st else l
            sums.append(sv)
            off += n
    sums.append(lambda: done(st['o'] / st['l']))
    return logits, sums


def interleave(a, b):
    i = j = 0
    while i < len(a) or j < len(b):
        if j >= len(b) or (i < len(a) and i * len(b) <= j * len(a)):
            a[i]()
            i += 1
        else:
            b[j]()
            j += 1


def run_tiles(tiles):
    before = []
    for logits, sums in tiles:
        interleave(logits, before)
        before = sums
    interleave([], before)


def on(cond, *calls):
    @pl.when(cond)
    def _():
        for c in calls:
            c()


def runs(steps, kind):
    out = []
    for i, s in enumerate(steps):
        if s == kind:
            if out and sum(out[-1]) == i:
                out[-1][1] += 1
            else:
                out.append([i, 1])
    return out


def scope(name):
    return jax.named_scope(name)


def main_kernel(beta_ref, x_ref, wk_ref, wv_ref, wq_ref, wout_ref, out_ref, lq_ref, lo_ref,
                xb, pm, xp, ws, q_s, kv_s, kvp_s, kvr_s, s_scr, t_scr,
                x_sem, w_sem, wo_sem, lq_send, lq_recv, lo_zsend, lo_zrecv, lo_send, lo_recv,
                kvp_send, kvp_recv, kvr_send, kvr_recv, kvf_send, kvf_recv, o_send, o_recv, y_send, y_recv, ready):
    dp, tp, sp = lax.axis_index('dp'), lax.axis_index('tp'), lax.axis_index('sp')
    idx = dp * 4 + sp
    side = tp // 2
    inner = (tp == 1) | (tp == 2)
    outer = jnp.logical_not(inner)
    W = (wk_ref, wv_ref, wq_ref)
    peer_x, peer_y, peer_c = {'dp': dp ^ 1}, {'sp': sp ^ 2}, {'sp': sp ^ 1}

    def remote(src, dst, ss, rs, dev):
        return pltpu.make_async_remote_copy(src_ref=src, dst_ref=dst, send_sem=ss, recv_sem=rs, device_id=dev, device_id_type=MESH)

    def lq_copy(t, src, dst, dev):
        return remote(lq_ref.at[src, t], lq_ref.at[dst, t], lq_send.at[t, dst], lq_recv.at[t, dst], dev)

    def lq_z(t):
        return remote(W[t].at[ds(idx * B, B), :], lq_ref.at[0, t], lq_send.at[t, 0], lq_recv.at[t, 0], {'tp': tp ^ 2})

    def lo_copy(u, src, dst, dev):
        return remote(lo_ref.at[src, u], lo_ref.at[dst, u], lo_send.at[u, dst], lo_recv.at[u, dst], dev)

    def lo_z(u, dst):
        far = 1 - dst // 2 if u == 0 else dst // 2
        b = (tp ^ dst) - 1
        return remote(wout_ref.at[:, ds(far * 1024 + idx * 128, 128)], lo_ref.at[0, u, b], lo_zsend.at[dst - 1, u], lo_zrecv.at[u, b], {'tp': dst})

    def lo_start(u):
        for dst in (1, 2):
            pl.when(tp != dst)(lambda dst=dst: lo_z(u, dst).start())

    def lo_zwait(u):
        for b in range(3):
            remote(lo_ref.at[0, u, b], lo_ref.at[0, u, b], lo_zsend.at[0, u], lo_zrecv.at[u, b], {'tp': tp}).wait_recv()

    hops = ((0, 2, peer_y), (0, 1, peer_x), (0, 4, peer_c), (2, 3, peer_x), (2, 6, peer_c), (1, 5, peer_c), (3, 7, peer_c))

    def hop(copy, p, i):
        return copy(p, *hops[i])

    def ev_z(copy, p):
        with scope(f'z_{copy.__name__}{p}'):
            lq_z(p).wait_recv() if copy is lq_copy else lo_zwait(p)
        for i in range(3):
            hop(copy, p, i).start()

    def ev_xy(copy, p):
        with scope(f'y_{copy.__name__}{p}'):
            hop(copy, p, 0).wait_recv()
        hop(copy, p, 3).start()
        hop(copy, p, 4).start()
        with scope(f'x_{copy.__name__}{p}'):
            hop(copy, p, 1).wait_recv()
        hop(copy, p, 5).start()

    def ev_done(copy, p):
        with scope(f'x2_{copy.__name__}{p}'):
            hop(copy, p, 3).wait_recv()
        hop(copy, p, 6).start()
        with scope(f'c_{copy.__name__}{p}'):
            for i in (2, 4, 5, 6):
                hop(copy, p, i).wait_recv()

    def sends_done(copy, p):
        for i in range(len(hops)):
            hop(copy, p, i).wait_send()

    def w_load(t):
        return [pltpu.make_async_copy(lq_ref.at[s, t], ws.at[t, ds((idx ^ m) * B, B), :], w_sem.at[t, s]) for s, m in enumerate(SLOT)]

    def own_load(t):
        return pltpu.make_async_copy(W[t], ws.at[t], w_sem.at[t, 0])

    def start(copies):
        for c in copies:
            c.start()

    def wait(copies):
        for c in copies:
            c.wait()

    def ev_weights(t):
        ev_done(lq_copy, t)
        start(w_load(t))
        wait(w_load(t))

    wo = xp.at[1 - side]

    def wo_own():
        return [pltpu.make_async_copy(wout_ref.at[pl.ds(r * B, B), pl.ds(c * H, H)], xp.at[1 - side, r, :, ds((c ^ tp ^ 2) * H, H)], wo_sem.at[2, r * 4 + c, 0, 0])
                for r in TWO for c in range(4)]

    def wo_load(u):
        out = []
        for s, m in enumerate(SLOT):
            col = (side if u else 1 - side) * 1024 + (idx ^ m) * 128
            pos = ((col // H) ^ tp ^ 2) * H + col % H
            for b in range(3):
                for r in TWO:
                    out.append(pltpu.make_async_copy(lo_ref.at[s, u, b, pl.ds(r * B, B)], xp.at[1 - side, 2 + 2 * b + r, :, ds(pos, 128)], wo_sem.at[u, s, b, r]))
        return out

    def kvp_copy(h, s):
        return remote(kv_s.at[h, pl.ds(8 * s, 2)], kvp_s.at[h, pl.ds(2 * s, 2)], kvp_send.at[h, s], kvp_recv.at[h, s], peer_c)

    def kvr_copy(h, s):
        return remote(kv_s.at[h, 8 * s], kvr_s.at[h, s], kvr_send.at[h, s], kvr_recv.at[h, s], peer_y)

    def kvf_copy(h, s):
        return remote(kvr_s.at[h, s], kvr_s.at[h, 2 + s], kvf_send.at[h, s], kvf_recv.at[h, s], peer_c)

    def kv_start(copy, heads):
        for h in heads:
            for s in TWO:
                copy(h, s).start()

    def kv_wait(copy, heads):
        with scope(f'w_{copy.__name__}{heads[0]}'):
            for h in heads:
                for s in TWO:
                    copy(h, s).wait_recv()

    def kv_forward(heads):
        kv_wait(kvr_copy, heads)
        kv_start(kvf_copy, heads)

    def order(k):
        return 2 * (k % 4) + ((k // 4) ^ side)

    def o_at(k, p, theirs, col, size):
        return ws.at[theirs, ds(k * B, B), ds(col, size)] if p else xb.at[k // 2, :, ds((k % 2) * 1024 + theirs * H + col, size)]

    def o_copy(k, p):
        return remote(o_at(k, p, 0, 0, H), o_at(k, p, 1, 0, H), o_send.at[k, p], o_recv.at[k, p], {'tp': tp ^ 1})

    def o_times(k, cols):
        y = nn(xb[k // 2, :, ds((k % 2) * 1024, 1024)], wo[0:4, :, cols].reshape(1024, 1024))
        for i in TWO:
            y = y + nn(ws[i, ds(k * B, B), :], wo[part(2 + i, 2), :, cols].reshape(H, 1024))
        return y.astype(BF)

    def y_src(k, v):
        return xp.at[side, k, :, pl.ds(v * H, H)]

    def y_copy(k, v, seg):
        return remote(y_src(k, v), out_ref.at[seg, k], y_send.at[k, v], y_recv.at[seg, k], {'tp': tp ^ v})

    def y_local(k):
        return pltpu.make_async_copy(y_src(k, 0), out_ref.at[side, k], y_send.at[k, 0])

    def x_copy(j):
        return pltpu.make_async_copy(x_ref.at[ds(j * B, B), :], xb.at[lax.rem(j, 4)], x_sem.at[lax.rem(j, 4)])

    for j in range(4):
        x_copy(j).start()
    for t in range(3):
        own_load(t).start()
    barrier = pltpu.get_barrier_semaphore()
    peers = [{'tp': tp ^ 1}, {'tp': tp ^ 2}, {'tp': tp ^ 3}, peer_x, peer_y, peer_c]
    for dev in peers:
        pl.semaphore_signal(barrier, inc=1, device_id=dev, device_id_type=MESH)
    with scope('barrier'):
        pl.semaphore_wait(barrier, len(peers))
    lq_z(KEY).start()

    pm[...] = phase_matrix(False)

    def permute_body(j, carry):
        x_copy(j).wait()
        y = nn(pm[...], xb[lax.rem(j, 4)]).astype(BF).reshape(8, 32, M)
        xp[j // 8, :, pl.ds(pl.multiple_of(lax.rem(j, 8) * 32, 32), 32), :] = y
        pl.when(j < 12)(lambda: x_copy(j + 4).start())
        return carry

    with scope('permute'):
        lax.fori_loop(0, 16, permute_body, None)

    def signal_ready(i):
        pl.when(inner)(lambda: pl.semaphore_signal(ready.at[i], inc=1, device_id={'tp': tp ^ 1}, device_id_type=MESH))

    def wait_ready(i):
        with scope(f'ready{i}'):
            pl.when(outer)(lambda: pl.semaphore_wait(ready.at[i], 1))

    signal_ready(0)

    def group(g):
        low = g < 4
        return jnp.where(low, g & 1, 0), jnp.where(low, g // 2, g - 2)

    def head_number(h):
        return 2 * (tp ^ (h // 2 * 2)) + h % 2

    def reverse(i):
        return (i % 2) * 2 + i // 2

    def project(heads, sigma, pair, kinds, chunk=None):
        for h in heads:
            if chunk is not None:
                pair = reverse((chunk - head_number(h)) & 3)
            t = head_number(h) + reverse(pair)
            x, swap = xp[side ^ sigma, pl.ds(2 * (t & 3), 2)].reshape(H, M), (t & 7) >> 2
            for t in kinds:
                y = nn(x, ws[t, :, part(h % 2, B)])
                for j in TWO:
                    piece = y[part(j, B)]
                    r = 2 * pair + (j ^ swap)
                    if t == QUE:
                        q_s[h, r] = piece.astype(BF)
                    else:
                        kv_s[h, 8 * sigma + r, t] = (piece.T if t == VAL else piece).astype(BF)

    with scope('own_w'):
        for t in range(3):
            own_load(t).wait()
    own, partner = HEADS[:2], HEADS[2:]

    def own_body(g, carry):
        sigma, pair = group(g)
        with scope('own_kv'):
            project(own, sigma, pair, (KEY, VAL))

        @pl.when(g == 1)
        def _():
            lq_z(VAL).start()
            kv_start(kvp_copy, own)

        @pl.when(g == 2)
        def _():
            ev_z(lq_copy, KEY)

        @pl.when(g == 4)
        def _():
            kvr_copy(0, 0).start()
        return carry

    lax.fori_loop(0, 6, own_body, None)
    lq_z(QUE).start()
    ev_xy(lq_copy, KEY)

    def own_q_body(pair, carry):
        with scope('own_q'):
            project(own, 0, pair, (QUE,))
        return carry

    lax.fori_loop(0, 4, own_q_body, None)

    def tile(h, c, kind):
        a = head_number(h)
        rel = (c - a) & 3
        b0, b01, b1, b012, b12, b2, b0123, b123, b23, b3 = [beta_ref[i, h] for i in range(10)]

        def group_of(ref, i, weights):
            parts = []
            n = 0
            for count, b in weights:
                def values(i=i + n, count=count):
                    v = [ref[h, i + j, VAL] for j in range(count)]
                    return v[0] if count == 1 else jnp.concatenate(v, axis=1)
                parts.append((values, count * B, b))
                n += count
            return (lambda: ref[h, i:i + n, KEY].reshape(n * B, B)), parts

        def put(k, ot):
            y = ot.T.astype(BF)
            col = (h % 2) * B
            pl.when(h >= 2)(lambda: o_at(k, 1, 0, col, B).__setitem__(..., y))
            pl.when(h < 2)(lambda: o_at(k, 0, 0, col, B).__setitem__(..., y))

        def both(ot):
            swap = ((a + rel) & 7) >> 2
            for j in TWO:
                put(2 * c + (j ^ swap), ot[:, part(j, B)])

        def wide(ref):
            return lambda off, n: ref.at[pl.ds(off, n), :]

        def narrow(off, n):
            lane = off // 3072
            return s_scr.at[pl.ds(off - lane * 3072, n), pl.ds(lane * B, B)]

        if kind == 'odd':
            groups = [group_of(kv_s, i, [(2, None)]) for i in range(0, 8, 2)]
            return tile_steps(lambda: q_s[h, pl.ds(jnp.where(rel == 1, 4, 6), 2)].reshape(H, B), groups, wide(t_scr), both)
        if kind == 'two':
            groups = [group_of(kv_s, i, [(2, b)]) for i, b in ((0, b01), (2, b01), (4, b0), (6, b0), (8, b1), (10, b1))]
            return tile_steps(lambda: q_s[h, 2:4].reshape(H, B), groups, wide(s_scr), both)
        if kind == 'one':
            groups = [group_of(kv_s, 0, [(2, b012), (2, b01)]), group_of(kv_s, 4, [(2, b0), (2, b0)]), group_of(kv_s, 8, [(2, b12), (2, b1)]),
                      group_of(kvp_s, 0, [(2, b2), (2, b2)])]
            return tile_steps(lambda: q_s[h, 1], groups, narrow, lambda ot: put(2 * c + ((a >> 2) ^ 1), ot))
        pair = [(1, b23), (1, b2)]
        groups = [group_of(kv_s, 0, [(1, b0123), (1, b012), (2, b01)]), group_of(kv_s, 4, [(2, b0), (2, b0)]), group_of(kv_s, 8, [(1, b123), (1, b12), (2, b1)]),
                  group_of(kvp_s, 0, pair + pair), group_of(kvr_s, 0, [(2, b3), (2, b3)])]
        return tile_steps(lambda: q_s[h, 0], groups, narrow, lambda ot: put(2 * c + (a >> 2), ot))

    def chunk_tiles(n):
        c, first = n % 4, n // 4 * 2
        special = first + (c & 1)
        rest = first + 1 - (c & 1)
        rel = (c - head_number(special)) & 3

        @pl.when(rel == 2)
        def _():
            with scope('tile2'):
                run_tiles([tile(rest, c, 'odd'), tile(special, c, 'two')])

        @pl.when(rel == 0)
        def _():
            with scope('tile1'):
                run_tiles([tile(rest, c, 'odd'), tile(special, c, 'one')])

    def send_o(ks, p):
        @pl.when(outer)
        def _():
            for k in ks:
                o_copy(order(k), p).start()

    def step_body(t, carry):
        def flag(kind):
            return functools.reduce(jnp.logical_or, [(t >= s) & (t < s + n) for s, n in runs(STEPS, kind)])

        def count(kind):
            return sum(jnp.clip(t - s, 0, n) for s, n in runs(STEPS, kind))

        @pl.when(flag('K'))
        def _():
            with scope('par_k'):
                project(partner, *group(count('K')), (KEY,))

        @pl.when(flag('V'))
        def _():
            with scope('par_v'):
                project(partner, *group(count('V')), (VAL,))

        @pl.when(flag('Q'))
        def _():
            with scope('par_q'):
                project(partner, 0, None, (QUE,), count('Q'))

        pl.when(flag('A') | flag('B'))(lambda: chunk_tiles(jnp.where(flag('B'), 4 + count('B'), count('A'))))

        @pl.when(flag('Z'))
        def _():
            with scope('tile0'):
                h = count('Z')
                run_tiles([tile(h, head_number(h) & 3, 'zero')])

        @pl.when(flag('R') & inner)
        def _():
            n = count('R')
            k = order(n)
            with scope('wait_o'):
                for p in TWO:
                    o_copy(k, p).wait_recv()
            with scope('proj_r'):
                y = o_times(k, slice(0, 1024))
                for v in (2, 3):
                    y_src(k, v)[...] = y[:, part(v - 2, H)]
                    y_copy(k, v, side).start()

        @pl.when(flag('L') & inner)
        def _():
            k = order(count('L'))
            with scope('proj_l'):
                y = o_times(k, slice(1024, M))
                y_src(k, 1)[...] = y[:, H:]
                y_copy(k, 1, side).start()
                y_src(k, 0)[...] = y[:, :H]
                y_local(k).start()

        call = functools.partial

        events = {
            'zv': [call(ev_z, lq_copy, VAL)],
            'zq': [call(ev_z, lq_copy, QUE), call(lo_start, 0)],
            'xv': [call(ev_xy, lq_copy, VAL)],
            'xq': [call(ev_xy, lq_copy, QUE)],
            'wk': [call(ev_weights, KEY)],
            'wv': [call(ev_weights, VAL)],
            'wq': [call(ev_weights, QUE)],
            'zl': [call(on, inner, call(ev_z, lo_copy, 0)), call(lo_start, 1)],
            'xl': [call(on, inner, call(ev_xy, lo_copy, 0))],
            'wl': [call(on, inner, call(ev_done, lo_copy, 0), lambda: start(wo_load(0)), lambda: wait(wo_load(0)), lambda: wait(wo_own()))],
            'zm': [call(on, inner, call(ev_z, lo_copy, 1))],
            'xm': [call(on, inner, call(ev_xy, lo_copy, 1))],
            'wm': [call(on, inner, call(ev_done, lo_copy, 1), lambda: start(wo_load(1)), lambda: wait(wo_load(1)))],
            'free': [call(signal_ready, 1), call(on, inner, lambda: start(wo_own())), call(wait_ready, 0), call(wait_ready, 1)],
            'po': [call(kv_wait, kvp_copy, own)],
            'pp': [call(kv_wait, kvp_copy, partner)],
            'sp': [call(kv_start, kvp_copy, partner)],
            's01': [lambda: kvr_copy(0, 1).start()],
            's1': [call(kv_start, kvr_copy, [1])],
            'sr': [call(kv_start, kvr_copy, partner)],
        }
        for h in HEADS:
            events[f'f{h}'] = [call(kv_forward, [h])]
            events[f'g{h}'] = [call(kv_wait, kvf_copy, [h])]
        for k in ROWS:
            for p in TWO:
                events['op'[p] + str(k)] = [call(send_o, (k,), p)]
        todo = [(i, s) for i, s in enumerate(AFTER) if s]
        for j in range(0, len(todo), 4):
            some = todo[j:j + 4]

            @pl.when((t >= some[0][0]) & (t <= some[-1][0]))
            def _(some=some):
                for i, s in some:
                    @pl.when(t == i)
                    def _(s=s):
                        for c in s.split(','):
                            for call_ in events[c]:
                                call_()
        return carry

    lax.fori_loop(0, len(STEPS), step_body, None)

    for t in range(3):
        lq_z(t).wait_send()
        sends_done(lq_copy, t)
    for u in TWO:
        for dst in (1, 2):
            pl.when(tp != dst)(lambda u=u, dst=dst: lo_z(u, dst).wait_send())
        pl.when(inner)(lambda u=u: sends_done(lo_copy, u))
    for h in HEADS:
        for s in TWO:
            for copy in (kvp_copy, kvr_copy, kvf_copy):
                copy(h, s).wait_send()

    @pl.when(outer)
    def _():
        for k in ROWS:
            for p in TWO:
                o_copy(k, p).wait_send()

    @pl.when(inner)
    def _():
        for k in ROWS:
            for v in (1, 2, 3):
                y_copy(k, v, side).wait_send()
            y_local(k).wait()

    for seg in TWO:
        @pl.when(tp != 1 + seg)
        def _(seg=seg):
            for k in ROWS:
                with scope(f'recv{k}_{seg}'):
                    y_copy(k, 1, seg).wait_recv()


PROGRAM = (
    '-.zv,s01,po', 'A.wk', 'K', 'K.xv', 'K', 'K', 'K.zq', 'K', 'A.wv', 'V', 'V.sp,xq', 'V.f0', 'V.zl,s1', 'V.g0', 'V.zm,sr,free', 'Z.o0,wq', 'Q.pp',
    'B.p0,xl', 'Q', 'Q', 'Q', 'B.p1', '-.wl', 'R.f1,xm,g1', 'Z.o1', 'A', 'B.o2,p2', 'R', 'A.wm', 'B.o3,p3', 'R', 'L.o4,o5,o6,o7', 'L.f2', 'L.f3',
    '-.g2,g3', 'Z', 'Z.p4,p5,p6,p7', 'R', 'L', 'R', 'L', 'R', 'L', 'R', 'L', 'R', 'L',
)
STEPS = [s.partition('.')[0] for s in PROGRAM]
AFTER = [s.partition('.')[-1] for s in PROGRAM]


def main(beta, x, wk, wv, wq, w_out):
    anyspec = pl.BlockSpec(memory_space=pl.ANY)
    vmem = [((4, B, M), BF), ((B, B), BF), ((2, 8, B, M), BF), ((3, M, H), BF), ((4, 8, B, B), BF), ((4, 12, 2, B, B), BF), ((4, 4, 2, B, B), BF), ((4, 4, 2, B, B), BF),
            ((3072, H), F32), ((M, H), F32)]
    dma = [(4,), (3, 8), (3, 8, 3, 2), (3, 8), (3, 8), (2, 2), (2, 3), (2, 8), (2, 8)] + [(4, 2)] * 6 + [(8, 2), (8, 2), (8, 4), (2, 8)]
    return pl.pallas_call(
        main_kernel,
        in_specs=[pl.BlockSpec(memory_space=pltpu.SMEM)] + [anyspec] * 5,
        out_specs=[anyspec] * 3,
        out_shape=[jax.ShapeDtypeStruct(s, BF) for s in ((2, 8, B, H), (8, 3, B, H), (8, 2, 3, H, 128))],
        scratch_shapes=[pltpu.VMEM(*v) for v in vmem] + [pltpu.SemaphoreType.DMA(d) for d in dma] + [pltpu.SemaphoreType.REGULAR((2,))],
        compiler_params=params(collective_id=0, has_side_effects=True),
        cost_estimate=pl.CostEstimate(flops=10**11, bytes_accessed=10**8, transcendentals=0),
        name='main',
    )(beta, x, wk, wv, wq, w_out)[0]


def solution(mesh):
    tp_size = mesh.shape['tp']

    def device_fn(hidden, w_query, w_key, w_value, w_out, branch_bias):
        tp = lax.axis_index('tp')
        heads = branch_bias.shape[1] // tp_size
        b = jnp.concatenate([lax.dynamic_slice_in_dim(branch_bias, t * heads, heads, axis=1) for t in (tp, tp ^ 2)], axis=1)
        beta = []
        for branches in ('0', '01', '1', '012', '12', '2', '0123', '123', '23', '3'):
            rows = [b[i:i + 1] for i in map(int, branches)]
            m = functools.reduce(jnp.maximum, rows)
            beta.append((m + jnp.log(sum(jnp.exp(r - m) for r in rows))) * math.log2(math.e))
        return unpermute(main(jnp.concatenate(beta), hidden, w_key, w_value, w_query, w_out))

    return jax.shard_map(device_fn, mesh=mesh, in_specs=(P(('dp', 'sp'), None), P(None, 'tp'), P(None, 'tp'), P(None, 'tp'), P('tp', None), P(None, None)), out_specs=P(('dp', 'sp'), 'tp'), check_vma=False)
```

```python
import functools
import math

import jax
import jax.numpy as jnp
from jax import lax
from jax.experimental import pallas as pl
from jax.experimental.pallas import tpu as pltpu
from jax.sharding import PartitionSpec as P

MESH = pl.DeviceIdType.MESH
BF = jnp.bfloat16
F32 = jnp.float32
B, H, M = 256, 512, 2048
KAPPA = math.log2(math.e) / 16
VMEM = 66_900_000
SLOT = (0, 4, 2, 6, 1, 5, 3, 7)
KEY, VAL, QUE = range(3)
HEADS = range(4)
TWO = range(2)
ROWS = range(8)


def nn(a, b):
    return lax.dot_general(a, b, (((1,), (0,)), ((), ())), preferred_element_type=F32)


def nt(a, b):
    return lax.dot_general(a, b, (((1,), (1,)), ((), ())), preferred_element_type=F32)


def params(**kw):
    return pltpu.CompilerParams(vmem_limit_bytes=VMEM, **kw)


def ds(start, size, align=128):
    return pl.ds(pl.multiple_of(start, align), size)


def part(i, size):
    return slice(i * size, i * size + size)


def phase_matrix(transposed):
    r = lax.broadcasted_iota(jnp.int32, (B, B), int(transposed))
    p = lax.broadcasted_iota(jnp.int32, (B, B), int(not transposed))
    k = r // 32
    return (p == (r % 32) * 8 + k // 2 + 4 * (k % 2)).astype(F32).astype(BF)


def unpermute_kernel(y_ref, o_ref, pm_ref):
    @pl.when(pl.program_id(0) + pl.program_id(1) == 0)
    def _():
        pm_ref[...] = phase_matrix(True)

    for j in range(y_ref.shape[1] // 32):
        y = y_ref[:, part(j, 32), :].reshape(B, y_ref.shape[-1])
        o_ref[part(j, B), :] = nn(pm_ref[...], y).astype(BF)


def unpermute(y):
    s, k, i, c = y.shape
    return pl.pallas_call(
        unpermute_kernel,
        grid=(s, 2),
        in_specs=[pl.BlockSpec((None, k, i // 2, c), lambda s, j: (s, 0, j, 0))],
        out_specs=pl.BlockSpec((k * i // 2, c), lambda s, j: (s * 2 + j, 0)),
        out_shape=jax.ShapeDtypeStruct((s * k * i, c), BF),
        scratch_shapes=[pltpu.VMEM((B, B), BF)],
        compiler_params=params(),
        name='unpermute',
    )(y)


def tile_steps(q, wide, narrow, s_ref, n_ref, done):
    st = {}
    logits, sums = [], []

    def add(name, x):
        st[name] = st[name] + x if name in st else x

    for groups, ref in ((wide, s_ref), (narrow, n_ref)):
        off = 0
        for keys, parts in groups:
            def qk(keys=keys, parts=parts, off=off, ref=ref):
                s = nt(keys(), q() if ref is s_ref else q()[:B])
                o = 0
                for _, n, b in parts:
                    piece = s[o:o + n]
                    ref[pl.ds(off + o, n), :] = piece
                    t = jnp.max(piece, axis=0, keepdims=True) * KAPPA
                    if b is not None:
                        t = t + b
                    if ref is n_ref:
                        t = jnp.concatenate([t, st['top'][:, B:]], axis=1)
                    st['top'] = jnp.maximum(st['top'], t) if 'top' in st else t
                    o += n
            logits.append(qk)
            for v, n, b in parts:
                def sv(v=v, n=n, b=b, off=off, ref=ref):
                    top = st['top'] if ref is s_ref else st['top'][:, :B]
                    e = jnp.exp2(ref[pl.ds(off, n), :] * KAPPA - (top if b is None else top - b))
                    name = 'w' if ref is s_ref else 'n'
                    add('l' + name, jnp.sum(e, axis=0, keepdims=True))
                    add('o' + name, nn(v(), e.astype(BF)))
                sums.append(sv)
                off += n

    def finish():
        o, l = st['ow'], st['lw']
        if narrow:
            o = jnp.concatenate([o[:, :B] + st['on'], o[:, B:]], axis=1)
            l = jnp.concatenate([l[:, :B] + st['ln'], l[:, B:]], axis=1)
        done(o / l)

    return logits, sums + [finish]


def interleave(a, b):
    i = j = 0
    while i < len(a) or j < len(b):
        if j >= len(b) or (i < len(a) and i * len(b) <= j * len(a)):
            a[i]()
            i += 1
        else:
            b[j]()
            j += 1


def run_tiles(tiles):
    before = []
    for logits, sums in tiles:
        interleave(logits, before)
        before = sums
    interleave([], before)


def on(cond, *calls):
    @pl.when(cond)
    def _():
        for c in calls:
            c()


def scope(name):
    return jax.named_scope(name)


def main_kernel(beta_ref, x_ref, wk_ref, wv_ref, wq_ref, wout_ref, out_ref, lq_ref, lo_ref,
                xb, pm, xp, ws, q_s, kv_s, kvp_s, kvr_s, s_scr, t_scr,
                x_sem, w_sem, wo_sem, lq_send, lq_recv, lo_zsend, lo_zrecv, lo_send, lo_recv,
                kvp_send, kvp_recv, kvr_send, kvr_recv, kvf_send, kvf_recv, o_send, o_recv, y_send, y_recv, ready):
    dp, tp, sp = lax.axis_index('dp'), lax.axis_index('tp'), lax.axis_index('sp')
    idx = dp * 4 + sp
    side = tp // 2
    inner = (tp == 1) | (tp == 2)
    outer = jnp.logical_not(inner)
    W = (wk_ref, wv_ref, wq_ref)
    peer_x, peer_y, peer_c = {'dp': dp ^ 1}, {'sp': sp ^ 2}, {'sp': sp ^ 1}

    def remote(src, dst, ss, rs, dev):
        return pltpu.make_async_remote_copy(src_ref=src, dst_ref=dst, send_sem=ss, recv_sem=rs, device_id=dev, device_id_type=MESH)

    def lq_copy(t, src, dst, dev):
        return remote(lq_ref.at[src, t], lq_ref.at[dst, t], lq_send.at[t, dst], lq_recv.at[t, dst], dev)

    def lq_z(t):
        return remote(W[t].at[ds(idx * B, B), :], lq_ref.at[0, t], lq_send.at[t, 0], lq_recv.at[t, 0], {'tp': tp ^ 2})

    def lo_copy(v, src, dst, dev):
        return remote(lo_ref.at[v, src], lo_ref.at[v, dst], lo_send.at[v, dst], lo_recv.at[v, dst], dev)

    def lo_z(v, dst):
        b = (tp ^ dst) - 1
        return remote(wout_ref.at[ds(idx * 64, 64, 64), ds((dst ^ v) * H, H)], lo_ref.at[v, 0, b], lo_zsend.at[dst - 1, v], lo_zrecv.at[v, b], {'tp': dst})

    def lo_start(*vs):
        for v in vs:
            for dst in (1, 2):
                pl.when(tp != dst)(lambda v=v, dst=dst: lo_z(v, dst).start())

    def lo_zwait(v):
        for b in range(3):
            remote(lo_ref.at[v, 0, b], lo_ref.at[v, 0, b], lo_zsend.at[0, v], lo_zrecv.at[v, b], {'tp': tp}).wait_recv()

    def hop(copy, p, i):
        near, far = (peer_y, peer_x) if copy is lq_copy or p < 2 else (peer_x, peer_y)
        n, f = (2, 1) if near is peer_y else (1, 2)
        return copy(p, *((0, n, near), (0, f, far), (0, 4, peer_c), (n, 3, far), (n, 4 + n, peer_c), (f, 4 + f, peer_c), (3, 7, peer_c))[i])

    def ev_z(copy, *ps):
        for p in ps:
            with scope(f'z_{copy.__name__}{p}'):
                lq_z(p).wait_recv() if copy is lq_copy else lo_zwait(p)
            for i in range(3):
                hop(copy, p, i).start()

    def ev_xy(copy, *ps):
        for p in ps:
            with scope(f'n_{copy.__name__}{p}'):
                hop(copy, p, 0).wait_recv()
            hop(copy, p, 3).start()
            hop(copy, p, 4).start()
        for p in ps:
            with scope(f'f_{copy.__name__}{p}'):
                hop(copy, p, 1).wait_recv()
            hop(copy, p, 5).start()

    def ev_done(copy, *ps):
        for p in ps:
            with scope(f'x2_{copy.__name__}{p}'):
                hop(copy, p, 3).wait_recv()
            hop(copy, p, 6).start()
        for p in ps:
            with scope(f'c_{copy.__name__}{p}'):
                for i in (2, 4, 5, 6):
                    hop(copy, p, i).wait_recv()

    def sends_done(copy, p):
        for i in range(7):
            hop(copy, p, i).wait_send()

    def w_load(t):
        return [pltpu.make_async_copy(lq_ref.at[s, t], ws.at[t, ds((idx ^ m) * B, B), :], w_sem.at[t, s]) for s, m in enumerate(SLOT)]

    def own_load(t):
        return pltpu.make_async_copy(W[t], ws.at[t], w_sem.at[t, 0])

    def start(copies):
        for c in copies:
            c.start()

    def wait(copies):
        for c in copies:
            c.wait()

    def ev_weights(t):
        ev_done(lq_copy, t)
        start(w_load(t))
        wait(w_load(t))

    wo = xp.at[1 - side]

    def wo_own():
        return [pltpu.make_async_copy(wout_ref.at[pl.ds(r * B, B), pl.ds(c * H, H)], xp.at[1 - side, r, :, ds((c ^ tp ^ 2) * H, H)], wo_sem.at[4, r * 4 + c, 0])
                for r in TWO for c in range(4)]

    def wo_load(*vs):
        out = []
        for v in vs:
            for s, m in enumerate(SLOT):
                for b in range(3):
                    row = (idx ^ m) * 64
                    out.append(pltpu.make_async_copy(lo_ref.at[v, s, b], xp.at[1 - side, 2 + 2 * b + row // B, ds(row % B, 64, 64), pl.ds((v ^ 2) * H, H)],
                                                     wo_sem.at[v, s, b]))
        return out

    def kvp_copy(h, s):
        return remote(kv_s.at[h, pl.ds(8 * s, 2)], kvp_s.at[h, pl.ds(2 * s, 2)], kvp_send.at[h, s], kvp_recv.at[h, s], peer_c)

    def kvr_copy(h, s):
        return remote(kv_s.at[h, 8 * s], kvr_s.at[h, s], kvr_send.at[h, s], kvr_recv.at[h, s], peer_y)

    def kvf_copy(h, s):
        return remote(kvr_s.at[h, s], kvr_s.at[h, 2 + s], kvf_send.at[h, s], kvf_recv.at[h, s], peer_c)

    def kv_start(copy, heads):
        for h in heads:
            for s in TWO:
                copy(h, s).start()

    def kv_wait(copy, heads):
        with scope(f'w_{copy.__name__}{heads[0]}'):
            for h in heads:
                for s in TWO:
                    copy(h, s).wait_recv()

    def kv_forward(heads):
        kv_wait(kvr_copy, heads)
        kv_start(kvf_copy, heads)

    def reverse(i):
        return (i % 2) * 2 + i // 2

    def order(n):
        return 2 * reverse(n % 4) + ((n // 4) ^ side)

    def o_at(k, p, theirs, col, size):
        return ws.at[theirs, ds(k * B, B), ds(col, size)] if p else xb.at[k // 2, :, ds((k % 2) * 1024 + theirs * H + col, size)]

    def o_copy(k, p):
        return remote(o_at(k, p, 0, 0, H), o_at(k, p, 1, 0, H), o_send.at[k, p], o_recv.at[k, p], {'tp': tp ^ 1})

    def o_times(k, v, n):
        cols = pl.ds((v ^ 2) * H, n * H)
        y = nn(xb[k // 2, :, ds((k % 2) * 1024, 1024)], wo[0:4, :, cols].reshape(1024, n * H))
        for i in TWO:
            y = y + nn(ws[i, ds(k * B, B), :], wo[part(2 + i, 2), :, cols].reshape(H, n * H))
        y = y.astype(BF)
        for i in range(n):
            y_src(k, v + i)[...] = y[:, part(i, H)]
            y_copy(k, v + i, side).start() if v else y_local(k).start()

    def y_src(k, v):
        return xp.at[side, k, :, pl.ds(v * H, H)]

    def y_copy(k, v, seg):
        return remote(y_src(k, v), out_ref.at[seg, k], y_send.at[k, v], y_recv.at[seg, k], {'tp': tp ^ v})

    def y_local(k):
        return pltpu.make_async_copy(y_src(k, 0), out_ref.at[side, k], y_send.at[k, 0])

    def x_copy(j):
        return pltpu.make_async_copy(x_ref.at[ds(j * B, B), :], xb.at[lax.rem(j, 4)], x_sem.at[lax.rem(j, 4)])

    for j in range(4):
        x_copy(j).start()
    for t in range(3):
        own_load(t).start()
    barrier = pltpu.get_barrier_semaphore()
    peers = [{'tp': tp ^ 1}, {'tp': tp ^ 2}, {'tp': tp ^ 3}, peer_x, peer_y, peer_c]
    for dev in peers:
        pl.semaphore_signal(barrier, inc=1, device_id=dev, device_id_type=MESH)
    with scope('barrier'):
        pl.semaphore_wait(barrier, len(peers))
    lq_z(KEY).start()

    pm[...] = phase_matrix(False)

    def permute_body(j, carry):
        x_copy(j).wait()
        y = nn(pm[...], xb[lax.rem(j, 4)]).astype(BF).reshape(8, 32, M)
        xp[j // 8, :, ds(lax.rem(j, 8) * 32, 32, 32), :] = y
        pl.when(j < 12)(lambda: x_copy(j + 4).start())
        return carry

    with scope('permute'):
        lax.fori_loop(0, 16, permute_body, None)

    def signal_ready(i):
        pl.when(inner)(lambda: pl.semaphore_signal(ready.at[i], inc=1, device_id={'tp': tp ^ 1}, device_id_type=MESH))

    def wait_ready(i):
        with scope(f'ready{i}'):
            pl.when(outer)(lambda: pl.semaphore_wait(ready.at[i], 1))

    signal_ready(0)

    def group(g):
        low = g < 4
        return jnp.where(low, g & 1, 0), jnp.where(low, g // 2, g - 2)

    def head_number(h):
        return 2 * (tp ^ (h // 2 * 2)) + h % 2

    def project(heads, sigma, pair, kinds):
        for h in heads:
            t = head_number(h) + reverse(pair)
            x, swap = xp[side ^ sigma, pl.ds(2 * (t & 3), 2)].reshape(H, M), (t & 7) >> 2
            for t in kinds:
                y = nn(x, ws[t, :, part(h % 2, B)])
                for j in TWO:
                    piece = y[part(j, B)]
                    kv_s[h, 8 * sigma + 2 * pair + (j ^ swap), t] = (piece.T if t == VAL else piece).astype(BF)

    def phases_of(j):
        return [j % 2 + 2 * i for i in TWO], (j // 2) ^ side

    def rank_of(phase, h):
        rel = (phase - head_number(h)) & 7
        return (rel & 1) * 4 + ((rel >> 1) & 1) * 2 + (rel >> 2)

    def queries(heads, j):
        phases, half = phases_of(j)
        x = jnp.concatenate([xp[side, 2 * f + half] for f in phases])
        for h in heads:
            y = nn(x, ws[QUE, :, part(h % 2, B)]).astype(BF)
            for i, f in enumerate(phases):
                q_s[h, rank_of(f + 4 * half, h)] = y[part(i, B)]

    with scope('own_w'):
        for t in range(3):
            own_load(t).wait()
    own, partner = HEADS[:2], HEADS[2:]

    def own_body(g, carry):
        sigma, pair = group(g)
        with scope('own_kv'):
            project(own, sigma, pair, (KEY, VAL))

        @pl.when(g == 1)
        def _():
            lq_z(VAL).start()
            kv_start(kvp_copy, own)

        @pl.when(g == 2)
        def _():
            ev_z(lq_copy, KEY)

        @pl.when(g == 4)
        def _():
            kvr_copy(0, 0).start()
        return carry

    lax.fori_loop(0, 6, own_body, None)
    ev_xy(lq_copy, KEY)

    def own_q_body(pair, carry):
        with scope('own_q'):
            queries(own, pair)
        return carry

    lax.fori_loop(0, 4, own_q_body, None)
    lq_z(QUE).start()

    lane = lax.broadcasted_iota(jnp.int32, (1, H), 1)

    def mix(b, c):
        return jnp.where(lane < B, b, c)

    def keys_of(ref, h, i, weights):
        parts = []
        n = 0
        for count, b in weights:
            def values(i=i + n, count=count):
                v = [ref[h, i + j, VAL] for j in range(count)]
                return v[0] if count == 1 else jnp.concatenate(v, axis=1)
            parts.append((values, count * B, b))
            n += count
        return (lambda: ref[h, i:i + n, KEY].reshape(n * B, B)), parts

    def chunk_tiles(p, j, kind):
        both_phases, half = phases_of(j)

        def put(h, phase, ot):
            k = 2 * (phase & 3) + half
            y = ot.T.astype(BF)
            for i in TWO:
                pl.when(p == i)(lambda i=i: o_at(k, i, 0, (h % 2) * B, B).__setitem__(..., y))

        def tile(h, phases, ranks, wide, narrow, s_ref, n_ref):
            def done(ot):
                for i, phase in enumerate(phases):
                    put(h, phase, ot[:, part(i, B)])
            return tile_steps(lambda: jnp.concatenate([q_s[h, r] for r in ranks]), wide, narrow, s_ref, n_ref, done)

        h = 2 * p + (j % 2) ^ 1
        rest = tile(h, both_phases, [rank_of(f + 4 * half, h) for f in both_phases], [keys_of(kv_s, h, i, [(2, None)]) for i in range(0, 8, 2)], [], t_scr, None)
        h = 2 * p + (j % 2)
        a = head_number(h)
        b0, b01, b1, b012, b12, b2, b0123, b123, b23, b3 = [beta_ref[i, h] for i in range(10)]
        phases = [a & 3, (a & 3) ^ 2]
        both = [keys_of(kv_s, h, i, [(2, b)]) for i, b in ((2, b01), (4, b0), (6, b0), (10, b1))]
        if kind == 0:
            both += [keys_of(kv_s, h, 0, [(1, mix(b0123, b01)), (1, mix(b012, b01))]), keys_of(kv_s, h, 8, [(1, mix(b123, b1)), (1, mix(b12, b1))])]
            first = [keys_of(kvp_s, h, 0, [(1, b23), (1, b2)] * 2), keys_of(kvr_s, h, 0, [(2, b3)] * 2)]
        else:
            both += [keys_of(kv_s, h, 0, [(2, mix(b012, b01))]), keys_of(kv_s, h, 8, [(2, mix(b12, b1))])]
            first = [keys_of(kvp_s, h, 0, [(2, b2)] * 2)]
        with scope(f'tile{kind}'):
            run_tiles([rest, tile(h, phases, [kind, rank_of(phases[1] + 4 * half, h)], both, first, s_scr, t_scr.at[:, pl.ds(0, B)])])

    def send_o(ks, p):
        @pl.when(outer)
        def _():
            for k in ks:
                o_copy(order(k), p).start()

    def step_body(t, carry):
        packed = functools.reduce(lambda x, i: jnp.where(t == i, TABLE[i], x), range(len(TABLE)), 0)
        code, n, event = packed % 16, packed // 16 % 16, packed // 256 - 1

        def kind(c):
            return code == KINDS.index(c)

        for c, t_ in (('K', KEY), ('V', VAL)):
            @pl.when(kind(c))
            def _(t_=t_):
                with scope(f'par_{t_}'):
                    project(partner, *group(n), (t_,))

        @pl.when(kind('Q'))
        def _():
            with scope('par_q'):
                queries(partner, n)

        for i in TWO:
            pl.when(kind('AB'[i]))(lambda i=i: chunk_tiles(n // 4, n % 4, i))

        for c, v, m in (('R', 2, 2), ('L', 1, 1), ('N', 0, 1)):
            @pl.when(kind(c) & inner)
            def _(c=c, v=v, m=m):
                k = order(n)
                if c == 'R':
                    with scope('wait_o'):
                        for p in TWO:
                            o_copy(k, p).wait_recv()
                with scope(f'out{v}'):
                    o_times(k, v, m)

        call = functools.partial

        events = {
            'zv': [call(ev_z, lq_copy, VAL)],
            'zq': [call(ev_z, lq_copy, QUE)],
            'xv': [call(ev_xy, lq_copy, VAL)],
            'xq': [call(ev_xy, lq_copy, QUE)],
            'wk': [call(ev_weights, KEY)],
            'wv': [call(ev_weights, VAL)],
            'wq': [call(ev_weights, QUE)],
            'free': [call(signal_ready, 1), call(on, inner, lambda: start(wo_own())), call(wait_ready, 1)],
            'rz': [call(wait_ready, 0)],
            'po': [call(kv_wait, kvp_copy, own)],
            'pp': [call(kv_wait, kvp_copy, partner)],
            'sp': [call(kv_start, kvp_copy, partner)],
            's01': [lambda: kvr_copy(0, 1).start()],
            's1': [call(kv_start, kvr_copy, [1])],
            'sr': [call(kv_start, kvr_copy, partner)],
        }
        for i, vs in enumerate(((2, 3), (1,), (0,))):
            events[f'b{i}'] = [call(lo_start, *vs)]
            events[f'z{i}'] = [call(on, inner, call(ev_z, lo_copy, *vs))]
            events[f'x{i}'] = [call(on, inner, call(ev_xy, lo_copy, *vs))]
            events[f'w{i}'] = [call(on, inner, call(ev_done, lo_copy, *vs), lambda vs=vs: start(wo_load(*vs)), lambda vs=vs: wait(wo_load(*vs)))]
        events['w0'] += [call(on, inner, lambda: wait(wo_own()))]
        for h in HEADS:
            events[f'f{h}'] = [call(kv_forward, [h])]
            events[f'g{h}'] = [call(kv_wait, kvf_copy, [h])]
        for k in ROWS:
            for p in TWO:
                events['op'[p] + str(k)] = [call(send_o, (k,), p)]
        @pl.when(event >= 0)
        def _():
            for i, names in enumerate(EVENTS):
                on(event == i, *[c for name in names.split(',') for c in events[name]])
        return carry

    lax.fori_loop(0, len(TABLE), step_body, None)

    for t in range(3):
        lq_z(t).wait_send()
        sends_done(lq_copy, t)
    for v in range(4):
        for dst in (1, 2):
            pl.when(tp != dst)(lambda v=v, dst=dst: lo_z(v, dst).wait_send())
        pl.when(inner)(lambda v=v: sends_done(lo_copy, v))
    for h in HEADS:
        for s in TWO:
            for copy in (kvp_copy, kvr_copy, kvf_copy):
                copy(h, s).wait_send()

    @pl.when(outer)
    def _():
        for k in ROWS:
            for p in TWO:
                o_copy(k, p).wait_send()

    @pl.when(inner)
    def _():
        for k in ROWS:
            for v in (1, 2, 3):
                y_copy(k, v, side).wait_send()
            y_local(k).wait()

    for seg in TWO:
        @pl.when(tp != 1 + seg)
        def _(seg=seg):
            for k in ROWS:
                with scope(f'recv{k}_{seg}'):
                    y_copy(k, 1, seg).wait_recv()


PROGRAM = (
    '-.zv,s01,po,rz', 'T2.o4,o5,wk', 'K', 'K.xv', 'K', 'K.b0', 'K', 'K.zq,f0,g0', 'T0.o0,o1,z0,wv', 'V', 'V.sp,xq', 'V', 'V', 'V', 'V.free', 'T3.wq',
    'Q.pp,x0,s1', 'T4.p0,p1,b1', 'Q', 'Q', 'Q', '-.w0', 'R', 'T5.p2,p3,z1,b2', 'R', '-.f1,g1', 'T1.o2,o3,x1', 'R.sr,z2', '-.w1', 'L', 'L', 'L',
    'R.o6,o7', 'L.x2', '-.f2,f3,g2,g3', 'T6.p4,p5', 'R.w2', 'L', 'T7.p6,p7', 'N', 'N', 'N', 'R', 'L', 'N', 'R', 'L', 'N', 'R', 'L', 'N', 'N', 'N',
)
KINDS = '-KVQABRLN'


def tables():
    table, seen = [], {}
    names = tuple(dict.fromkeys(s.partition('.')[2] for s in PROGRAM if '.' in s))
    for s in PROGRAM:
        name, _, after = s.partition('.')
        kind, n = name[0], seen.get(name[0], 0)
        seen[kind] = n + 1
        if kind == 'T':
            n = int(name[1:])
            kind = 'AB'[n in (2, 3, 4, 5)]
        table.append(KINDS.index(kind) + 16 * n + 256 * (names.index(after) + 1 if after else 0))
    return table, names


TABLE, EVENTS = tables()


def main(beta, x, wk, wv, wq, w_out):
    anyspec = pl.BlockSpec(memory_space=pl.ANY)
    vmem = [((4, B, M), BF), ((B, B), BF), ((2, 8, B, M), BF), ((3, M, H), BF), ((4, 8, B, B), BF), ((4, 12, 2, B, B), BF), ((4, 4, 2, B, B), BF), ((4, 4, 2, B, B), BF),
            ((3072, H), F32), ((M, H), F32)]
    dma = [(4,), (3, 8), (5, 8, 3), (3, 8), (3, 8), (2, 4), (4, 3), (4, 8), (4, 8)] + [(4, 2)] * 6 + [(8, 2), (8, 2), (8, 4), (2, 8)]
    return pl.pallas_call(
        main_kernel,
        in_specs=[pl.BlockSpec(memory_space=pltpu.SMEM)] + [anyspec] * 5,
        out_specs=[anyspec] * 3,
        out_shape=[jax.ShapeDtypeStruct(s, BF) for s in ((2, 8, B, H), (8, 3, B, H), (4, 8, 3, 64, H))],
        scratch_shapes=[pltpu.VMEM(*v) for v in vmem] + [pltpu.SemaphoreType.DMA(d) for d in dma] + [pltpu.SemaphoreType.REGULAR((2,))],
        compiler_params=params(collective_id=0, has_side_effects=True),
        cost_estimate=pl.CostEstimate(flops=10**11, bytes_accessed=10**8, transcendentals=0),
        name='main',
    )(beta, x, wk, wv, wq, w_out)[0]


def solution(mesh):
    tp_size = mesh.shape['tp']

    def device_fn(hidden, w_query, w_key, w_value, w_out, branch_bias):
        tp = lax.axis_index('tp')
        heads = branch_bias.shape[1] // tp_size
        b = jnp.concatenate([lax.dynamic_slice_in_dim(branch_bias, t * heads, heads, axis=1) for t in (tp, tp ^ 2)], axis=1)
        beta = []
        for branches in ('0', '01', '1', '012', '12', '2', '0123', '123', '23', '3'):
            rows = [b[i:i + 1] for i in map(int, branches)]
            m = functools.reduce(jnp.maximum, rows)
            beta.append((m + jnp.log(sum(jnp.exp(r - m) for r in rows))) * math.log2(math.e))
        return unpermute(main(jnp.concatenate(beta), hidden, w_key, w_value, w_query, w_out))

    return jax.shard_map(device_fn, mesh=mesh, in_specs=(P(('dp', 'sp'), None), P(None, 'tp'), P(None, 'tp'), P(None, 'tp'), P('tp', None), P(None, None)), out_specs=P(('dp', 'sp'), 'tp'), check_vma=False)
```

```python
import functools
import math

import jax
import jax.numpy as jnp
from jax import lax
from jax.experimental import pallas as pl
from jax.experimental.pallas import tpu as pltpu
from jax.sharding import PartitionSpec as P

MESH = pl.DeviceIdType.MESH
BF = jnp.bfloat16
F32 = jnp.float32
B, H, M = 256, 512, 2048
KAPPA = math.log2(math.e) / 16
VMEM = 66_900_000
SLOT = (0, 4, 2, 6, 1, 5, 3, 7)
KEY, VAL, QUE = range(3)
HEADS = range(4)
TWO = range(2)
ROWS = range(8)


def nn(a, b):
    return lax.dot_general(a, b, (((1,), (0,)), ((), ())), preferred_element_type=F32)


def nt(a, b):
    return lax.dot_general(a, b, (((1,), (1,)), ((), ())), preferred_element_type=F32)


def params(**kw):
    return pltpu.CompilerParams(vmem_limit_bytes=VMEM, **kw)


def ds(start, size, align=128):
    return pl.ds(pl.multiple_of(start, align), size)


def part(i, size):
    return slice(i * size, i * size + size)


def phase_matrix(transposed):
    r = lax.broadcasted_iota(jnp.int32, (B, B), int(transposed))
    p = lax.broadcasted_iota(jnp.int32, (B, B), int(not transposed))
    k = r // 32
    return (p == (r % 32) * 8 + k // 2 + 4 * (k % 2)).astype(F32).astype(BF)


def unpermute_kernel(y_ref, o_ref, pm_ref):
    @pl.when(pl.program_id(0) + pl.program_id(1) == 0)
    def _():
        pm_ref[...] = phase_matrix(True)

    for j in range(y_ref.shape[1] // 32):
        y = y_ref[:, part(j, 32), :].reshape(B, y_ref.shape[-1])
        o_ref[part(j, B), :] = nn(pm_ref[...], y).astype(BF)


def unpermute(y):
    s, k, i, c = y.shape
    return pl.pallas_call(
        unpermute_kernel,
        grid=(s, 2),
        in_specs=[pl.BlockSpec((None, k, i // 2, c), lambda s, j: (s, 0, j, 0))],
        out_specs=pl.BlockSpec((k * i // 2, c), lambda s, j: (s * 2 + j, 0)),
        out_shape=jax.ShapeDtypeStruct((s * k * i, c), BF),
        scratch_shapes=[pltpu.VMEM((B, B), BF)],
        compiler_params=params(),
        name='unpermute',
    )(y)


def tile_steps(q, wide, narrow, s_ref, n_ref, done):
    st = {}
    logits, sums = [], []

    def add(name, x):
        st[name] = st[name] + x if name in st else x

    for groups, ref in ((wide, s_ref), (narrow, n_ref)):
        off = 0
        for keys, parts in groups:
            def qk(keys=keys, parts=parts, off=off, ref=ref):
                s = nt(keys(), q() if ref is s_ref else q()[:B])
                o = 0
                for _, n, b in parts:
                    piece = s[o:o + n]
                    ref[pl.ds(off + o, n), :] = piece
                    t = jnp.max(piece, axis=0, keepdims=True) * KAPPA
                    if b is not None:
                        t = t + b
                    if ref is n_ref:
                        t = jnp.concatenate([t, st['top'][:, B:]], axis=1)
                    st['top'] = jnp.maximum(st['top'], t) if 'top' in st else t
                    o += n
            logits.append(qk)
            for v, n, b in parts:
                def sv(v=v, n=n, b=b, off=off, ref=ref):
                    top = st['top'] if ref is s_ref else st['top'][:, :B]
                    e = jnp.exp2(ref[pl.ds(off, n), :] * KAPPA - (top if b is None else top - b))
                    name = 'w' if ref is s_ref else 'n'
                    add('l' + name, jnp.sum(e, axis=0, keepdims=True))
                    add('o' + name, nn(v(), e.astype(BF)))
                sums.append(sv)
                off += n

    def finish():
        o, l = st['ow'], st['lw']
        if narrow:
            o = jnp.concatenate([o[:, :B] + st['on'], o[:, B:]], axis=1)
            l = jnp.concatenate([l[:, :B] + st['ln'], l[:, B:]], axis=1)
        done(o / l)

    return logits, sums + [finish]


def interleave(a, b):
    i = j = 0
    while i < len(a) or j < len(b):
        if j >= len(b) or (i < len(a) and i * len(b) <= j * len(a)):
            a[i]()
            i += 1
        else:
            b[j]()
            j += 1


def run_tiles(tiles):
    before = []
    for logits, sums in tiles:
        interleave(logits, before)
        before = sums
    interleave([], before)


def on(cond, *calls):
    @pl.when(cond)
    def _():
        for c in calls:
            c()


def scope(name):
    return jax.named_scope(name)


def main_kernel(beta_ref, x_ref, wk_ref, wv_ref, wq_ref, wout_ref, out_ref, lq_ref, lo_ref,
                xb, pm, xp, ws, q_s, kv_s, kvp_s, kvr_s, s_scr, t_scr,
                x_sem, w_sem, wo_sem, lq_send, lq_recv, lo_zsend, lo_zrecv, lo_send, lo_recv,
                kvp_send, kvp_recv, kvr_send, kvr_recv, kvf_send, kvf_recv, o_send, o_recv, y_send, y_recv, ready):
    dp, tp, sp = lax.axis_index('dp'), lax.axis_index('tp'), lax.axis_index('sp')
    idx = dp * 4 + sp
    side = tp // 2
    inner = (tp == 1) | (tp == 2)
    outer = jnp.logical_not(inner)
    W = (wk_ref, wv_ref, wq_ref)
    peer_x, peer_y, peer_c = {'dp': dp ^ 1}, {'sp': sp ^ 2}, {'sp': sp ^ 1}

    def remote(src, dst, ss, rs, dev):
        return pltpu.make_async_remote_copy(src_ref=src, dst_ref=dst, send_sem=ss, recv_sem=rs, device_id=dev, device_id_type=MESH)

    def lq_copy(t, src, dst, dev):
        return remote(lq_ref.at[src, t], lq_ref.at[dst, t], lq_send.at[t, dst], lq_recv.at[t, dst], dev)

    def lq_z(t):
        return remote(W[t // 2].at[ds(idx * B, B), pl.ds(t % 2 * B, B)], lq_ref.at[0, t], lq_send.at[t, 0], lq_recv.at[t, 0], {'tp': tp ^ 2})

    def lq_start(t):
        for i in TWO:
            lq_z(2 * t + i).start()

    def lo_copy(v, src, dst, dev):
        return remote(lo_ref.at[v, src], lo_ref.at[v, dst], lo_send.at[v, dst], lo_recv.at[v, dst], dev)

    def lo_z(v, dst):
        b = (tp ^ dst) - 1
        return remote(wout_ref.at[ds(idx * 64, 64, 64), ds((dst ^ v) * H, H)], lo_ref.at[v, 0, b], lo_zsend.at[dst - 1, v], lo_zrecv.at[v, b], {'tp': dst})

    def lo_start(*vs):
        for v in vs:
            for dst in (1, 2):
                pl.when(tp != dst)(lambda v=v, dst=dst: lo_z(v, dst).start())

    def lo_zwait(v):
        for b in range(3):
            remote(lo_ref.at[v, 0, b], lo_ref.at[v, 0, b], lo_zsend.at[0, v], lo_zrecv.at[v, b], {'tp': tp}).wait_recv()

    def hop(copy, p, i):
        near, far = (peer_y, peer_x) if copy is lq_copy or p < 2 else (peer_x, peer_y)
        n, f = (2, 1) if near is peer_y else (1, 2)
        return copy(p, *((0, n, near), (0, f, far), (0, 4, peer_c), (n, 3, far), (n, 4 + n, peer_c), (f, 4 + f, peer_c), (3, 7, peer_c))[i])

    def ev_z(copy, *ps):
        for p in ps:
            with scope(f'z_{copy.__name__}{p}'):
                lq_z(p).wait_recv() if copy is lq_copy else lo_zwait(p)
            for i in range(3):
                hop(copy, p, i).start()

    def ev_xy(copy, *ps):
        for p in ps:
            with scope(f'n_{copy.__name__}{p}'):
                hop(copy, p, 0).wait_recv()
            hop(copy, p, 3).start()
            hop(copy, p, 4).start()
        for p in ps:
            with scope(f'f_{copy.__name__}{p}'):
                hop(copy, p, 1).wait_recv()
            hop(copy, p, 5).start()

    def ev_done(copy, *ps):
        for p in ps:
            with scope(f'x2_{copy.__name__}{p}'):
                hop(copy, p, 3).wait_recv()
            hop(copy, p, 6).start()
        for p in ps:
            with scope(f'c_{copy.__name__}{p}'):
                for i in (2, 4, 5, 6):
                    hop(copy, p, i).wait_recv()

    def sends_done(copy, p):
        for i in range(7):
            hop(copy, p, i).wait_send()

    def w_load(t):
        return [pltpu.make_async_copy(lq_ref.at[s, 2 * t + i], ws.at[t, ds((idx ^ m) * B, B), pl.ds(i * B, B)], w_sem.at[2 * t + i, s]) for s, m in enumerate(SLOT) for i in TWO]

    def own_load(t):
        return pltpu.make_async_copy(W[t], ws.at[t], w_sem.at[t, 0])

    def start(copies):
        for c in copies:
            c.start()

    def wait(copies):
        for c in copies:
            c.wait()

    def ev_weights(t):
        ev_done(lq_copy, 2 * t, 2 * t + 1)
        start(w_load(t))
        wait(w_load(t))

    wo = xp.at[1 - side]

    def wo_own():
        return [pltpu.make_async_copy(wout_ref.at[pl.ds(r * B, B), pl.ds(c * H, H)], xp.at[1 - side, r, :, ds((c ^ tp ^ 2) * H, H)], wo_sem.at[4, r * 4 + c, 0])
                for r in TWO for c in range(4)]

    def wo_load(*vs):
        out = []
        for v in vs:
            for s, m in enumerate(SLOT):
                for b in range(3):
                    row = (idx ^ m) * 64
                    out.append(pltpu.make_async_copy(lo_ref.at[v, s, b], xp.at[1 - side, 2 + 2 * b + row // B, ds(row % B, 64, 64), pl.ds((v ^ 2) * H, H)],
                                                     wo_sem.at[v, s, b]))
        return out

    def kvp_copy(h, s):
        return remote(kv_s.at[h, pl.ds(8 * s, 2)], kvp_s.at[h, pl.ds(2 * s, 2)], kvp_send.at[h, s], kvp_recv.at[h, s], peer_c)

    def kvr_copy(h, s):
        return remote(kv_s.at[h, 8 * s], kvr_s.at[h, s], kvr_send.at[h, s], kvr_recv.at[h, s], peer_y)

    def kvf_copy(h, s):
        return remote(kvr_s.at[h, s], kvr_s.at[h, 2 + s], kvf_send.at[h, s], kvf_recv.at[h, s], peer_c)

    def kv_start(copy, heads):
        for h in heads:
            for s in TWO:
                copy(h, s).start()

    def kv_wait(copy, heads):
        with scope(f'w_{copy.__name__}{heads[0]}'):
            for h in heads:
                for s in TWO:
                    copy(h, s).wait_recv()

    def kv_forward(heads):
        kv_wait(kvr_copy, heads)
        kv_start(kvf_copy, heads)

    def reverse(i):
        return (i % 2) * 2 + i // 2

    def order(n):
        return 2 * reverse(n % 4) + ((n // 4) ^ side)

    def o_at(k, p, theirs, col, size):
        return ws.at[theirs, ds(k * B, B), ds(col, size)] if p else xb.at[k // 2, :, ds((k % 2) * 1024 + theirs * H + col, size)]

    def o_copy(k, p):
        return remote(o_at(k, p, 0, 0, H), o_at(k, p, 1, 0, H), o_send.at[k, p], o_recv.at[k, p], {'tp': tp ^ 1})

    def o_times(k, v, n):
        cols = pl.ds((v ^ 2) * H, n * H)
        y = nn(xb[k // 2, :, ds((k % 2) * 1024, 1024)], wo[0:4, :, cols].reshape(1024, n * H))
        for i in TWO:
            y = y + nn(ws[i, ds(k * B, B), :], wo[part(2 + i, 2), :, cols].reshape(H, n * H))
        y = y.astype(BF)
        for i in range(n):
            y_src(k, v + i)[...] = y[:, part(i, H)]
            y_copy(k, v + i, side).start() if v else y_local(k).start()

    def y_src(k, v):
        return xp.at[side, k, :, pl.ds(v * H, H)]

    def y_copy(k, v, seg):
        return remote(y_src(k, v), out_ref.at[seg, k], y_send.at[k, v], y_recv.at[seg, k], {'tp': tp ^ v})

    def y_local(k):
        return pltpu.make_async_copy(y_src(k, 0), out_ref.at[side, k], y_send.at[k, 0])

    def x_copy(j):
        return pltpu.make_async_copy(x_ref.at[ds(j * B, B), :], xb.at[lax.rem(j, 4)], x_sem.at[lax.rem(j, 4)])

    for j in range(4):
        x_copy(j).start()
    for t in range(3):
        own_load(t).start()
    barrier = pltpu.get_barrier_semaphore()
    peers = [{'tp': tp ^ 1}, {'tp': tp ^ 2}, {'tp': tp ^ 3}, peer_x, peer_y, peer_c]
    for dev in peers:
        pl.semaphore_signal(barrier, inc=1, device_id=dev, device_id_type=MESH)
    with scope('barrier'):
        pl.semaphore_wait(barrier, len(peers))
    lq_start(KEY)

    pm[...] = phase_matrix(False)

    def permute_body(j, carry):
        x_copy(j).wait()
        y = nn(pm[...], xb[lax.rem(j, 4)]).astype(BF).reshape(8, 32, M)
        xp[j // 8, :, ds(lax.rem(j, 8) * 32, 32, 32), :] = y
        pl.when(j < 12)(lambda: x_copy(j + 4).start())
        return carry

    with scope('permute'):
        lax.fori_loop(0, 16, permute_body, None)

    def signal_ready(i):
        pl.when(inner)(lambda: pl.semaphore_signal(ready.at[i], inc=1, device_id={'tp': tp ^ 1}, device_id_type=MESH))

    def wait_ready(i):
        with scope(f'ready{i}'):
            pl.when(outer)(lambda: pl.semaphore_wait(ready.at[i], 1))

    signal_ready(0)

    def group(g):
        low = g < 4
        return jnp.where(low, g & 1, 0), jnp.where(low, g // 2, g - 2)

    def head_number(h):
        return 2 * (tp ^ (h // 2 * 2)) + h % 2

    def project(heads, sigma, pair, kinds):
        for h in heads:
            t = head_number(h) + reverse(pair)
            x, swap = xp[side ^ sigma, pl.ds(2 * (t & 3), 2)].reshape(H, M), (t & 7) >> 2
            for t in kinds:
                y = nn(x, ws[t, :, part(h % 2, B)])
                for j in TWO:
                    piece = y[part(j, B)]
                    kv_s[h, 8 * sigma + 2 * pair + (j ^ swap), t] = (piece.T if t == VAL else piece).astype(BF)

    def phases_of(j):
        return [j % 2 + 2 * i for i in TWO], (j // 2) ^ side

    def rank_of(phase, h):
        rel = (phase - head_number(h)) & 7
        return (rel & 1) * 4 + ((rel >> 1) & 1) * 2 + (rel >> 2)

    def queries(heads, j):
        phases, half = phases_of(j)
        x = jnp.concatenate([xp[side, 2 * f + half] for f in phases])
        for h in heads:
            y = nn(x, ws[QUE, :, part(h % 2, B)]).astype(BF)
            for i, f in enumerate(phases):
                q_s[h, rank_of(f + 4 * half, h)] = y[part(i, B)]

    with scope('own_w'):
        for t in range(3):
            own_load(t).wait()
    own, partner = HEADS[:2], HEADS[2:]

    def own_body(g, carry):
        sigma, pair = group(g)
        with scope('own_kv'):
            project(own, sigma, pair, (KEY, VAL))

        @pl.when(g == 0)
        def _():
            kvr_copy(0, 0).start()

        @pl.when(g == 1)
        def _():
            lq_start(VAL)
            ev_z(lq_copy, 0)
            kv_start(kvp_copy, own)

        @pl.when(g == 2)
        def _():
            ev_z(lq_copy, 1)
            kvr_copy(0, 1).start()

        @pl.when(g == 3)
        def _():
            ev_xy(lq_copy, 0)

        @pl.when(g == 4)
        def _():
            ev_xy(lq_copy, 1)
        return carry

    lax.fori_loop(0, 6, own_body, None)

    def own_q_body(pair, carry):
        with scope('own_q'):
            queries(own, pair)
        pl.when(pair == 0)(lambda: lq_start(QUE))
        return carry

    lax.fori_loop(0, 4, own_q_body, None)

    lane = lax.broadcasted_iota(jnp.int32, (1, H), 1)

    def mix(b, c):
        return jnp.where(lane < B, b, c)

    def keys_of(ref, h, i, weights):
        parts = []
        n = 0
        for count, b in weights:
            def values(i=i + n, count=count):
                v = [ref[h, i + j, VAL] for j in range(count)]
                return v[0] if count == 1 else jnp.concatenate(v, axis=1)
            parts.append((values, count * B, b))
            n += count
        return (lambda: ref[h, i:i + n, KEY].reshape(n * B, B)), parts

    def chunk_tiles(p, j, kind):
        both_phases, half = phases_of(j)

        def put(h, phase, ot):
            k = 2 * (phase & 3) + half
            y = ot.T.astype(BF)
            for i in TWO:
                pl.when(p == i)(lambda i=i: o_at(k, i, 0, (h % 2) * B, B).__setitem__(..., y))

        def tile(h, phases, ranks, wide, narrow, s_ref, n_ref):
            def done(ot):
                for i, phase in enumerate(phases):
                    put(h, phase, ot[:, part(i, B)])
            return tile_steps(lambda: jnp.concatenate([q_s[h, r] for r in ranks]), wide, narrow, s_ref, n_ref, done)

        h = 2 * p + (j % 2) ^ 1
        rest = tile(h, both_phases, [rank_of(f + 4 * half, h) for f in both_phases], [keys_of(kv_s, h, i, [(2, None)]) for i in range(0, 8, 2)], [], t_scr, None)
        h = 2 * p + (j % 2)
        a = head_number(h)
        b0, b01, b1, b012, b12, b2, b0123, b123, b23, b3 = [beta_ref[i, h] for i in range(10)]
        phases = [a & 3, (a & 3) ^ 2]
        both = [keys_of(kv_s, h, i, [(2, b)]) for i, b in ((2, b01), (4, b0), (6, b0), (10, b1))]
        if kind == 0:
            both += [keys_of(kv_s, h, 0, [(1, mix(b0123, b01)), (1, mix(b012, b01))]), keys_of(kv_s, h, 8, [(1, mix(b123, b1)), (1, mix(b12, b1))])]
            first = [keys_of(kvp_s, h, i, [(1, b23), (1, b2)]) for i in (0, 2)] + [keys_of(kvr_s, h, i, [(2, b3)]) for i in (0, 2)]
        else:
            both += [keys_of(kv_s, h, 0, [(2, mix(b012, b01))]), keys_of(kv_s, h, 8, [(2, mix(b12, b1))])]
            first = [keys_of(kvp_s, h, i, [(2, b2)]) for i in (0, 2)]
        with scope(f'tile{kind}'):
            run_tiles([rest, tile(h, phases, [kind, rank_of(phases[1] + 4 * half, h)], both, first, s_scr, t_scr.at[:, pl.ds(0, B)])])

    def send_o(ks, p):
        @pl.when(outer)
        def _():
            for k in ks:
                o_copy(order(k), p).start()

    def step_body(t, carry):
        packed = functools.reduce(lambda x, i: jnp.where(t == i, TABLE[i], x), range(len(TABLE)), 0)
        code, n, event = packed % 16, packed // 16 % 16, packed // 256 - 1

        def kind(c):
            return code == KINDS.index(c)

        for c, t_ in (('K', KEY), ('V', VAL)):
            @pl.when(kind(c))
            def _(t_=t_):
                with scope(f'par_{t_}'):
                    for i in TWO:
                        project(partner, *group(2 * n + i), (t_,))

        @pl.when(kind('Q'))
        def _():
            with scope('par_q'):
                queries(partner, n)

        for i in TWO:
            pl.when(kind('AB'[i]))(lambda i=i: chunk_tiles(n // 4, n % 4, i))

        for c, v, m in (('R', 2, 2), ('L', 1, 1), ('N', 0, 1)):
            @pl.when(kind(c) & inner)
            def _(c=c, v=v, m=m):
                k = order(n)
                if c == 'R':
                    with scope('wait_o'):
                        for p in TWO:
                            o_copy(k, p).wait_recv()
                with scope(f'out{v}'):
                    o_times(k, v, m)

        call = functools.partial

        events = {
            'wk': [call(ev_weights, KEY)],
            'wv': [call(ev_weights, VAL)],
            'wq': [call(ev_weights, QUE)],
            'free': [call(signal_ready, 1), call(on, inner, lambda: start(wo_own())), call(wait_ready, 1)],
            'rz': [call(wait_ready, 0)],
            'po': [call(kv_wait, kvp_copy, own)],
            'pp': [call(kv_wait, kvp_copy, partner)],
            'sp': [call(kv_start, kvp_copy, partner)],
            's1': [call(kv_start, kvr_copy, [1])],
            'sr': [call(kv_start, kvr_copy, partner)],
        }
        for t_, c in enumerate('kvq'):
            for i in TWO:
                events[f'z{c}{i}'] = [call(ev_z, lq_copy, 2 * t_ + i)]
                events[f'x{c}{i}'] = [call(ev_xy, lq_copy, 2 * t_ + i)]
        for i, vs in enumerate(((2, 3), (1,), (0,))):
            events[f'b{i}'] = [call(lo_start, *vs)]
            events[f'z{i}'] = [call(on, inner, call(ev_z, lo_copy, *vs))]
            events[f'x{i}'] = [call(on, inner, call(ev_xy, lo_copy, *vs))]
            events[f'w{i}'] = [call(on, inner, call(ev_done, lo_copy, *vs), lambda vs=vs: start(wo_load(*vs)), lambda vs=vs: wait(wo_load(*vs)))]
        events['w0'] += [call(on, inner, lambda: wait(wo_own()))]
        for h in HEADS:
            events[f'f{h}'] = [call(kv_forward, [h])]
            events[f'g{h}'] = [call(kv_wait, kvf_copy, [h])]
        for k in ROWS:
            for p in TWO:
                events['op'[p] + str(k)] = [call(send_o, (k,), p)]
        @pl.when(event >= 0)
        def _():
            for i, names in enumerate(EVENTS):
                on(event == i, *[c for name in names.split(',') for c in events[name]])
        return carry

    lax.fori_loop(0, len(TABLE), step_body, None)

    for t in range(6):
        lq_z(t).wait_send()
        sends_done(lq_copy, t)
    for v in range(4):
        for dst in (1, 2):
            pl.when(tp != dst)(lambda v=v, dst=dst: lo_z(v, dst).wait_send())
        pl.when(inner)(lambda v=v: sends_done(lo_copy, v))
    for h in HEADS:
        for s in TWO:
            for copy in (kvp_copy, kvr_copy, kvf_copy):
                copy(h, s).wait_send()

    @pl.when(outer)
    def _():
        for k in ROWS:
            for p in TWO:
                o_copy(k, p).wait_send()

    @pl.when(inner)
    def _():
        for k in ROWS:
            for v in (1, 2, 3):
                y_copy(k, v, side).wait_send()
            y_local(k).wait()

    for seg in TWO:
        @pl.when(tp != 1 + seg)
        def _(seg=seg):
            for k in ROWS:
                with scope(f'recv{k}_{seg}'):
                    y_copy(k, 1, seg).wait_recv()


PROGRAM = (
    '-.wk,zv0,zv1,po,rz', 'K', 'K.xv0,f0', 'K.xv1,zq0,b0,g0', 'T0.o0,o1,zq1,wv', 'V.xq0,xq1,z0', 'V', 'V.sp,free,wq', 'Q.pp', 'T4.p0,p1,x0,s1,b1,sr',
    'Q', 'Q', 'Q', 'T2', '-.w0', 'R', 'T5.p2,p3,z1,b2', 'R.f1', 'T3.g1', 'T1.o2,o3,x1', 'R.z2', '-.w1', 'L', 'L', 'L', 'R.o4,o5', 'L.f2,f3',
    '-.g2,g3', 'T6.p4,p5,o6,o7', 'R', 'L', 'T7.p6,p7', 'R.x2', 'L', '-.w2', 'N', 'N', 'N', 'R', 'L', 'N', 'R', 'L', 'N', 'N', 'N', 'N',
)
KINDS = '-KVQABRLN'


def tables():
    table, seen = [], {}
    names = tuple(dict.fromkeys(s.partition('.')[2] for s in PROGRAM if '.' in s))
    for s in PROGRAM:
        name, _, after = s.partition('.')
        kind, n = name[0], seen.get(name[0], 0)
        seen[kind] = n + 1
        if kind == 'T':
            n = int(name[1:])
            kind = 'AB'[n in (2, 3, 4, 5)]
        table.append(KINDS.index(kind) + 16 * n + 256 * (names.index(after) + 1 if after else 0))
    return table, names


TABLE, EVENTS = tables()


def main(beta, x, wk, wv, wq, w_out):
    anyspec = pl.BlockSpec(memory_space=pl.ANY)
    vmem = [((4, B, M), BF), ((B, B), BF), ((2, 8, B, M), BF), ((3, M, H), BF), ((4, 8, B, B), BF), ((4, 12, 2, B, B), BF), ((4, 4, 2, B, B), BF), ((4, 4, 2, B, B), BF),
            ((3072, H), F32), ((M, H), F32)]
    dma = [(4,), (6, 8), (5, 8, 3), (6, 8), (6, 8), (2, 4), (4, 3), (4, 8), (4, 8)] + [(4, 2)] * 6 + [(8, 2), (8, 2), (8, 4), (2, 8)]
    return pl.pallas_call(
        main_kernel,
        in_specs=[pl.BlockSpec(memory_space=pltpu.SMEM)] + [anyspec] * 5,
        out_specs=[anyspec] * 3,
        out_shape=[jax.ShapeDtypeStruct(s, BF) for s in ((2, 8, B, H), (8, 6, B, B), (4, 8, 3, 64, H))],
        scratch_shapes=[pltpu.VMEM(*v) for v in vmem] + [pltpu.SemaphoreType.DMA(d) for d in dma] + [pltpu.SemaphoreType.REGULAR((2,))],
        compiler_params=params(collective_id=0, has_side_effects=True),
        cost_estimate=pl.CostEstimate(flops=10**11, bytes_accessed=10**8, transcendentals=0),
        name='main',
    )(beta, x, wk, wv, wq, w_out)[0]


def solution(mesh):
    tp_size = mesh.shape['tp']

    def device_fn(hidden, w_query, w_key, w_value, w_out, branch_bias):
        tp = lax.axis_index('tp')
        heads = branch_bias.shape[1] // tp_size
        b = jnp.concatenate([lax.dynamic_slice_in_dim(branch_bias, t * heads, heads, axis=1) for t in (tp, tp ^ 2)], axis=1)
        beta = []
        for branches in ('0', '01', '1', '012', '12', '2', '0123', '123', '23', '3'):
            rows = [b[i:i + 1] for i in map(int, branches)]
            m = functools.reduce(jnp.maximum, rows)
            beta.append((m + jnp.log(sum(jnp.exp(r - m) for r in rows))) * math.log2(math.e))
        return unpermute(main(jnp.concatenate(beta), hidden, w_key, w_value, w_query, w_out))

    return jax.shard_map(device_fn, mesh=mesh, in_specs=(P(('dp', 'sp'), None), P(None, 'tp'), P(None, 'tp'), P(None, 'tp'), P('tp', None), P(None, None)), out_specs=P(('dp', 'sp'), 'tp'), check_vma=False)
```

```python
import functools
import math

import jax
import jax.numpy as jnp
from jax import lax
from jax.experimental import pallas as pl
from jax.experimental.pallas import tpu as pltpu
from jax.sharding import PartitionSpec as P

MESH = pl.DeviceIdType.MESH
BF = jnp.bfloat16
F32 = jnp.float32
B, H, M = 256, 512, 2048
KAPPA = math.log2(math.e) / 16
VMEM = 66_900_000
SLOT = (0, 4, 2, 6, 1, 5, 3, 7)
KEY, VAL, QUE = range(3)
HEADS = range(4)
TWO = range(2)
ROWS = range(8)


def nn(a, b):
    return lax.dot_general(a, b, (((1,), (0,)), ((), ())), preferred_element_type=F32)


def nt(a, b):
    return lax.dot_general(a, b, (((1,), (1,)), ((), ())), preferred_element_type=F32)


def params(**kw):
    return pltpu.CompilerParams(vmem_limit_bytes=VMEM, **kw)


def ds(start, size, align=128):
    return pl.ds(pl.multiple_of(start, align), size)


def part(i, size):
    return slice(i * size, i * size + size)


def phase_matrix(transposed):
    r = lax.broadcasted_iota(jnp.int32, (B, B), int(transposed))
    p = lax.broadcasted_iota(jnp.int32, (B, B), int(not transposed))
    k = r // 32
    return (p == (r % 32) * 8 + k // 2 + 4 * (k % 2)).astype(F32).astype(BF)


def unpermute_kernel(y_ref, o_ref, pm_ref):
    @pl.when(pl.program_id(0) + pl.program_id(1) == 0)
    def _():
        pm_ref[...] = phase_matrix(True)

    for j in range(y_ref.shape[1] // 32):
        y = y_ref[:, part(j, 32), :].reshape(B, y_ref.shape[-1])
        o_ref[part(j, B), :] = nn(pm_ref[...], y).astype(BF)


def unpermute(y):
    s, k, i, c = y.shape
    return pl.pallas_call(
        unpermute_kernel,
        grid=(s, 2),
        in_specs=[pl.BlockSpec((None, k, i // 2, c), lambda s, j: (s, 0, j, 0))],
        out_specs=pl.BlockSpec((k * i // 2, c), lambda s, j: (s * 2 + j, 0)),
        out_shape=jax.ShapeDtypeStruct((s * k * i, c), BF),
        scratch_shapes=[pltpu.VMEM((B, B), BF)],
        compiler_params=params(),
        name='unpermute',
    )(y)


def tile_steps(q, wide, narrow, s_ref, n_ref, done):
    st = {}
    logits, sums = [], []

    def add(name, x):
        st[name] = st[name] + x if name in st else x

    for groups, ref in ((wide, s_ref), (narrow, n_ref)):
        off = 0
        for keys, parts in groups:
            def qk(keys=keys, parts=parts, off=off, ref=ref):
                s = nt(keys(), q() if ref is s_ref else q()[:B])
                o = 0
                for _, n, b in parts:
                    piece = s[o:o + n]
                    ref[pl.ds(off + o, n), :] = piece
                    t = jnp.max(piece, axis=0, keepdims=True) * KAPPA
                    if b is not None:
                        t = t + b
                    if ref is n_ref:
                        t = jnp.concatenate([t, st['top'][:, B:]], axis=1)
                    st['top'] = jnp.maximum(st['top'], t) if 'top' in st else t
                    o += n
            logits.append(qk)
            for v, n, b in parts:
                def sv(v=v, n=n, b=b, off=off, ref=ref):
                    top = st['top'] if ref is s_ref else st['top'][:, :B]
                    e = jnp.exp2(ref[pl.ds(off, n), :] * KAPPA - (top if b is None else top - b))
                    name = 'w' if ref is s_ref else 'n'
                    add('l' + name, jnp.sum(e, axis=0, keepdims=True))
                    add('o' + name, nn(v(), e.astype(BF)))
                sums.append(sv)
                off += n

    def finish():
        o, l = st['ow'], st['lw']
        if narrow:
            o = jnp.concatenate([o[:, :B] + st['on'], o[:, B:]], axis=1)
            l = jnp.concatenate([l[:, :B] + st['ln'], l[:, B:]], axis=1)
        done(o / l)

    return logits, sums + [finish]


def interleave(a, b):
    i = j = 0
    while i < len(a) or j < len(b):
        if j >= len(b) or (i < len(a) and i * len(b) <= j * len(a)):
            a[i]()
            i += 1
        else:
            b[j]()
            j += 1


def run_tiles(tiles):
    before = []
    for logits, sums in tiles:
        interleave(logits, before)
        before = sums
    interleave([], before)


def on(cond, *calls):
    @pl.when(cond)
    def _():
        for c in calls:
            c()


def scope(name):
    return jax.named_scope(name)


def main_kernel(beta_ref, x_ref, wk_ref, wv_ref, wq_ref, wout_ref, out_ref, lq_ref, lo_ref, lb_ref,
                xb, pm, xp, ws, q_s, kv_s, kvp_s, kvr_s, s_scr, t_scr,
                x_sem, w_sem, wo_sem, lq_send, lq_recv, lo_zsend, lo_zrecv, lo_send, lo_recv, lb_send, lb_recv,
                kvp_send, kvp_recv, kvr_send, kvr_recv, kvf_send, kvf_recv, o_send, o_recv, y_send, y_recv, ready):
    dp, tp, sp = lax.axis_index('dp'), lax.axis_index('tp'), lax.axis_index('sp')
    idx = dp * 4 + sp
    side = tp // 2
    inner = (tp == 1) | (tp == 2)
    outer = jnp.logical_not(inner)
    W = (wk_ref, wv_ref, wq_ref)
    peer_x, peer_y, peer_c = {'dp': dp ^ 1}, {'sp': sp ^ 2}, {'sp': sp ^ 1}

    def remote(src, dst, ss, rs, dev):
        return pltpu.make_async_remote_copy(src_ref=src, dst_ref=dst, send_sem=ss, recv_sem=rs, device_id=dev, device_id_type=MESH)

    def lq_copy(t, src, dst, dev):
        return remote(lq_ref.at[src, t], lq_ref.at[dst, t], lq_send.at[t, dst], lq_recv.at[t, dst], dev)

    def lq_z(t):
        return remote(W[t // 2].at[ds(idx * B, B), pl.ds(t % 2 * B, B)], lq_ref.at[0, t], lq_send.at[t, 0], lq_recv.at[t, 0], {'tp': tp ^ 2})

    def lq_start(t):
        for i in TWO:
            lq_z(2 * t + i).start()

    def lo_copy(v, src, dst, dev):
        return remote(lo_ref.at[v, src], lo_ref.at[v, dst], lo_send.at[v, dst], lo_recv.at[v, dst], dev)

    def lo_z(v):
        dst = 2 - side
        b = (tp ^ dst) - 2
        return remote(wout_ref.at[ds(idx * 64, 64, 64), ds((dst ^ v) * H, H)], lo_ref.at[v, 0, b], lo_zsend.at[v], lo_zrecv.at[v, b], {'tp': dst})

    def lb_z(v):
        return remote(wout_ref.at[ds(sp % 2 * B, B), ds((tp ^ 1 ^ v) * H, H)], lb_ref.at[v, sp % 2], lb_send.at[v, 0], lb_recv.at[v, 0], {'tp': tp ^ 1})

    def lb_core(v):
        return remote(lb_ref.at[v, sp % 2], lb_ref.at[v, sp % 2], lb_send.at[v, 1], lb_recv.at[v, 1], peer_c)

    def lo_start(*vs):
        for v in vs:
            lo_z(v).start()
            pl.when(outer)(lambda v=v: lb_z(v).start())

    def lo_zwait(v):
        for b in TWO:
            remote(lo_ref.at[v, 0, b], lo_ref.at[v, 0, b], lo_zsend.at[v], lo_zrecv.at[v, b], {'tp': tp}).wait_recv()

    def hop(copy, p, i):
        near, far = (peer_y, peer_x) if copy is lq_copy else (peer_x, peer_y)
        n, f = (2, 1) if near is peer_y else (1, 2)
        return copy(p, *((0, n, near), (0, f, far), (0, 4, peer_c), (n, 3, far), (n, 4 + n, peer_c), (f, 4 + f, peer_c), (3, 7, peer_c))[i])

    def ev_z(copy, *ps):
        for p in ps:
            with scope(f'z_{copy.__name__}{p}'):
                lq_z(p).wait_recv() if copy is lq_copy else lo_zwait(p)
            for i in range(3):
                hop(copy, p, i).start()

    def ev_xy(copy, *ps):
        for p in ps:
            with scope(f'n_{copy.__name__}{p}'):
                hop(copy, p, 0).wait_recv()
            hop(copy, p, 3).start()
            hop(copy, p, 4).start()
        for p in ps:
            with scope(f'f_{copy.__name__}{p}'):
                hop(copy, p, 1).wait_recv()
            hop(copy, p, 5).start()

    def ev_y(copy, *ps):
        for p in ps:
            with scope(f'y_{copy.__name__}{p}'):
                hop(copy, p, 3).wait_recv()
            hop(copy, p, 6).start()
            if copy is lq_copy and p >= 2:
                start(w_load(p, SLOT[:4]))

    def ev_done(copy, *ps):
        for p in ps:
            with scope(f'c_{copy.__name__}{p}'):
                for i in (2, 4, 5, 6):
                    hop(copy, p, i).wait_recv()

    def sends_done(copy, p):
        for i in range(7):
            hop(copy, p, i).wait_send()

    def w_load(p, slots):
        return [pltpu.make_async_copy(lq_ref.at[SLOT.index(m), p], ws.at[p // 2 % 2, ds((idx ^ m) * B, B), pl.ds(p % 2 * B, B)], w_sem.at[p, SLOT.index(m)]) for m in slots]

    def own_load(t):
        return pltpu.make_async_copy(W[t], ws.at[t], w_sem.at[t, 0])

    def start(copies):
        for c in copies:
            c.start()

    def wait(copies):
        for c in copies:
            c.wait()

    def ev_weights(t):
        pieces = [2 * t + i for i in TWO]
        ev_done(lq_copy, *pieces)
        for p in pieces:
            start(w_load(p, SLOT[4:] if t else SLOT))
        with scope(f'load{t}'):
            for p in pieces:
                wait(w_load(p, SLOT))

    def ev_wo(*vs):
        ev_done(lo_copy, *vs)
        for v in vs:
            lb_core(v).wait_recv()
        start(wo_load(*vs))
        with scope(f'wo{vs[0]}'):
            wait(wo_load(*vs))

    def ev_lb(*vs):
        for v in vs:
            with scope(f'lb{v}'):
                lb_z(v).wait_recv()
            lb_core(v).start()

    wo = xp.at[1 - side]

    def wo_own():
        return [pltpu.make_async_copy(wout_ref.at[pl.ds(r * B, B), pl.ds(c * H, H)], xp.at[1 - side, r, :, ds((c ^ tp ^ 2) * H, H)], wo_sem.at[4, r * 4 + c, 0])
                for r in TWO for c in range(4)]

    def wo_load(*vs):
        out = []
        for v in vs:
            cols = pl.ds((v ^ 2) * H, H)
            for s, m in enumerate(SLOT):
                row = (idx ^ m) * 64
                for b in TWO:
                    out.append(pltpu.make_async_copy(lo_ref.at[v, s, b], xp.at[1 - side, 4 + 2 * b + row // B, ds(row % B, 64, 64), cols], wo_sem.at[v, s, b]))
            for r in TWO:
                out.append(pltpu.make_async_copy(lb_ref.at[v, r], xp.at[1 - side, 2 + r, :, cols], wo_sem.at[v, r, 2]))
        return out

    def kvp_copy(h, s):
        return remote(kv_s.at[h, pl.ds(8 * s, 2)], kvp_s.at[h, pl.ds(2 * s, 2)], kvp_send.at[h, s], kvp_recv.at[h, s], peer_c)

    def kvr_copy(h, s):
        return remote(kv_s.at[h, 8 * s], kvr_s.at[h, s], kvr_send.at[h, s], kvr_recv.at[h, s], peer_y)

    def kvf_copy(h, s):
        return remote(kvr_s.at[h, s], kvr_s.at[h, 2 + s], kvf_send.at[h, s], kvf_recv.at[h, s], peer_c)

    def kv_start(copy, heads):
        for h in heads:
            for s in TWO:
                copy(h, s).start()

    def kv_wait(copy, heads):
        with scope(f'w_{copy.__name__}{heads[0]}'):
            for h in heads:
                for s in TWO:
                    copy(h, s).wait_recv()

    def kv_forward(heads):
        kv_wait(kvr_copy, heads)
        kv_start(kvf_copy, heads)

    def reverse(i):
        return (i % 2) * 2 + i // 2

    def order(n):
        return 2 * reverse(n % 4) + ((n // 4) ^ side)

    def o_at(k, p, theirs, col, size):
        return ws.at[1 + theirs, ds(k * B, B), ds(col, size)] if p else xb.at[k // 2, :, ds((k % 2) * 1024 + theirs * H + col, size)]

    def o_copy(k, p):
        return remote(o_at(k, p, 0, 0, H), o_at(k, p, 1, 0, H), o_send.at[k, p], o_recv.at[k, p], {'tp': tp ^ 1})

    def o_times(k, v, n):
        cols = pl.ds((v ^ 2) * H, n * H)
        y = nn(xb[k // 2, :, ds((k % 2) * 1024, 1024)], wo[0:4, :, cols].reshape(1024, n * H))
        for i in TWO:
            y = y + nn(ws[1 + i, ds(k * B, B), :], wo[part(2 + i, 2), :, cols].reshape(H, n * H))
        y = y.astype(BF)
        for i in range(n):
            y_src(k, v + i)[...] = y[:, part(i, H)]
            y_copy(k, v + i, side).start() if v else y_local(k).start()

    def y_src(k, v):
        return xp.at[side, k, :, pl.ds(v * H, H)]

    def y_copy(k, v, seg):
        return remote(y_src(k, v), out_ref.at[seg, k], y_send.at[k, v], y_recv.at[seg, k], {'tp': tp ^ v})

    def y_local(k):
        return pltpu.make_async_copy(y_src(k, 0), out_ref.at[side, k], y_send.at[k, 0])

    def x_copy(j):
        return pltpu.make_async_copy(x_ref.at[ds(j * B, B), :], xb.at[lax.rem(j, 4)], x_sem.at[lax.rem(j, 4)])

    for j in range(4):
        x_copy(j).start()
    for t in range(3):
        own_load(t).start()
    barrier = pltpu.get_barrier_semaphore()
    peers = [{'tp': tp ^ 1}, {'tp': tp ^ 2}, {'tp': tp ^ 3}, peer_x, peer_y, peer_c]
    for dev in peers:
        pl.semaphore_signal(barrier, inc=1, device_id=dev, device_id_type=MESH)
    with scope('barrier'):
        pl.semaphore_wait(barrier, len(peers))
    lq_start(KEY)

    pm[...] = phase_matrix(False)

    def permute_body(j, carry):
        x_copy(j).wait()
        y = nn(pm[...], xb[lax.rem(j, 4)]).astype(BF).reshape(8, 32, M)
        xp[j // 8, :, ds(lax.rem(j, 8) * 32, 32, 32), :] = y
        pl.when(j < 12)(lambda: x_copy(j + 4).start())
        return carry

    with scope('permute'):
        lax.fori_loop(0, 16, permute_body, None)

    def signal_ready(i):
        pl.when(inner)(lambda: pl.semaphore_signal(ready.at[i], inc=1, device_id={'tp': tp ^ 1}, device_id_type=MESH))

    def wait_ready(i):
        with scope(f'ready{i}'):
            pl.when(outer)(lambda: pl.semaphore_wait(ready.at[i], 1))

    signal_ready(0)

    def group(g):
        low = g < 4
        return jnp.where(low, g & 1, 0), jnp.where(low, g // 2, g - 2)

    def head_number(h):
        return 2 * (tp ^ (h // 2 * 2)) + h % 2

    def project(heads, sigma, pair, kinds):
        for h in heads:
            t = head_number(h) + reverse(pair)
            x, swap = xp[side ^ sigma, pl.ds(2 * (t & 3), 2)].reshape(H, M), (t & 7) >> 2
            for t in kinds:
                y = nn(x, ws[t, :, part(h % 2, B)])
                for j in TWO:
                    piece = y[part(j, B)]
                    kv_s[h, 8 * sigma + 2 * pair + (j ^ swap), t] = (piece.T if t == VAL else piece).astype(BF)

    def phases_of(j):
        return [j % 2 + 2 * i for i in TWO], (j // 2) ^ side

    def rank_of(phase, h):
        rel = (phase - head_number(h)) & 7
        return (rel & 1) * 4 + ((rel >> 1) & 1) * 2 + (rel >> 2)

    def queries(heads, w, j):
        phases, half = phases_of(j)
        x = jnp.concatenate([xp[side, 2 * f + half] for f in phases])
        for h in heads:
            y = nn(x, ws[w, :, part(h % 2, B)]).astype(BF)
            for i, f in enumerate(phases):
                q_s[h, rank_of(f + 4 * half, h)] = y[part(i, B)]

    with scope('own_w'):
        for t in range(3):
            own_load(t).wait()
    own, partner = HEADS[:2], HEADS[2:]

    lane = lax.broadcasted_iota(jnp.int32, (1, H), 1)

    def mix(b, c):
        return jnp.where(lane < B, b, c)

    def keys_of(ref, h, i, weights):
        parts = []
        n = 0
        for count, b in weights:
            def values(i=i + n, count=count):
                v = [ref[h, i + j, VAL] for j in range(count)]
                return v[0] if count == 1 else jnp.concatenate(v, axis=1)
            parts.append((values, count * B, b))
            n += count
        return (lambda: ref[h, i:i + n, KEY].reshape(n * B, B)), parts

    def chunk_tiles(p, j, kind):
        both_phases, half = phases_of(j)

        def put(h, phase, ot):
            k = 2 * (phase & 3) + half
            y = ot.T.astype(BF)
            for i in TWO:
                pl.when(p == i)(lambda i=i: o_at(k, i, 0, (h % 2) * B, B).__setitem__(..., y))

        def tile(h, phases, ranks, wide, narrow, s_ref, n_ref):
            def done(ot):
                for i, phase in enumerate(phases):
                    put(h, phase, ot[:, part(i, B)])
            return tile_steps(lambda: jnp.concatenate([q_s[h, r] for r in ranks]), wide, narrow, s_ref, n_ref, done)

        h = 2 * p + (j % 2) ^ 1
        rest = tile(h, both_phases, [rank_of(f + 4 * half, h) for f in both_phases], [keys_of(kv_s, h, i, [(2, None)]) for i in range(0, 8, 2)], [], t_scr, None)
        h = 2 * p + (j % 2)
        a = head_number(h)
        b0, b01, b1, b012, b12, b2, b0123, b123, b23, b3 = [beta_ref[i, h] for i in range(10)]
        phases = [a & 3, (a & 3) ^ 2]
        both = [keys_of(kv_s, h, i, [(2, b)]) for i, b in ((2, b01), (4, b0), (6, b0), (10, b1))]
        if kind == 0:
            both += [keys_of(kv_s, h, 0, [(1, mix(b0123, b01)), (1, mix(b012, b01))]), keys_of(kv_s, h, 8, [(1, mix(b123, b1)), (1, mix(b12, b1))])]
            first = [keys_of(kvp_s, h, i, [(1, b23), (1, b2)]) for i in (0, 2)] + [keys_of(kvr_s, h, i, [(2, b3)]) for i in (0, 2)]
        else:
            both += [keys_of(kv_s, h, 0, [(2, mix(b012, b01))]), keys_of(kv_s, h, 8, [(2, mix(b12, b1))])]
            first = [keys_of(kvp_s, h, i, [(2, b2)]) for i in (0, 2)]
        with scope(f'tile{kind}'):
            run_tiles([rest, tile(h, phases, [kind, rank_of(phases[1] + 4 * half, h)], both, first, s_scr, t_scr.at[:, pl.ds(0, B)])])

    def send_o(ks, p):
        @pl.when(outer)
        def _():
            for k in ks:
                o_copy(order(k), p).start()

    def step_body(t, carry):
        packed = functools.reduce(lambda x, i: jnp.where(t == i, TABLE[i], x), range(len(TABLE)), 0)
        code, n, event = packed % 16, packed // 16 % 16, packed // 256 - 1

        def kind(c):
            return code == KINDS.index(c)

        @pl.when(kind('O'))
        def _():
            with scope('own_kv'):
                project(own, *group(n), (KEY, VAL))

        for c, t_ in (('K', KEY), ('V', VAL)):
            @pl.when(kind(c))
            def _(t_=t_):
                with scope(f'par_{t_}'):
                    for i in TWO:
                        project(partner, *group(2 * n + i), (t_,))

        for c, heads, w in (('P', own, QUE), ('Q', partner, KEY)):
            @pl.when(kind(c))
            def _(c=c, heads=heads, w=w):
                with scope(f'que_{c}'):
                    queries(heads, w, n)

        for i in TWO:
            pl.when(kind('AB'[i]))(lambda i=i: chunk_tiles(n // 4, n % 4, i))

        for c, v, m in (('R', 2, 2), ('L', 1, 1), ('N', 0, 1)):
            @pl.when(kind(c) & inner)
            def _(c=c, v=v, m=m):
                k = order(n)
                if c == 'R':
                    with scope('wait_o'):
                        for p in TWO:
                            o_copy(k, p).wait_recv()
                with scope(f'out{v}'):
                    o_times(k, v, m)

        call = functools.partial

        events = {
            'free': [call(signal_ready, 1), call(on, inner, lambda: start(wo_own())), call(wait_ready, 1)],
            'rz': [call(wait_ready, 0)],
            'so': [call(kv_start, kvp_copy, own)],
            'po': [call(kv_wait, kvp_copy, own)],
            'sp': [call(kv_start, kvp_copy, partner)],
            'pp': [call(kv_wait, kvp_copy, partner)],
        }
        for t_, c in enumerate('kvq'):
            events['b' + c] = [call(lq_start, t_)]
            events['w' + c] = [call(ev_weights, t_)]
            for i in TWO:
                for e, f in zip('zxy', (ev_z, ev_xy, ev_y)):
                    events[f'{e}{c}{i}'] = [call(f, lq_copy, 2 * t_ + i)]
        for i, vs in enumerate(((2, 3), (1,), (0,))):
            events[f'b{i}'] = [call(lo_start, *vs)]
            for e, f in zip('zxycw', (call(ev_z, lo_copy), call(ev_xy, lo_copy), call(ev_y, lo_copy), ev_lb, ev_wo)):
                events[f'{e}{i}'] = [call(on, inner, call(f, *vs))]
        events['w0'] += [call(on, inner, lambda: wait(wo_own()))]
        for h in HEADS:
            for z in TWO:
                events[f's{h}{z}'] = [kvr_copy(h, z).start]
            events[f'f{h}'] = [call(kv_forward, [h])]
            events[f'g{h}'] = [call(kv_wait, kvf_copy, [h])]
        for k in ROWS:
            for p in TWO:
                events['op'[p] + str(k)] = [call(send_o, (k,), p)]
        @pl.when(event >= 0)
        def _():
            for i, names in enumerate(EVENTS):
                calls = []
                for name in names.split(','):
                    where, _, name = name.rpartition(':')
                    c = events[name]
                    calls += [call(on, inner if where == 'i' else outer, *c)] if where else c
                on(event == i, *calls)
        return carry

    lax.fori_loop(0, len(TABLE), step_body, None)

    def call_sends(copy, p):
        return functools.partial(sends_done, copy, p)

    for t in range(6):
        lq_z(t).wait_send()
        sends_done(lq_copy, t)
    for v in range(4):
        lo_z(v).wait_send()
        on(outer, lb_z(v).wait_send)
        on(inner, lb_core(v).wait_send, call_sends(lo_copy, v))
    for h in HEADS:
        for s in TWO:
            for copy in (kvp_copy, kvr_copy, kvf_copy):
                copy(h, s).wait_send()

    @pl.when(outer)
    def _():
        for k in ROWS:
            for p in TWO:
                o_copy(k, p).wait_send()

    @pl.when(inner)
    def _():
        for k in ROWS:
            for v in (1, 2, 3):
                y_copy(k, v, side).wait_send()
            y_local(k).wait()

    for seg in TWO:
        @pl.when(tp != 1 + seg)
        def _(seg=seg):
            for k in ROWS:
                with scope(f'recv{k}_{seg}'):
                    y_copy(k, 1, seg).wait_recv()


PROGRAM = (
    'O.i:zk0,i:zk1', 'O.o:zk0,bv,so', 'O.o:zk1,s00,i:xk0', 'O.o:xk0,i:xk1', 'O.o:xk1,i:yk0,i:zv0,i:zv1', 'O.o:yk0,i:yk1', 'P.bq', 'P.o:yk1,o:zv0',
    'P.wk,o:zv1,s01', 'K.i:xv0,i:xv1', 'K.o:xv0,i:zq0,i:zq1', 'K.o:xv1,o:zq0,i:yv0,i:yv1,b0,rz,po', 'P.o:yv0,o:zq1,b1', 'T2.o:yv1,wv,xq0',
    'V.xq1,z0,f0', 'V.o:yq0,z1,c0', 'V.i:yq0,yq1,sp,free,g0', 'T0.o0,o1,x0,wq', 'Q.pp,c1', 'T4.p0,p1,x1,s10,s11', 'Q', 'Q', 'Q.y0', '-.w0,y1', 'R',
    'T5.p2,p3,b2,s20,s21', 'R.w1', 'L', 'L.f1', 'T3.s30,s31,g1', 'T1.o2,o3,o4,o5', 'R', 'L.z2,c2', '-.f2', 'R', 'L.x2', '-.g2', 'T6.p4,p5,o6,o7,f3',
    'R', 'L.y2', '-.g3', 'T7.p6,p7', 'R', 'L', '-.w2', 'N', 'N', 'N', 'R', 'L', 'N', 'R', 'L', 'N', 'N', 'N', 'N',
)
KINDS = '-OPKVQABRLN'


def tables():
    table, seen = [], {}
    names = tuple(dict.fromkeys(s.partition('.')[2] for s in PROGRAM if '.' in s))
    for s in PROGRAM:
        name, _, after = s.partition('.')
        kind, n = name[0], seen.get(name[0], 0)
        seen[kind] = n + 1
        if kind == 'T':
            n = int(name[1:])
            kind = 'AB'[n in (2, 3, 4, 5)]
        table.append(KINDS.index(kind) + 16 * n + 256 * (names.index(after) + 1 if after else 0))
    return table, names


TABLE, EVENTS = tables()


def main(beta, x, wk, wv, wq, w_out):
    anyspec = pl.BlockSpec(memory_space=pl.ANY)
    vmem = [((4, B, M), BF), ((B, B), BF), ((2, 8, B, M), BF), ((3, M, H), BF), ((4, 8, B, B), BF), ((4, 12, 2, B, B), BF), ((4, 4, 2, B, B), BF), ((4, 4, 2, B, B), BF),
            ((3072, H), F32), ((M, H), F32)]
    dma = [(4,), (6, 8), (5, 8, 3), (6, 8), (6, 8), (4,), (4, 2), (4, 8), (4, 8), (4, 2), (4, 2)] + [(4, 2)] * 6 + [(8, 2), (8, 2), (8, 4), (2, 8)]
    return pl.pallas_call(
        main_kernel,
        in_specs=[pl.BlockSpec(memory_space=pltpu.SMEM)] + [anyspec] * 5,
        out_specs=[anyspec] * 4,
        out_shape=[jax.ShapeDtypeStruct(s, BF) for s in ((2, 8, B, H), (8, 6, B, B), (4, 8, 2, 64, H), (4, 2, B, H))],
        scratch_shapes=[pltpu.VMEM(*v) for v in vmem] + [pltpu.SemaphoreType.DMA(d) for d in dma] + [pltpu.SemaphoreType.REGULAR((2,))],
        compiler_params=params(collective_id=0, has_side_effects=True),
        cost_estimate=pl.CostEstimate(flops=10**11, bytes_accessed=10**8, transcendentals=0),
        name='main',
    )(beta, x, wk, wv, wq, w_out)[0]


def solution(mesh):
    tp_size = mesh.shape['tp']

    def device_fn(hidden, w_query, w_key, w_value, w_out, branch_bias):
        tp = lax.axis_index('tp')
        heads = branch_bias.shape[1] // tp_size
        b = jnp.concatenate([lax.dynamic_slice_in_dim(branch_bias, t * heads, heads, axis=1) for t in (tp, tp ^ 2)], axis=1)
        beta = []
        for branches in ('0', '01', '1', '012', '12', '2', '0123', '123', '23', '3'):
            rows = [b[i:i + 1] for i in map(int, branches)]
            m = functools.reduce(jnp.maximum, rows)
            beta.append((m + jnp.log(sum(jnp.exp(r - m) for r in rows))) * math.log2(math.e))
        return unpermute(main(jnp.concatenate(beta), hidden, w_key, w_value, w_query, w_out))

    return jax.shard_map(device_fn, mesh=mesh, in_specs=(P(('dp', 'sp'), None), P(None, 'tp'), P(None, 'tp'), P(None, 'tp'), P('tp', None), P(None, None)), out_specs=P(('dp', 'sp'), 'tp'), check_vma=False)
```

```python
import functools
import math

import jax
import jax.numpy as jnp
from jax import lax
from jax.experimental import pallas as pl
from jax.experimental.pallas import tpu as pltpu
from jax.sharding import PartitionSpec as P

MESH = pl.DeviceIdType.MESH
BF = jnp.bfloat16
F32 = jnp.float32
B, H, M = 256, 512, 2048
KAPPA = math.log2(math.e) / 16
VMEM = 66_900_000
SLOT = (0, 4, 2, 6, 1, 5, 3, 7)
KEY, VAL, QUE = range(3)
HEADS = range(4)
TWO = range(2)
ROWS = range(8)


def nn(a, b):
    return lax.dot_general(a, b, (((1,), (0,)), ((), ())), preferred_element_type=F32)


def nt(a, b):
    return lax.dot_general(a, b, (((1,), (1,)), ((), ())), preferred_element_type=F32)


def params(**kw):
    return pltpu.CompilerParams(vmem_limit_bytes=VMEM, **kw)


def ds(start, size, align=128):
    return pl.ds(pl.multiple_of(start, align), size)


def part(i, size):
    return slice(i * size, i * size + size)


def phase_matrix(transposed):
    r = lax.broadcasted_iota(jnp.int32, (B, B), int(transposed))
    p = lax.broadcasted_iota(jnp.int32, (B, B), int(not transposed))
    k = r // 32
    return (p == (r % 32) * 8 + k // 2 + 4 * (k % 2)).astype(F32).astype(BF)


def unpermute_kernel(y_ref, o_ref, pm_ref):
    @pl.when(pl.program_id(0) + pl.program_id(1) == 0)
    def _():
        pm_ref[...] = phase_matrix(True)

    for j in range(y_ref.shape[1] // 32):
        y = y_ref[:, part(j, 32), :].reshape(B, y_ref.shape[-1])
        o_ref[part(j, B), :] = nn(pm_ref[...], y).astype(BF)


def unpermute(y):
    s, k, i, c = y.shape
    return pl.pallas_call(
        unpermute_kernel,
        grid=(s, 2),
        in_specs=[pl.BlockSpec((None, k, i // 2, c), lambda s, j: (s, 0, j, 0))],
        out_specs=pl.BlockSpec((k * i // 2, c), lambda s, j: (s * 2 + j, 0)),
        out_shape=jax.ShapeDtypeStruct((s * k * i, c), BF),
        scratch_shapes=[pltpu.VMEM((B, B), BF)],
        compiler_params=params(),
        name='unpermute',
    )(y)


def tile_steps(q, wide, narrow, s_ref, n_ref, done):
    st = {}
    logits, sums = [], []

    def add(name, x):
        st[name] = st[name] + x if name in st else x

    for groups, ref in ((wide, s_ref), (narrow, n_ref)):
        off = 0
        for keys, parts in groups:
            def qk(keys=keys, parts=parts, off=off, ref=ref):
                s = nt(keys(), q() if ref is s_ref else q()[:B])
                o = 0
                for _, n, b in parts:
                    piece = s[o:o + n]
                    ref[pl.ds(off + o, n), :] = piece
                    t = jnp.max(piece, axis=0, keepdims=True) * KAPPA
                    if b is not None:
                        t = t + b
                    if ref is n_ref:
                        t = jnp.concatenate([t, st['top'][:, B:]], axis=1)
                    st['top'] = jnp.maximum(st['top'], t) if 'top' in st else t
                    o += n
            logits.append(qk)
            for v, n, b in parts:
                def sv(v=v, n=n, b=b, off=off, ref=ref):
                    top = st['top'] if ref is s_ref else st['top'][:, :B]
                    e = jnp.exp2(ref[pl.ds(off, n), :] * KAPPA - (top if b is None else top - b))
                    name = 'w' if ref is s_ref else 'n'
                    add('l' + name, jnp.sum(e, axis=0, keepdims=True))
                    add('o' + name, nn(v(), e.astype(BF)))
                sums.append(sv)
                off += n

    def finish():
        o, l = st['ow'], st['lw']
        if narrow:
            o = jnp.concatenate([o[:, :B] + st['on'], o[:, B:]], axis=1)
            l = jnp.concatenate([l[:, :B] + st['ln'], l[:, B:]], axis=1)
        done(o / l)

    return logits, sums + [finish]


def interleave(a, b):
    i = j = 0
    while i < len(a) or j < len(b):
        if j >= len(b) or (i < len(a) and i * len(b) <= j * len(a)):
            a[i]()
            i += 1
        else:
            b[j]()
            j += 1


def run_tiles(tiles):
    before = []
    for logits, sums in tiles:
        interleave(logits, before)
        before = sums
    interleave([], before)


def choose(x, cases):
    def among(lo, hi):
        mid = (lo + hi) // 2
        if hi - lo == 1:
            cases[lo]()
        else:
            pl.when(x < mid)(lambda: among(lo, mid))
            pl.when(x >= mid)(lambda: among(mid, hi))
    among(0, len(cases))


def on(cond, *calls):
    @pl.when(cond)
    def _():
        for c in calls:
            c()


def scope(name):
    return jax.named_scope(name)


def main_kernel(beta_ref, x_ref, wk_ref, wv_ref, wq_ref, wout_ref, out_ref, lq_ref, lo_ref, lb_ref,
                xb, pm, xp, ws, q_s, kv_s, kvp_s, kvr_s, s_scr, t_scr,
                x_sem, w_sem, wo_sem, lq_send, lq_recv, lo_zsend, lo_zrecv, lo_send, lo_recv, lb_send, lb_recv,
                kvp_send, kvp_recv, kvr_send, kvr_recv, kvf_send, kvf_recv, o_send, o_recv, y_send, y_recv, ready, tab):
    dp, tp, sp = lax.axis_index('dp'), lax.axis_index('tp'), lax.axis_index('sp')
    idx = dp * 4 + sp
    side = tp // 2
    inner = (tp == 1) | (tp == 2)
    outer = jnp.logical_not(inner)
    W = (wk_ref, wv_ref, wq_ref)
    peer_x, peer_y, peer_c = {'dp': dp ^ 1}, {'sp': sp ^ 2}, {'sp': sp ^ 1}

    def remote(src, dst, ss, rs, dev):
        return pltpu.make_async_remote_copy(src_ref=src, dst_ref=dst, send_sem=ss, recv_sem=rs, device_id=dev, device_id_type=MESH)

    def lq_copy(t, src, dst, dev):
        return remote(lq_ref.at[src, t], lq_ref.at[dst, t], lq_send.at[t, dst], lq_recv.at[t, dst], dev)

    def lq_z(t):
        return remote(W[t // 2].at[ds(idx * B, B), pl.ds(t % 2 * B, B)], lq_ref.at[0, t], lq_send.at[t, 0], lq_recv.at[t, 0], {'tp': tp ^ 2})

    def lq_start(t):
        for i in TWO:
            lq_z(2 * t + i).start()

    def lo_copy(v, src, dst, dev):
        return remote(lo_ref.at[v, src], lo_ref.at[v, dst], lo_send.at[v, dst], lo_recv.at[v, dst], dev)

    def lo_z(v):
        dst = 2 - side
        b = (tp ^ dst) - 2
        return remote(wout_ref.at[ds(idx * 64, 64, 64), ds((dst ^ v) * H, H)], lo_ref.at[v, 0, b], lo_zsend.at[v], lo_zrecv.at[v, b], {'tp': dst})

    def lb_z(v):
        return remote(wout_ref.at[ds(sp % 2 * B, B), ds((tp ^ 1 ^ v) * H, H)], lb_ref.at[v, sp % 2], lb_send.at[v, 0], lb_recv.at[v, 0], {'tp': tp ^ 1})

    def lb_core(v):
        return remote(lb_ref.at[v, sp % 2], lb_ref.at[v, sp % 2], lb_send.at[v, 1], lb_recv.at[v, 1], peer_c)

    def lo_start(*vs):
        for v in vs:
            lo_z(v).start()
            pl.when(outer)(lambda v=v: lb_z(v).start())

    def lo_zwait(v):
        for b in TWO:
            remote(lo_ref.at[v, 0, b], lo_ref.at[v, 0, b], lo_zsend.at[v], lo_zrecv.at[v, b], {'tp': tp}).wait_recv()

    def hop(copy, p, i):
        near, far = (peer_y, peer_x) if copy is lq_copy else (peer_x, peer_y)
        n, f = (2, 1) if near is peer_y else (1, 2)
        return copy(p, *((0, n, near), (0, f, far), (0, 4, peer_c), (n, 3, far), (n, 4 + n, peer_c), (f, 4 + f, peer_c), (3, 7, peer_c))[i])

    def ev_z(copy, *ps):
        for p in ps:
            with scope(f'z_{copy.__name__}{p}'):
                lq_z(p).wait_recv() if copy is lq_copy else lo_zwait(p)
            for i in range(3):
                hop(copy, p, i).start()

    def ev_xy(copy, *ps):
        for p in ps:
            with scope(f'n_{copy.__name__}{p}'):
                hop(copy, p, 0).wait_recv()
            hop(copy, p, 3).start()
            hop(copy, p, 4).start()
        for p in ps:
            with scope(f'f_{copy.__name__}{p}'):
                hop(copy, p, 1).wait_recv()
            hop(copy, p, 5).start()

    def ev_y(copy, *ps):
        for p in ps:
            with scope(f'y_{copy.__name__}{p}'):
                hop(copy, p, 3).wait_recv()
            hop(copy, p, 6).start()
            if copy is lq_copy and p >= 2:
                start(w_load(p, SLOT[:4]))

    def ev_done(copy, *ps):
        for p in ps:
            with scope(f'c_{copy.__name__}{p}'):
                for i in (2, 4, 5, 6):
                    hop(copy, p, i).wait_recv()

    def sends_done(copy, p):
        for i in range(7):
            hop(copy, p, i).wait_send()

    def w_load(p, slots):
        return [pltpu.make_async_copy(lq_ref.at[SLOT.index(m), p], ws.at[p // 2 % 2, ds((idx ^ m) * B, B), pl.ds(p % 2 * B, B)], w_sem.at[p, SLOT.index(m)]) for m in slots]

    def own_load(t):
        return pltpu.make_async_copy(W[t], ws.at[t], w_sem.at[t, 0])

    def start(copies):
        for c in copies:
            c.start()

    def wait(copies):
        for c in copies:
            c.wait()

    def ev_weights(t):
        pieces = [2 * t + i for i in TWO]
        ev_done(lq_copy, *pieces)
        for p in pieces:
            start(w_load(p, SLOT[4:] if t else SLOT))
        with scope(f'load{t}'):
            for p in pieces:
                wait(w_load(p, SLOT))

    def ev_wo(*vs):
        ev_done(lo_copy, *vs)
        for v in vs:
            lb_core(v).wait_recv()
        start(wo_load(*vs))
        with scope(f'wo{vs[0]}'):
            wait(wo_load(*vs))

    def ev_lb(*vs):
        for v in vs:
            with scope(f'lb{v}'):
                lb_z(v).wait_recv()
            lb_core(v).start()

    wo = xp.at[1 - side]

    def wo_own():
        return [pltpu.make_async_copy(wout_ref.at[pl.ds(r * B, B), pl.ds(c * H, H)], xp.at[1 - side, r, :, ds((c ^ tp ^ 2) * H, H)], wo_sem.at[4, r * 4 + c, 0])
                for r in TWO for c in range(4)]

    def wo_load(*vs):
        out = []
        for v in vs:
            cols = pl.ds((v ^ 2) * H, H)
            for s, m in enumerate(SLOT):
                row = (idx ^ m) * 64
                for b in TWO:
                    out.append(pltpu.make_async_copy(lo_ref.at[v, s, b], xp.at[1 - side, 4 + 2 * b + row // B, ds(row % B, 64, 64), cols], wo_sem.at[v, s, b]))
            for r in TWO:
                out.append(pltpu.make_async_copy(lb_ref.at[v, r], xp.at[1 - side, 2 + r, :, cols], wo_sem.at[v, r, 2]))
        return out

    def kvp_copy(h, s):
        return remote(kv_s.at[h, pl.ds(8 * s, 2)], kvp_s.at[h, pl.ds(2 * s, 2)], kvp_send.at[h, s], kvp_recv.at[h, s], peer_c)

    def kvr_copy(h, s):
        return remote(kv_s.at[h, 8 * s], kvr_s.at[h, s], kvr_send.at[h, s], kvr_recv.at[h, s], peer_y)

    def kvf_copy(h, s):
        return remote(kvr_s.at[h, s], kvr_s.at[h, 2 + s], kvf_send.at[h, s], kvf_recv.at[h, s], peer_c)

    def kv_start(copy, heads):
        for h in heads:
            for s in TWO:
                copy(h, s).start()

    def kv_wait(copy, heads):
        with scope(f'w_{copy.__name__}{heads[0]}'):
            for h in heads:
                for s in TWO:
                    copy(h, s).wait_recv()

    def kv_forward(heads):
        kv_wait(kvr_copy, heads)
        kv_start(kvf_copy, heads)

    def reverse(i):
        return (i % 2) * 2 + i // 2

    def order(n):
        return 2 * reverse(n % 4) + ((n // 4) ^ side)

    def o_at(k, p, theirs, col, size):
        return ws.at[1 + theirs, ds(k * B, B), ds(col, size)] if p else xb.at[k // 2, :, ds((k % 2) * 1024 + theirs * H + col, size)]

    def o_copy(k, p):
        return remote(o_at(k, p, 0, 0, H), o_at(k, p, 1, 0, H), o_send.at[k, p], o_recv.at[k, p], {'tp': tp ^ 1})

    def o_times(k, v, n):
        cols = pl.ds((v ^ 2) * H, n * H)
        y = nn(xb[k // 2, :, ds((k % 2) * 1024, 1024)], wo[0:4, :, cols].reshape(1024, n * H))
        for i in TWO:
            y = y + nn(ws[1 + i, ds(k * B, B), :], wo[part(2 + i, 2), :, cols].reshape(H, n * H))
        y = y.astype(BF)
        for i in range(n):
            y_src(k, v + i)[...] = y[:, part(i, H)]
            y_copy(k, v + i, side).start() if v else y_local(k).start()

    def y_src(k, v):
        return xp.at[side, k, :, pl.ds(v * H, H)]

    def y_copy(k, v, seg):
        return remote(y_src(k, v), out_ref.at[seg, k], y_send.at[k, v], y_recv.at[seg, k], {'tp': tp ^ v})

    def y_local(k):
        return pltpu.make_async_copy(y_src(k, 0), out_ref.at[side, k], y_send.at[k, 0])

    def x_copy(j):
        return pltpu.make_async_copy(x_ref.at[ds(j * B, B), :], xb.at[lax.rem(j, 4)], x_sem.at[lax.rem(j, 4)])

    for j in range(4):
        x_copy(j).start()
    for t in range(3):
        own_load(t).start()
    barrier = pltpu.get_barrier_semaphore()
    peers = [{'tp': tp ^ 1}, {'tp': tp ^ 2}, {'tp': tp ^ 3}, peer_x, peer_y, peer_c]
    for dev in peers:
        pl.semaphore_signal(barrier, inc=1, device_id=dev, device_id_type=MESH)
    with scope('barrier'):
        pl.semaphore_wait(barrier, len(peers))
    lq_start(KEY)

    pm[...] = phase_matrix(False)

    def permute_body(j, carry):
        x_copy(j).wait()
        y = nn(pm[...], xb[lax.rem(j, 4)]).astype(BF).reshape(8, 32, M)
        xp[j // 8, :, ds(lax.rem(j, 8) * 32, 32, 32), :] = y
        pl.when(j < 12)(lambda: x_copy(j + 4).start())
        return carry

    with scope('permute'):
        lax.fori_loop(0, 16, permute_body, None)

    def signal_ready(i):
        pl.when(inner)(lambda: pl.semaphore_signal(ready.at[i], inc=1, device_id={'tp': tp ^ 1}, device_id_type=MESH))

    def wait_ready(i):
        with scope(f'ready{i}'):
            pl.when(outer)(lambda: pl.semaphore_wait(ready.at[i], 1))

    signal_ready(0)

    def group(g):
        low = g < 4
        return jnp.where(low, g & 1, 0), jnp.where(low, g // 2, g - 2)

    def head_number(h):
        return 2 * (tp ^ (h // 2 * 2)) + h % 2

    def project(heads, sigma, pair, kinds):
        for h in heads:
            t = head_number(h) + reverse(pair)
            x, swap = xp[side ^ sigma, pl.ds(2 * (t & 3), 2)].reshape(H, M), (t & 7) >> 2
            for t in kinds:
                y = nn(x, ws[t, :, part(h % 2, B)])
                for j in TWO:
                    piece = y[part(j, B)]
                    kv_s[h, 8 * sigma + 2 * pair + (j ^ swap), t] = (piece.T if t == VAL else piece).astype(BF)

    def phases_of(j):
        return [j % 2 + 2 * i for i in TWO], (j // 2) ^ side

    def rank_of(phase, h):
        rel = (phase - head_number(h)) & 7
        return (rel & 1) * 4 + ((rel >> 1) & 1) * 2 + (rel >> 2)

    def queries(heads, w, j):
        phases, half = phases_of(j)
        x = jnp.concatenate([xp[side, 2 * f + half] for f in phases])
        for h in heads:
            y = nn(x, ws[w, :, part(h % 2, B)]).astype(BF)
            for i, f in enumerate(phases):
                q_s[h, rank_of(f + 4 * half, h)] = y[part(i, B)]

    with scope('own_w'):
        for t in range(3):
            own_load(t).wait()
    own, partner = HEADS[:2], HEADS[2:]

    lane = lax.broadcasted_iota(jnp.int32, (1, H), 1)

    def mix(b, c):
        return jnp.where(lane < B, b, c)

    def keys_of(ref, h, i, weights):
        parts = []
        n = 0
        for count, b in weights:
            def values(i=i + n, count=count):
                v = [ref[h, i + j, VAL] for j in range(count)]
                return v[0] if count == 1 else jnp.concatenate(v, axis=1)
            parts.append((values, count * B, b))
            n += count
        return (lambda: ref[h, i:i + n, KEY].reshape(n * B, B)), parts

    def chunk_tiles(p, j, kind):
        both_phases, half = phases_of(j)

        def put(h, phase, ot):
            k = 2 * (phase & 3) + half
            y = ot.T.astype(BF)
            for i in TWO:
                pl.when(p == i)(lambda i=i: o_at(k, i, 0, (h % 2) * B, B).__setitem__(..., y))

        def tile(h, phases, ranks, wide, narrow, s_ref, n_ref):
            def done(ot):
                for i, phase in enumerate(phases):
                    put(h, phase, ot[:, part(i, B)])
            return tile_steps(lambda: jnp.concatenate([q_s[h, r] for r in ranks]), wide, narrow, s_ref, n_ref, done)

        h = 2 * p + (j % 2) ^ 1
        rest = tile(h, both_phases, [rank_of(f + 4 * half, h) for f in both_phases], [keys_of(kv_s, h, i, [(2, None)]) for i in range(0, 8, 2)], [], t_scr, None)
        h = 2 * p + (j % 2)
        a = head_number(h)
        b0, b01, b1, b012, b12, b2, b0123, b123, b23, b3 = [beta_ref[i, h] for i in range(10)]
        phases = [a & 3, (a & 3) ^ 2]
        both = [keys_of(kv_s, h, i, [(2, b)]) for i, b in ((2, b01), (4, b0), (6, b0), (10, b1))]
        if kind == 0:
            both += [keys_of(kv_s, h, 0, [(1, mix(b0123, b01)), (1, mix(b012, b01))]), keys_of(kv_s, h, 8, [(1, mix(b123, b1)), (1, mix(b12, b1))])]
            first = [keys_of(kvp_s, h, i, [(1, b23), (1, b2)]) for i in (0, 2)] + [keys_of(kvr_s, h, i, [(2, b3)]) for i in (0, 2)]
        else:
            both += [keys_of(kv_s, h, 0, [(2, mix(b012, b01))]), keys_of(kv_s, h, 8, [(2, mix(b12, b1))])]
            first = [keys_of(kvp_s, h, i, [(2, b2)]) for i in (0, 2)]
        with scope(f'tile{kind}'):
            run_tiles([rest, tile(h, phases, [kind, rank_of(phases[1] + 4 * half, h)], both, first, s_scr, t_scr.at[:, pl.ds(0, B)])])

    def send_o(ks, p):
        @pl.when(outer)
        def _():
            for k in ks:
                o_copy(order(k), p).start()

    def step_body(t, carry):
        packed = functools.reduce(lambda x, i: jnp.where(t == i, TABLE[i], x), range(len(TABLE)), 0)
        code, n, event = packed % 16, packed // 16 % 16, packed // 256

        def step_o():
            with scope('own_kv'):
                project(own, *group(n), (KEY, VAL))

        def step_kv(t_):
            with scope(f'par_{t_}'):
                for i in TWO:
                    project(partner, *group(2 * n + i), (t_,))

        def step_q(heads, w):
            with scope(f'que_{w}'):
                queries(heads, w, n)

        def step_out(v, m):
            @pl.when(inner)
            def _():
                k = order(n)
                if m == 2:
                    with scope('wait_o'):
                        for p in TWO:
                            o_copy(k, p).wait_recv()
                with scope(f'out{v}'):
                    o_times(k, v, m)

        f = functools.partial
        kinds = {'-': lambda: None, 'O': step_o, 'P': f(step_q, own, QUE), 'K': f(step_kv, KEY), 'V': f(step_kv, VAL), 'Q': f(step_q, partner, KEY),
                 'A': lambda: chunk_tiles(n // 4, n % 4, 0), 'B': lambda: chunk_tiles(n // 4, n % 4, 1), 'R': f(step_out, 2, 2), 'L': f(step_out, 1, 1), 'N': f(step_out, 0, 1)}
        choose(code, [kinds[c] for c in KINDS])
        call = functools.partial

        events = {
            'free': [call(signal_ready, 1), call(on, inner, lambda: start(wo_own()))],
            'r0': [call(wait_ready, 0)],
            'r1': [call(wait_ready, 1)],
            'so': [call(kv_start, kvp_copy, own)],
            'po': [call(kv_wait, kvp_copy, own)],
            'sp': [call(kv_start, kvp_copy, partner)],
            'pp': [call(kv_wait, kvp_copy, partner)],
        }
        for t_, c in enumerate('kvq'):
            events['b' + c] = [call(lq_start, t_)]
            events['w' + c] = [call(ev_weights, t_)]
            for i in TWO:
                for e, f in zip('zxy', (ev_z, ev_xy, ev_y)):
                    events[f'{e}{c}{i}'] = [call(f, lq_copy, 2 * t_ + i)]
        for i, vs in enumerate(((2, 3), (1,), (0,))):
            events[f'b{i}'] = [call(lo_start, *vs)]
            for e, f in zip('zxycw', (call(ev_z, lo_copy), call(ev_xy, lo_copy), call(ev_y, lo_copy), ev_lb, ev_wo)):
                events[f'{e}{i}'] = [call(on, inner, call(f, *vs))]
        events['w0'] += [call(on, inner, lambda: wait(wo_own()))]
        for h in HEADS:
            for z in TWO:
                events[f's{h}{z}'] = [kvr_copy(h, z).start]
            events[f'f{h}'] = [call(kv_forward, [h])]
            events[f'g{h}'] = [call(kv_wait, kvf_copy, [h])]
        for k in ROWS:
            for p in TWO:
                events['op'[p] + str(k)] = [call(send_o, (k,), p)]
        def run(names):
            for name in names.split(','):
                where, _, name = name.rpartition(':')
                if where:
                    on(inner if where == 'i' else outer, *events[name])
                else:
                    for c in events[name]:
                        c()

        @pl.when(event > 0)
        def _():
            choose(event - 1, [functools.partial(run, names) for names in EVENTS])
        return carry

    lax.fori_loop(0, len(TABLE), step_body, None)

    def call_sends(copy, p):
        return functools.partial(sends_done, copy, p)

    for t in range(6):
        lq_z(t).wait_send()
        sends_done(lq_copy, t)
    for v in range(4):
        lo_z(v).wait_send()
        on(outer, lb_z(v).wait_send)
        on(inner, lb_core(v).wait_send, call_sends(lo_copy, v))
    for h in HEADS:
        for s in TWO:
            for copy in (kvp_copy, kvr_copy, kvf_copy):
                copy(h, s).wait_send()

    @pl.when(outer)
    def _():
        for k in ROWS:
            for p in TWO:
                o_copy(k, p).wait_send()

    @pl.when(inner)
    def _():
        for k in ROWS:
            for v in (1, 2, 3):
                y_copy(k, v, side).wait_send()
            y_local(k).wait()

    for seg in TWO:
        @pl.when(tp != 1 + seg)
        def _(seg=seg):
            for k in ROWS:
                with scope(f'recv{k}_{seg}'):
                    y_copy(k, 1, seg).wait_recv()


PROGRAM = (
    'O.i:zk0,i:zk1', 'O.o:zk0,bv,so', 'O.o:zk1,s00,i:xk0', 'O.o:xk0,i:xk1', 'O.o:xk1,i:yk0,i:zv0,i:zv1', 'O.o:yk0,i:yk1,s01', 'P.bq',
    'P.o:yk1,o:zv0', 'P.wk,o:zv1', 'K.i:xv0,i:xv1', 'K.o:xv0,i:zq0,i:zq1,f0', 'K.o:xv1,o:zq0,i:yv0,i:yv1,b0,r0,po', 'P.o:yv0,o:zq1,b1,g0',
    'T0.o0,o1,o:yv1,wv,xq0', 'V.xq1,z0', 'V.o:yq0,z1,c0', 'V.i:yq0,yq1,sp,free,x0,wq', 'Q.pp,c1,r1', 'T4.p0,p1,x1,s10,s11', 'Q', 'Q.y0', 'Q',
    '-.w0,y1', 'R', 'T5.p2,p3,b2,s20,s21', 'R.w1', 'L', 'L.f1', 'T2.s30,s31,g1', 'T1.o2,o3,o4,o5', 'R', 'L.z2,c2,f2', 'R', 'L.x2,g2', 'T6.p4,p5',
    'T3.o6,o7,f3', 'R', 'L.y2,g3', 'T7.p6,p7', 'R', 'L', '-.w2', 'N', 'N', 'N', 'R', 'L', 'N', 'R', 'L', 'N', 'N', 'N', 'N',
)
KINDS = '-OPKVQABRLN'


def tables():
    table, seen = [], {}
    names = tuple(dict.fromkeys(s.partition('.')[2] for s in PROGRAM if '.' in s))
    for s in PROGRAM:
        name, _, after = s.partition('.')
        kind, n = name[0], seen.get(name[0], 0)
        seen[kind] = n + 1
        if kind == 'T':
            n = int(name[1:])
            kind = 'AB'[n in (2, 3, 4, 5)]
        table.append(KINDS.index(kind) + 16 * n + 256 * (names.index(after) + 1 if after else 0))
    return table, names


TABLE, EVENTS = tables()


def main(beta, x, wk, wv, wq, w_out):
    anyspec = pl.BlockSpec(memory_space=pl.ANY)
    vmem = [((4, B, M), BF), ((B, B), BF), ((2, 8, B, M), BF), ((3, M, H), BF), ((4, 8, B, B), BF), ((4, 12, 2, B, B), BF), ((4, 4, 2, B, B), BF), ((4, 4, 2, B, B), BF),
            ((3072, H), F32), ((M, H), F32)]
    dma = [(4,), (6, 8), (5, 8, 3), (6, 8), (6, 8), (4,), (4, 2), (4, 8), (4, 8), (4, 2), (4, 2)] + [(4, 2)] * 6 + [(8, 2), (8, 2), (8, 4), (2, 8)]
    return pl.pallas_call(
        main_kernel,
        in_specs=[pl.BlockSpec(memory_space=pltpu.SMEM)] + [anyspec] * 5,
        out_specs=[anyspec] * 4,
        out_shape=[jax.ShapeDtypeStruct(s, BF) for s in ((2, 8, B, H), (8, 6, B, B), (4, 8, 2, 64, H), (4, 2, B, H))],
        scratch_shapes=[pltpu.VMEM(*v) for v in vmem] + [pltpu.SemaphoreType.DMA(d) for d in dma] + [pltpu.SemaphoreType.REGULAR((2,)), pltpu.SMEM((len(TABLE),), jnp.int32)],
        compiler_params=params(collective_id=0, has_side_effects=True),
        cost_estimate=pl.CostEstimate(flops=10**11, bytes_accessed=10**8, transcendentals=0),
        name='main',
    )(beta, x, wk, wv, wq, w_out)[0]


def solution(mesh):
    tp_size = mesh.shape['tp']

    def device_fn(hidden, w_query, w_key, w_value, w_out, branch_bias):
        tp = lax.axis_index('tp')
        heads = branch_bias.shape[1] // tp_size
        b = jnp.concatenate([lax.dynamic_slice_in_dim(branch_bias, t * heads, heads, axis=1) for t in (tp, tp ^ 2)], axis=1)
        beta = []
        for branches in ('0', '01', '1', '012', '12', '2', '0123', '123', '23', '3'):
            rows = [b[i:i + 1] for i in map(int, branches)]
            m = functools.reduce(jnp.maximum, rows)
            beta.append((m + jnp.log(sum(jnp.exp(r - m) for r in rows))) * math.log2(math.e))
        return unpermute(main(jnp.concatenate(beta), hidden, w_key, w_value, w_query, w_out))

    return jax.shard_map(device_fn, mesh=mesh, in_specs=(P(('dp', 'sp'), None), P(None, 'tp'), P(None, 'tp'), P(None, 'tp'), P('tp', None), P(None, None)), out_specs=P(('dp', 'sp'), 'tp'), check_vma=False)
```

```python
import functools
import math

import jax
import jax.numpy as jnp
from jax import lax
from jax.experimental import pallas as pl
from jax.experimental.pallas import tpu as pltpu
from jax.sharding import PartitionSpec as P

MESH = pl.DeviceIdType.MESH
BF = jnp.bfloat16
F32 = jnp.float32
B, H, M = 256, 512, 2048
KAPPA = math.log2(math.e) / 16
VMEM = 66_900_000
SLOT = (0, 4, 2, 6, 1, 5, 3, 7)
KEY, VAL, QUE = range(3)
HEADS = range(4)
TWO = range(2)
ROWS = range(8)


def nn(a, b):
    return lax.dot_general(a, b, (((1,), (0,)), ((), ())), preferred_element_type=F32)


def nt(a, b):
    return lax.dot_general(a, b, (((1,), (1,)), ((), ())), preferred_element_type=F32)


def params(**kw):
    return pltpu.CompilerParams(vmem_limit_bytes=VMEM, **kw)


def ds(start, size, align=128):
    return pl.ds(pl.multiple_of(start, align), size)


def part(i, size):
    return slice(i * size, i * size + size)


def phase_matrix(transposed):
    r = lax.broadcasted_iota(jnp.int32, (B, B), int(transposed))
    p = lax.broadcasted_iota(jnp.int32, (B, B), int(not transposed))
    k = r // 32
    return (p == (r % 32) * 8 + k // 2 + 4 * (k % 2)).astype(F32).astype(BF)


def unpermute_kernel(y_ref, o_ref, y_s, o_s, load, store):
    pieces = [(s, j) for s in TWO for j in range(4)]

    def get(i):
        s, j = pieces[i]
        return pltpu.make_async_copy(y_ref.at[s, :, pl.ds(j * 64, 64)], y_s.at[i], load.at[i])

    def put(i):
        return pltpu.make_async_copy(o_s.at[i], o_ref.at[pl.ds(i * H, H)], store.at[i])

    for i in ROWS:
        get(i).start()
    pm = phase_matrix(True)
    for i in ROWS:
        get(i).wait()
        for j in TWO:
            o_s[i, part(j, B), :] = nn(pm, y_s[i, :, part(j, 32), :].reshape(B, H)).astype(BF)
        put(i).start()
    for i in ROWS:
        put(i).wait()


def unpermute(y):
    anyspec = pl.BlockSpec(memory_space=pl.ANY)
    return pl.pallas_call(
        unpermute_kernel,
        in_specs=[anyspec],
        out_specs=anyspec,
        out_shape=jax.ShapeDtypeStruct((2 * M, H), BF),
        scratch_shapes=[pltpu.VMEM((8, 8, 64, H), BF), pltpu.VMEM((8, H, H), BF), pltpu.SemaphoreType.DMA((8,)), pltpu.SemaphoreType.DMA((8,))],
        compiler_params=params(),
        name='unpermute',
    )(y)


def tile_steps(q, wide, narrow, s_ref, n_ref, done):
    st = {}
    logits, sums = [], []

    def add(name, x):
        st[name] = st[name] + x if name in st else x

    for groups, ref in ((wide, s_ref), (narrow, n_ref)):
        off = 0
        for keys, parts in groups:
            def qk(keys=keys, parts=parts, off=off, ref=ref):
                s = nt(keys(), q() if ref is s_ref else q()[:B])
                o = 0
                for _, n, b in parts:
                    piece = s[o:o + n]
                    ref[pl.ds(off + o, n), :] = piece
                    t = jnp.max(piece, axis=0, keepdims=True) * KAPPA
                    if b is not None:
                        t = t + fit(b, t)
                    if ref is n_ref:
                        t = jnp.concatenate([t, st['top'][:, B:]], axis=1)
                    st['top'] = jnp.maximum(st['top'], t) if 'top' in st else t
                    o += n
            logits.append(qk)
            for v, n, b in parts:
                def sv(v=v, n=n, b=b, off=off, ref=ref):
                    top = st['top'] if ref is s_ref else st['top'][:, :B]
                    e = jnp.exp2(ref[pl.ds(off, n), :] * KAPPA - (top if b is None else top - fit(b, top)))
                    name = 'w' if ref is s_ref else 'n'
                    add('l' + name, jnp.sum(e, axis=0, keepdims=True))
                    add('o' + name, nn(v(), e.astype(BF)))
                sums.append(sv)
                off += n

    def finish():
        o, l = st['ow'], st['lw']
        if narrow:
            o = jnp.concatenate([o[:, :B] + st['on'], o[:, B:]], axis=1)
            l = jnp.concatenate([l[:, :B] + st['ln'], l[:, B:]], axis=1)
        done(o / l)

    return logits, sums + [finish]


def fit(b, like):
    return b if b.shape == like.shape else jnp.concatenate([b] * (like.shape[1] // 128), axis=1)


def interleave(a, b):
    i = j = 0
    while i < len(a) or j < len(b):
        if j >= len(b) or (i < len(a) and i * len(b) <= j * len(a)):
            a[i]()
            i += 1
        else:
            b[j]()
            j += 1


def run_tiles(tiles):
    before = []
    for logits, sums in tiles:
        interleave(logits, before)
        before = sums
    interleave([], before)


def choose(x, cases):
    def among(lo, hi):
        mid = (lo + hi) // 2
        if hi - lo == 1:
            cases[lo]()
        else:
            pl.when(x < mid)(lambda: among(lo, mid))
            pl.when(x >= mid)(lambda: among(mid, hi))
    among(0, len(cases))


def on(cond, *calls):
    @pl.when(cond)
    def _():
        for c in calls:
            c()


def scope(name):
    return jax.named_scope(name)


def main_kernel(bias_ref, x_ref, wk_ref, wv_ref, wq_ref, wout_ref, out_ref, lq_ref, lo_ref, lb_ref,
                xb, pm, xp, ws, q_s, kv_s, kvp_s, kvr_s, s_scr, t_scr,
                beta_s, x_sem, w_sem, wo_sem, sent, lq_recv, lo_recv, lb_recv, kv_recv, o_recv, y_recv, ready):
    dp, tp, sp = lax.axis_index('dp'), lax.axis_index('tp'), lax.axis_index('sp')
    idx = dp * 4 + sp
    side = tp // 2
    inner = (tp == 1) | (tp == 2)
    outer = jnp.logical_not(inner)
    W = (wk_ref, wv_ref, wq_ref)
    peer_x, peer_y, peer_c = {'dp': dp ^ 1}, {'sp': sp ^ 2}, {'sp': sp ^ 1}

    def remote(src, dst, ss, rs, dev):
        return pltpu.make_async_remote_copy(src_ref=src, dst_ref=dst, send_sem=ss, recv_sem=rs, device_id=dev, device_id_type=MESH)

    def lq_copy(t, src, dst, dev):
        return remote(lq_ref.at[src, t], lq_ref.at[dst, t], sent.at[0], lq_recv.at[t, min(dst, 4)], dev)

    def lq_z(t):
        return remote(W[t // 2].at[ds(idx * B, B), pl.ds(t % 2 * B, B)], lq_ref.at[0, t], sent.at[0], lq_recv.at[t, 0], {'tp': tp ^ 2})

    def lq_start(t):
        for i in TWO:
            lq_z(2 * t + i).start()

    def lo_copy(v, src, dst, dev):
        return remote(lo_ref.at[v, src], lo_ref.at[v, dst], sent.at[1], lo_recv.at[v, min(dst, 4)], dev)

    def lo_z(v):
        dst = 2 - side
        b = (tp ^ dst) - 2
        return remote(wout_ref.at[ds(idx * 64, 64, 64), ds((dst ^ v) * H, H)], lo_ref.at[v, 0, b], sent.at[2], lo_recv.at[v, 0], {'tp': dst})

    def lb_z(v):
        return remote(wout_ref.at[ds(sp % 2 * B, B), ds((tp ^ 1 ^ v) * H, H)], lb_ref.at[v, sp % 2], sent.at[3], lb_recv.at[v, 0], {'tp': tp ^ 1})

    def lb_core(v):
        return remote(lb_ref.at[v, sp % 2], lb_ref.at[v, sp % 2], sent.at[3], lb_recv.at[v, 1], peer_c)

    def lo_start(*vs):
        for v in vs:
            lo_z(v).start()

    def arrived(ref, sem):
        remote(ref, ref, sent.at[0], sem, peer_c).wait_recv()

    def all_sent(ref, i):
        remote(ref, ref, sent.at[i], sent.at[i], peer_c).wait_send()

    def lo_zwait(v):
        arrived(lo_ref.at[v, 0], lo_recv.at[v, 0])

    def hop(copy, p, i):
        near, far = (peer_y, peer_x) if copy is lq_copy else (peer_x, peer_y)
        n, f = (2, 1) if near is peer_y else (1, 2)
        return copy(p, *((0, n, near), (0, f, far), (0, 4, peer_c), (n, 3, far), (n, 4 + n, peer_c), (f, 4 + f, peer_c), (3, 7, peer_c))[i])

    def ev_z(copy, *ps):
        for p in ps:
            with scope(f'z_{copy.__name__}{p}'):
                lq_z(p).wait_recv() if copy is lq_copy else lo_zwait(p)
            for i in range(3):
                hop(copy, p, i).start()

    def ev_xy(copy, *ps):
        for p in ps:
            with scope(f'n_{copy.__name__}{p}'):
                hop(copy, p, 0).wait_recv()
            hop(copy, p, 3).start()
            hop(copy, p, 4).start()
        for p in ps:
            with scope(f'f_{copy.__name__}{p}'):
                hop(copy, p, 1).wait_recv()
            hop(copy, p, 5).start()

    def ev_y(copy, *ps):
        for p in ps:
            with scope(f'y_{copy.__name__}{p}'):
                hop(copy, p, 3).wait_recv()
            hop(copy, p, 6).start()
            if copy is lq_copy and p >= 2:
                start(w_load(p, SLOT[:4]))

    def ev_done(copy, *ps):
        for p in ps:
            with scope(f'c_{copy.__name__}{p}'):
                if copy is lq_copy:
                    arrived(lq_ref.at[pl.ds(4, 4), p], lq_recv.at[p, 4])
                else:
                    arrived(lo_ref.at[p, pl.ds(4, 4)], lo_recv.at[p, 4])

    def w_load(p, slots):
        return [pltpu.make_async_copy(lq_ref.at[SLOT.index(m), p], ws.at[p // 2 % 2, ds((idx ^ m) * B, B), pl.ds(p % 2 * B, B)], w_sem.at[p]) for m in slots]

    def own_load(t):
        return pltpu.make_async_copy(W[t], ws.at[t], w_sem.at[6 + t])

    def start(copies):
        for c in copies:
            c.start()

    def wait(copies):
        for c in copies:
            c.wait()

    def ev_last(t):
        pieces = [2 * t + i for i in TWO]
        ev_done(lq_copy, *pieces)
        for p in pieces:
            start(w_load(p, SLOT[4:] if t else SLOT))

    def local(ref, sem):
        pltpu.make_async_copy(ref, ref, sem).wait()

    def ev_weights(t):
        with scope(f'load{t}'):
            for i in TWO:
                local(ws.at[t % 2, :, pl.ds(i * B, B)], w_sem.at[2 * t + i])

    def ev_wo(*vs):
        ev_done(lo_copy, *vs)
        for v in vs:
            lb_core(v).wait_recv()
        start(wo_load(*vs))

    def ev_wo_ready(*vs):
        with scope(f'wo{vs[0]}'):
            for v in vs:
                local(xp.at[1 - side, pl.ds(2, 6), :, pl.ds((v ^ 2) * H, H)], wo_sem.at[v])

    def ev_lb(*vs):
        for v in vs:
            with scope(f'lb{v}'):
                lb_z(v).wait_recv()
            lb_core(v).start()

    wo = xp.at[1 - side]

    def wo_own():
        return [pltpu.make_async_copy(wout_ref.at[pl.ds(r * B, B), pl.ds(c * H, H)], xp.at[1 - side, r, :, ds((c ^ tp ^ 2) * H, H)], wo_sem.at[4])
                for r in TWO for c in range(4)]

    def wo_load(*vs):
        out = []
        for v in vs:
            cols = pl.ds((v ^ 2) * H, H)
            for s, m in enumerate(SLOT):
                row = (idx ^ m) * 64
                for b in TWO:
                    out.append(pltpu.make_async_copy(lo_ref.at[v, s, b], xp.at[1 - side, 4 + 2 * b + row // B, ds(row % B, 64, 64), cols], wo_sem.at[v]))
            for r in TWO:
                out.append(pltpu.make_async_copy(lb_ref.at[v, r], xp.at[1 - side, 2 + r, :, cols], wo_sem.at[v]))
        return out

    def kvp_copy(h, s):
        return remote(kv_s.at[h, pl.ds(8 * s, 2)], kvp_s.at[h, pl.ds(2 * s, 2)], sent.at[4], kv_recv.at[0, h], peer_c)

    def kvr_copy(h, s):
        return remote(kv_s.at[h, 8 * s], kvr_s.at[h, s], sent.at[5], kv_recv.at[1, h], peer_y)

    def kvf_copy(h, s):
        return remote(kvr_s.at[h, s], kvr_s.at[h, 2 + s], sent.at[6], kv_recv.at[2, h], peer_c)

    def kv_start(copy, heads):
        for h in heads:
            for s in TWO:
                copy(h, s).start()

    def kv_wait(copy, heads):
        with scope(f'w_{copy.__name__}{heads[0]}'):
            for h in heads:
                i = (kvp_copy, kvr_copy, kvf_copy).index(copy)
                arrived((kvp_s.at[h], kvr_s.at[h, pl.ds(0, 2)], kvr_s.at[h, pl.ds(2, 2)])[i], kv_recv.at[i, h])

    def kv_forward(heads):
        kv_wait(kvr_copy, heads)
        kv_start(kvf_copy, heads)

    def reverse(i):
        return (i % 2) * 2 + i // 2

    def order(n):
        return 2 * reverse(n % 4) + ((n // 4) ^ side)

    def o_at(k, p, theirs, col, size):
        return ws.at[1 + theirs, ds(k * B, B), ds(col, size)] if p else xb.at[k // 2, :, ds((k % 2) * 1024 + theirs * H + col, size)]

    def o_copy(k, p):
        return remote(o_at(k, p, 0, 0, H), o_at(k, p, 1, 0, H), sent.at[7], o_recv.at[k], {'tp': tp ^ 1})

    def o_times(k, v, n):
        cols = pl.ds((v ^ 2) * H, n * H)
        y = nn(xb[k // 2, :, ds((k % 2) * 1024, 1024)], wo[0:4, :, cols].reshape(1024, n * H))
        for i in TWO:
            y = y + nn(ws[1 + i, ds(k * B, B), :], wo[part(2 + i, 2), :, cols].reshape(H, n * H))
        y = y.astype(BF)
        for i in range(n):
            y_src(k, v + i)[...] = y[:, part(i, H)]
            y_copy(k, v + i, side).start() if v else y_local(k).start()

    def y_src(k, v):
        return xp.at[side, k, :, pl.ds(v * H, H)]

    def y_copy(k, v, seg):
        return remote(y_src(k, v), out_ref.at[seg, k], sent.at[8], y_recv.at[seg], {'tp': tp ^ v})

    def y_local(k):
        return pltpu.make_async_copy(y_src(k, 0), out_ref.at[side, k], sent.at[9])

    def x_copy(j):
        return pltpu.make_async_copy(x_ref.at[ds(j * B, B), :], xb.at[lax.rem(j, 4)], x_sem.at[lax.rem(j, 4)])

    for j in range(4):
        x_copy(j).start()
    barrier = pltpu.get_barrier_semaphore()
    peers = [{'tp': tp ^ 1}, {'tp': tp ^ 2}, {'tp': tp ^ 3}, peer_x, peer_y, peer_c]
    for dev in peers:
        pl.semaphore_signal(barrier, inc=1, device_id=dev, device_id_type=MESH)
    for t in range(3):
        own_load(t).start()

    pm[...] = phase_matrix(False)

    def permute_body(j, carry):
        x_copy(j).wait()
        y = nn(pm[...], xb[lax.rem(j, 4)]).astype(BF).reshape(8, 32, M)
        xp[j // 8, :, ds(lax.rem(j, 8) * 32, 32, 32), :] = y
        pl.when(j < 12)(lambda: x_copy(j + 4).start())

        @pl.when(j == 7)
        def _():
            with scope('barrier'):
                pl.semaphore_wait(barrier, len(peers))
            lq_start(KEY)
            on(outer, lb_z(2).start)
        return carry

    with scope('permute'):
        lax.fori_loop(0, 16, permute_body, None)

    for h in HEADS:
        column = 2 * (tp ^ (h // 2 * 2)) + h % 2
        for i, branches in enumerate(('0', '01', '1', '012', '12', '2', '0123', '123', '23', '3')):
            rows = [jnp.full((1, 128), bias_ref[j, column], F32) for j in map(int, branches)]
            m = functools.reduce(jnp.maximum, rows)
            beta_s[pl.ds(h * 16 + i, 1), :] = (m + jnp.log(sum(jnp.exp(r - m) for r in rows))) * math.log2(math.e)

    def signal_ready(i):
        pl.when(inner)(lambda: pl.semaphore_signal(ready.at[i], inc=1, device_id={'tp': tp ^ 1}, device_id_type=MESH))

    def wait_ready(i):
        with scope(f'ready{i}'):
            pl.when(outer)(lambda: pl.semaphore_wait(ready.at[i], 1))

    signal_ready(0)

    def group(g):
        low = g < 4
        return jnp.where(low, g & 1, 0), jnp.where(low, g // 2, g - 2)

    def head_number(h):
        return 2 * (tp ^ (h // 2 * 2)) + h % 2

    def project(heads, sigma, pair, kinds):
        for h in heads:
            t = head_number(h) + reverse(pair)
            x, swap = xp[side ^ sigma, pl.ds(2 * (t & 3), 2)].reshape(H, M), (t & 7) >> 2
            for t in kinds:
                y = nn(x, ws[t, :, part(h % 2, B)])
                for j in TWO:
                    piece = y[part(j, B)]
                    kv_s[h, 8 * sigma + 2 * pair + (j ^ swap), t] = (piece.T if t == VAL else piece).astype(BF)

    def phases_of(j):
        return [j % 2 + 2 * i for i in TWO], (j // 2) ^ side

    def rank_of(phase, h):
        rel = (phase - head_number(h)) & 7
        return (rel & 1) * 4 + ((rel >> 1) & 1) * 2 + (rel >> 2)

    def queries(heads, w, j):
        phases, half = phases_of(j)
        x = jnp.concatenate([xp[side, 2 * f + half] for f in phases])
        for h in heads:
            y = nn(x, ws[w, :, part(h % 2, B)]).astype(BF)
            for i, f in enumerate(phases):
                q_s[h, rank_of(f + 4 * half, h)] = y[part(i, B)]

    with scope('own_w'):
        for t in range(3):
            own_load(t).wait()
    own, partner = HEADS[:2], HEADS[2:]

    def mix(b, c):
        return jnp.concatenate([b, b, c, c], axis=1)

    def keys_of(ref, h, i, weights):
        parts = []
        n = 0
        for count, b in weights:
            def values(i=i + n, count=count):
                v = [ref[h, i + j, VAL] for j in range(count)]
                return v[0] if count == 1 else jnp.concatenate(v, axis=1)
            parts.append((values, count * B, b))
            n += count
        return (lambda: ref[h, i:i + n, KEY].reshape(n * B, B)), parts

    def chunk_tiles(p, j, kind):
        both_phases, half = phases_of(j)

        def put(h, phase, ot):
            k = 2 * (phase & 3) + half
            y = ot.T.astype(BF)
            for i in TWO:
                pl.when(p == i)(lambda i=i: o_at(k, i, 0, (h % 2) * B, B).__setitem__(..., y))

        def tile(h, phases, ranks, wide, narrow, s_ref, n_ref):
            def done(ot):
                for i, phase in enumerate(phases):
                    put(h, phase, ot[:, part(i, B)])
            return tile_steps(lambda: jnp.concatenate([q_s[h, r] for r in ranks]), wide, narrow, s_ref, n_ref, done)

        h = 2 * p + (j % 2) ^ 1
        rest = tile(h, both_phases, [rank_of(f + 4 * half, h) for f in both_phases], [keys_of(kv_s, h, i, [(2, None)]) for i in range(0, 8, 2)], [], t_scr, None)
        h = 2 * p + (j % 2)
        a = head_number(h)
        b0, b01, b1, b012, b12, b2, b0123, b123, b23, b3 = [beta_s[pl.ds(h * 16 + i, 1), :] for i in range(10)]
        phases = [a & 3, (a & 3) ^ 2]
        both = [keys_of(kv_s, h, i, [(2, b)]) for i, b in ((2, b01), (4, b0), (6, b0), (10, b1))]
        if kind == 0:
            both += [keys_of(kv_s, h, 0, [(1, mix(b0123, b01)), (1, mix(b012, b01))]), keys_of(kv_s, h, 8, [(1, mix(b123, b1)), (1, mix(b12, b1))])]
            first = [keys_of(kvp_s, h, i, [(1, b23), (1, b2)]) for i in (0, 2)] + [keys_of(kvr_s, h, i, [(2, b3)]) for i in (0, 2)]
        else:
            both += [keys_of(kv_s, h, 0, [(2, mix(b012, b01))]), keys_of(kv_s, h, 8, [(2, mix(b12, b1))])]
            first = [keys_of(kvp_s, h, i, [(2, b2)]) for i in (0, 2)]
        with scope(f'tile{kind}'):
            run_tiles([rest, tile(h, phases, [kind, rank_of(phases[1] + 4 * half, h)], both, first, s_scr, t_scr.at[:, pl.ds(0, B)])])

    def send_o(ks, p):
        @pl.when(outer)
        def _():
            for k in ks:
                o_copy(order(k), p).start()

    def step_body(t, carry):
        packed = functools.reduce(lambda x, i: jnp.where(t == i, TABLE[i], x), range(len(TABLE)), 0)
        code, n, event = packed % 16, packed // 16 % 16, packed // 256

        def step_o():
            with scope('own_kv'):
                project(own, *group(n), (KEY, VAL))

        def step_kv(t_):
            with scope(f'par_{t_}'):
                for i in TWO:
                    project(partner, *group(2 * n + i), (t_,))

        def step_q(heads, w):
            with scope(f'que_{w}'):
                queries(heads, w, n)

        def step_out(v, m):
            @pl.when(inner)
            def _():
                k = order(n)
                if m == 2:
                    with scope('wait_o'):
                        arrived(ws.at[0, pl.ds(0, H), :], o_recv.at[k])
                with scope(f'out{v}'):
                    o_times(k, v, m)

        f = functools.partial
        kinds = {'-': lambda: None, 'O': step_o, 'P': f(step_q, own, QUE), 'K': f(step_kv, KEY), 'V': f(step_kv, VAL), 'Q': f(step_q, partner, KEY),
                 'A': lambda: chunk_tiles(n // 4, n % 4, 0), 'B': lambda: chunk_tiles(n // 4, n % 4, 1), 'R': f(step_out, 2, 2), 'L': f(step_out, 1, 1), 'N': f(step_out, 0, 1)}
        choose(code, [kinds[c] for c in KINDS])
        call = functools.partial

        events = {
            'free': [call(signal_ready, 1), call(on, inner, lambda: start(wo_own()))],
            'r0': [call(wait_ready, 0)],
            'r1': [call(wait_ready, 1)],
            'so': [call(kv_start, kvp_copy, own)],
            'po': [call(kv_wait, kvp_copy, own)],
            'sp': [call(kv_start, kvp_copy, partner)],
            'pp': [call(kv_wait, kvp_copy, partner)],
        }
        for t_, c in enumerate('kvq'):
            events['b' + c] = [call(lq_start, t_)]
            events['l' + c] = [call(ev_last, t_)]
            events['w' + c] = [call(ev_weights, t_)]
            for i in TWO:
                for e, f in zip('zxy', (ev_z, ev_xy, ev_y)):
                    events[f'{e}{c}{i}'] = [call(f, lq_copy, 2 * t_ + i)]
        for i, vs in enumerate(((2, 3), (1,), (0,))):
            events[f'b{i}'] = [call(lo_start, *vs)]
            for e, f in zip('zxycwv', (call(ev_z, lo_copy), call(ev_xy, lo_copy), call(ev_y, lo_copy), ev_lb, ev_wo, ev_wo_ready)):
                events[f'{e}{i}'] = [call(on, inner, call(f, *vs))]
        events['v0'] += [call(on, inner, lambda: local(xp.at[1 - side, pl.ds(0, 2)], wo_sem.at[4]))]
        for v in (0, 1, 3):
            events[f'd{v}'] = [call(on, outer, lambda v=v: lb_z(v).start())]
        for h in HEADS:
            for z in TWO:
                events[f's{h}{z}'] = [kvr_copy(h, z).start]
            events[f'f{h}'] = [call(kv_forward, [h])]
            events[f'g{h}'] = [call(kv_wait, kvf_copy, [h])]
        for k in ROWS:
            for p in TWO:
                events['op'[p] + str(k)] = [call(send_o, (k,), p)]
        def run(names):
            for name in names.split(','):
                where, _, name = name.rpartition(':')
                if where:
                    on(inner if where == 'i' else outer, *events[name])
                else:
                    for c in events[name]:
                        c()

        @pl.when(event > 0)
        def _():
            choose(event - 1, [functools.partial(run, names) for names in EVENTS])
        return carry

    lax.fori_loop(0, len(TABLE), step_body, None)

    all_sent(lq_ref, 0)
    all_sent(lo_ref.at[:, 0, 0], 2)
    all_sent(lb_ref.at[:, 0], 3)
    all_sent(kvp_s, 4)
    all_sent(kvr_s.at[:, pl.ds(0, 2)], 5)
    all_sent(kvr_s.at[:, pl.ds(0, 2)], 6)

    @pl.when(outer)
    def _():
        all_sent(xb, 7)

    @pl.when(inner)
    def _():
        all_sent(lo_ref.at[:, pl.ds(0, 7)], 1)
        with scope('y_sent'):
            all_sent(xp.at[side, :, :, pl.ds(H, 3 * H)], 8)
        local(xp.at[side, :, :, pl.ds(0, H)], sent.at[9])

    for seg in TWO:
        @pl.when(tp != 1 + seg)
        def _(seg=seg):
            with scope(f'recv{seg}'):
                arrived(out_ref.at[seg], y_recv.at[seg])


PROGRAM = (
    'O.i:zk0,i:zk1', 'O.o:zk0,bv,d3,so', 'O.o:zk1,s00,i:xk0', 'O.o:xk0,i:xk1', 'O.o:xk1,i:yk0,i:zv0', 'O.o:yk0,i:yk1,i:zv1,s01', 'P.bq,d1,o:yk1,lk',
    'P.wk,o:zv0,i:xv0', 'K.o:zv1,i:xv1', 'K.f0,i:zq0,i:zq1', 'K.o:xv0,o:zq0,i:yv0,i:yv1,b0,r0,po,g0', 'P.o:xv1',
    'T0.o0,o1,o:yv0,o:yv1,o:zq1,b1,lv,wv,i:xq0,i:xq1', 'V.o:xq0,o:xq1,z0,o:s10,o:s11', 'V.o:yq0,c0,z1', 'V.i:yq0,i:yq1,o:yq1,sp,lq,o:s20,o:s21',
    'P.free,x0,wq,c1', 'Q.pp,r1,o:s30,o:s31', 'T4.p0,p1,x1', 'Q.y0,i:s10,i:s11,w0', 'T5.p2,p3,v0,y1,w1,o:f1', 'R', 'Q.v1', 'L', 'R', 'L',
    'Q.i:f1,o:g1,i:s20,i:s21,b2,d0', 'T2.i:g1,o:f2', 'T1.o2,o3,o:g2,o:f3', 'R.i:s30,i:s31', 'L.z2,c2,i:f2', 'R.x2', 'L.i:g2',
    'T6.p4,o4,p5,o5,y2,o:g3', 'T3.w2,i:f3', 'R.v2', 'L.i:g3', 'T7.p6,o6,p7,o7', 'R', 'L', 'N', 'N', 'N', 'N', 'R', 'L', 'N', 'R', 'L', 'N', 'N', 'N',
)
KINDS = '-OPKVQABRLN'


def tables():
    table, seen = [], {}
    names = tuple(dict.fromkeys(s.partition('.')[2] for s in PROGRAM if '.' in s))
    for s in PROGRAM:
        name, _, after = s.partition('.')
        kind, n = name[0], seen.get(name[0], 0)
        seen[kind] = n + 1
        if kind == 'T':
            n = int(name[1:])
            kind = 'AB'[n in (2, 3, 4, 5)]
        table.append(KINDS.index(kind) + 16 * n + 256 * (names.index(after) + 1 if after else 0))
    return table, names


TABLE, EVENTS = tables()


def main(bias, x, wk, wv, wq, w_out):
    anyspec = pl.BlockSpec(memory_space=pl.ANY)
    vmem = [((4, B, M), BF), ((B, B), BF), ((2, 8, B, M), BF), ((3, M, H), BF), ((4, 8, B, B), BF), ((4, 12, 2, B, B), BF), ((4, 4, 2, B, B), BF), ((4, 4, 2, B, B), BF),
            ((3072, H), F32), ((M, H), F32), ((64, 128), F32)]
    dma = [(4,), (9,), (5,), (10,), (6, 5), (4, 5), (4, 2), (3, 4), (8,), (2,)]
    return pl.pallas_call(
        main_kernel,
        in_specs=[pl.BlockSpec(memory_space=pltpu.SMEM)] + [anyspec] * 5,
        out_specs=[anyspec] * 4,
        out_shape=[jax.ShapeDtypeStruct(s, BF) for s in ((2, 8, B, H), (8, 6, B, B), (4, 8, 2, 64, H), (4, 2, B, H))],
        scratch_shapes=[pltpu.VMEM(*v) for v in vmem] + [pltpu.SemaphoreType.DMA(d) for d in dma] + [pltpu.SemaphoreType.REGULAR((2,))],
        compiler_params=params(collective_id=0, has_side_effects=True),
        cost_estimate=pl.CostEstimate(flops=10**11, bytes_accessed=10**8, transcendentals=0),
        name='main',
    )(bias, x, wk, wv, wq, w_out)[0]


def solution(mesh):
    def device_fn(hidden, w_query, w_key, w_value, w_out, branch_bias):
        return unpermute(main(branch_bias, hidden, w_key, w_value, w_query, w_out))

    return jax.shard_map(device_fn, mesh=mesh, in_specs=(P(('dp', 'sp'), None), P(None, 'tp'), P(None, 'tp'), P(None, 'tp'), P('tp', None), P(None, None)), out_specs=P(('dp', 'sp'), 'tp'), check_vma=False)
```

```python
import functools
import math

import jax
import jax.numpy as jnp
from jax import lax
from jax.experimental import pallas as pl
from jax.experimental.pallas import tpu as pltpu
from jax.sharding import PartitionSpec as P

MESH = pl.DeviceIdType.MESH
BF = jnp.bfloat16
F32 = jnp.float32
B, H, M = 256, 512, 2048
KAPPA = math.log2(math.e) / 16
VMEM = 66_900_000
SLOT = (0, 4, 2, 6, 1, 5, 3, 7)
KEY, VAL, QUE = range(3)
HEADS = range(4)
TWO = range(2)
ROWS = range(8)


def nn(a, b):
    return lax.dot_general(a, b, (((1,), (0,)), ((), ())), preferred_element_type=F32)


def nt(a, b):
    return lax.dot_general(a, b, (((1,), (1,)), ((), ())), preferred_element_type=F32)


def params(**kw):
    return pltpu.CompilerParams(vmem_limit_bytes=VMEM, **kw)


def ds(start, size, align=128):
    return pl.ds(pl.multiple_of(start, align), size)


def part(i, size):
    return slice(i * size, i * size + size)


def phase_matrix(transposed):
    r = lax.broadcasted_iota(jnp.int32, (B, B), int(transposed))
    p = lax.broadcasted_iota(jnp.int32, (B, B), int(not transposed))
    k = r // 32
    return (p == (r % 32) * 8 + k // 2 + 4 * (k % 2)).astype(F32).astype(BF)


def unpermute_kernel(y_ref, o_ref, y_s, o_s, load, store):
    pieces = [(s, j) for s in TWO for j in range(4)]

    def get(i):
        s, j = pieces[i]
        return pltpu.make_async_copy(y_ref.at[s, :, pl.ds(j * 64, 64)], y_s.at[i], load.at[i])

    def put(i):
        return pltpu.make_async_copy(o_s.at[i], o_ref.at[pl.ds(i * H, H)], store.at[i])

    for i in ROWS:
        get(i).start()
    pm = phase_matrix(True)
    for i in ROWS:
        get(i).wait()
        for j in TWO:
            o_s[i, part(j, B), :] = nn(pm, y_s[i, :, part(j, 32), :].reshape(B, H)).astype(BF)
        put(i).start()
    for i in ROWS:
        put(i).wait()


def unpermute(y):
    anyspec = pl.BlockSpec(memory_space=pl.ANY)
    return pl.pallas_call(
        unpermute_kernel,
        in_specs=[anyspec],
        out_specs=anyspec,
        out_shape=jax.ShapeDtypeStruct((2 * M, H), BF),
        scratch_shapes=[pltpu.VMEM((8, 8, 64, H), BF), pltpu.VMEM((8, H, H), BF), pltpu.SemaphoreType.DMA((8,)), pltpu.SemaphoreType.DMA((8,))],
        compiler_params=params(),
        name='unpermute',
    )(y)


def tile_steps(q, wide, narrow, s_ref, n_ref, done):
    st = {}
    logits, sums = [], []

    def add(name, x):
        st[name] = st[name] + x if name in st else x

    for groups, ref in ((wide, s_ref), (narrow, n_ref)):
        off = 0
        for keys, parts in groups:
            def qk(keys=keys, parts=parts, off=off, ref=ref):
                s = nt(keys(), q() if ref is s_ref else q()[:B])
                o = 0
                for _, n, b in parts:
                    piece = s[o:o + n]
                    ref[pl.ds(off + o, n), :] = piece
                    t = jnp.max(piece, axis=0, keepdims=True) * KAPPA
                    if b is not None:
                        t = t + fit(b, t)
                    if ref is n_ref:
                        t = jnp.concatenate([t, st['top'][:, B:]], axis=1)
                    st['top'] = jnp.maximum(st['top'], t) if 'top' in st else t
                    o += n
            logits.append(qk)
            for v, n, b in parts:
                def sv(v=v, n=n, b=b, off=off, ref=ref):
                    top = st['top'] if ref is s_ref else st['top'][:, :B]
                    e = jnp.exp2(ref[pl.ds(off, n), :] * KAPPA - (top if b is None else top - fit(b, top)))
                    name = 'w' if ref is s_ref else 'n'
                    add('l' + name, jnp.sum(e, axis=0, keepdims=True))
                    add('o' + name, nn(v(), e.astype(BF)))
                sums.append(sv)
                off += n

    def finish():
        o, l = st['ow'], st['lw']
        if narrow:
            o = jnp.concatenate([o[:, :B] + st['on'], o[:, B:]], axis=1)
            l = jnp.concatenate([l[:, :B] + st['ln'], l[:, B:]], axis=1)
        done(o / l)

    return logits, sums + [finish]


def fit(b, like):
    return b if b.shape == like.shape else jnp.concatenate([b] * (like.shape[1] // 128), axis=1)


def interleave(a, b):
    i = j = 0
    while i < len(a) or j < len(b):
        if j >= len(b) or (i < len(a) and i * len(b) <= j * len(a)):
            a[i]()
            i += 1
        else:
            b[j]()
            j += 1


def run_tiles(tiles):
    before = []
    for logits, sums in tiles:
        interleave(logits, before)
        before = sums
    interleave([], before)


def choose(x, cases):
    def among(lo, hi):
        mid = (lo + hi) // 2
        if hi - lo == 1:
            cases[lo]()
        else:
            pl.when(x < mid)(lambda: among(lo, mid))
            pl.when(x >= mid)(lambda: among(mid, hi))
    among(0, len(cases))


def on(cond, *calls):
    @pl.when(cond)
    def _():
        for c in calls:
            c()


def scope(name):
    return jax.named_scope(name)


def main_kernel(bias_ref, x_ref, wk_ref, wv_ref, wq_ref, wout_ref, out_ref, lq_ref, lo_ref, lb_ref,
                xb, pm, xp, ws, q_s, kv_s, kvp_s, kvr_s, s_scr, t_scr,
                beta_s, x_sem, w_sem, wo_sem, sent, lq_recv, lo_recv, lb_recv, kv_recv, o_recv, y_recv, ready):
    dp, tp, sp = lax.axis_index('dp'), lax.axis_index('tp'), lax.axis_index('sp')
    idx = dp * 4 + sp
    side = tp // 2
    inner = (tp == 1) | (tp == 2)
    outer = jnp.logical_not(inner)
    W = (wk_ref, wv_ref, wq_ref)
    peer_x, peer_y, peer_c = {'dp': dp ^ 1}, {'sp': sp ^ 2}, {'sp': sp ^ 1}

    def remote(src, dst, ss, rs, dev):
        return pltpu.make_async_remote_copy(src_ref=src, dst_ref=dst, send_sem=ss, recv_sem=rs, device_id=dev, device_id_type=MESH)

    def lq_copy(t, src, dst, dev):
        return remote(lq_ref.at[src, t], lq_ref.at[dst, t], sent.at[0], lq_recv.at[t, min(dst, 4)], dev)

    def lq_z(t):
        return remote(W[t // 2].at[ds(idx * B, B), pl.ds(t % 2 * B, B)], lq_ref.at[0, t], sent.at[0], lq_recv.at[t, 0], {'tp': tp ^ 2})

    def lq_start(t):
        for i in TWO:
            lq_z(2 * t + i).start()

    def lo_copy(v, src, dst, dev):
        return remote(lo_ref.at[v, src], lo_ref.at[v, dst], sent.at[1], lo_recv.at[v, min(dst, 4)], dev)

    def lo_z(v):
        dst = 2 - side
        b = (tp ^ dst) - 2
        return remote(wout_ref.at[ds(idx * 64, 64, 64), ds((dst ^ v) * H, H)], lo_ref.at[v, 0, b], sent.at[2], lo_recv.at[v, 0], {'tp': dst})

    def lb_z(v):
        return remote(wout_ref.at[ds(sp % 2 * B, B), ds((tp ^ 1 ^ v) * H, H)], lb_ref.at[v, sp % 2], sent.at[3], lb_recv.at[v, 0], {'tp': tp ^ 1})

    def lb_core(v):
        return remote(lb_ref.at[v, sp % 2], lb_ref.at[v, sp % 2], sent.at[3], lb_recv.at[v, 1], peer_c)

    def lo_start(*vs):
        for v in vs:
            lo_z(v).start()

    def arrived(ref, sem):
        remote(ref, ref, sent.at[0], sem, peer_c).wait_recv()

    def all_sent(ref, i):
        remote(ref, ref, sent.at[i], sent.at[i], peer_c).wait_send()

    def lo_zwait(v):
        arrived(lo_ref.at[v, 0], lo_recv.at[v, 0])

    def hop(copy, p, i):
        near, far = (peer_y, peer_x) if copy is lq_copy else (peer_x, peer_y)
        n, f = (2, 1) if near is peer_y else (1, 2)
        return copy(p, *((0, n, near), (0, f, far), (0, 4, peer_c), (n, 3, far), (n, 4 + n, peer_c), (f, 4 + f, peer_c), (3, 7, peer_c))[i])

    def ev_z(copy, *ps):
        for p in ps:
            with scope(f'z_{copy.__name__}{p}'):
                lq_z(p).wait_recv() if copy is lq_copy else lo_zwait(p)
            for i in range(3):
                hop(copy, p, i).start()

    def ev_xy(copy, *ps):
        for p in ps:
            with scope(f'n_{copy.__name__}{p}'):
                hop(copy, p, 0).wait_recv()
            hop(copy, p, 3).start()
            hop(copy, p, 4).start()
        for p in ps:
            with scope(f'f_{copy.__name__}{p}'):
                hop(copy, p, 1).wait_recv()
            hop(copy, p, 5).start()

    def ev_y(copy, *ps):
        for p in ps:
            with scope(f'y_{copy.__name__}{p}'):
                hop(copy, p, 3).wait_recv()
            hop(copy, p, 6).start()
            if copy is lq_copy and p >= 2:
                start(w_load(p, SLOT[:4]))

    def ev_done(copy, *ps):
        for p in ps:
            with scope(f'c_{copy.__name__}{p}'):
                if copy is lq_copy:
                    arrived(lq_ref.at[pl.ds(4, 4), p], lq_recv.at[p, 4])
                else:
                    arrived(lo_ref.at[p, pl.ds(4, 4)], lo_recv.at[p, 4])

    def w_load(p, slots):
        return [pltpu.make_async_copy(lq_ref.at[SLOT.index(m), p], ws.at[p // 2 % 2, ds((idx ^ m) * B, B), pl.ds(p % 2 * B, B)], w_sem.at[p]) for m in slots]

    def own_load(t):
        return pltpu.make_async_copy(W[t], ws.at[t], w_sem.at[6 + t])

    def start(copies):
        for c in copies:
            c.start()

    def wait(copies):
        for c in copies:
            c.wait()

    def ev_last(t):
        pieces = [2 * t + i for i in TWO]
        ev_done(lq_copy, *pieces)
        for p in pieces:
            start(w_load(p, SLOT[4:] if t else SLOT))

    def local(ref, sem):
        pltpu.make_async_copy(ref, ref, sem).wait()

    def ev_weights(t):
        with scope(f'load{t}'):
            for i in TWO:
                local(ws.at[t % 2, :, pl.ds(i * B, B)], w_sem.at[2 * t + i])

    def ev_wo(*vs):
        ev_done(lo_copy, *vs)
        for v in vs:
            lb_core(v).wait_recv()
        start(wo_load(*vs))

    def ev_wo_ready(*vs):
        with scope(f'wo{vs[0]}'):
            for v in vs:
                local(xp.at[1 - side, pl.ds(2, 6), :, pl.ds((v ^ 2) * H, H)], wo_sem.at[v])

    def ev_lb(*vs):
        for v in vs:
            with scope(f'lb{v}'):
                lb_z(v).wait_recv()
            lb_core(v).start()

    wo = xp.at[1 - side]

    def wo_own():
        return [pltpu.make_async_copy(wout_ref.at[pl.ds(r * B, B), pl.ds(c * H, H)], xp.at[1 - side, r, :, ds((c ^ tp ^ 2) * H, H)], wo_sem.at[4])
                for r in TWO for c in range(4)]

    def wo_load(*vs):
        out = []
        for v in vs:
            cols = pl.ds((v ^ 2) * H, H)
            for s, m in enumerate(SLOT):
                row = (idx ^ m) * 64
                for b in TWO:
                    out.append(pltpu.make_async_copy(lo_ref.at[v, s, b], xp.at[1 - side, 4 + 2 * b + row // B, ds(row % B, 64, 64), cols], wo_sem.at[v]))
            for r in TWO:
                out.append(pltpu.make_async_copy(lb_ref.at[v, r], xp.at[1 - side, 2 + r, :, cols], wo_sem.at[v]))
        return out

    def kvp_copy(h, s):
        return remote(kv_s.at[h, pl.ds(8 * s, 2)], kvp_s.at[h, pl.ds(2 * s, 2)], sent.at[4], kv_recv.at[0, h], peer_c)

    def kvr_copy(h, s):
        return remote(kv_s.at[h, 8 * s], kvr_s.at[h, s], sent.at[5], kv_recv.at[1, h], peer_y)

    def kvf_copy(h, s):
        return remote(kvr_s.at[h, s], kvr_s.at[h, 2 + s], sent.at[6], kv_recv.at[2, h], peer_c)

    def kv_start(copy, heads):
        for h in heads:
            for s in TWO:
                copy(h, s).start()

    def kv_wait(copy, heads):
        with scope(f'w_{copy.__name__}{heads[0]}'):
            for h in heads:
                i = (kvp_copy, kvr_copy, kvf_copy).index(copy)
                arrived((kvp_s.at[h], kvr_s.at[h, pl.ds(0, 2)], kvr_s.at[h, pl.ds(2, 2)])[i], kv_recv.at[i, h])

    def kv_forward(heads):
        kv_wait(kvr_copy, heads)
        kv_start(kvf_copy, heads)

    def reverse(i):
        return (i % 2) * 2 + i // 2

    def order(n):
        return 2 * reverse(n % 4) + ((n // 4) ^ side)

    def o_at(k, p, theirs, col, size):
        return ws.at[1 + theirs, ds(k * B, B), ds(col, size)] if p else xb.at[k // 2, :, ds((k % 2) * 1024 + theirs * H + col, size)]

    def o_copy(k, p):
        return remote(o_at(k, p, 0, 0, H), o_at(k, p, 1, 0, H), sent.at[7], o_recv.at[k], {'tp': tp ^ 1})

    def o_times(k, v, n):
        cols = pl.ds((v ^ 2) * H, n * H)
        y = nn(xb[k // 2, :, ds((k % 2) * 1024, 1024)], wo[0:4, :, cols].reshape(1024, n * H))
        for i in TWO:
            y = y + nn(ws[1 + i, ds(k * B, B), :], wo[part(2 + i, 2), :, cols].reshape(H, n * H))
        y = y.astype(BF)
        for i in range(n):
            y_src(k, v + i)[...] = y[:, part(i, H)]
            y_copy(k, v + i, side).start() if v else y_local(k).start()

    def y_src(k, v):
        return xp.at[side, k, :, pl.ds(v * H, H)]

    def y_copy(k, v, seg):
        return remote(y_src(k, v), out_ref.at[seg, k], sent.at[8], y_recv.at[seg], {'tp': tp ^ v})

    def y_local(k):
        return pltpu.make_async_copy(y_src(k, 0), out_ref.at[side, k], sent.at[9])

    def x_copy(j):
        return pltpu.make_async_copy(x_ref.at[ds(j * B, B), :], xb.at[lax.rem(j, 4)], x_sem.at[lax.rem(j, 4)])

    for j in range(4):
        x_copy(j).start()
    barrier = pltpu.get_barrier_semaphore()
    peers = [{'tp': tp ^ 1}, {'tp': tp ^ 2}, {'tp': tp ^ 3}, peer_x, peer_y, peer_c]
    for dev in peers:
        pl.semaphore_signal(barrier, inc=1, device_id=dev, device_id_type=MESH)
    for t in range(3):
        own_load(t).start()

    pm[...] = phase_matrix(False)

    def permute_body(j, carry):
        x_copy(j).wait()
        y = nn(pm[...], xb[lax.rem(j, 4)]).astype(BF).reshape(8, 32, M)
        xp[j // 8, :, ds(lax.rem(j, 8) * 32, 32, 32), :] = y
        pl.when(j < 12)(lambda: x_copy(j + 4).start())

        @pl.when(j == 7)
        def _():
            with scope('barrier'):
                pl.semaphore_wait(barrier, len(peers))
            lq_start(KEY)
        return carry

    with scope('permute'):
        lax.fori_loop(0, 16, permute_body, None)

    for h in HEADS:
        column = 2 * (tp ^ (h // 2 * 2)) + h % 2
        for i, branches in enumerate(('0', '01', '1', '012', '12', '2', '0123', '123', '23', '3')):
            rows = [jnp.full((1, 128), bias_ref[j, column], F32) for j in map(int, branches)]
            m = functools.reduce(jnp.maximum, rows)
            beta_s[pl.ds(h * 16 + i, 1), :] = (m + jnp.log(sum(jnp.exp(r - m) for r in rows))) * math.log2(math.e)

    def signal_ready(i):
        pl.when(inner)(lambda: pl.semaphore_signal(ready.at[i], inc=1, device_id={'tp': tp ^ 1}, device_id_type=MESH))

    def wait_ready(i):
        with scope(f'ready{i}'):
            pl.when(outer)(lambda: pl.semaphore_wait(ready.at[i], 1))

    signal_ready(0)

    def group(g):
        low = g < 4
        return jnp.where(low, g & 1, 0), jnp.where(low, g // 2, g - 2)

    def head_number(h):
        return 2 * (tp ^ (h // 2 * 2)) + h % 2

    def project(heads, sigma, pair, kinds):
        for h in heads:
            t = head_number(h) + reverse(pair)
            x, swap = xp[side ^ sigma, pl.ds(2 * (t & 3), 2)].reshape(H, M), (t & 7) >> 2
            for t in kinds:
                y = nn(x, ws[t, :, part(h % 2, B)])
                for j in TWO:
                    piece = y[part(j, B)]
                    kv_s[h, 8 * sigma + 2 * pair + (j ^ swap), t] = (piece.T if t == VAL else piece).astype(BF)

    def phases_of(j):
        return [j % 2 + 2 * i for i in TWO], (j // 2) ^ side

    def rank_of(phase, h):
        rel = (phase - head_number(h)) & 7
        return (rel & 1) * 4 + ((rel >> 1) & 1) * 2 + (rel >> 2)

    def queries(heads, w, j):
        phases, half = phases_of(j)
        x = jnp.concatenate([xp[side, 2 * f + half] for f in phases])
        for h in heads:
            y = nn(x, ws[w, :, part(h % 2, B)]).astype(BF)
            for i, f in enumerate(phases):
                q_s[h, rank_of(f + 4 * half, h)] = y[part(i, B)]

    with scope('own_w'):
        for t in range(3):
            own_load(t).wait()
    own, partner = HEADS[:2], HEADS[2:]

    def mix(b, c):
        return jnp.concatenate([b, b, c, c], axis=1)

    def keys_of(ref, h, i, weights):
        parts = []
        n = 0
        for count, b in weights:
            def values(i=i + n, count=count):
                v = [ref[h, i + j, VAL] for j in range(count)]
                return v[0] if count == 1 else jnp.concatenate(v, axis=1)
            parts.append((values, count * B, b))
            n += count
        return (lambda: ref[h, i:i + n, KEY].reshape(n * B, B)), parts

    def chunk_tiles(p, j, kind):
        both_phases, half = phases_of(j)

        def put(h, phase, ot):
            k = 2 * (phase & 3) + half
            y = ot.T.astype(BF)
            for i in TWO:
                pl.when(p == i)(lambda i=i: o_at(k, i, 0, (h % 2) * B, B).__setitem__(..., y))

        def tile(h, phases, ranks, wide, narrow, s_ref, n_ref):
            def done(ot):
                for i, phase in enumerate(phases):
                    put(h, phase, ot[:, part(i, B)])
            return tile_steps(lambda: jnp.concatenate([q_s[h, r] for r in ranks]), wide, narrow, s_ref, n_ref, done)

        h = 2 * p + (j % 2) ^ 1
        rest = tile(h, both_phases, [rank_of(f + 4 * half, h) for f in both_phases], [keys_of(kv_s, h, i, [(2, None)]) for i in range(0, 8, 2)], [], t_scr, None)
        h = 2 * p + (j % 2)
        a = head_number(h)
        b0, b01, b1, b012, b12, b2, b0123, b123, b23, b3 = [beta_s[pl.ds(h * 16 + i, 1), :] for i in range(10)]
        phases = [a & 3, (a & 3) ^ 2]
        both = [keys_of(kv_s, h, i, [(2, b)]) for i, b in ((2, b01), (4, b0), (6, b0), (10, b1))]
        if kind == 0:
            both += [keys_of(kv_s, h, 0, [(1, mix(b0123, b01)), (1, mix(b012, b01))]), keys_of(kv_s, h, 8, [(1, mix(b123, b1)), (1, mix(b12, b1))])]
            first = [keys_of(kvp_s, h, i, [(1, b23), (1, b2)]) for i in (0, 2)] + [keys_of(kvr_s, h, i, [(2, b3)]) for i in (0, 2)]
        else:
            both += [keys_of(kv_s, h, 0, [(2, mix(b012, b01))]), keys_of(kv_s, h, 8, [(2, mix(b12, b1))])]
            first = [keys_of(kvp_s, h, i, [(2, b2)]) for i in (0, 2)]
        with scope(f'tile{kind}'):
            run_tiles([rest, tile(h, phases, [kind, rank_of(phases[1] + 4 * half, h)], both, first, s_scr, t_scr.at[:, pl.ds(0, B)])])

    def send_o(ks, p):
        @pl.when(outer)
        def _():
            for k in ks:
                o_copy(order(k), p).start()

    def step_body(t, carry):
        packed = functools.reduce(lambda x, i: jnp.where(t == i, TABLE[i], x), range(len(TABLE)), 0)
        code, n, event = packed % 16, packed // 16 % 16, packed // 256

        def step_o():
            with scope('own_kv'):
                project(own, *group(n), (KEY, VAL))

        def step_kv(t_):
            with scope(f'par_{t_}'):
                for i in TWO:
                    project(partner, *group(2 * n + i), (t_,))

        def step_q(heads, w):
            with scope(f'que_{w}'):
                queries(heads, w, n)

        def step_out(v, m):
            @pl.when(inner)
            def _():
                k = order(n)
                if m == 2:
                    with scope('wait_o'):
                        arrived(ws.at[0, pl.ds(0, H), :], o_recv.at[k])
                with scope(f'out{v}'):
                    o_times(k, v, m)

        f = functools.partial
        kinds = {'-': lambda: None, 'O': step_o, 'P': f(step_q, own, QUE), 'K': f(step_kv, KEY), 'V': f(step_kv, VAL), 'Q': f(step_q, partner, KEY),
                 'A': lambda: chunk_tiles(n // 4, n % 4, 0), 'B': lambda: chunk_tiles(n // 4, n % 4, 1), 'R': f(step_out, 2, 2), 'L': f(step_out, 1, 1), 'N': f(step_out, 0, 1)}
        choose(code, [kinds[c] for c in KINDS])
        call = functools.partial

        events = {
            'free': [call(signal_ready, 1), call(on, inner, lambda: start(wo_own()))],
            'r0': [call(wait_ready, 0)],
            'r1': [call(wait_ready, 1)],
            'so': [call(kv_start, kvp_copy, own)],
            'po': [call(kv_wait, kvp_copy, own)],
            'sp': [call(kv_start, kvp_copy, partner)],
            'pp': [call(kv_wait, kvp_copy, partner)],
        }
        for t_, c in enumerate('kvq'):
            events['b' + c] = [call(lq_start, t_)]
            events['l' + c] = [call(ev_last, t_)]
            events['w' + c] = [call(ev_weights, t_)]
            for i in TWO:
                for e, f in zip('zxy', (ev_z, ev_xy, ev_y)):
                    events[f'{e}{c}{i}'] = [call(f, lq_copy, 2 * t_ + i)]
        for i, vs in enumerate(((2, 3), (1,), (0,))):
            events[f'b{i}'] = [call(lo_start, *vs)]
            for e, f in zip('zxycwv', (call(ev_z, lo_copy), call(ev_xy, lo_copy), call(ev_y, lo_copy), ev_lb, ev_wo, ev_wo_ready)):
                events[f'{e}{i}'] = [call(on, inner, call(f, *vs))]
        events['v0'] += [call(on, inner, lambda: local(xp.at[1 - side, pl.ds(0, 2)], wo_sem.at[4]))]
        for v in range(4):
            events[f'd{v}'] = [call(on, outer, lambda v=v: lb_z(v).start())]
        for h in HEADS:
            for z in TWO:
                events[f's{h}{z}'] = [kvr_copy(h, z).start]
            events[f'f{h}'] = [call(kv_forward, [h])]
            events[f'g{h}'] = [call(kv_wait, kvf_copy, [h])]
        for k in ROWS:
            for p in TWO:
                events['op'[p] + str(k)] = [call(send_o, (k,), p)]
        def run(names):
            for name in names.split(','):
                where, _, name = name.rpartition(':')
                if where:
                    on(inner if where == 'i' else outer, *events[name])
                else:
                    for c in events[name]:
                        c()

        @pl.when(event > 0)
        def _():
            choose(event - 1, [functools.partial(run, names) for names in EVENTS])
        return carry

    lax.fori_loop(0, len(TABLE), step_body, None)

    all_sent(lq_ref, 0)
    all_sent(lo_ref.at[:, 0, 0], 2)
    all_sent(lb_ref.at[:, 0], 3)
    all_sent(kvp_s, 4)
    all_sent(kvr_s.at[:, pl.ds(0, 2)], 5)
    all_sent(kvr_s.at[:, pl.ds(0, 2)], 6)

    @pl.when(outer)
    def _():
        all_sent(xb, 7)

    @pl.when(inner)
    def _():
        all_sent(lo_ref.at[:, pl.ds(0, 7)], 1)
        with scope('y_sent'):
            all_sent(xp.at[side, :, :, pl.ds(H, 3 * H)], 8)
        local(xp.at[side, :, :, pl.ds(0, H)], sent.at[9])

    for seg in TWO:
        @pl.when(tp != 1 + seg)
        def _(seg=seg):
            with scope(f'recv{seg}'):
                arrived(out_ref.at[seg], y_recv.at[seg])


PROGRAM = (
    'O.i:zk0,i:zk1', 'O.bv,o:zk0,so', 'O.o:zk1,s00,i:xk0', 'O.o:xk0,i:xk1,s01,d2', 'O.i:yk0,i:zv0', 'O.bq,o:xk1,o:yk0,i:yk1,i:zv1', 'P.i:xv0',
    'P.o:yk1,lk,o:zv0,d3', 'P.wk,o:zv1', 'K.i:xv1,i:zq0', 'K.o:xv0,f0,i:zq1,d1', 'K.o:xv1,o:zq0,o:zq1,i:yv0,i:yv1,b0,b1,r0,po,g0',
    'T0.o0,d0,o:yv0,o:yv1,lv,wv,i:xq0,i:xq1', 'V.o:xq0,o:xq1,z0,o:s10,o:s11', 'V.i:yq0,c0,z1', 'V.i:yq1,o:yq0,o:yq1,sp,lq,o:s20,o:s21',
    'P.free,x0,wq,c1', 'Q.pp,r1,o:s30,o:s31', 'T4.p0,o1,p1,x1', 'Q.y0,i:s10,i:s11,w0', 'T5.p2,p3,v0,y1,w1,o:f1', 'R', 'Q.v1', 'L', 'R', 'L',
    'Q.i:f1,o:g1,i:s20,i:s21,b2', 'T2.i:g1,o:f2', 'T1.o2,o3,o:g2,o:f3', 'R.i:s30,i:s31', 'L.i:f2', 'R', 'L.i:g2', 'T6.p4,o4,p5,o5,o:g3', 'R',
    'T3.i:f3,z2,c2', 'L.i:g3', 'T7.p6,o6,p7,o7', 'R.x2', 'L', 'R.y2', 'L.w2', '-.v2', 'N', 'N', 'N', 'N', 'R', 'L', 'N', 'N', 'N', 'N',
)
KINDS = '-OPKVQABRLN'


def tables():
    table, seen = [], {}
    names = tuple(dict.fromkeys(s.partition('.')[2] for s in PROGRAM if '.' in s))
    for s in PROGRAM:
        name, _, after = s.partition('.')
        kind, n = name[0], seen.get(name[0], 0)
        seen[kind] = n + 1
        if kind == 'T':
            n = int(name[1:])
            kind = 'AB'[n in (2, 3, 4, 5)]
        table.append(KINDS.index(kind) + 16 * n + 256 * (names.index(after) + 1 if after else 0))
    return table, names


TABLE, EVENTS = tables()


def main(bias, x, wk, wv, wq, w_out):
    anyspec = pl.BlockSpec(memory_space=pl.ANY)
    vmem = [((4, B, M), BF), ((B, B), BF), ((2, 8, B, M), BF), ((3, M, H), BF), ((4, 8, B, B), BF), ((4, 12, 2, B, B), BF), ((4, 4, 2, B, B), BF), ((4, 4, 2, B, B), BF),
            ((3072, H), F32), ((M, H), F32), ((64, 128), F32)]
    dma = [(4,), (9,), (5,), (10,), (6, 5), (4, 5), (4, 2), (3, 4), (8,), (2,)]
    return pl.pallas_call(
        main_kernel,
        in_specs=[pl.BlockSpec(memory_space=pltpu.SMEM)] + [anyspec] * 5,
        out_specs=[anyspec] * 4,
        out_shape=[jax.ShapeDtypeStruct(s, BF) for s in ((2, 8, B, H), (8, 6, B, B), (4, 8, 2, 64, H), (4, 2, B, H))],
        scratch_shapes=[pltpu.VMEM(*v) for v in vmem] + [pltpu.SemaphoreType.DMA(d) for d in dma] + [pltpu.SemaphoreType.REGULAR((2,))],
        compiler_params=params(collective_id=0, has_side_effects=True),
        cost_estimate=pl.CostEstimate(flops=10**11, bytes_accessed=10**8, transcendentals=0),
        name='main',
    )(bias, x, wk, wv, wq, w_out)[0]


def solution(mesh):
    def device_fn(hidden, w_query, w_key, w_value, w_out, branch_bias):
        return unpermute(main(branch_bias, hidden, w_key, w_value, w_query, w_out))

    return jax.shard_map(device_fn, mesh=mesh, in_specs=(P(('dp', 'sp'), None), P(None, 'tp'), P(None, 'tp'), P(None, 'tp'), P('tp', None), P(None, None)), out_specs=P(('dp', 'sp'), 'tp'), check_vma=False)
```

```python
import functools
import math

import jax
import jax.numpy as jnp
from jax import lax
from jax.experimental import pallas as pl
from jax.experimental.pallas import tpu as pltpu
from jax.sharding import PartitionSpec as P

MESH = pl.DeviceIdType.MESH
BF = jnp.bfloat16
F32 = jnp.float32
B, H, M = 256, 512, 2048
KAPPA = math.log2(math.e) / 16
VMEM = 66_900_000
SLOT = (0, 4, 2, 6, 1, 5, 3, 7)
KEY, VAL, QUE = range(3)
HEADS = range(4)
TWO = range(2)
ROWS = range(8)


def nn(a, b):
    return lax.dot_general(a, b, (((1,), (0,)), ((), ())), preferred_element_type=F32)


def nt(a, b):
    return lax.dot_general(a, b, (((1,), (1,)), ((), ())), preferred_element_type=F32)


def params(**kw):
    return pltpu.CompilerParams(vmem_limit_bytes=VMEM, **kw)


def ds(start, size, align=128):
    return pl.ds(pl.multiple_of(start, align), size)


def part(i, size):
    return slice(i * size, i * size + size)


def phase_matrix(transposed):
    r = lax.broadcasted_iota(jnp.int32, (B, B), int(transposed))
    p = lax.broadcasted_iota(jnp.int32, (B, B), int(not transposed))
    k = r // 32
    return (p == (r % 32) * 8 + k // 2 + 4 * (k % 2)).astype(F32).astype(BF)


def unpermute_kernel(y_ref, o_ref, y_s, o_s, load, store):
    pieces = [(s, j) for s in TWO for j in range(4)]

    def get(i):
        s, j = pieces[i]
        return pltpu.make_async_copy(y_ref.at[s, :, pl.ds(j * 64, 64)], y_s.at[i], load.at[i])

    def put(i):
        return pltpu.make_async_copy(o_s.at[i], o_ref.at[pl.ds(i * H, H)], store.at[i])

    for i in ROWS:
        get(i).start()
    pm = phase_matrix(True)
    for i in ROWS:
        get(i).wait()
        for j in TWO:
            o_s[i, part(j, B), :] = nn(pm, y_s[i, :, part(j, 32), :].reshape(B, H)).astype(BF)
        put(i).start()
    for i in ROWS:
        put(i).wait()


def unpermute(y):
    anyspec = pl.BlockSpec(memory_space=pl.ANY)
    return pl.pallas_call(
        unpermute_kernel,
        in_specs=[anyspec],
        out_specs=anyspec,
        out_shape=jax.ShapeDtypeStruct((2 * M, H), BF),
        scratch_shapes=[pltpu.VMEM((8, 8, 64, H), BF), pltpu.VMEM((8, H, H), BF), pltpu.SemaphoreType.DMA((8,)), pltpu.SemaphoreType.DMA((8,))],
        compiler_params=params(),
        name='unpermute',
    )(y)


def tile_steps(q, wide, narrow, s_ref, n_ref, done):
    st = {}
    logits, sums = [], []

    def add(name, x):
        st[name] = st[name] + x if name in st else x

    for groups, ref in ((wide, s_ref), (narrow, n_ref)):
        off = 0
        for keys, parts in groups:
            def qk(keys=keys, parts=parts, off=off, ref=ref):
                s = nt(keys(), q() if ref is s_ref else q()[:B])
                o = 0
                for _, n, b in parts:
                    piece = s[o:o + n]
                    ref[pl.ds(off + o, n), :] = piece
                    t = jnp.max(piece, axis=0, keepdims=True) * KAPPA
                    if b is not None:
                        t = t + fit(b, t)
                    if ref is n_ref:
                        t = jnp.concatenate([t, st['top'][:, B:]], axis=1)
                    st['top'] = jnp.maximum(st['top'], t) if 'top' in st else t
                    o += n
            logits.append(qk)
            for v, n, b in parts:
                def sv(v=v, n=n, b=b, off=off, ref=ref):
                    top = st['top'] if ref is s_ref else st['top'][:, :B]
                    e = jnp.exp2(ref[pl.ds(off, n), :] * KAPPA - (top if b is None else top - fit(b, top)))
                    name = 'w' if ref is s_ref else 'n'
                    add('l' + name, jnp.sum(e, axis=0, keepdims=True))
                    add('o' + name, nn(v(), e.astype(BF)))
                sums.append(sv)
                off += n

    def finish():
        o, l = st['ow'], st['lw']
        if narrow:
            o = jnp.concatenate([o[:, :B] + st['on'], o[:, B:]], axis=1)
            l = jnp.concatenate([l[:, :B] + st['ln'], l[:, B:]], axis=1)
        done(o / l)

    return logits, sums + [finish]


def fit(b, like):
    return b if b.shape == like.shape else jnp.concatenate([b] * (like.shape[1] // 128), axis=1)


def interleave(a, b):
    i = j = 0
    while i < len(a) or j < len(b):
        if j >= len(b) or (i < len(a) and i * len(b) <= j * len(a)):
            a[i]()
            i += 1
        else:
            b[j]()
            j += 1


def run_tiles(tiles):
    before = []
    for logits, sums in tiles:
        interleave(logits, before)
        before = sums
    interleave([], before)


def choose(x, cases):
    def among(lo, hi):
        mid = (lo + hi) // 2
        if hi - lo == 1:
            cases[lo]()
        else:
            pl.when(x < mid)(lambda: among(lo, mid))
            pl.when(x >= mid)(lambda: among(mid, hi))
    among(0, len(cases))


def on(cond, *calls):
    @pl.when(cond)
    def _():
        for c in calls:
            c()


def scope(name):
    return jax.named_scope(name)


def main_kernel(bias_ref, x_ref, wk_ref, wv_ref, wq_ref, wout_ref, out_ref, lq_ref, lo_ref, lb_ref,
                xb, pm, xp, ws, q_s, kv_s, kvp_s, kvr_s, s_scr, t_scr,
                beta_s, x_sem, w_sem, wo_sem, sent, lq_recv, lo_recv, lb_recv, kv_recv, o_recv, y_recv, ready):
    dp, tp, sp = lax.axis_index('dp'), lax.axis_index('tp'), lax.axis_index('sp')
    idx = dp * 4 + sp
    side = tp // 2
    inner = (tp == 1) | (tp == 2)
    outer = jnp.logical_not(inner)
    W = (wk_ref, wv_ref, wq_ref)
    peer_x, peer_y, peer_c = {'dp': dp ^ 1}, {'sp': sp ^ 2}, {'sp': sp ^ 1}

    def remote(src, dst, ss, rs, dev):
        return pltpu.make_async_remote_copy(src_ref=src, dst_ref=dst, send_sem=ss, recv_sem=rs, device_id=dev, device_id_type=MESH)

    def lq_copy(t, src, dst, dev):
        return remote(lq_ref.at[src, t], lq_ref.at[dst, t], sent.at[0], lq_recv.at[t, min(dst, 4)], dev)

    def lq_z(t):
        return remote(W[t // 2].at[ds(idx * B, B), pl.ds(t % 2 * B, B)], lq_ref.at[0, t], sent.at[0], lq_recv.at[t, 0], {'tp': tp ^ 2})

    def lq_start(t):
        for i in TWO:
            lq_z(2 * t + i).start()

    def lo_copy(v, src, dst, dev):
        return remote(lo_ref.at[v, src], lo_ref.at[v, dst], sent.at[1], lo_recv.at[v, min(dst, 4)], dev)

    def lo_z(v):
        dst = 2 - side
        b = (tp ^ dst) - 2
        return remote(wout_ref.at[ds(idx * 64, 64, 64), ds((dst ^ v) * H, H)], lo_ref.at[v, 0, b], sent.at[2], lo_recv.at[v, 0], {'tp': dst})

    def lb_z(v):
        return remote(wout_ref.at[ds(sp % 2 * B, B), ds((tp ^ 1 ^ v) * H, H)], lb_ref.at[v, sp % 2], sent.at[3], lb_recv.at[v, 0], {'tp': tp ^ 1})

    def lb_core(v):
        return remote(lb_ref.at[v, sp % 2], lb_ref.at[v, sp % 2], sent.at[3], lb_recv.at[v, 1], peer_c)

    def lo_start(*vs):
        for v in vs:
            lo_z(v).start()

    def arrived(ref, sem):
        remote(ref, ref, sent.at[0], sem, peer_c).wait_recv()

    def all_sent(ref, i):
        remote(ref, ref, sent.at[i], sent.at[i], peer_c).wait_send()

    def lo_zwait(v):
        arrived(lo_ref.at[v, 0], lo_recv.at[v, 0])

    def hop(copy, p, i):
        near, far = (peer_y, peer_x) if copy is lq_copy else (peer_x, peer_y)
        n, f = (2, 1) if near is peer_y else (1, 2)
        return copy(p, *((0, n, near), (0, f, far), (0, 4, peer_c), (n, 3, far), (n, 4 + n, peer_c), (f, 4 + f, peer_c), (3, 7, peer_c))[i])

    def ev_z(copy, *ps):
        for p in ps:
            with scope(f'z_{copy.__name__}{p}'):
                lq_z(p).wait_recv() if copy is lq_copy else lo_zwait(p)
            for i in range(3):
                hop(copy, p, i).start()

    def ev_xy(copy, *ps):
        for p in ps:
            with scope(f'n_{copy.__name__}{p}'):
                hop(copy, p, 0).wait_recv()
            hop(copy, p, 3).start()
            hop(copy, p, 4).start()
        for p in ps:
            with scope(f'f_{copy.__name__}{p}'):
                hop(copy, p, 1).wait_recv()
            hop(copy, p, 5).start()

    def ev_y(copy, *ps):
        for p in ps:
            with scope(f'y_{copy.__name__}{p}'):
                hop(copy, p, 3).wait_recv()
            hop(copy, p, 6).start()
            if copy is lq_copy and p >= 2:
                start(w_load(p, SLOT[:4]))

    def ev_done(copy, *ps):
        for p in ps:
            with scope(f'c_{copy.__name__}{p}'):
                if copy is lq_copy:
                    arrived(lq_ref.at[pl.ds(4, 4), p], lq_recv.at[p, 4])
                else:
                    arrived(lo_ref.at[p, pl.ds(4, 4)], lo_recv.at[p, 4])

    def w_load(p, slots):
        return [pltpu.make_async_copy(lq_ref.at[SLOT.index(m), p], ws.at[p // 2 % 2, ds((idx ^ m) * B, B), pl.ds(p % 2 * B, B)], w_sem.at[p]) for m in slots]

    def own_load(t):
        return pltpu.make_async_copy(W[t], ws.at[t], w_sem.at[6 + t])

    def start(copies):
        for c in copies:
            c.start()

    def wait(copies):
        for c in copies:
            c.wait()

    def ev_last(t):
        pieces = [2 * t + i for i in TWO]
        ev_done(lq_copy, *pieces)
        for p in pieces:
            start(w_load(p, SLOT[4:] if t else SLOT))

    def local(ref, sem):
        pltpu.make_async_copy(ref, ref, sem).wait()

    def ev_weights(t):
        with scope(f'load{t}'):
            for i in TWO:
                local(ws.at[t % 2, :, pl.ds(i * B, B)], w_sem.at[2 * t + i])

    def ev_wo(*vs):
        ev_done(lo_copy, *vs)
        for v in vs:
            lb_core(v).wait_recv()
        start(wo_load(*vs))

    def ev_wo_ready(*vs):
        with scope(f'wo{vs[0]}'):
            for v in vs:
                local(xp.at[1 - side, pl.ds(2, 6), :, pl.ds((v ^ 2) * H, H)], wo_sem.at[v])

    def ev_lb(*vs):
        for v in vs:
            with scope(f'lb{v}'):
                lb_z(v).wait_recv()
            lb_core(v).start()

    wo = xp.at[1 - side]

    def wo_own():
        return [pltpu.make_async_copy(wout_ref.at[pl.ds(r * B, B), pl.ds(c * H, H)], xp.at[1 - side, r, :, ds((c ^ tp ^ 2) * H, H)], wo_sem.at[4])
                for r in TWO for c in range(4)]

    def wo_load(*vs):
        out = []
        for v in vs:
            cols = pl.ds((v ^ 2) * H, H)
            for s, m in enumerate(SLOT):
                row = (idx ^ m) * 64
                for b in TWO:
                    out.append(pltpu.make_async_copy(lo_ref.at[v, s, b], xp.at[1 - side, 4 + 2 * b + row // B, ds(row % B, 64, 64), cols], wo_sem.at[v]))
            for r in TWO:
                out.append(pltpu.make_async_copy(lb_ref.at[v, r], xp.at[1 - side, 2 + r, :, cols], wo_sem.at[v]))
        return out

    def kvp_copy(h, s):
        return remote(kv_s.at[h, pl.ds(8 * s, 2)], kvp_s.at[h, pl.ds(2 * s, 2)], sent.at[4], kv_recv.at[0, h], peer_c)

    def kvr_copy(h, s):
        return remote(kv_s.at[h, 8 * s], kvr_s.at[h, s], sent.at[5], kv_recv.at[1, h], peer_y)

    def kvf_copy(h, s):
        return remote(kvr_s.at[h, s], kvr_s.at[h, 2 + s], sent.at[6], kv_recv.at[2, h], peer_c)

    def kv_start(copy, heads):
        for h in heads:
            for s in TWO:
                copy(h, s).start()

    def kv_wait(copy, heads):
        with scope(f'w_{copy.__name__}{heads[0]}'):
            for h in heads:
                i = (kvp_copy, kvr_copy, kvf_copy).index(copy)
                arrived((kvp_s.at[h], kvr_s.at[h, pl.ds(0, 2)], kvr_s.at[h, pl.ds(2, 2)])[i], kv_recv.at[i, h])

    def kv_forward(heads):
        kv_wait(kvr_copy, heads)
        kv_start(kvf_copy, heads)

    def reverse(i):
        return (i % 2) * 2 + i // 2

    def order(n):
        return 2 * reverse(n % 4) + ((n // 4) ^ side)

    def o_at(k, p, theirs, col, size):
        return ws.at[1 + theirs, ds(k * B, B), ds(col, size)] if p else xb.at[k // 2, :, ds((k % 2) * 1024 + theirs * H + col, size)]

    def o_copy(k, p):
        return remote(o_at(k, p, 0, 0, H), o_at(k, p, 1, 0, H), sent.at[7], o_recv.at[k], {'tp': tp ^ 1})

    def o_times(k, v, n):
        cols = pl.ds((v ^ 2) * H, n * H)
        y = nn(xb[k // 2, :, ds((k % 2) * 1024, 1024)], wo[0:4, :, cols].reshape(1024, n * H))
        for i in TWO:
            y = y + nn(ws[1 + i, ds(k * B, B), :], wo[part(2 + i, 2), :, cols].reshape(H, n * H))
        y = y.astype(BF)
        for i in range(n):
            y_src(k, v + i)[...] = y[:, part(i, H)]
            y_copy(k, v + i, side).start() if v else y_local(k).start()

    def y_src(k, v):
        return xp.at[side, k, :, pl.ds(v * H, H)]

    def y_copy(k, v, seg):
        return remote(y_src(k, v), out_ref.at[seg, k], sent.at[8], y_recv.at[seg], {'tp': tp ^ v})

    def y_local(k):
        return pltpu.make_async_copy(y_src(k, 0), out_ref.at[side, k], sent.at[9])

    def x_copy(j):
        return pltpu.make_async_copy(x_ref.at[ds(j * B, B), :], xb.at[lax.rem(j, 4)], x_sem.at[lax.rem(j, 4)])

    for j in range(4):
        x_copy(j).start()
    barrier = pltpu.get_barrier_semaphore()
    peers = [{'tp': tp ^ 1}, {'tp': tp ^ 2}, {'tp': tp ^ 3}, peer_x, peer_y, peer_c]
    for dev in peers:
        pl.semaphore_signal(barrier, inc=1, device_id=dev, device_id_type=MESH)
    for t in range(3):
        own_load(t).start()

    pm[...] = phase_matrix(False)

    def permute_body(j, carry):
        x_copy(j).wait()
        y = nn(pm[...], xb[lax.rem(j, 4)]).astype(BF).reshape(8, 32, M)
        xp[j // 8, :, ds(lax.rem(j, 8) * 32, 32, 32), :] = y
        pl.when(j < 12)(lambda: x_copy(j + 4).start())

        @pl.when(j == 7)
        def _():
            with scope('barrier'):
                pl.semaphore_wait(barrier, len(peers))
            lq_start(KEY)
            on(outer, lb_z(2).start)
        return carry

    with scope('permute'):
        lax.fori_loop(0, 16, permute_body, None)

    for h in HEADS:
        column = 2 * (tp ^ (h // 2 * 2)) + h % 2
        for i, branches in enumerate(('0', '01', '1', '012', '12', '2', '0123', '123', '23', '3')):
            rows = [jnp.full((1, 128), bias_ref[j, column], F32) for j in map(int, branches)]
            m = functools.reduce(jnp.maximum, rows)
            beta_s[pl.ds(h * 16 + i, 1), :] = (m + jnp.log(sum(jnp.exp(r - m) for r in rows))) * math.log2(math.e)

    def signal_ready(i):
        pl.when(inner)(lambda: pl.semaphore_signal(ready.at[i], inc=1, device_id={'tp': tp ^ 1}, device_id_type=MESH))

    def wait_ready(i):
        with scope(f'ready{i}'):
            pl.when(outer)(lambda: pl.semaphore_wait(ready.at[i], 1))

    signal_ready(0)

    def group(g):
        low = g < 4
        return jnp.where(low, g & 1, 0), jnp.where(low, g // 2, g - 2)

    def head_number(h):
        return 2 * (tp ^ (h // 2 * 2)) + h % 2

    def project(heads, sigma, pair, kinds):
        for h in heads:
            t = head_number(h) + reverse(pair)
            x, swap = xp[side ^ sigma, pl.ds(2 * (t & 3), 2)].reshape(H, M), (t & 7) >> 2
            for t in kinds:
                y = nn(x, ws[t, :, part(h % 2, B)])
                for j in TWO:
                    piece = y[part(j, B)]
                    kv_s[h, 8 * sigma + 2 * pair + (j ^ swap), t] = (piece.T if t == VAL else piece).astype(BF)

    def phases_of(j):
        return [j % 2 + 2 * i for i in TWO], (j // 2) ^ side

    def rank_of(phase, h):
        rel = (phase - head_number(h)) & 7
        return (rel & 1) * 4 + ((rel >> 1) & 1) * 2 + (rel >> 2)

    def queries(heads, w, j):
        phases, half = phases_of(j)
        x = jnp.concatenate([xp[side, 2 * f + half] for f in phases])
        for h in heads:
            y = nn(x, ws[w, :, part(h % 2, B)]).astype(BF)
            for i, f in enumerate(phases):
                q_s[h, rank_of(f + 4 * half, h)] = y[part(i, B)]

    with scope('own_w'):
        for t in range(3):
            own_load(t).wait()
    own, partner = HEADS[:2], HEADS[2:]

    def mix(b, c):
        return jnp.concatenate([b, b, c, c], axis=1)

    def keys_of(ref, h, i, weights):
        parts = []
        n = 0
        for count, b in weights:
            def values(i=i + n, count=count):
                v = [ref[h, i + j, VAL] for j in range(count)]
                return v[0] if count == 1 else jnp.concatenate(v, axis=1)
            parts.append((values, count * B, b))
            n += count
        return (lambda: ref[h, i:i + n, KEY].reshape(n * B, B)), parts

    def chunk_tiles(p, j, kind):
        both_phases, half = phases_of(j)

        def put(h, phase, ot):
            k = 2 * (phase & 3) + half
            y = ot.T.astype(BF)
            for i in TWO:
                pl.when(p == i)(lambda i=i: o_at(k, i, 0, (h % 2) * B, B).__setitem__(..., y))

        def tile(h, phases, ranks, wide, narrow, s_ref, n_ref):
            def done(ot):
                for i, phase in enumerate(phases):
                    put(h, phase, ot[:, part(i, B)])
            return tile_steps(lambda: jnp.concatenate([q_s[h, r] for r in ranks]), wide, narrow, s_ref, n_ref, done)

        h = 2 * p + (j % 2) ^ 1
        rest = tile(h, both_phases, [rank_of(f + 4 * half, h) for f in both_phases], [keys_of(kv_s, h, i, [(2, None)]) for i in range(0, 8, 2)], [], t_scr, None)
        h = 2 * p + (j % 2)
        a = head_number(h)
        b0, b01, b1, b012, b12, b2, b0123, b123, b23, b3 = [beta_s[pl.ds(h * 16 + i, 1), :] for i in range(10)]
        phases = [a & 3, (a & 3) ^ 2]
        both = [keys_of(kv_s, h, i, [(2, b)]) for i, b in ((2, b01), (4, b0), (6, b0), (10, b1))]
        if kind == 0:
            both += [keys_of(kv_s, h, 0, [(1, mix(b0123, b01)), (1, mix(b012, b01))]), keys_of(kv_s, h, 8, [(1, mix(b123, b1)), (1, mix(b12, b1))])]
            first = [keys_of(kvp_s, h, i, [(1, b23), (1, b2)]) for i in (0, 2)] + [keys_of(kvr_s, h, i, [(2, b3)]) for i in (0, 2)]
        else:
            both += [keys_of(kv_s, h, 0, [(2, mix(b012, b01))]), keys_of(kv_s, h, 8, [(2, mix(b12, b1))])]
            first = [keys_of(kvp_s, h, i, [(2, b2)]) for i in (0, 2)]
        with scope(f'tile{kind}'):
            run_tiles([rest, tile(h, phases, [kind, rank_of(phases[1] + 4 * half, h)], both, first, s_scr, t_scr.at[:, pl.ds(0, B)])])

    def send_o(ks, p):
        @pl.when(outer)
        def _():
            for k in ks:
                o_copy(order(k), p).start()

    def step_body(t, carry):
        packed = functools.reduce(lambda x, i: jnp.where(t == i, TABLE[i], x), range(len(TABLE)), 0)
        code, n, event = packed % 16, packed // 16 % 16, packed // 256

        def step_o():
            with scope('own_kv'):
                project(own, *group(n), (KEY, VAL))

        def step_kv(t_):
            with scope(f'par_{t_}'):
                for i in TWO:
                    project(partner, *group(2 * n + i), (t_,))

        def step_q(heads, w):
            with scope(f'que_{w}'):
                queries(heads, w, n)

        def step_out(v, m):
            @pl.when(inner)
            def _():
                k = order(n)
                if m == 2:
                    with scope('wait_o'):
                        arrived(ws.at[0, pl.ds(0, H), :], o_recv.at[k])
                with scope(f'out{v}'):
                    o_times(k, v, m)

        f = functools.partial
        kinds = {'-': lambda: None, 'O': step_o, 'P': f(step_q, own, QUE), 'K': f(step_kv, KEY), 'V': f(step_kv, VAL), 'Q': f(step_q, partner, KEY),
                 'A': lambda: chunk_tiles(n // 4, n % 4, 0), 'B': lambda: chunk_tiles(n // 4, n % 4, 1), 'R': f(step_out, 2, 2), 'L': f(step_out, 1, 1), 'N': f(step_out, 0, 1)}
        choose(code, [kinds[c] for c in KINDS])
        call = functools.partial

        events = {
            'free': [call(signal_ready, 1), call(on, inner, lambda: start(wo_own()))],
            'r0': [call(wait_ready, 0)],
            'r1': [call(wait_ready, 1)],
            'so': [call(kv_start, kvp_copy, own)],
            'po': [call(kv_wait, kvp_copy, own)],
            'sp': [call(kv_start, kvp_copy, partner)],
            'pp': [call(kv_wait, kvp_copy, partner)],
        }
        for t_, c in enumerate('kvq'):
            events['b' + c] = [call(lq_start, t_)]
            events['l' + c] = [call(ev_last, t_)]
            events['w' + c] = [call(ev_weights, t_)]
            for i in TWO:
                for e, f in zip('zxy', (ev_z, ev_xy, ev_y)):
                    events[f'{e}{c}{i}'] = [call(f, lq_copy, 2 * t_ + i)]
        for i, vs in enumerate(((2, 3), (1,), (0,))):
            events[f'b{i}'] = [call(lo_start, *vs)]
            for e, f in zip('zxycwv', (call(ev_z, lo_copy), call(ev_xy, lo_copy), call(ev_y, lo_copy), ev_lb, ev_wo, ev_wo_ready)):
                events[f'{e}{i}'] = [call(on, inner, call(f, *vs))]
        events['v0'] += [call(on, inner, lambda: local(xp.at[1 - side, pl.ds(0, 2)], wo_sem.at[4]))]
        for v in range(4):
            events[f'd{v}'] = [call(on, outer, lambda v=v: lb_z(v).start())]
        for h in HEADS:
            for z in TWO:
                events[f's{h}{z}'] = [kvr_copy(h, z).start]
            events[f'f{h}'] = [call(kv_forward, [h])]
            events[f'g{h}'] = [call(kv_wait, kvf_copy, [h])]
        for k in ROWS:
            for p in TWO:
                events['op'[p] + str(k)] = [call(send_o, (k,), p)]
        def run(names):
            for name in names.split(','):
                where, _, name = name.rpartition(':')
                if where:
                    on(inner if where == 'i' else outer, *events[name])
                else:
                    for c in events[name]:
                        c()

        @pl.when(event > 0)
        def _():
            choose(event - 1, [functools.partial(run, names) for names in EVENTS])
        return carry

    lax.fori_loop(0, len(TABLE), step_body, None)

    all_sent(lq_ref, 0)
    all_sent(lo_ref.at[:, 0, 0], 2)
    all_sent(lb_ref.at[:, 0], 3)
    all_sent(kvp_s, 4)
    all_sent(kvr_s.at[:, pl.ds(0, 2)], 5)
    all_sent(kvr_s.at[:, pl.ds(0, 2)], 6)

    @pl.when(outer)
    def _():
        all_sent(xb, 7)

    @pl.when(inner)
    def _():
        all_sent(lo_ref.at[:, pl.ds(0, 7)], 1)
        with scope('y_sent'):
            all_sent(xp.at[side, :, :, pl.ds(H, 3 * H)], 8)
        local(xp.at[side, :, :, pl.ds(0, H)], sent.at[9])

    for seg in TWO:
        @pl.when(tp != 1 + seg)
        def _(seg=seg):
            with scope(f'recv{seg}'):
                arrived(out_ref.at[seg], y_recv.at[seg])


PROGRAM = (
    'O.i:zk0,i:zk1', 'O.i:bv,o:zk0,so', 'O.o:zk1,s00,i:xk0', 'O.o:bv,o:xk0,i:xk1,o:s01,d3', 'O.i:yk0,i:zv0', 'O.o:xk1,o:yk0,i:yk1,i:zv1,i:s01,i:bq',
    'P.o:bq', 'P.o:yk1,lk,o:zv0,d1,i:xv0', 'P.wk,o:zv1,i:xv1', 'K.i:zq0', 'K.o:xv0,i:zq1,f0', 'K.o:xv1,o:zq0,o:zq1,i:yv0,i:yv1,b0,b1,r0,po,g0',
    'T0.o0,o1,d0,o:yv0,o:yv1,lv,wv,i:xq0,i:xq1,o:xq0', 'V.o:xq1,z0,o:s10,o:s11', 'V.i:yq0,i:yq1,o:yq0,c0,z1', 'V.o:yq1,sp,lq,o:s20,o:s21',
    'P.free,wq,c1', 'Q.pp,r1,x0,o:s30,o:s31', 'T4.p0,p1,x1', 'Q.y0,i:s10,i:s11,w0', 'T5.p2,p3,v0,y1,o:f1', 'R.w1', 'Q.v1', 'L', 'R', 'L',
    'Q.i:f1,o:g1,i:s20,i:s21,b2', 'T2.i:g1,o:f2', 'T1.o2,o3,o:g2,o:f3', 'R.i:s30,i:s31', 'L.i:f2', 'R', 'L.i:g2', 'T6.p4,o4,p5,o5,o:g3', 'R',
    'T3.i:f3,z2,c2', 'L.i:g3', 'T7.p6,o6,p7,o7', 'R.x2', 'L', 'R.y2', 'L.w2', '-.v2', 'N', 'N', 'N', 'R', 'L', 'N', 'N', 'N', 'N', 'N',
)
KINDS = '-OPKVQABRLN'


def tables():
    table, seen = [], {}
    names = tuple(dict.fromkeys(s.partition('.')[2] for s in PROGRAM if '.' in s))
    for s in PROGRAM:
        name, _, after = s.partition('.')
        kind, n = name[0], seen.get(name[0], 0)
        seen[kind] = n + 1
        if kind == 'T':
            n = int(name[1:])
            kind = 'AB'[n in (2, 3, 4, 5)]
        table.append(KINDS.index(kind) + 16 * n + 256 * (names.index(after) + 1 if after else 0))
    return table, names


TABLE, EVENTS = tables()


def main(bias, x, wk, wv, wq, w_out):
    anyspec = pl.BlockSpec(memory_space=pl.ANY)
    vmem = [((4, B, M), BF), ((B, B), BF), ((2, 8, B, M), BF), ((3, M, H), BF), ((4, 8, B, B), BF), ((4, 12, 2, B, B), BF), ((4, 4, 2, B, B), BF), ((4, 4, 2, B, B), BF),
            ((3072, H), F32), ((M, H), F32), ((64, 128), F32)]
    dma = [(4,), (9,), (5,), (10,), (6, 5), (4, 5), (4, 2), (3, 4), (8,), (2,)]
    return pl.pallas_call(
        main_kernel,
        in_specs=[pl.BlockSpec(memory_space=pltpu.SMEM)] + [anyspec] * 5,
        out_specs=[anyspec] * 4,
        out_shape=[jax.ShapeDtypeStruct(s, BF) for s in ((2, 8, B, H), (8, 6, B, B), (4, 8, 2, 64, H), (4, 2, B, H))],
        scratch_shapes=[pltpu.VMEM(*v) for v in vmem] + [pltpu.SemaphoreType.DMA(d) for d in dma] + [pltpu.SemaphoreType.REGULAR((2,))],
        compiler_params=params(collective_id=0, has_side_effects=True),
        cost_estimate=pl.CostEstimate(flops=10**11, bytes_accessed=10**8, transcendentals=0),
        name='main',
    )(bias, x, wk, wv, wq, w_out)[0]


def solution(mesh):
    def device_fn(hidden, w_query, w_key, w_value, w_out, branch_bias):
        return unpermute(main(branch_bias, hidden, w_key, w_value, w_query, w_out))

    return jax.shard_map(device_fn, mesh=mesh, in_specs=(P(('dp', 'sp'), None), P(None, 'tp'), P(None, 'tp'), P(None, 'tp'), P('tp', None), P(None, None)), out_specs=P(('dp', 'sp'), 'tp'), check_vma=False)
```

```python
import functools
import math

import jax
import jax.numpy as jnp
from jax import lax
from jax.experimental import pallas as pl
from jax.experimental.pallas import tpu as pltpu
from jax.sharding import PartitionSpec as P

MESH = pl.DeviceIdType.MESH
BF = jnp.bfloat16
F32 = jnp.float32
B, H, M = 256, 512, 2048
KAPPA = math.log2(math.e) / 16
VMEM = 66_900_000
SLOT = (0, 4, 2, 6, 1, 5, 3, 7)
KEY, VAL, QUE = range(3)
HEADS = range(4)
TWO = range(2)
ROWS = range(8)


def nn(a, b):
    return lax.dot_general(a, b, (((1,), (0,)), ((), ())), preferred_element_type=F32)


def nt(a, b):
    return lax.dot_general(a, b, (((1,), (1,)), ((), ())), preferred_element_type=F32)


def params(**kw):
    return pltpu.CompilerParams(vmem_limit_bytes=VMEM, **kw)


def ds(start, size, align=128):
    return pl.ds(pl.multiple_of(start, align), size)


def part(i, size):
    return slice(i * size, i * size + size)


def phase_matrix(transposed):
    r = lax.broadcasted_iota(jnp.int32, (B, B), int(transposed))
    p = lax.broadcasted_iota(jnp.int32, (B, B), int(not transposed))
    k = r // 32
    return (p == (r % 32) * 8 + k // 2 + 4 * (k % 2)).astype(F32).astype(BF)


def unpermute_kernel(y_ref, o_ref, y_s, o_s, load, store):
    pieces = [(s, j) for s in TWO for j in range(4)]

    def get(i):
        s, j = pieces[i]
        return pltpu.make_async_copy(y_ref.at[s, :, pl.ds(j * 64, 64)], y_s.at[i], load.at[i])

    def put(i):
        return pltpu.make_async_copy(o_s.at[i], o_ref.at[pl.ds(i * H, H)], store.at[i])

    for i in ROWS:
        get(i).start()
    pm = phase_matrix(True)
    for i in ROWS:
        get(i).wait()
        for j in TWO:
            o_s[i, part(j, B), :] = nn(pm, y_s[i, :, part(j, 32), :].reshape(B, H)).astype(BF)
        put(i).start()
    for i in ROWS:
        put(i).wait()


def unpermute(y):
    anyspec = pl.BlockSpec(memory_space=pl.ANY)
    return pl.pallas_call(
        unpermute_kernel,
        in_specs=[anyspec],
        out_specs=anyspec,
        out_shape=jax.ShapeDtypeStruct((2 * M, H), BF),
        scratch_shapes=[pltpu.VMEM((8, 8, 64, H), BF), pltpu.VMEM((8, H, H), BF), pltpu.SemaphoreType.DMA((8,)), pltpu.SemaphoreType.DMA((8,))],
        compiler_params=params(),
        name='unpermute',
    )(y)


def tile_steps(q, wide, narrow, s_ref, n_ref, done):
    st = {}
    logits, sums = [], []

    def add(name, x):
        st[name] = st[name] + x if name in st else x

    for groups, ref in ((wide, s_ref), (narrow, n_ref)):
        off = 0
        for keys, parts in groups:
            def qk(keys=keys, parts=parts, off=off, ref=ref):
                s = nt(keys(), q() if ref is s_ref else q()[:B])
                o = 0
                for _, n, b in parts:
                    piece = s[o:o + n]
                    ref[pl.ds(off + o, n), :] = piece
                    t = jnp.max(piece, axis=0, keepdims=True) * KAPPA
                    if b is not None:
                        t = t + fit(b, t)
                    if ref is n_ref:
                        t = jnp.concatenate([t, st['top'][:, B:]], axis=1)
                    st['top'] = jnp.maximum(st['top'], t) if 'top' in st else t
                    o += n
            logits.append(qk)
            for v, n, b in parts:
                def sv(v=v, n=n, b=b, off=off, ref=ref):
                    top = st['top'] if ref is s_ref else st['top'][:, :B]
                    e = jnp.exp2(ref[pl.ds(off, n), :] * KAPPA - (top if b is None else top - fit(b, top)))
                    name = 'w' if ref is s_ref else 'n'
                    add('l' + name, jnp.sum(e, axis=0, keepdims=True))
                    add('o' + name, nn(v(), e.astype(BF)))
                sums.append(sv)
                off += n

    def finish():
        o, l = st['ow'], st['lw']
        if narrow:
            o = jnp.concatenate([o[:, :B] + st['on'], o[:, B:]], axis=1)
            l = jnp.concatenate([l[:, :B] + st['ln'], l[:, B:]], axis=1)
        done(o / l)

    return logits, sums + [finish]


def fit(b, like):
    return b if b.shape == like.shape else jnp.concatenate([b] * (like.shape[1] // 128), axis=1)


def interleave(a, b):
    i = j = 0
    while i < len(a) or j < len(b):
        if j >= len(b) or (i < len(a) and i * len(b) <= j * len(a)):
            a[i]()
            i += 1
        else:
            b[j]()
            j += 1


def run_tiles(tiles):
    before = []
    for logits, sums in tiles:
        interleave(logits, before)
        before = sums
    interleave([], before)


def choose(x, cases):
    def among(lo, hi):
        mid = (lo + hi) // 2
        if hi - lo == 1:
            cases[lo]()
        else:
            pl.when(x < mid)(lambda: among(lo, mid))
            pl.when(x >= mid)(lambda: among(mid, hi))
    among(0, len(cases))


def on(cond, *calls):
    @pl.when(cond)
    def _():
        for c in calls:
            c()


def scope(name):
    return jax.named_scope(name)


def main_kernel(bias_ref, x_ref, wk_ref, wv_ref, wq_ref, wout_ref, out_ref, lq_ref, lo_ref, lb_ref,
                xb, pm, xp, ws, q_s, kv_s, kvp_s, kvr_s, s_scr, t_scr,
                beta_s, x_sem, w_sem, wo_sem, sent, lq_recv, lo_recv, lb_recv, kv_recv, o_recv, y_recv, ready):
    dp, tp, sp = lax.axis_index('dp'), lax.axis_index('tp'), lax.axis_index('sp')
    idx = dp * 4 + sp
    side = tp // 2
    inner = (tp == 1) | (tp == 2)
    outer = jnp.logical_not(inner)
    W = (wk_ref, wv_ref, wq_ref)
    peer_x, peer_y, peer_c = {'dp': dp ^ 1}, {'sp': sp ^ 2}, {'sp': sp ^ 1}

    def remote(src, dst, ss, rs, dev):
        return pltpu.make_async_remote_copy(src_ref=src, dst_ref=dst, send_sem=ss, recv_sem=rs, device_id=dev, device_id_type=MESH)

    def lq_copy(t, src, dst, dev):
        return remote(lq_ref.at[src, t], lq_ref.at[dst, t], sent.at[0], lq_recv.at[t, min(dst, 4)], dev)

    def lq_z(t):
        return remote(W[t // 2].at[ds(idx * B, B), pl.ds(t % 2 * B, B)], lq_ref.at[0, t], sent.at[0], lq_recv.at[t, 0], {'tp': tp ^ 2})

    def lq_start(t):
        for i in TWO:
            lq_z(2 * t + i).start()

    def lo_copy(v, src, dst, dev):
        return remote(lo_ref.at[v, src], lo_ref.at[v, dst], sent.at[1], lo_recv.at[v, min(dst, 4)], dev)

    def lo_z(v):
        dst = 2 - side
        b = (tp ^ dst) - 2
        return remote(wout_ref.at[ds(idx * 64, 64, 64), ds((dst ^ v) * H, H)], lo_ref.at[v, 0, b], sent.at[2], lo_recv.at[v, 0], {'tp': dst})

    def lb_z(v):
        return remote(wout_ref.at[ds(sp % 2 * B, B), ds((tp ^ 1 ^ v) * H, H)], lb_ref.at[v, sp % 2], sent.at[3], lb_recv.at[v, 0], {'tp': tp ^ 1})

    def lb_core(v):
        return remote(lb_ref.at[v, sp % 2], lb_ref.at[v, sp % 2], sent.at[3], lb_recv.at[v, 1], peer_c)

    def lo_start(*vs):
        for v in vs:
            lo_z(v).start()

    def arrived(ref, sem):
        remote(ref, ref, sent.at[0], sem, peer_c).wait_recv()

    def all_sent(ref, i):
        remote(ref, ref, sent.at[i], sent.at[i], peer_c).wait_send()

    def lo_zwait(v):
        arrived(lo_ref.at[v, 0], lo_recv.at[v, 0])

    def hop(copy, p, i):
        return copy(p, *((0, 2, peer_y), (0, 1, peer_x), (0, 4, peer_c), (2, 3, peer_x), (2, 6, peer_c), (1, 5, peer_c), (3, 7, peer_c))[i])

    def ev_z(copy, *ps):
        for p in ps:
            with scope(f'z_{copy.__name__}{p}'):
                lq_z(p).wait_recv() if copy is lq_copy else lo_zwait(p)
            for i in range(3):
                hop(copy, p, i).start()

    def ev_near(copy, *ps):
        for p in ps:
            with scope(f'n_{copy.__name__}{p}'):
                hop(copy, p, 0).wait_recv()
            hop(copy, p, 3).start()
            hop(copy, p, 4).start()

    def ev_far(copy, *ps):
        for p in ps:
            with scope(f'f_{copy.__name__}{p}'):
                hop(copy, p, 1).wait_recv()
            hop(copy, p, 5).start()

    def ev_xy(copy, *ps):
        ev_near(copy, *ps)
        ev_far(copy, *ps)

    def ev_y(copy, *ps):
        for p in ps:
            with scope(f'y_{copy.__name__}{p}'):
                hop(copy, p, 3).wait_recv()
            hop(copy, p, 6).start()
            if copy is lq_copy and p >= 2:
                start(w_load(p, SLOT[:4]))

    def ev_done(copy, *ps):
        for p in ps:
            with scope(f'c_{copy.__name__}{p}'):
                if copy is lq_copy:
                    arrived(lq_ref.at[pl.ds(4, 4), p], lq_recv.at[p, 4])
                else:
                    arrived(lo_ref.at[p, pl.ds(4, 4)], lo_recv.at[p, 4])

    def w_load(p, slots):
        return [pltpu.make_async_copy(lq_ref.at[SLOT.index(m), p], ws.at[p // 2 % 2, ds((idx ^ m) * B, B), pl.ds(p % 2 * B, B)], w_sem.at[p]) for m in slots]

    def own_load(t):
        return pltpu.make_async_copy(W[t], ws.at[t], w_sem.at[6 + t])

    def start(copies):
        for c in copies:
            c.start()

    def wait(copies):
        for c in copies:
            c.wait()

    def ev_last(t):
        pieces = [2 * t + i for i in TWO]
        ev_done(lq_copy, *pieces)
        for p in pieces:
            start(w_load(p, SLOT[4:] if t else SLOT))

    def local(ref, sem):
        pltpu.make_async_copy(ref, ref, sem).wait()

    def ev_weights(t):
        with scope(f'load{t}'):
            for i in TWO:
                local(ws.at[t % 2, :, pl.ds(i * B, B)], w_sem.at[2 * t + i])

    def ev_wo(*vs):
        ev_done(lo_copy, *vs)
        for v in vs:
            lb_core(v).wait_recv()
        start(wo_load(*vs))

    def ev_wo_ready(*vs):
        with scope(f'wo{vs[0]}'):
            for v in vs:
                local(xp.at[1 - side, pl.ds(2, 6), :, pl.ds((v ^ 2) * H, H)], wo_sem.at[v])

    def ev_lb(*vs):
        for v in vs:
            with scope(f'lb{v}'):
                lb_z(v).wait_recv()
            lb_core(v).start()

    wo = xp.at[1 - side]

    def wo_own():
        return [pltpu.make_async_copy(wout_ref.at[pl.ds(r * B, B), pl.ds(c * H, H)], xp.at[1 - side, r, :, ds((c ^ tp ^ 2) * H, H)], wo_sem.at[4])
                for r in TWO for c in range(4)]

    def wo_load(*vs):
        out = []
        for v in vs:
            cols = pl.ds((v ^ 2) * H, H)
            for s, m in enumerate(SLOT):
                row = (idx ^ m) * 64
                for b in TWO:
                    out.append(pltpu.make_async_copy(lo_ref.at[v, s, b], xp.at[1 - side, 4 + 2 * b + row // B, ds(row % B, 64, 64), cols], wo_sem.at[v]))
            for r in TWO:
                out.append(pltpu.make_async_copy(lb_ref.at[v, r], xp.at[1 - side, 2 + r, :, cols], wo_sem.at[v]))
        return out

    def kvp_copy(h, s):
        return remote(kv_s.at[h, pl.ds(8 * s, 2)], kvp_s.at[h, pl.ds(2 * s, 2)], sent.at[4], kv_recv.at[0, h], peer_c)

    def kvr_copy(h, s):
        return remote(kv_s.at[h, 8 * s], kvr_s.at[h, s], sent.at[5], kv_recv.at[1, h], peer_y)

    def kvf_copy(h, s):
        return remote(kvr_s.at[h, s], kvr_s.at[h, 2 + s], sent.at[6], kv_recv.at[2, h], peer_c)

    def kv_start(copy, heads):
        for h in heads:
            for s in TWO:
                copy(h, s).start()

    def kv_wait(copy, heads):
        with scope(f'w_{copy.__name__}{heads[0]}'):
            for h in heads:
                i = (kvp_copy, kvr_copy, kvf_copy).index(copy)
                arrived((kvp_s.at[h], kvr_s.at[h, pl.ds(0, 2)], kvr_s.at[h, pl.ds(2, 2)])[i], kv_recv.at[i, h])

    def kv_forward(heads):
        kv_wait(kvr_copy, heads)
        kv_start(kvf_copy, heads)

    def reverse(i):
        return (i % 2) * 2 + i // 2

    def order(n):
        return 2 * reverse(n % 4) + ((n // 4) ^ side)

    def o_at(k, p, theirs, col, size):
        return ws.at[1 + theirs, ds(k * B, B), ds(col, size)] if p else xb.at[k // 2, :, ds((k % 2) * 1024 + theirs * H + col, size)]

    def o_copy(k, p):
        return remote(o_at(k, p, 0, 0, H), o_at(k, p, 1, 0, H), sent.at[7], o_recv.at[k], {'tp': tp ^ 1})

    def o_times(k, v, n):
        cols = pl.ds((v ^ 2) * H, n * H)
        y = nn(xb[k // 2, :, ds((k % 2) * 1024, 1024)], wo[0:4, :, cols].reshape(1024, n * H))
        for i in TWO:
            y = y + nn(ws[1 + i, ds(k * B, B), :], wo[part(2 + i, 2), :, cols].reshape(H, n * H))
        y = y.astype(BF)
        for i in range(n):
            y_src(k, v + i)[...] = y[:, part(i, H)]
            y_copy(k, v + i, side).start() if v else y_local(k).start()

    def y_src(k, v):
        return xp.at[side, k, :, pl.ds(v * H, H)]

    def y_copy(k, v, seg):
        return remote(y_src(k, v), out_ref.at[seg, k], sent.at[8], y_recv.at[seg], {'tp': tp ^ v})

    def y_local(k):
        return pltpu.make_async_copy(y_src(k, 0), out_ref.at[side, k], sent.at[9])

    def x_copy(j):
        return pltpu.make_async_copy(x_ref.at[ds(j * B, B), :], xb.at[lax.rem(j, 4)], x_sem.at[lax.rem(j, 4)])

    for j in range(4):
        x_copy(j).start()
    barrier = pltpu.get_barrier_semaphore()
    peers = [{'tp': tp ^ 1}, {'tp': tp ^ 2}, {'tp': tp ^ 3}, peer_x, peer_y, peer_c]
    for dev in peers:
        pl.semaphore_signal(barrier, inc=1, device_id=dev, device_id_type=MESH)
    for t in range(3):
        own_load(t).start()

    pm[...] = phase_matrix(False)

    def permute_body(j, carry):
        x_copy(j).wait()
        y = nn(pm[...], xb[lax.rem(j, 4)]).astype(BF).reshape(8, 32, M)
        xp[j // 8, :, ds(lax.rem(j, 8) * 32, 32, 32), :] = y
        pl.when(j < 12)(lambda: x_copy(j + 4).start())

        @pl.when(j == 7)
        def _():
            with scope('barrier'):
                pl.semaphore_wait(barrier, len(peers))
            lq_start(KEY)
            on(outer, lb_z(2).start)
        return carry

    with scope('permute'):
        lax.fori_loop(0, 16, permute_body, None)

    for h in HEADS:
        column = 2 * (tp ^ (h // 2 * 2)) + h % 2
        for i, branches in enumerate(('0', '01', '1', '012', '12', '2', '0123', '123', '23', '3')):
            rows = [jnp.full((1, 128), bias_ref[j, column], F32) for j in map(int, branches)]
            m = functools.reduce(jnp.maximum, rows)
            beta_s[pl.ds(h * 16 + i, 1), :] = (m + jnp.log(sum(jnp.exp(r - m) for r in rows))) * math.log2(math.e)

    def signal_ready(i):
        pl.when(inner)(lambda: pl.semaphore_signal(ready.at[i], inc=1, device_id={'tp': tp ^ 1}, device_id_type=MESH))

    def wait_ready(i):
        with scope(f'ready{i}'):
            pl.when(outer)(lambda: pl.semaphore_wait(ready.at[i], 1))

    signal_ready(0)

    def group(g):
        low = g < 4
        return jnp.where(low, g & 1, 0), jnp.where(low, g // 2, g - 2)

    def head_number(h):
        return 2 * (tp ^ (h // 2 * 2)) + h % 2

    def project(heads, sigma, pair, kinds):
        for h in heads:
            t = head_number(h) + reverse(pair)
            x, swap = xp[side ^ sigma, pl.ds(2 * (t & 3), 2)].reshape(H, M), (t & 7) >> 2
            for t in kinds:
                y = nn(x, ws[t, :, part(h % 2, B)])
                for j in TWO:
                    piece = y[part(j, B)]
                    kv_s[h, 8 * sigma + 2 * pair + (j ^ swap), t] = (piece.T if t == VAL else piece).astype(BF)

    def phases_of(j):
        return [j % 2 + 2 * i for i in TWO], (j // 2) ^ side

    def rank_of(phase, h):
        rel = (phase - head_number(h)) & 7
        return (rel & 1) * 4 + ((rel >> 1) & 1) * 2 + (rel >> 2)

    def queries(heads, w, j):
        phases, half = phases_of(j)
        x = jnp.concatenate([xp[side, 2 * f + half] for f in phases])
        for h in heads:
            y = nn(x, ws[w, :, part(h % 2, B)]).astype(BF)
            for i, f in enumerate(phases):
                q_s[h, rank_of(f + 4 * half, h)] = y[part(i, B)]

    with scope('own_w'):
        for t in range(3):
            own_load(t).wait()
    own, partner = HEADS[:2], HEADS[2:]

    def mix(b, c):
        return jnp.concatenate([b, b, c, c], axis=1)

    def keys_of(ref, h, i, weights):
        parts = []
        n = 0
        for count, b in weights:
            def values(i=i + n, count=count):
                v = [ref[h, i + j, VAL] for j in range(count)]
                return v[0] if count == 1 else jnp.concatenate(v, axis=1)
            parts.append((values, count * B, b))
            n += count
        return (lambda: ref[h, i:i + n, KEY].reshape(n * B, B)), parts

    def chunk_tiles(p, j, kind):
        both_phases, half = phases_of(j)

        def put(h, phase, ot):
            k = 2 * (phase & 3) + half
            y = ot.T.astype(BF)
            for i in TWO:
                pl.when(p == i)(lambda i=i: o_at(k, i, 0, (h % 2) * B, B).__setitem__(..., y))

        def tile(h, phases, ranks, wide, narrow, s_ref, n_ref):
            def done(ot):
                for i, phase in enumerate(phases):
                    put(h, phase, ot[:, part(i, B)])
            return tile_steps(lambda: jnp.concatenate([q_s[h, r] for r in ranks]), wide, narrow, s_ref, n_ref, done)

        h = 2 * p + (j % 2) ^ 1
        rest = tile(h, both_phases, [rank_of(f + 4 * half, h) for f in both_phases], [keys_of(kv_s, h, i, [(2, None)]) for i in range(0, 8, 2)], [], t_scr, None)
        h = 2 * p + (j % 2)
        a = head_number(h)
        b0, b01, b1, b012, b12, b2, b0123, b123, b23, b3 = [beta_s[pl.ds(h * 16 + i, 1), :] for i in range(10)]
        phases = [a & 3, (a & 3) ^ 2]
        both = [keys_of(kv_s, h, i, [(2, b)]) for i, b in ((2, b01), (4, b0), (6, b0), (10, b1))]
        if kind == 0:
            both += [keys_of(kv_s, h, 0, [(1, mix(b0123, b01)), (1, mix(b012, b01))]), keys_of(kv_s, h, 8, [(1, mix(b123, b1)), (1, mix(b12, b1))])]
            first = [keys_of(kvp_s, h, i, [(1, b23), (1, b2)]) for i in (0, 2)] + [keys_of(kvr_s, h, i, [(2, b3)]) for i in (0, 2)]
        else:
            both += [keys_of(kv_s, h, 0, [(2, mix(b012, b01))]), keys_of(kv_s, h, 8, [(2, mix(b12, b1))])]
            first = [keys_of(kvp_s, h, i, [(2, b2)]) for i in (0, 2)]
        with scope(f'tile{kind}'):
            run_tiles([rest, tile(h, phases, [kind, rank_of(phases[1] + 4 * half, h)], both, first, s_scr, t_scr.at[:, pl.ds(0, B)])])

    def send_o(ks, p):
        @pl.when(outer)
        def _():
            for k in ks:
                o_copy(order(k), p).start()

    def step_body(t, carry):
        packed = functools.reduce(lambda x, i: jnp.where(t == i, TABLE[i], x), range(len(TABLE)), 0)
        code, n, event = packed % 16, packed // 16 % 16, packed // 256

        def step_o():
            with scope('own_kv'):
                project(own, *group(n), (KEY, VAL))

        def step_kv(t_):
            with scope(f'par_{t_}'):
                for i in TWO:
                    project(partner, *group(2 * n + i), (t_,))

        def step_q(heads, w):
            with scope(f'que_{w}'):
                queries(heads, w, n)

        def step_out(v, m):
            @pl.when(inner)
            def _():
                k = order(n)
                if m == 2:
                    with scope('wait_o'):
                        arrived(ws.at[0, pl.ds(0, H), :], o_recv.at[k])
                with scope(f'out{v}'):
                    o_times(k, v, m)

        f = functools.partial
        kinds = {'-': lambda: None, 'O': step_o, 'P': f(step_q, own, QUE), 'K': f(step_kv, KEY), 'V': f(step_kv, VAL), 'Q': f(step_q, partner, KEY),
                 'A': lambda: chunk_tiles(n // 4, n % 4, 0), 'B': lambda: chunk_tiles(n // 4, n % 4, 1), 'R': f(step_out, 2, 2), 'L': f(step_out, 1, 1), 'N': f(step_out, 0, 1)}
        choose(code, [kinds[c] for c in KINDS])
        call = functools.partial

        events = {
            'free': [call(signal_ready, 1), call(on, inner, lambda: start(wo_own()))],
            'r0': [call(wait_ready, 0)],
            'r1': [call(wait_ready, 1)],
            'so': [call(kv_start, kvp_copy, own)],
            'po': [call(kv_wait, kvp_copy, own)],
            'sp': [call(kv_start, kvp_copy, partner)],
            'pp': [call(kv_wait, kvp_copy, partner)],
        }
        for t_, c in enumerate('kvq'):
            events['b' + c] = [call(lq_start, t_)]
            events['l' + c] = [call(ev_last, t_)]
            events['w' + c] = [call(ev_weights, t_)]
            for i in TWO:
                for e, f in zip('zxy', (ev_z, ev_xy, ev_y)):
                    events[f'{e}{c}{i}'] = [call(f, lq_copy, 2 * t_ + i)]
        for i, vs in enumerate(((2, 3), (1,), (0,))):
            events[f'b{i}'] = [call(lo_start, *vs)]
            for e, f in zip('zmxycwv', (call(ev_z, lo_copy), call(ev_near, lo_copy), call(ev_far, lo_copy), call(ev_y, lo_copy), ev_lb, ev_wo, ev_wo_ready)):
                events[f'{e}{i}'] = [call(on, inner, call(f, *vs))]
        events['v0'] += [call(on, inner, lambda: local(xp.at[1 - side, pl.ds(0, 2)], wo_sem.at[4]))]
        for v in range(4):
            events[f'd{v}'] = [call(on, outer, lambda v=v: lb_z(v).start())]
        for h in HEADS:
            for z in TWO:
                events[f's{h}{z}'] = [kvr_copy(h, z).start]
            events[f'f{h}'] = [call(kv_forward, [h])]
            events[f'g{h}'] = [call(kv_wait, kvf_copy, [h])]
        for k in ROWS:
            for p in TWO:
                events['op'[p] + str(k)] = [call(send_o, (k,), p)]
        def run(names):
            for name in names.split(','):
                where, _, name = name.rpartition(':')
                if where:
                    on(inner if where == 'i' else outer, *events[name])
                else:
                    for c in events[name]:
                        c()

        @pl.when(event > 0)
        def _():
            choose(event - 1, [functools.partial(run, names) for names in EVENTS])
        return carry

    lax.fori_loop(0, len(TABLE), step_body, None)

    all_sent(lq_ref, 0)
    all_sent(lo_ref.at[:, 0, 0], 2)
    all_sent(lb_ref.at[:, 0], 3)
    all_sent(kvp_s, 4)
    all_sent(kvr_s.at[:, pl.ds(0, 2)], 5)
    all_sent(kvr_s.at[:, pl.ds(0, 2)], 6)

    @pl.when(outer)
    def _():
        all_sent(xb, 7)

    @pl.when(inner)
    def _():
        all_sent(lo_ref.at[:, pl.ds(0, 7)], 1)
        with scope('y_sent'):
            all_sent(xp.at[side, :, :, pl.ds(H, 3 * H)], 8)
        local(xp.at[side, :, :, pl.ds(0, H)], sent.at[9])

    for seg in TWO:
        @pl.when(tp != 1 + seg)
        def _(seg=seg):
            with scope(f'recv{seg}'):
                arrived(out_ref.at[seg], y_recv.at[seg])


PROGRAM = (
    'O.i:zk0,i:zk1', 'O.i:bv,o:zk0,so', 'O.o:zk1,s00,i:xk0', 'O.o:bv,o:xk0,i:xk1,o:s01,d3', 'O.i:yk0,i:zv0', 'O.o:xk1,o:yk0,i:yk1,i:zv1,i:s01,i:bq',
    'P.o:bq', 'P.o:yk1,lk,o:zv0,d1,i:xv0', 'P.wk,o:zv1,i:xv1', 'K.i:zq0', 'K.o:xv0,i:zq1,f0', 'K.o:xv1,o:zq0,i:yv0,i:yv1,b0,b1,r0,po,g0,o:zq1',
    'T0.o0,o1,d0,o:yv0,o:yv1,lv,i:xq0,i:xq1,o:xq0', 'P.wv,z0', 'V.o:xq1,o:s10,o:s11', 'V.c0,z1', 'V.yq0,yq1,m0,sp,free,lq,o:s20,o:s21,wq',
    'Q.pp,r1,x0,c1,o:s30,o:s31', 'T4.p0,p1,y0,w0,m1,x1,i:s10,i:s11,v0', 'R', 'Q.y1', 'T5.p2,p3,w1,o:f1', 'R.v1', 'Q', 'L', 'L',
    'Q.i:f1,o:g1,i:s20,i:s21,b2', 'T2.i:g1,o:f2', 'T1.o2,o3,o:g2,o:f3', 'R.i:s30,i:s31', 'L.i:f2', 'R', 'L.i:g2', 'T6.p4,o4,p5,o5,o:g3', 'R',
    'T3.i:f3,z2,c2', 'L.i:g3', 'T7.p6,o6,p7,o7', 'R.m2,x2', 'L', 'R.y2', 'L.w2', '-.v2', 'N', 'N', 'N', 'R', 'L', 'N', 'N', 'N', 'N', 'N',
)
KINDS = '-OPKVQABRLN'


def tables():
    table, seen = [], {}
    names = tuple(dict.fromkeys(s.partition('.')[2] for s in PROGRAM if '.' in s))
    for s in PROGRAM:
        name, _, after = s.partition('.')
        kind, n = name[0], seen.get(name[0], 0)
        seen[kind] = n + 1
        if kind == 'T':
            n = int(name[1:])
            kind = 'AB'[n in (2, 3, 4, 5)]
        table.append(KINDS.index(kind) + 16 * n + 256 * (names.index(after) + 1 if after else 0))
    return table, names


TABLE, EVENTS = tables()


def main(bias, x, wk, wv, wq, w_out):
    anyspec = pl.BlockSpec(memory_space=pl.ANY)
    vmem = [((4, B, M), BF), ((B, B), BF), ((2, 8, B, M), BF), ((3, M, H), BF), ((4, 8, B, B), BF), ((4, 12, 2, B, B), BF), ((4, 4, 2, B, B), BF), ((4, 4, 2, B, B), BF),
            ((3072, H), F32), ((M, H), F32), ((64, 128), F32)]
    dma = [(4,), (9,), (5,), (10,), (6, 5), (4, 5), (4, 2), (3, 4), (8,), (2,)]
    return pl.pallas_call(
        main_kernel,
        in_specs=[pl.BlockSpec(memory_space=pltpu.SMEM)] + [anyspec] * 5,
        out_specs=[anyspec] * 4,
        out_shape=[jax.ShapeDtypeStruct(s, BF) for s in ((2, 8, B, H), (8, 6, B, B), (4, 8, 2, 64, H), (4, 2, B, H))],
        scratch_shapes=[pltpu.VMEM(*v) for v in vmem] + [pltpu.SemaphoreType.DMA(d) for d in dma] + [pltpu.SemaphoreType.REGULAR((2,))],
        compiler_params=params(collective_id=0, has_side_effects=True),
        cost_estimate=pl.CostEstimate(flops=10**11, bytes_accessed=10**8, transcendentals=0),
        name='main',
    )(bias, x, wk, wv, wq, w_out)[0]


def solution(mesh):
    def device_fn(hidden, w_query, w_key, w_value, w_out, branch_bias):
        return unpermute(main(branch_bias, hidden, w_key, w_value, w_query, w_out))

    return jax.shard_map(device_fn, mesh=mesh, in_specs=(P(('dp', 'sp'), None), P(None, 'tp'), P(None, 'tp'), P(None, 'tp'), P('tp', None), P(None, None)), out_specs=P(('dp', 'sp'), 'tp'), check_vma=False)
```

```python
import functools
import math

import jax
import jax.numpy as jnp
from jax import lax
from jax.experimental import pallas as pl
from jax.experimental.pallas import tpu as pltpu
from jax.sharding import PartitionSpec as P

MESH = pl.DeviceIdType.MESH
BF = jnp.bfloat16
F32 = jnp.float32
B, H, M = 256, 512, 2048
KAPPA = math.log2(math.e) / 16
VMEM = 66_900_000
SLOT = (0, 4, 2, 6, 1, 5, 3, 7)
KEY, VAL, QUE = range(3)
HEADS = range(4)
TWO = range(2)
ROWS = range(8)


def nn(a, b):
    return lax.dot_general(a, b, (((1,), (0,)), ((), ())), preferred_element_type=F32)


def nt(a, b):
    return lax.dot_general(a, b, (((1,), (1,)), ((), ())), preferred_element_type=F32)


def params(**kw):
    return pltpu.CompilerParams(vmem_limit_bytes=VMEM, **kw)


def ds(start, size, align=128):
    return pl.ds(pl.multiple_of(start, align), size)


def part(i, size):
    return slice(i * size, i * size + size)


def phase_matrix(transposed):
    r = lax.broadcasted_iota(jnp.int32, (B, B), int(transposed))
    p = lax.broadcasted_iota(jnp.int32, (B, B), int(not transposed))
    k = r // 32
    return (p == (r % 32) * 8 + k // 2 + 4 * (k % 2)).astype(F32).astype(BF)


def unpermute_kernel(y_ref, o_ref, y_s, o_s, load, store):
    pieces = [(s, j) for s in TWO for j in range(4)]

    def get(i):
        s, j = pieces[i]
        return pltpu.make_async_copy(y_ref.at[s, :, pl.ds(j * 64, 64)], y_s.at[i], load.at[i])

    def put(i):
        return pltpu.make_async_copy(o_s.at[i], o_ref.at[pl.ds(i * H, H)], store.at[i])

    for i in ROWS:
        get(i).start()
    pm = phase_matrix(True)
    for i in range(0, 8, 2):
        group = (i, i + 1)
        for k in group:
            get(k).wait()
        for k in group:
            for j in TWO:
                o_s[k, part(j, B), :] = nn(pm, y_s[k, :, part(j, 32), :].reshape(B, H)).astype(BF)
        for k in group:
            put(k).start()
    for i in ROWS:
        put(i).wait()


def unpermute(y):
    anyspec = pl.BlockSpec(memory_space=pl.ANY)
    return pl.pallas_call(
        unpermute_kernel,
        in_specs=[anyspec],
        out_specs=anyspec,
        out_shape=jax.ShapeDtypeStruct((2 * M, H), BF),
        scratch_shapes=[pltpu.VMEM((8, 8, 64, H), BF), pltpu.VMEM((8, H, H), BF), pltpu.SemaphoreType.DMA((8,)), pltpu.SemaphoreType.DMA((8,))],
        compiler_params=params(),
        name='unpermute',
    )(y)


def tile_steps(q, wide, narrow, s_ref, n_ref, done):
    st = {}
    logits, sums = [], []

    def add(name, x):
        st[name] = st[name] + x if name in st else x

    for groups, ref in ((wide, s_ref), (narrow, n_ref)):
        off = 0
        for keys, parts in groups:
            def qk(keys=keys, parts=parts, off=off, ref=ref):
                s = nt(keys(), q() if ref is s_ref else q()[:B])
                o = 0
                for _, n, b in parts:
                    piece = s[o:o + n]
                    ref[pl.ds(off + o, n), :] = piece
                    t = jnp.max(piece, axis=0, keepdims=True) * KAPPA
                    if b is not None:
                        t = t + fit(b, t)
                    if ref is n_ref:
                        t = jnp.concatenate([t, st['top'][:, B:]], axis=1)
                    st['top'] = jnp.maximum(st['top'], t) if 'top' in st else t
                    o += n
            logits.append(qk)
            for v, n, b in parts:
                def sv(v=v, n=n, b=b, off=off, ref=ref):
                    top = st['top'] if ref is s_ref else st['top'][:, :B]
                    e = jnp.exp2(ref[pl.ds(off, n), :] * KAPPA - (top if b is None else top - fit(b, top)))
                    name = 'w' if ref is s_ref else 'n'
                    add('l' + name, jnp.sum(e, axis=0, keepdims=True))
                    add('o' + name, nn(v(), e.astype(BF)))
                sums.append(sv)
                off += n

    def finish():
        o, l = st['ow'], st['lw']
        if narrow:
            o = jnp.concatenate([o[:, :B] + st['on'], o[:, B:]], axis=1)
            l = jnp.concatenate([l[:, :B] + st['ln'], l[:, B:]], axis=1)
        done(o / l)

    return logits, sums + [finish]


def fit(b, like):
    return b if b.shape == like.shape else jnp.concatenate([b] * (like.shape[1] // 128), axis=1)


def interleave(a, b):
    i = j = 0
    while i < len(a) or j < len(b):
        if j >= len(b) or (i < len(a) and i * len(b) <= j * len(a)):
            a[i]()
            i += 1
        else:
            b[j]()
            j += 1


def run_tiles(tiles):
    before = []
    for logits, sums in tiles:
        interleave(logits, before)
        before = sums
    interleave([], before)


def choose(x, cases):
    def among(lo, hi):
        mid = (lo + hi) // 2
        if hi - lo == 1:
            cases[lo]()
        else:
            pl.when(x < mid)(lambda: among(lo, mid))
            pl.when(x >= mid)(lambda: among(mid, hi))
    among(0, len(cases))


def on(cond, *calls):
    @pl.when(cond)
    def _():
        for c in calls:
            c()


def scope(name):
    return jax.named_scope(name)


def main_kernel(bias_ref, x_ref, wk_ref, wv_ref, wq_ref, wout_ref, out_ref, lq_ref, lo_ref, lb_ref,
                xb, pm, xp, ws, q_s, kv_s, kvp_s, kvr_s, s_scr, t_scr,
                beta_s, x_sem, w_sem, wo_sem, sent, lq_recv, lo_recv, lb_recv, kv_recv, o_recv, y_recv, ready):
    dp, tp, sp = lax.axis_index('dp'), lax.axis_index('tp'), lax.axis_index('sp')
    idx = dp * 4 + sp
    side = tp // 2
    inner = (tp == 1) | (tp == 2)
    outer = jnp.logical_not(inner)
    W = (wk_ref, wv_ref, wq_ref)
    peer_x, peer_y, peer_c = {'dp': dp ^ 1}, {'sp': sp ^ 2}, {'sp': sp ^ 1}

    def remote(src, dst, ss, rs, dev):
        return pltpu.make_async_remote_copy(src_ref=src, dst_ref=dst, send_sem=ss, recv_sem=rs, device_id=dev, device_id_type=MESH)

    def lq_copy(t, src, dst, dev):
        return remote(lq_ref.at[src, t], lq_ref.at[dst, t], sent.at[0], lq_recv.at[t, min(dst, 4)], dev)

    def lq_z(t):
        return remote(W[t // 2].at[ds(idx * B, B), pl.ds(t % 2 * B, B)], lq_ref.at[0, t], sent.at[0], lq_recv.at[t, 0], {'tp': tp ^ 2})

    def lq_start(t):
        for i in TWO:
            lq_z(2 * t + i).start()

    def lo_copy(v, src, dst, dev):
        return remote(lo_ref.at[v, src], lo_ref.at[v, dst], sent.at[1], lo_recv.at[v, min(dst, 4)], dev)

    def lo_z(v):
        dst = 2 - side
        b = (tp ^ dst) - 2
        return remote(wout_ref.at[ds(idx * 64, 64, 64), ds((dst ^ v) * H, H)], lo_ref.at[v, 0, b], sent.at[2], lo_recv.at[v, 0], {'tp': dst})

    def lb_z(v):
        return remote(wout_ref.at[ds(sp % 2 * B, B), ds((tp ^ 1 ^ v) * H, H)], lb_ref.at[v, sp % 2], sent.at[3], lb_recv.at[v, 0], {'tp': tp ^ 1})

    def lb_core(v):
        return remote(lb_ref.at[v, sp % 2], lb_ref.at[v, sp % 2], sent.at[3], lb_recv.at[v, 1], peer_c)

    def lo_start(*vs):
        for v in vs:
            lo_z(v).start()

    def arrived(ref, sem):
        remote(ref, ref, sent.at[0], sem, peer_c).wait_recv()

    def all_sent(ref, i):
        remote(ref, ref, sent.at[i], sent.at[i], peer_c).wait_send()

    def lo_zwait(v):
        arrived(lo_ref.at[v, 0], lo_recv.at[v, 0])

    def hop(copy, p, i):
        return copy(p, *((0, 2, peer_y), (0, 1, peer_x), (0, 4, peer_c), (2, 3, peer_x), (2, 6, peer_c), (1, 5, peer_c), (3, 7, peer_c))[i])

    def ev_z(copy, *ps):
        for p in ps:
            with scope(f'z_{copy.__name__}{p}'):
                lq_z(p).wait_recv() if copy is lq_copy else lo_zwait(p)
            for i in range(3):
                hop(copy, p, i).start()

    def ev_near(copy, *ps):
        for p in ps:
            with scope(f'n_{copy.__name__}{p}'):
                hop(copy, p, 0).wait_recv()
            hop(copy, p, 3).start()
            hop(copy, p, 4).start()

    def ev_far(copy, *ps):
        for p in ps:
            with scope(f'f_{copy.__name__}{p}'):
                hop(copy, p, 1).wait_recv()
            hop(copy, p, 5).start()

    def ev_xy(copy, *ps):
        ev_near(copy, *ps)
        ev_far(copy, *ps)

    def ev_y(copy, *ps):
        for p in ps:
            with scope(f'y_{copy.__name__}{p}'):
                hop(copy, p, 3).wait_recv()
            hop(copy, p, 6).start()
            if copy is lq_copy and p >= 2:
                start(w_load(p, SLOT[:4]))

    def ev_done(copy, *ps):
        for p in ps:
            with scope(f'c_{copy.__name__}{p}'):
                if copy is lq_copy:
                    arrived(lq_ref.at[pl.ds(4, 4), p], lq_recv.at[p, 4])
                else:
                    arrived(lo_ref.at[p, pl.ds(4, 4)], lo_recv.at[p, 4])

    def w_load(p, slots):
        return [pltpu.make_async_copy(lq_ref.at[SLOT.index(m), p], ws.at[p // 2 % 2, ds((idx ^ m) * B, B), pl.ds(p % 2 * B, B)], w_sem.at[p]) for m in slots]

    def own_load(t):
        return pltpu.make_async_copy(W[t], ws.at[t], w_sem.at[6 + t])

    def start(copies):
        for c in copies:
            c.start()

    def wait(copies):
        for c in copies:
            c.wait()

    def ev_last(t):
        pieces = [2 * t + i for i in TWO]
        ev_done(lq_copy, *pieces)
        for p in pieces:
            start(w_load(p, SLOT[4:] if t else SLOT))

    def local(ref, sem):
        pltpu.make_async_copy(ref, ref, sem).wait()

    def ev_weights(t):
        with scope(f'load{t}'):
            for i in TWO:
                local(ws.at[t % 2, :, pl.ds(i * B, B)], w_sem.at[2 * t + i])

    def ev_wo(*vs):
        ev_done(lo_copy, *vs)
        for v in vs:
            lb_core(v).wait_recv()
        start(wo_load(*vs))

    def ev_wo_ready(*vs):
        with scope(f'wo{vs[0]}'):
            for v in vs:
                local(xp.at[1 - side, pl.ds(2, 6), :, pl.ds((v ^ 2) * H, H)], wo_sem.at[v])

    def ev_lb(*vs):
        for v in vs:
            with scope(f'lb{v}'):
                lb_z(v).wait_recv()
            lb_core(v).start()

    wo = xp.at[1 - side]

    def wo_own():
        return [pltpu.make_async_copy(wout_ref.at[pl.ds(r * B, B), pl.ds(c * H, H)], xp.at[1 - side, r, :, ds((c ^ tp ^ 2) * H, H)], wo_sem.at[4])
                for r in TWO for c in range(4)]

    def wo_load(*vs):
        out = []
        for v in vs:
            cols = pl.ds((v ^ 2) * H, H)
            for s, m in enumerate(SLOT):
                row = (idx ^ m) * 64
                for b in TWO:
                    out.append(pltpu.make_async_copy(lo_ref.at[v, s, b], xp.at[1 - side, 4 + 2 * b + row // B, ds(row % B, 64, 64), cols], wo_sem.at[v]))
            for r in TWO:
                out.append(pltpu.make_async_copy(lb_ref.at[v, r], xp.at[1 - side, 2 + r, :, cols], wo_sem.at[v]))
        return out

    def kvp_copy(h, s):
        return remote(kv_s.at[h, pl.ds(8 * s, 2)], kvp_s.at[h, pl.ds(2 * s, 2)], sent.at[4], kv_recv.at[0, h], peer_c)

    def kvr_copy(h, s):
        return remote(kv_s.at[h, 8 * s], kvr_s.at[h, s], sent.at[5], kv_recv.at[1, h], peer_y)

    def kvf_copy(h, s):
        return remote(kvr_s.at[h, s], kvr_s.at[h, 2 + s], sent.at[6], kv_recv.at[2, h], peer_c)

    def kv_start(copy, heads):
        for h in heads:
            for s in TWO:
                copy(h, s).start()

    def kv_wait(copy, heads):
        with scope(f'w_{copy.__name__}{heads[0]}'):
            for h in heads:
                i = (kvp_copy, kvr_copy, kvf_copy).index(copy)
                arrived((kvp_s.at[h], kvr_s.at[h, pl.ds(0, 2)], kvr_s.at[h, pl.ds(2, 2)])[i], kv_recv.at[i, h])

    def kv_forward(heads):
        kv_wait(kvr_copy, heads)
        kv_start(kvf_copy, heads)

    def reverse(i):
        return (i % 2) * 2 + i // 2

    def order(n):
        return 2 * reverse(n % 4) + ((n // 4) ^ side)

    def o_at(k, p, theirs, col, size, row=0, rows=B):
        if p:
            return ws.at[1 + theirs, ds(k * B + row, rows), ds(col, size)]
        return xb.at[k // 2, pl.ds(row, rows), ds((k % 2) * 1024 + theirs * H + col, size)]

    def o_copy(k, p, half):
        row = half * 128
        return remote(o_at(k, p, 0, 0, H, row, 128), o_at(k, p, 1, 0, H, row, 128), sent.at[7], o_recv.at[k, half], {'tp': tp ^ 1})

    def o_times(k, v, n, row=0, rows=B):
        cols = pl.ds((v ^ 2) * H, n * H)
        y = nn(xb[k // 2, pl.ds(row, rows), ds((k % 2) * 1024, 1024)], wo[0:4, :, cols].reshape(1024, n * H))
        for i in TWO:
            y = y + nn(ws[1 + i, ds(k * B + row, rows), :], wo[part(2 + i, 2), :, cols].reshape(H, n * H))
        y = y.astype(BF)
        for i in range(n):
            y_src(k, v + i, row, rows)[...] = y[:, part(i, H)]
            y_copy(k, v + i, side, row, rows).start() if v else y_local(k).start()

    def y_src(k, v, row=0, rows=B):
        return xp.at[side, k, pl.ds(row, rows), pl.ds(v * H, H)]

    def y_copy(k, v, seg, row, rows):
        return remote(y_src(k, v, row, rows), out_ref.at[seg, k, pl.ds(row, rows)], sent.at[8], y_recv.at[seg], {'tp': tp ^ v})

    def y_local(k):
        return pltpu.make_async_copy(y_src(k, 0), out_ref.at[side, k], sent.at[9])

    def x_copy(j):
        return pltpu.make_async_copy(x_ref.at[ds(j * B, B), :], xb.at[lax.rem(j, 4)], x_sem.at[lax.rem(j, 4)])

    for j in range(4):
        x_copy(j).start()
    barrier = pltpu.get_barrier_semaphore()
    peers = [{'tp': tp ^ 1}, {'tp': tp ^ 2}, {'tp': tp ^ 3}, peer_x, peer_y, peer_c]
    for dev in peers:
        pl.semaphore_signal(barrier, inc=1, device_id=dev, device_id_type=MESH)
    for t in range(3):
        own_load(t).start()

    pm[...] = phase_matrix(False)

    def permute_body(j, carry):
        x_copy(j).wait()
        y = nn(pm[...], xb[lax.rem(j, 4)]).astype(BF).reshape(8, 32, M)
        xp[j // 8, :, ds(lax.rem(j, 8) * 32, 32, 32), :] = y
        pl.when(j < 12)(lambda: x_copy(j + 4).start())

        @pl.when(j == 7)
        def _():
            with scope('barrier'):
                pl.semaphore_wait(barrier, len(peers))
            lq_start(KEY)
            on(outer, lb_z(2).start)
        return carry

    with scope('permute'):
        lax.fori_loop(0, 16, permute_body, None)

    for h in HEADS:
        column = 2 * (tp ^ (h // 2 * 2)) + h % 2
        for i, branches in enumerate(('0', '01', '1', '012', '12', '2', '0123', '123', '23', '3')):
            rows = [jnp.full((1, 128), bias_ref[j, column], F32) for j in map(int, branches)]
            m = functools.reduce(jnp.maximum, rows)
            beta_s[pl.ds(h * 16 + i, 1), :] = (m + jnp.log(sum(jnp.exp(r - m) for r in rows))) * math.log2(math.e)

    def signal_ready(i):
        pl.when(inner)(lambda: pl.semaphore_signal(ready.at[i], inc=1, device_id={'tp': tp ^ 1}, device_id_type=MESH))

    def wait_ready(i):
        with scope(f'ready{i}'):
            pl.when(outer)(lambda: pl.semaphore_wait(ready.at[i], 1))

    signal_ready(0)

    def group(g):
        low = g < 4
        return jnp.where(low, g & 1, 0), jnp.where(low, g // 2, g - 2)

    def head_number(h):
        return 2 * (tp ^ (h // 2 * 2)) + h % 2

    def project(heads, sigma, pair, kinds):
        for h in heads:
            t = head_number(h) + reverse(pair)
            x, swap = xp[side ^ sigma, pl.ds(2 * (t & 3), 2)].reshape(H, M), (t & 7) >> 2
            for t in kinds:
                y = nn(x, ws[t, :, part(h % 2, B)])
                for j in TWO:
                    piece = y[part(j, B)]
                    kv_s[h, 8 * sigma + 2 * pair + (j ^ swap), t] = (piece.T if t == VAL else piece).astype(BF)

    def phases_of(j):
        return [j % 2 + 2 * i for i in TWO], (j // 2) ^ side

    def rank_of(phase, h):
        rel = (phase - head_number(h)) & 7
        return (rel & 1) * 4 + ((rel >> 1) & 1) * 2 + (rel >> 2)

    def queries(heads, w, j):
        phases, half = phases_of(j)
        x = jnp.concatenate([xp[side, 2 * f + half] for f in phases])
        for h in heads:
            y = nn(x, ws[w, :, part(h % 2, B)]).astype(BF)
            for i, f in enumerate(phases):
                q_s[h, rank_of(f + 4 * half, h)] = y[part(i, B)]

    with scope('own_w'):
        for t in range(3):
            own_load(t).wait()
    own, partner = HEADS[:2], HEADS[2:]

    def mix(b, c):
        return jnp.concatenate([b, b, c, c], axis=1)

    def keys_of(ref, h, i, weights):
        parts = []
        n = 0
        for count, b in weights:
            def values(i=i + n, count=count):
                v = [ref[h, i + j, VAL] for j in range(count)]
                return v[0] if count == 1 else jnp.concatenate(v, axis=1)
            parts.append((values, count * B, b))
            n += count
        return (lambda: ref[h, i:i + n, KEY].reshape(n * B, B)), parts

    def chunk_tiles(p, j, kind):
        both_phases, half = phases_of(j)

        def put(h, phase, ot):
            k = 2 * (phase & 3) + half
            y = ot.T.astype(BF)
            for i in TWO:
                pl.when(p == i)(lambda i=i: o_at(k, i, 0, (h % 2) * B, B).__setitem__(..., y))

        def tile(h, phases, ranks, wide, narrow, s_ref, n_ref):
            def done(ot):
                for i, phase in enumerate(phases):
                    put(h, phase, ot[:, part(i, B)])
            return tile_steps(lambda: jnp.concatenate([q_s[h, r] for r in ranks]), wide, narrow, s_ref, n_ref, done)

        h = 2 * p + (j % 2) ^ 1
        rest = tile(h, both_phases, [rank_of(f + 4 * half, h) for f in both_phases], [keys_of(kv_s, h, i, [(2, None)]) for i in range(0, 8, 2)], [], t_scr, None)
        h = 2 * p + (j % 2)
        a = head_number(h)
        b0, b01, b1, b012, b12, b2, b0123, b123, b23, b3 = [beta_s[pl.ds(h * 16 + i, 1), :] for i in range(10)]
        phases = [a & 3, (a & 3) ^ 2]
        both = [keys_of(kv_s, h, i, [(2, b)]) for i, b in ((2, b01), (4, b0), (6, b0), (10, b1))]
        if kind == 0:
            both += [keys_of(kv_s, h, 0, [(1, mix(b0123, b01)), (1, mix(b012, b01))]), keys_of(kv_s, h, 8, [(1, mix(b123, b1)), (1, mix(b12, b1))])]
            first = [keys_of(kvp_s, h, i, [(1, b23), (1, b2)]) for i in (0, 2)] + [keys_of(kvr_s, h, i, [(2, b3)]) for i in (0, 2)]
        else:
            both += [keys_of(kv_s, h, 0, [(2, mix(b012, b01))]), keys_of(kv_s, h, 8, [(2, mix(b12, b1))])]
            first = [keys_of(kvp_s, h, i, [(2, b2)]) for i in (0, 2)]
        with scope(f'tile{kind}'):
            run_tiles([rest, tile(h, phases, [kind, rank_of(phases[1] + 4 * half, h)], both, first, s_scr, t_scr.at[:, pl.ds(0, B)])])

    def send_o(ks, p):
        @pl.when(outer)
        def _():
            for k in ks:
                for half in TWO:
                    o_copy(order(k), p, half).start()

    def step_body(t, carry):
        packed = functools.reduce(lambda x, i: jnp.where(t == i, TABLE[i], x), range(len(TABLE)), 0)
        code, n, event = packed % 16, packed // 16 % 16, packed // 256

        def step_o():
            with scope('own_kv'):
                project(own, *group(n), (KEY, VAL))

        def step_kv(t_):
            with scope(f'par_{t_}'):
                for i in TWO:
                    project(partner, *group(2 * n + i), (t_,))

        def step_q(heads, w):
            with scope(f'que_{w}'):
                queries(heads, w, n)

        def step_out(v, m):
            @pl.when(inner)
            def _():
                k = order(n)

                def halves():
                    for half in TWO:
                        with scope(f'wait_h{half}'):
                            arrived(ws.at[0, pl.ds(0, B), :], o_recv.at[k, half])
                        o_times(k, v, m, half * 128, 128)

                def whole():
                    with scope('wait_o'):
                        for half in TWO:
                            arrived(ws.at[0, pl.ds(0, B), :], o_recv.at[k, half])
                    with scope(f'out{v}'):
                        o_times(k, v, m)

                if m == 2:
                    pl.when(n == 0)(halves)
                    pl.when(n > 0)(whole)
                else:
                    with scope(f'out{v}'):
                        o_times(k, v, m)

        f = functools.partial
        kinds = {'-': lambda: None, 'O': step_o, 'P': f(step_q, own, QUE), 'K': f(step_kv, KEY), 'V': f(step_kv, VAL), 'Q': f(step_q, partner, KEY),
                 'A': lambda: chunk_tiles(n // 4, n % 4, 0), 'B': lambda: chunk_tiles(n // 4, n % 4, 1), 'R': f(step_out, 2, 2), 'L': f(step_out, 1, 1), 'N': f(step_out, 0, 1)}
        choose(code, [kinds[c] for c in KINDS])
        call = functools.partial

        events = {
            'free': [call(signal_ready, 1), call(on, inner, lambda: start(wo_own()))],
            'r0': [call(wait_ready, 0)],
            'r1': [call(wait_ready, 1)],
            'so': [call(kv_start, kvp_copy, own)],
            'po': [call(kv_wait, kvp_copy, own)],
            'sp': [call(kv_start, kvp_copy, partner)],
            'pp': [call(kv_wait, kvp_copy, partner)],
        }
        for t_, c in enumerate('kvq'):
            events['b' + c] = [call(lq_start, t_)]
            events['l' + c] = [call(ev_last, t_)]
            events['w' + c] = [call(ev_weights, t_)]
            for i in TWO:
                for e, f in zip('zxy', (ev_z, ev_xy, ev_y)):
                    events[f'{e}{c}{i}'] = [call(f, lq_copy, 2 * t_ + i)]
        for i, vs in enumerate(((2, 3), (1,), (0,))):
            events[f'b{i}'] = [call(lo_start, *vs)]
            for e, f in zip('zmxycwv', (call(ev_z, lo_copy), call(ev_near, lo_copy), call(ev_far, lo_copy), call(ev_y, lo_copy), ev_lb, ev_wo, ev_wo_ready)):
                events[f'{e}{i}'] = [call(on, inner, call(f, *vs))]
        events['v0'] += [call(on, inner, lambda: local(xp.at[1 - side, pl.ds(0, 2)], wo_sem.at[4]))]
        for v in range(4):
            events[f'd{v}'] = [call(on, outer, lambda v=v: lb_z(v).start())]
        for h in HEADS:
            for z in TWO:
                events[f's{h}{z}'] = [kvr_copy(h, z).start]
            events[f'f{h}'] = [call(kv_forward, [h])]
            events[f'g{h}'] = [call(kv_wait, kvf_copy, [h])]
        for k in ROWS:
            for p in TWO:
                events['op'[p] + str(k)] = [call(send_o, (k,), p)]
        def run(names):
            for name in names.split(','):
                where, _, name = name.rpartition(':')
                if where:
                    on(inner if where == 'i' else outer, *events[name])
                else:
                    for c in events[name]:
                        c()

        @pl.when(event > 0)
        def _():
            choose(event - 1, [functools.partial(run, names) for names in EVENTS])
        return carry

    lax.fori_loop(0, len(TABLE), step_body, None)

    all_sent(lq_ref, 0)
    all_sent(lo_ref.at[:, 0, 0], 2)
    all_sent(lb_ref.at[:, 0], 3)
    all_sent(kvp_s, 4)
    all_sent(kvr_s.at[:, pl.ds(0, 2)], 5)
    all_sent(kvr_s.at[:, pl.ds(0, 2)], 6)

    @pl.when(outer)
    def _():
        all_sent(xb, 7)

    @pl.when(inner)
    def _():
        all_sent(lo_ref.at[:, pl.ds(0, 7)], 1)
        with scope('y_sent'):
            all_sent(xp.at[side, :, :, pl.ds(H, 3 * H)], 8)
        local(xp.at[side, :, :, pl.ds(0, H)], sent.at[9])

    for seg in TWO:
        @pl.when(tp != 1 + seg)
        def _(seg=seg):
            with scope(f'recv{seg}'):
                arrived(out_ref.at[seg], y_recv.at[seg])


PROGRAM = (
    'O.i:zk0,i:zk1', 'O.i:bv,o:zk0,so', 'O.o:zk1,s00,i:xk0', 'O.o:bv,o:xk0,i:xk1,o:s01,d3', 'O.i:yk0,i:zv0', 'O.o:xk1,o:yk0,i:yk1,i:zv1,i:s01,i:bq',
    'P.o:bq', 'P.o:yk1,lk,o:zv0,d1,i:xv0', 'P.wk,o:zv1,i:xv1', 'K.i:zq0', 'K.o:xv0,i:zq1,f0', 'K.o:xv1,o:zq0,i:yv0,i:yv1,b0,b1,r0,po,g0,o:zq1',
    'T0.o0,o1,d0,o:yv0,o:yv1,lv,i:xq0,i:xq1', 'P.wv,z0,o:xq0,b2', 'V.o:xq1,o:s10,o:s11', 'V.c0,z1', 'V.yq0,yq1,m0,sp,free,lq,o:s20,o:s21,wq',
    'Q.pp,r1,x0,c1,m1,i:s10,i:s11,o:s30,o:s31', 'T4.p0,p1,x1,y0,y1,w0,w1,v0,v1', 'R', 'L', 'Q', 'T5.p2,p3,o:f1', 'R', 'L', 'Q',
    'Q.i:f1,o:g1,i:s20,i:s21', 'T2.i:g1,o:f2', 'T1.o2,o3,o:g2,o:f3', 'R.i:s30,i:s31', 'L.i:f2', 'R', 'L.i:g2', 'T6.p4,o4,p5,o5,o:g3', 'R',
    'T3.i:f3,z2,c2', 'L.i:g3', 'T7.p6,o6,p7,o7', 'R.m2,x2', 'L', 'R.y2', 'L.w2', '-.v2', 'N', 'N', 'N', 'R', 'L', 'N', 'N', 'N', 'N', 'N',
)
KINDS = '-OPKVQABRLN'


def tables():
    table, seen = [], {}
    names = tuple(dict.fromkeys(s.partition('.')[2] for s in PROGRAM if '.' in s))
    for s in PROGRAM:
        name, _, after = s.partition('.')
        kind, n = name[0], seen.get(name[0], 0)
        seen[kind] = n + 1
        if kind == 'T':
            n = int(name[1:])
            kind = 'AB'[n in (2, 3, 4, 5)]
        table.append(KINDS.index(kind) + 16 * n + 256 * (names.index(after) + 1 if after else 0))
    return table, names


TABLE, EVENTS = tables()


def main(bias, x, wk, wv, wq, w_out):
    anyspec = pl.BlockSpec(memory_space=pl.ANY)
    vmem = [((4, B, M), BF), ((B, B), BF), ((2, 8, B, M), BF), ((3, M, H), BF), ((4, 8, B, B), BF), ((4, 12, 2, B, B), BF), ((4, 4, 2, B, B), BF), ((4, 4, 2, B, B), BF),
            ((3072, H), F32), ((M, H), F32), ((64, 128), F32)]
    dma = [(4,), (9,), (5,), (10,), (6, 5), (4, 5), (4, 2), (3, 4), (8, 2), (2,)]
    return pl.pallas_call(
        main_kernel,
        in_specs=[pl.BlockSpec(memory_space=pltpu.SMEM)] + [anyspec] * 5,
        out_specs=[anyspec] * 4,
        out_shape=[jax.ShapeDtypeStruct(s, BF) for s in ((2, 8, B, H), (8, 6, B, B), (4, 8, 2, 64, H), (4, 2, B, H))],
        scratch_shapes=[pltpu.VMEM(*v) for v in vmem] + [pltpu.SemaphoreType.DMA(d) for d in dma] + [pltpu.SemaphoreType.REGULAR((2,))],
        compiler_params=params(collective_id=0, has_side_effects=True),
        cost_estimate=pl.CostEstimate(flops=10**11, bytes_accessed=10**8, transcendentals=0),
        name='main',
    )(bias, x, wk, wv, wq, w_out)[0]


def solution(mesh):
    def device_fn(hidden, w_query, w_key, w_value, w_out, branch_bias):
        return unpermute(main(branch_bias, hidden, w_key, w_value, w_query, w_out))

    return jax.shard_map(device_fn, mesh=mesh, in_specs=(P(('dp', 'sp'), None), P(None, 'tp'), P(None, 'tp'), P(None, 'tp'), P('tp', None), P(None, None)), out_specs=P(('dp', 'sp'), 'tp'), check_vma=False)
```

```python
import functools
import math

import jax
import jax.numpy as jnp
from jax import lax
from jax.experimental import pallas as pl
from jax.experimental.pallas import tpu as pltpu
from jax.sharding import PartitionSpec as P

MESH = pl.DeviceIdType.MESH
BF = jnp.bfloat16
F32 = jnp.float32
B, H, M = 256, 512, 2048
KAPPA = math.log2(math.e) / 16
VMEM = 66_900_000
SLOT = (0, 4, 2, 6, 1, 5, 3, 7)
KEY, VAL, QUE = range(3)
HEADS = range(4)
TWO = range(2)
ROWS = range(8)


def nn(a, b):
    return lax.dot_general(a, b, (((1,), (0,)), ((), ())), preferred_element_type=F32)


def nt(a, b):
    return lax.dot_general(a, b, (((1,), (1,)), ((), ())), preferred_element_type=F32)


def params(**kw):
    return pltpu.CompilerParams(vmem_limit_bytes=VMEM, **kw)


def ds(start, size, align=128):
    return pl.ds(pl.multiple_of(start, align), size)


def part(i, size):
    return slice(i * size, i * size + size)


def phase_matrix(transposed):
    r = lax.broadcasted_iota(jnp.int32, (B, B), int(transposed))
    p = lax.broadcasted_iota(jnp.int32, (B, B), int(not transposed))
    k = r // 32
    return (p == (r % 32) * 8 + k // 2 + 4 * (k % 2)).astype(F32).astype(BF)


def unpermute_kernel(y_ref, o_ref, y_s, o_s, load, store):
    pieces = [(s, j) for s in TWO for j in range(4)]

    def get(i):
        s, j = pieces[i]
        return pltpu.make_async_copy(y_ref.at[s, :, pl.ds(j * 64, 64)], y_s.at[i], load.at[i])

    def put(i):
        return pltpu.make_async_copy(o_s.at[i], o_ref.at[pl.ds(i * H, H)], store.at[i])

    for i in ROWS:
        get(i).start()
    pm = phase_matrix(True)
    for i in range(0, 8, 2):
        group = (i, i + 1)
        for k in group:
            get(k).wait()
        for k in group:
            for j in TWO:
                o_s[k, part(j, B), :] = nn(pm, y_s[k, :, part(j, 32), :].reshape(B, H)).astype(BF)
        for k in group:
            put(k).start()
    for i in ROWS:
        put(i).wait()


def unpermute(y):
    anyspec = pl.BlockSpec(memory_space=pl.ANY)
    return pl.pallas_call(
        unpermute_kernel,
        in_specs=[anyspec],
        out_specs=anyspec,
        out_shape=jax.ShapeDtypeStruct((2 * M, H), BF),
        scratch_shapes=[pltpu.VMEM((8, 8, 64, H), BF), pltpu.VMEM((8, H, H), BF), pltpu.SemaphoreType.DMA((8,)), pltpu.SemaphoreType.DMA((8,))],
        compiler_params=params(),
        name='unpermute',
    )(y)


def tile_steps(q, wide, narrow, s_ref, n_ref, done):
    st = {}
    logits, sums = [], []

    def add(name, x):
        st[name] = st[name] + x if name in st else x

    for groups, ref in ((wide, s_ref), (narrow, n_ref)):
        off = 0
        for keys, parts in groups:
            def qk(keys=keys, parts=parts, off=off, ref=ref):
                s = nt(keys(), q() if ref is s_ref else q()[:B])
                o = 0
                for _, n, b in parts:
                    piece = s[o:o + n]
                    ref[pl.ds(off + o, n), :] = piece
                    t = jnp.max(piece, axis=0, keepdims=True) * KAPPA
                    if b is not None:
                        t = t + fit(b, t)
                    if ref is n_ref:
                        t = jnp.concatenate([t, st['top'][:, B:]], axis=1)
                    st['top'] = jnp.maximum(st['top'], t) if 'top' in st else t
                    o += n
            logits.append(qk)
            for v, n, b in parts:
                def sv(v=v, n=n, b=b, off=off, ref=ref):
                    top = st['top'] if ref is s_ref else st['top'][:, :B]
                    e = jnp.exp2(ref[pl.ds(off, n), :] * KAPPA - (top if b is None else top - fit(b, top)))
                    name = 'w' if ref is s_ref else 'n'
                    add('l' + name, jnp.sum(e, axis=0, keepdims=True))
                    add('o' + name, nn(v(), e.astype(BF)))
                sums.append(sv)
                off += n

    def finish():
        o, l = st['ow'], st['lw']
        if narrow:
            o = jnp.concatenate([o[:, :B] + st['on'], o[:, B:]], axis=1)
            l = jnp.concatenate([l[:, :B] + st['ln'], l[:, B:]], axis=1)
        done(o / l)

    return logits, sums + [finish]


def fit(b, like):
    return b if b.shape == like.shape else jnp.concatenate([b] * (like.shape[1] // 128), axis=1)


def interleave(a, b):
    i = j = 0
    while i < len(a) or j < len(b):
        if j >= len(b) or (i < len(a) and i * len(b) <= j * len(a)):
            a[i]()
            i += 1
        else:
            b[j]()
            j += 1


def run_tiles(tiles):
    before = []
    for logits, sums in tiles:
        interleave(logits, before)
        before = sums
    interleave([], before)


def choose(x, cases):
    def among(lo, hi):
        mid = (lo + hi) // 2
        if hi - lo == 1:
            cases[lo]()
        else:
            pl.when(x < mid)(lambda: among(lo, mid))
            pl.when(x >= mid)(lambda: among(mid, hi))
    among(0, len(cases))


def on(cond, *calls):
    @pl.when(cond)
    def _():
        for c in calls:
            c()


def scope(name):
    return jax.named_scope(name)


def main_kernel(bias_ref, x_ref, wk_ref, wv_ref, wq_ref, wout_ref, out_ref, lq_ref, lo_ref, lb_ref,
                xb, pm, xp, ws, q_s, kv_s, kvp_s, kvr_s, s_scr, t_scr,
                beta_s, x_sem, w_sem, wo_sem, sent, lq_recv, lo_recv, lb_recv, kv_recv, o_recv, y_recv, ready):
    dp, tp, sp = lax.axis_index('dp'), lax.axis_index('tp'), lax.axis_index('sp')
    idx = dp * 4 + sp
    side = tp // 2
    inner = (tp == 1) | (tp == 2)
    outer = jnp.logical_not(inner)
    W = (wk_ref, wv_ref, wq_ref)
    peer_x, peer_y, peer_c = {'dp': dp ^ 1}, {'sp': sp ^ 2}, {'sp': sp ^ 1}

    def remote(src, dst, ss, rs, dev):
        return pltpu.make_async_remote_copy(src_ref=src, dst_ref=dst, send_sem=ss, recv_sem=rs, device_id=dev, device_id_type=MESH)

    def lq_copy(t, src, dst, dev):
        return remote(lq_ref.at[src, t], lq_ref.at[dst, t], sent.at[0], lq_recv.at[t, min(dst, 4)], dev)

    def lq_z(t):
        return remote(W[t // 2].at[ds(idx * B, B), pl.ds(t % 2 * B, B)], lq_ref.at[0, t], sent.at[0], lq_recv.at[t, 0], {'tp': tp ^ 2})

    def lq_start(t):
        for i in TWO:
            lq_z(2 * t + i).start()

    def lo_copy(v, src, dst, dev):
        return remote(lo_ref.at[v, src], lo_ref.at[v, dst], sent.at[1], lo_recv.at[v, min(dst, 4)], dev)

    def lo_z(v):
        dst = 2 - side
        b = (tp ^ dst) - 2
        return remote(wout_ref.at[ds(idx * 64, 64, 64), ds((dst ^ v) * H, H)], lo_ref.at[v, 0, b], sent.at[2], lo_recv.at[v, 0], {'tp': dst})

    def lb_z(v):
        return remote(wout_ref.at[ds(sp % 2 * B, B), ds((tp ^ 1 ^ v) * H, H)], lb_ref.at[v, sp % 2], sent.at[3], lb_recv.at[v, 0], {'tp': tp ^ 1})

    def lb_core(v):
        return remote(lb_ref.at[v, sp % 2], lb_ref.at[v, sp % 2], sent.at[3], lb_recv.at[v, 1], peer_c)

    def lo_start(*vs):
        for v in vs:
            lo_z(v).start()

    def arrived(ref, sem):
        remote(ref, ref, sent.at[0], sem, peer_c).wait_recv()

    def all_sent(ref, i):
        remote(ref, ref, sent.at[i], sent.at[i], peer_c).wait_send()

    def lo_zwait(v):
        arrived(lo_ref.at[v, 0], lo_recv.at[v, 0])

    def hop(copy, p, i):
        near, far, n = (peer_x, peer_y, 1) if copy is lo_copy and p in (1, 2) else (peer_y, peer_x, 2)
        f = 3 - n
        return copy(p, *((0, n, near), (0, f, far), (0, 4, peer_c), (n, 3, far), (n, 4 + n, peer_c), (f, 4 + f, peer_c), (3, 7, peer_c))[i])

    def ev_z(copy, *ps):
        for p in ps:
            with scope(f'z_{copy.__name__}{p}'):
                lq_z(p).wait_recv() if copy is lq_copy else lo_zwait(p)
            hop(copy, p, 0).start()
        for p in ps:
            hop(copy, p, 1).start()
            hop(copy, p, 2).start()

    def ev_near(copy, *ps):
        for p in ps:
            with scope(f'n_{copy.__name__}{p}'):
                hop(copy, p, 0).wait_recv()
            hop(copy, p, 3).start()
            hop(copy, p, 4).start()

    def ev_far(copy, *ps):
        for p in ps:
            with scope(f'f_{copy.__name__}{p}'):
                hop(copy, p, 1).wait_recv()
            hop(copy, p, 5).start()

    def ev_xy(copy, *ps):
        ev_near(copy, *ps)
        ev_far(copy, *ps)

    def ev_y(copy, *ps):
        for p in ps:
            with scope(f'y_{copy.__name__}{p}'):
                hop(copy, p, 3).wait_recv()
            hop(copy, p, 6).start()
            if copy is lq_copy and p >= 2:
                start(w_load(p, SLOT[:4]))

    def ev_done(copy, *ps):
        for p in ps:
            with scope(f'c_{copy.__name__}{p}'):
                if copy is lq_copy:
                    arrived(lq_ref.at[pl.ds(4, 4), p], lq_recv.at[p, 4])
                else:
                    arrived(lo_ref.at[p, pl.ds(4, 4)], lo_recv.at[p, 4])

    def w_load(p, slots):
        return [pltpu.make_async_copy(lq_ref.at[SLOT.index(m), p], ws.at[p // 2 % 2, ds((idx ^ m) * B, B), pl.ds(p % 2 * B, B)], w_sem.at[p]) for m in slots]

    def own_load(t):
        return pltpu.make_async_copy(W[t], ws.at[t], w_sem.at[6 + t])

    def start(copies):
        for c in copies:
            c.start()

    def wait(copies):
        for c in copies:
            c.wait()

    def ev_last(t):
        pieces = [2 * t + i for i in TWO]
        ev_done(lq_copy, *pieces)
        for p in pieces:
            start(w_load(p, SLOT[4:] if t else SLOT))

    def local(ref, sem):
        pltpu.make_async_copy(ref, ref, sem).wait()

    def ev_weights(t):
        with scope(f'load{t}'):
            for i in TWO:
                local(ws.at[t % 2, :, pl.ds(i * B, B)], w_sem.at[2 * t + i])

    def ev_wo(*vs):
        ev_done(lo_copy, *vs)
        for v in vs:
            lb_core(v).wait_recv()
        start(wo_load(*vs))

    def ev_wo_ready(*vs):
        with scope(f'wo{vs[0]}'):
            for v in vs:
                local(xp.at[1 - side, pl.ds(2, 6), :, pl.ds((v ^ 2) * H, H)], wo_sem.at[v])

    def ev_lb(*vs):
        for v in vs:
            with scope(f'lb{v}'):
                lb_z(v).wait_recv()
            lb_core(v).start()

    wo = xp.at[1 - side]

    def wo_own():
        return [pltpu.make_async_copy(wout_ref.at[pl.ds(r * B, B), pl.ds(c * H, H)], xp.at[1 - side, r, :, ds((c ^ tp ^ 2) * H, H)], wo_sem.at[4])
                for r in TWO for c in range(4)]

    def wo_load(*vs):
        out = []
        for v in vs:
            cols = pl.ds((v ^ 2) * H, H)
            for s, m in enumerate(SLOT):
                row = (idx ^ m) * 64
                for b in TWO:
                    out.append(pltpu.make_async_copy(lo_ref.at[v, s, b], xp.at[1 - side, 4 + 2 * b + row // B, ds(row % B, 64, 64), cols], wo_sem.at[v]))
            for r in TWO:
                out.append(pltpu.make_async_copy(lb_ref.at[v, r], xp.at[1 - side, 2 + r, :, cols], wo_sem.at[v]))
        return out

    def kvp_copy(h, s):
        return remote(kv_s.at[h, pl.ds(8 * s, 2)], kvp_s.at[h, pl.ds(2 * s, 2)], sent.at[4], kv_recv.at[0, h], peer_c)

    def kvr_copy(h, s):
        return remote(kv_s.at[h, 8 * s], kvr_s.at[h, s], sent.at[5], kv_recv.at[1, h], peer_y)

    def kvf_copy(h, s):
        return remote(kvr_s.at[h, s], kvr_s.at[h, 2 + s], sent.at[6], kv_recv.at[2, h], peer_c)

    def kv_start(copy, heads):
        for h in heads:
            for s in TWO:
                copy(h, s).start()

    def kv_wait(copy, heads):
        with scope(f'w_{copy.__name__}{heads[0]}'):
            for h in heads:
                i = (kvp_copy, kvr_copy, kvf_copy).index(copy)
                arrived((kvp_s.at[h], kvr_s.at[h, pl.ds(0, 2)], kvr_s.at[h, pl.ds(2, 2)])[i], kv_recv.at[i, h])

    def kv_forward(heads):
        kv_wait(kvr_copy, heads)
        kv_start(kvf_copy, heads)

    def reverse(i):
        return (i % 2) * 2 + i // 2

    def order(n):
        return 2 * reverse(n % 4) + ((n // 4) ^ side)

    def o_at(k, p, theirs, col, size, row=0, rows=B):
        if p:
            return ws.at[1 + theirs, ds(k * B + row, rows), ds(col, size)]
        return xb.at[k // 2, pl.ds(row, rows), ds((k % 2) * 1024 + theirs * H + col, size)]

    def o_copy(k, p, half):
        row = half * 128
        return remote(o_at(k, p, 0, 0, H, row, 128), o_at(k, p, 1, 0, H, row, 128), sent.at[7], o_recv.at[k, half], {'tp': tp ^ 1})

    def o_times(k, v, n, row=0, rows=B):
        cols = pl.ds((v ^ 2) * H, n * H)
        y = nn(xb[k // 2, pl.ds(row, rows), ds((k % 2) * 1024, 1024)], wo[0:4, :, cols].reshape(1024, n * H))
        for i in TWO:
            y = y + nn(ws[1 + i, ds(k * B + row, rows), :], wo[part(2 + i, 2), :, cols].reshape(H, n * H))
        y = y.astype(BF)
        for i in range(n):
            y_src(k, v + i, row, rows)[...] = y[:, part(i, H)]
            y_copy(k, v + i, side, row, rows).start() if v else y_local(k).start()

    def y_src(k, v, row=0, rows=B):
        return xp.at[side, k, pl.ds(row, rows), pl.ds(v * H, H)]

    def y_copy(k, v, seg, row, rows):
        return remote(y_src(k, v, row, rows), out_ref.at[seg, k, pl.ds(row, rows)], sent.at[8], y_recv.at[seg], {'tp': tp ^ v})

    def y_local(k):
        return pltpu.make_async_copy(y_src(k, 0), out_ref.at[side, k], sent.at[9])

    def x_copy(j):
        return pltpu.make_async_copy(x_ref.at[ds(j * B, B), :], xb.at[lax.rem(j, 4)], x_sem.at[lax.rem(j, 4)])

    for j in range(4):
        x_copy(j).start()
    barrier = pltpu.get_barrier_semaphore()
    peers = [{'tp': tp ^ 1}, {'tp': tp ^ 2}, {'tp': tp ^ 3}, peer_x, peer_y, peer_c]
    for dev in peers:
        pl.semaphore_signal(barrier, inc=1, device_id=dev, device_id_type=MESH)
    for t in range(3):
        own_load(t).start()

    pm[...] = phase_matrix(False)

    def permute_body(j, carry):
        x_copy(j).wait()
        y = nn(pm[...], xb[lax.rem(j, 4)]).astype(BF).reshape(8, 32, M)
        xp[j // 8, :, ds(lax.rem(j, 8) * 32, 32, 32), :] = y
        pl.when(j < 12)(lambda: x_copy(j + 4).start())

        @pl.when(j == 7)
        def _():
            with scope('barrier'):
                pl.semaphore_wait(barrier, len(peers))
            lq_start(KEY)
            on(outer, lb_z(2).start)
        return carry

    with scope('permute'):
        lax.fori_loop(0, 16, permute_body, None)

    for h in HEADS:
        column = 2 * (tp ^ (h // 2 * 2)) + h % 2
        for i, branches in enumerate(('0', '01', '1', '012', '12', '2', '0123', '123', '23', '3')):
            rows = [jnp.full((1, 128), bias_ref[j, column], F32) for j in map(int, branches)]
            m = functools.reduce(jnp.maximum, rows)
            beta_s[pl.ds(h * 16 + i, 1), :] = (m + jnp.log(sum(jnp.exp(r - m) for r in rows))) * math.log2(math.e)

    def signal_ready(i):
        pl.when(inner)(lambda: pl.semaphore_signal(ready.at[i], inc=1, device_id={'tp': tp ^ 1}, device_id_type=MESH))

    def wait_ready(i):
        with scope(f'ready{i}'):
            pl.when(outer)(lambda: pl.semaphore_wait(ready.at[i], 1))

    signal_ready(0)

    def group(g):
        low = g < 4
        return jnp.where(low, g & 1, 0), jnp.where(low, g // 2, g - 2)

    def head_number(h):
        return 2 * (tp ^ (h // 2 * 2)) + h % 2

    def project(heads, sigma, pair, kinds):
        for h in heads:
            t = head_number(h) + reverse(pair)
            x, swap = xp[side ^ sigma, pl.ds(2 * (t & 3), 2)].reshape(H, M), (t & 7) >> 2
            for t in kinds:
                y = nn(x, ws[t, :, part(h % 2, B)])
                for j in TWO:
                    piece = y[part(j, B)]
                    kv_s[h, 8 * sigma + 2 * pair + (j ^ swap), t] = (piece.T if t == VAL else piece).astype(BF)

    def phases_of(j):
        return [j % 2 + 2 * i for i in TWO], (j // 2) ^ side

    def rank_of(phase, h):
        rel = (phase - head_number(h)) & 7
        return (rel & 1) * 4 + ((rel >> 1) & 1) * 2 + (rel >> 2)

    def queries(heads, w, j):
        phases, half = phases_of(j)
        x = jnp.concatenate([xp[side, 2 * f + half] for f in phases])
        for h in heads:
            y = nn(x, ws[w, :, part(h % 2, B)]).astype(BF)
            for i, f in enumerate(phases):
                q_s[h, rank_of(f + 4 * half, h)] = y[part(i, B)]

    with scope('own_w'):
        for t in range(3):
            own_load(t).wait()
    own, partner = HEADS[:2], HEADS[2:]

    def mix(b, c):
        return jnp.concatenate([b, b, c, c], axis=1)

    def keys_of(ref, h, i, weights):
        parts = []
        n = 0
        for count, b in weights:
            def values(i=i + n, count=count):
                v = [ref[h, i + j, VAL] for j in range(count)]
                return v[0] if count == 1 else jnp.concatenate(v, axis=1)
            parts.append((values, count * B, b))
            n += count
        return (lambda: ref[h, i:i + n, KEY].reshape(n * B, B)), parts

    def chunk_tiles(p, j, kind):
        both_phases, half = phases_of(j)

        def put(h, phase, ot):
            k = 2 * (phase & 3) + half
            y = ot.T.astype(BF)
            for i in TWO:
                pl.when(p == i)(lambda i=i: o_at(k, i, 0, (h % 2) * B, B).__setitem__(..., y))

        def tile(h, phases, ranks, wide, narrow, s_ref, n_ref):
            def done(ot):
                for i, phase in enumerate(phases):
                    put(h, phase, ot[:, part(i, B)])
            return tile_steps(lambda: jnp.concatenate([q_s[h, r] for r in ranks]), wide, narrow, s_ref, n_ref, done)

        h = 2 * p + (j % 2) ^ 1
        rest = tile(h, both_phases, [rank_of(f + 4 * half, h) for f in both_phases], [keys_of(kv_s, h, i, [(2, None)]) for i in range(0, 8, 2)], [], t_scr, None)
        h = 2 * p + (j % 2)
        a = head_number(h)
        b0, b01, b1, b012, b12, b2, b0123, b123, b23, b3 = [beta_s[pl.ds(h * 16 + i, 1), :] for i in range(10)]
        phases = [a & 3, (a & 3) ^ 2]
        both = [keys_of(kv_s, h, i, [(2, b)]) for i, b in ((2, b01), (4, b0), (6, b0), (10, b1))]
        if kind == 0:
            both += [keys_of(kv_s, h, 0, [(1, mix(b0123, b01)), (1, mix(b012, b01))]), keys_of(kv_s, h, 8, [(1, mix(b123, b1)), (1, mix(b12, b1))])]
            first = [keys_of(kvp_s, h, i, [(1, b23), (1, b2)]) for i in (0, 2)] + [keys_of(kvr_s, h, i, [(2, b3)]) for i in (0, 2)]
        else:
            both += [keys_of(kv_s, h, 0, [(2, mix(b012, b01))]), keys_of(kv_s, h, 8, [(2, mix(b12, b1))])]
            first = [keys_of(kvp_s, h, i, [(2, b2)]) for i in (0, 2)]
        with scope(f'tile{kind}'):
            run_tiles([rest, tile(h, phases, [kind, rank_of(phases[1] + 4 * half, h)], both, first, s_scr, t_scr.at[:, pl.ds(0, B)])])

    def send_o(ks, p):
        @pl.when(outer)
        def _():
            for k in ks:
                for half in TWO:
                    o_copy(order(k), p, half).start()

    def step_body(t, carry):
        packed = functools.reduce(lambda x, i: jnp.where(t == i, TABLE[i], x), range(len(TABLE)), 0)
        code, n, event = packed % 16, packed // 16 % 16, packed // 256

        def step_o():
            with scope('own_kv'):
                project(own, *group(n), (KEY, VAL))

        def step_kv(t_):
            with scope(f'par_{t_}'):
                for i in TWO:
                    project(partner, *group(2 * n + i), (t_,))

        def step_q(heads, w):
            with scope(f'que_{w}'):
                queries(heads, w, n)

        def step_out(v, m):
            @pl.when(inner)
            def _():
                k = order(n)

                def halves():
                    for half in TWO:
                        with scope(f'wait_h{half}'):
                            arrived(ws.at[0, pl.ds(0, B), :], o_recv.at[k, half])
                        o_times(k, v, m, half * 128, 128)

                def whole():
                    with scope('wait_o'):
                        for half in TWO:
                            arrived(ws.at[0, pl.ds(0, B), :], o_recv.at[k, half])
                    with scope(f'out{v}'):
                        o_times(k, v, m)

                if m == 2:
                    pl.when(n == 0)(halves)
                    pl.when(n > 0)(whole)
                else:
                    with scope(f'out{v}'):
                        o_times(k, v, m)

        f = functools.partial
        kinds = {'-': lambda: None, 'O': step_o, 'P': f(step_q, own, QUE), 'K': f(step_kv, KEY), 'V': f(step_kv, VAL), 'Q': f(step_q, partner, KEY),
                 'A': lambda: chunk_tiles(n // 4, n % 4, 0), 'B': lambda: chunk_tiles(n // 4, n % 4, 1), 'R': f(step_out, 2, 2), 'L': f(step_out, 1, 1), 'N': f(step_out, 0, 1)}
        choose(code, [kinds[c] for c in KINDS])
        call = functools.partial

        events = {
            'free': [call(signal_ready, 1), call(on, inner, lambda: start(wo_own()))],
            'r0': [call(wait_ready, 0)],
            'r1': [call(wait_ready, 1)],
            'so': [call(kv_start, kvp_copy, own)],
            'po': [call(kv_wait, kvp_copy, own)],
            'sp': [call(kv_start, kvp_copy, partner)],
            'pp': [call(kv_wait, kvp_copy, partner)],
        }
        for t_, c in enumerate('kvq'):
            events['b' + c] = [call(lq_start, t_)]
            events['l' + c] = [call(ev_last, t_)]
            events['w' + c] = [call(ev_weights, t_)]
            for i in TWO:
                for e, f in zip('zxy', (ev_z, ev_xy, ev_y)):
                    events[f'{e}{c}{i}'] = [call(f, lq_copy, 2 * t_ + i)]
        for i, vs in enumerate(((2, 3), (1,), (0,))):
            events[f'b{i}'] = [call(lo_start, *vs)]
            for e, f in zip('zmxycwv', (call(ev_z, lo_copy), call(ev_near, lo_copy), call(ev_far, lo_copy), call(ev_y, lo_copy), ev_lb, ev_wo, ev_wo_ready)):
                events[f'{e}{i}'] = [call(on, inner, call(f, *vs))]
        events['v0'] += [call(on, inner, lambda: local(xp.at[1 - side, pl.ds(0, 2)], wo_sem.at[4]))]
        for v in range(4):
            events[f'd{v}'] = [call(on, outer, lambda v=v: lb_z(v).start())]
        for h in HEADS:
            for z in TWO:
                events[f's{h}{z}'] = [kvr_copy(h, z).start]
            events[f'f{h}'] = [call(kv_forward, [h])]
            events[f'g{h}'] = [call(kv_wait, kvf_copy, [h])]
        for k in ROWS:
            for p in TWO:
                events['op'[p] + str(k)] = [call(send_o, (k,), p)]
        def run(names):
            for name in names.split(','):
                where, _, name = name.rpartition(':')
                if where:
                    on(inner if where == 'i' else outer, *events[name])
                else:
                    for c in events[name]:
                        c()

        @pl.when(event > 0)
        def _():
            choose(event - 1, [functools.partial(run, names) for names in EVENTS])
        return carry

    lax.fori_loop(0, len(TABLE), step_body, None)

    all_sent(lq_ref, 0)
    all_sent(lo_ref.at[:, 0, 0], 2)
    all_sent(lb_ref.at[:, 0], 3)
    all_sent(kvp_s, 4)
    all_sent(kvr_s.at[:, pl.ds(0, 2)], 5)
    all_sent(kvr_s.at[:, pl.ds(0, 2)], 6)

    @pl.when(outer)
    def _():
        all_sent(xb, 7)

    @pl.when(inner)
    def _():
        all_sent(lo_ref.at[:, pl.ds(0, 7)], 1)
        with scope('y_sent'):
            all_sent(xp.at[side, :, :, pl.ds(H, 3 * H)], 8)
        local(xp.at[side, :, :, pl.ds(0, H)], sent.at[9])

    for seg in TWO:
        @pl.when(tp != 1 + seg)
        def _(seg=seg):
            with scope(f'recv{seg}'):
                arrived(out_ref.at[seg], y_recv.at[seg])


PROGRAM = (
    'O.i:zk0,i:zk1', 'O.i:bv,o:zk0', 'O.o:zk1,s00,i:xk0', 'O.o:bv,o:xk0,i:xk1,o:s01,d3', 'O.o:xk1,i:yk0,i:zv0', 'O.o:yk0,i:yk1,i:zv1,i:s01,i:bq',
    'P.o:bq,so', 'P.o:yk1,lk,o:zv0,d1,i:xv0', 'P.wk,o:zv1,i:xv1', 'K.i:zq0', 'K.o:xv0,i:zq1,f0', 'K.o:xv1,o:zq0,i:yv0,i:yv1,b0,b1,r0,po,g0,o:zq1',
    'T0.o0,o1,d0,o:yv0,o:yv1,lv,i:xq0,i:xq1', 'P.wv,z0,o:xq0,b2', 'V.o:xq1,o:s10,o:s11', 'V.c0', 'V.yq0,yq1,m0,z1,sp,free,lq,o:s20,o:s21,wq',
    'Q.pp,r1,x0,c1,i:s10,i:s11,o:s30,o:s31', 'T4.p0,p1,m1,x1,y0,w0,v0', 'R.y1,w1', 'Q.v1', 'L', 'T5.p2,p3,o:f1', 'R', 'L', 'Q',
    'Q.i:f1,o:g1,i:s20,i:s21', 'T2.i:g1,o:f2', 'T1.o2,o3,o:g2,o:f3', 'R.i:s30,i:s31', 'L.i:f2', 'R', 'L.i:g2', 'T6.p4,o4,p5,o5,o:g3', 'R',
    'T3.i:f3,z2,c2', 'L.i:g3', 'T7.p6,o6,p7,o7', 'R.m2,x2', 'L', 'R.y2', 'L.w2', '-.v2', 'N', 'N', 'N', 'R', 'L', 'N', 'N', 'N', 'N', 'N',
)
KINDS = '-OPKVQABRLN'


def tables():
    table, seen = [], {}
    names = tuple(dict.fromkeys(s.partition('.')[2] for s in PROGRAM if '.' in s))
    for s in PROGRAM:
        name, _, after = s.partition('.')
        kind, n = name[0], seen.get(name[0], 0)
        seen[kind] = n + 1
        if kind == 'T':
            n = int(name[1:])
            kind = 'AB'[n in (2, 3, 4, 5)]
        table.append(KINDS.index(kind) + 16 * n + 256 * (names.index(after) + 1 if after else 0))
    return table, names


TABLE, EVENTS = tables()


def main(bias, x, wk, wv, wq, w_out):
    anyspec = pl.BlockSpec(memory_space=pl.ANY)
    vmem = [((4, B, M), BF), ((B, B), BF), ((2, 8, B, M), BF), ((3, M, H), BF), ((4, 8, B, B), BF), ((4, 12, 2, B, B), BF), ((4, 4, 2, B, B), BF), ((4, 4, 2, B, B), BF),
            ((3072, H), F32), ((M, H), F32), ((64, 128), F32)]
    dma = [(4,), (9,), (5,), (10,), (6, 5), (4, 5), (4, 2), (3, 4), (8, 2), (2,)]
    return pl.pallas_call(
        main_kernel,
        in_specs=[pl.BlockSpec(memory_space=pltpu.SMEM)] + [anyspec] * 5,
        out_specs=[anyspec] * 4,
        out_shape=[jax.ShapeDtypeStruct(s, BF) for s in ((2, 8, B, H), (8, 6, B, B), (4, 8, 2, 64, H), (4, 2, B, H))],
        scratch_shapes=[pltpu.VMEM(*v) for v in vmem] + [pltpu.SemaphoreType.DMA(d) for d in dma] + [pltpu.SemaphoreType.REGULAR((2,))],
        compiler_params=params(collective_id=0, has_side_effects=True),
        cost_estimate=pl.CostEstimate(flops=10**11, bytes_accessed=10**8, transcendentals=0),
        name='main',
    )(bias, x, wk, wv, wq, w_out)[0]


def solution(mesh):
    def device_fn(hidden, w_query, w_key, w_value, w_out, branch_bias):
        return unpermute(main(branch_bias, hidden, w_key, w_value, w_query, w_out))

    return jax.shard_map(device_fn, mesh=mesh, in_specs=(P(('dp', 'sp'), None), P(None, 'tp'), P(None, 'tp'), P(None, 'tp'), P('tp', None), P(None, None)), out_specs=P(('dp', 'sp'), 'tp'), check_vma=False)
```

```python
import functools
import math

import jax
import jax.numpy as jnp
from jax import lax
from jax.experimental import pallas as pl
from jax.experimental.pallas import tpu as pltpu
from jax.sharding import PartitionSpec as P

MESH = pl.DeviceIdType.MESH
BF = jnp.bfloat16
F32 = jnp.float32
B, H, M = 256, 512, 2048
KAPPA = math.log2(math.e) / 16
VMEM = 66_900_000
SLOT = (0, 4, 2, 6, 1, 5, 3, 7)
KEY, VAL, QUE = range(3)
HEADS = range(4)
TWO = range(2)
ROWS = range(8)


def nn(a, b):
    return lax.dot_general(a, b, (((1,), (0,)), ((), ())), preferred_element_type=F32)


def nt(a, b):
    return lax.dot_general(a, b, (((1,), (1,)), ((), ())), preferred_element_type=F32)


def params(**kw):
    return pltpu.CompilerParams(vmem_limit_bytes=VMEM, **kw)


def ds(start, size, align=128):
    return pl.ds(pl.multiple_of(start, align), size)


def part(i, size):
    return slice(i * size, i * size + size)


def phase_matrix(transposed):
    r = lax.broadcasted_iota(jnp.int32, (B, B), int(transposed))
    p = lax.broadcasted_iota(jnp.int32, (B, B), int(not transposed))
    k = r // 32
    return (p == (r % 32) * 8 + k // 2 + 4 * (k % 2)).astype(F32).astype(BF)


def unpermute_kernel(y_ref, o_ref, y_s, o_s, load, store):
    pieces = [(s, j) for s in TWO for j in range(4)]

    def get(i):
        s, j = pieces[i]
        return pltpu.make_async_copy(y_ref.at[s, :, pl.ds(j * 64, 64)], y_s.at[i], load.at[i])

    def put(i):
        return pltpu.make_async_copy(o_s.at[i], o_ref.at[pl.ds(i * H, H)], store.at[i])

    for i in ROWS:
        get(i).start()
    pm = phase_matrix(True)
    for i in range(0, 8, 2):
        group = (i, i + 1)
        for k in group:
            get(k).wait()
        for k in group:
            for j in TWO:
                o_s[k, part(j, B), :] = nn(pm, y_s[k, :, part(j, 32), :].reshape(B, H)).astype(BF)
        for k in group:
            put(k).start()
    for i in ROWS:
        put(i).wait()


def unpermute(y):
    anyspec = pl.BlockSpec(memory_space=pl.ANY)
    return pl.pallas_call(
        unpermute_kernel,
        in_specs=[anyspec],
        out_specs=anyspec,
        out_shape=jax.ShapeDtypeStruct((2 * M, H), BF),
        scratch_shapes=[pltpu.VMEM((8, 8, 64, H), BF), pltpu.VMEM((8, H, H), BF), pltpu.SemaphoreType.DMA((8,)), pltpu.SemaphoreType.DMA((8,))],
        compiler_params=params(),
        name='unpermute',
    )(y)


def tile_steps(q, wide, narrow, s_ref, n_ref, done):
    st = {}
    logits, sums = [], []

    def add(name, x):
        st[name] = st[name] + x if name in st else x

    for groups, ref in ((wide, s_ref), (narrow, n_ref)):
        off = 0
        for keys, parts in groups:
            def qk(keys=keys, parts=parts, off=off, ref=ref):
                s = nt(keys(), q() if ref is s_ref else q()[:B])
                o = 0
                for _, n, b in parts:
                    piece = s[o:o + n]
                    ref[pl.ds(off + o, n), :] = piece
                    t = jnp.max(piece, axis=0, keepdims=True) * KAPPA
                    if b is not None:
                        t = t + fit(b, t)
                    if ref is n_ref:
                        t = jnp.concatenate([t, st['top'][:, B:]], axis=1)
                    st['top'] = jnp.maximum(st['top'], t) if 'top' in st else t
                    o += n
            logits.append(qk)
            for v, n, b in parts:
                def sv(v=v, n=n, b=b, off=off, ref=ref):
                    top = st['top'] if ref is s_ref else st['top'][:, :B]
                    e = jnp.exp2(ref[pl.ds(off, n), :] * KAPPA - (top if b is None else top - fit(b, top)))
                    name = 'w' if ref is s_ref else 'n'
                    add('l' + name, jnp.sum(e, axis=0, keepdims=True))
                    add('o' + name, nn(v(), e.astype(BF)))
                sums.append(sv)
                off += n

    def finish():
        o, l = st['ow'], st['lw']
        if narrow:
            o = jnp.concatenate([o[:, :B] + st['on'], o[:, B:]], axis=1)
            l = jnp.concatenate([l[:, :B] + st['ln'], l[:, B:]], axis=1)
        done(o / l)

    return logits, sums + [finish]


def fit(b, like):
    return b if b.shape == like.shape else jnp.concatenate([b] * (like.shape[1] // 128), axis=1)


def interleave(a, b):
    i = j = 0
    while i < len(a) or j < len(b):
        if j >= len(b) or (i < len(a) and i * len(b) <= j * len(a)):
            a[i]()
            i += 1
        else:
            b[j]()
            j += 1


def run_tiles(tiles):
    before = []
    for logits, sums in tiles:
        interleave(logits, before)
        before = sums
    interleave([], before)


def choose(x, cases):
    def among(lo, hi):
        mid = (lo + hi) // 2
        if hi - lo == 1:
            cases[lo]()
        else:
            pl.when(x < mid)(lambda: among(lo, mid))
            pl.when(x >= mid)(lambda: among(mid, hi))
    among(0, len(cases))


def on(cond, *calls):
    @pl.when(cond)
    def _():
        for c in calls:
            c()


def scope(name):
    return jax.named_scope(name)


def main_kernel(bias_ref, x_ref, wk_ref, wv_ref, wq_ref, wout_ref, out_ref, lq_ref, lo_ref, lb_ref,
                xb, pm, xp, ws, q_s, kv_s, kvp_s, kvr_s, s_scr, t_scr,
                beta_s, x_sem, w_sem, wo_sem, sent, lq_recv, lo_recv, lb_recv, kv_recv, o_recv, y_recv, ready):
    dp, tp, sp = lax.axis_index('dp'), lax.axis_index('tp'), lax.axis_index('sp')
    idx = dp * 4 + sp
    side = tp // 2
    inner = (tp == 1) | (tp == 2)
    outer = jnp.logical_not(inner)
    W = (wk_ref, wv_ref, wq_ref)
    peer_x, peer_y, peer_c = {'dp': dp ^ 1}, {'sp': sp ^ 2}, {'sp': sp ^ 1}

    def remote(src, dst, ss, rs, dev):
        return pltpu.make_async_remote_copy(src_ref=src, dst_ref=dst, send_sem=ss, recv_sem=rs, device_id=dev, device_id_type=MESH)

    def lq_copy(t, src, dst, dev):
        return remote(lq_ref.at[src, t], lq_ref.at[dst, t], sent.at[0], lq_recv.at[t, min(dst, 4)], dev)

    def lq_z(t):
        return remote(W[t // 2].at[ds(idx * B, B), pl.ds(t % 2 * B, B)], lq_ref.at[0, t], sent.at[0], lq_recv.at[t, 0], {'tp': tp ^ 2})

    def lq_start(t):
        for i in TWO:
            lq_z(2 * t + i).start()

    def lo_copy(v, src, dst, dev):
        return remote(lo_ref.at[v, src], lo_ref.at[v, dst], sent.at[1], lo_recv.at[v, min(dst, 4)], dev)

    def lo_z(v):
        dst = 2 - side
        b = (tp ^ dst) - 2
        return remote(wout_ref.at[ds(idx * 64, 64, 64), ds((dst ^ v) * H, H)], lo_ref.at[v, 0, b], sent.at[2], lo_recv.at[v, 0], {'tp': dst})

    def lb_z(v):
        return remote(wout_ref.at[ds(sp % 2 * B, B), ds((tp ^ 1 ^ v) * H, H)], lb_ref.at[v, sp % 2], sent.at[3], lb_recv.at[v, 0], {'tp': tp ^ 1})

    def lb_core(v):
        return remote(lb_ref.at[v, sp % 2], lb_ref.at[v, sp % 2], sent.at[3], lb_recv.at[v, 1], peer_c)

    def lo_start(*vs):
        for v in vs:
            lo_z(v).start()

    def arrived(ref, sem):
        remote(ref, ref, sent.at[0], sem, peer_c).wait_recv()

    def all_sent(ref, i):
        remote(ref, ref, sent.at[i], sent.at[i], peer_c).wait_send()

    def lo_zwait(v):
        arrived(lo_ref.at[v, 0], lo_recv.at[v, 0])

    def hop(copy, p, i):
        near, far, n = (peer_x, peer_y, 1) if copy is lo_copy and p == 2 else (peer_y, peer_x, 2)
        f = 3 - n
        return copy(p, *((0, n, near), (0, f, far), (0, 4, peer_c), (n, 3, far), (n, 4 + n, peer_c), (f, 4 + f, peer_c), (3, 7, peer_c))[i])

    def ev_z(copy, *ps):
        for p in ps:
            with scope(f'z_{copy.__name__}{p}'):
                lq_z(p).wait_recv() if copy is lq_copy else lo_zwait(p)
            hop(copy, p, 0).start()
        for p in ps:
            hop(copy, p, 1).start()
            hop(copy, p, 2).start()

    def ev_near(copy, *ps):
        for p in ps:
            with scope(f'n_{copy.__name__}{p}'):
                hop(copy, p, 0).wait_recv()
            hop(copy, p, 3).start()
            hop(copy, p, 4).start()

    def ev_far(copy, *ps):
        for p in ps:
            with scope(f'f_{copy.__name__}{p}'):
                hop(copy, p, 1).wait_recv()
            hop(copy, p, 5).start()

    def ev_xy(copy, *ps):
        ev_near(copy, *ps)
        ev_far(copy, *ps)

    def ev_y(copy, *ps):
        for p in ps:
            with scope(f'y_{copy.__name__}{p}'):
                hop(copy, p, 3).wait_recv()
            hop(copy, p, 6).start()
            if copy is lq_copy and p >= 2:
                start(w_load(p, SLOT[:4]))

    def ev_done(copy, *ps):
        for p in ps:
            with scope(f'c_{copy.__name__}{p}'):
                if copy is lq_copy:
                    arrived(lq_ref.at[pl.ds(4, 4), p], lq_recv.at[p, 4])
                else:
                    arrived(lo_ref.at[p, pl.ds(4, 4)], lo_recv.at[p, 4])

    def w_load(p, slots):
        return [pltpu.make_async_copy(lq_ref.at[SLOT.index(m), p], ws.at[p // 2 % 2, ds((idx ^ m) * B, B), pl.ds(p % 2 * B, B)], w_sem.at[p]) for m in slots]

    def own_load(t):
        return pltpu.make_async_copy(W[t], ws.at[t], w_sem.at[6 + t])

    def start(copies):
        for c in copies:
            c.start()

    def wait(copies):
        for c in copies:
            c.wait()

    def ev_last(t):
        pieces = [2 * t + i for i in TWO]
        ev_done(lq_copy, *pieces)
        for p in pieces:
            start(w_load(p, SLOT[4:] if t else SLOT))

    def local(ref, sem):
        pltpu.make_async_copy(ref, ref, sem).wait()

    def ev_weights(t):
        with scope(f'load{t}'):
            for i in TWO:
                local(ws.at[t % 2, :, pl.ds(i * B, B)], w_sem.at[2 * t + i])

    def ev_wo(*vs):
        ev_done(lo_copy, *vs)
        for v in vs:
            lb_core(v).wait_recv()
        start(wo_load(*vs))

    def ev_wo_ready(*vs):
        with scope(f'wo{vs[0]}'):
            for v in vs:
                local(xp.at[1 - side, pl.ds(2, 6), :, pl.ds((v ^ 2) * H, H)], wo_sem.at[v])

    def ev_lb(*vs):
        for v in vs:
            with scope(f'lb{v}'):
                lb_z(v).wait_recv()
            lb_core(v).start()

    wo = xp.at[1 - side]

    def wo_own():
        return [pltpu.make_async_copy(wout_ref.at[pl.ds(r * B, B), pl.ds(c * H, H)], xp.at[1 - side, r, :, ds((c ^ tp ^ 2) * H, H)], wo_sem.at[4])
                for r in TWO for c in range(4)]

    def wo_load(*vs):
        out = []
        for v in vs:
            cols = pl.ds((v ^ 2) * H, H)
            for s, m in enumerate(SLOT):
                row = (idx ^ m) * 64
                for b in TWO:
                    out.append(pltpu.make_async_copy(lo_ref.at[v, s, b], xp.at[1 - side, 4 + 2 * b + row // B, ds(row % B, 64, 64), cols], wo_sem.at[v]))
            for r in TWO:
                out.append(pltpu.make_async_copy(lb_ref.at[v, r], xp.at[1 - side, 2 + r, :, cols], wo_sem.at[v]))
        return out

    def kvp_copy(h, s):
        return remote(kv_s.at[h, pl.ds(8 * s, 2)], kvp_s.at[h, pl.ds(2 * s, 2)], sent.at[4], kv_recv.at[0, h], peer_c)

    def kvr_copy(h, s):
        return remote(kv_s.at[h, 8 * s], kvr_s.at[h, s], sent.at[5], kv_recv.at[1, h], peer_y)

    def kvf_copy(h, s):
        return remote(kvr_s.at[h, s], kvr_s.at[h, 2 + s], sent.at[6], kv_recv.at[2, h], peer_c)

    def kv_start(copy, heads):
        for h in heads:
            for s in TWO:
                copy(h, s).start()

    def kv_wait(copy, heads):
        with scope(f'w_{copy.__name__}{heads[0]}'):
            for h in heads:
                i = (kvp_copy, kvr_copy, kvf_copy).index(copy)
                arrived((kvp_s.at[h], kvr_s.at[h, pl.ds(0, 2)], kvr_s.at[h, pl.ds(2, 2)])[i], kv_recv.at[i, h])

    def kv_forward(heads):
        kv_wait(kvr_copy, heads)
        kv_start(kvf_copy, heads)

    def reverse(i):
        return (i % 2) * 2 + i // 2

    def order(n):
        return 2 * reverse(n % 4) + ((n // 4) ^ side)

    def o_at(k, p, theirs, col, size, row=0, rows=B):
        if p:
            return ws.at[1 + theirs, ds(k * B + row, rows), ds(col, size)]
        return xb.at[k // 2, pl.ds(row, rows), ds((k % 2) * 1024 + theirs * H + col, size)]

    def o_copy(k, p, half):
        row = half * 128
        return remote(o_at(k, p, 0, 0, H, row, 128), o_at(k, p, 1, 0, H, row, 128), sent.at[7], o_recv.at[k, half], {'tp': tp ^ 1})

    def o_times(k, v, n, row=0, rows=B):
        cols = pl.ds((v ^ 2) * H, n * H)
        y = nn(xb[k // 2, pl.ds(row, rows), ds((k % 2) * 1024, 1024)], wo[0:4, :, cols].reshape(1024, n * H))
        for i in TWO:
            y = y + nn(ws[1 + i, ds(k * B + row, rows), :], wo[part(2 + i, 2), :, cols].reshape(H, n * H))
        y = y.astype(BF)
        for i in range(n):
            y_src(k, v + i, row, rows)[...] = y[:, part(i, H)]
            y_copy(k, v + i, side, row, rows).start() if v else y_local(k).start()

    def y_src(k, v, row=0, rows=B):
        return xp.at[side, k, pl.ds(row, rows), pl.ds(v * H, H)]

    def y_copy(k, v, seg, row, rows):
        return remote(y_src(k, v, row, rows), out_ref.at[seg, k, pl.ds(row, rows)], sent.at[8], y_recv.at[seg], {'tp': tp ^ v})

    def y_local(k):
        return pltpu.make_async_copy(y_src(k, 0), out_ref.at[side, k], sent.at[9])

    def x_copy(j):
        return pltpu.make_async_copy(x_ref.at[ds(j * B, B), :], xb.at[lax.rem(j, 4)], x_sem.at[lax.rem(j, 4)])

    for j in range(4):
        x_copy(j).start()
    barrier = pltpu.get_barrier_semaphore()
    peers = [{'tp': tp ^ 1}, {'tp': tp ^ 2}, {'tp': tp ^ 3}, peer_x, peer_y, peer_c]
    for dev in peers:
        pl.semaphore_signal(barrier, inc=1, device_id=dev, device_id_type=MESH)
    for t in range(3):
        own_load(t).start()

    pm[...] = phase_matrix(False)

    def permute_body(j, carry):
        x_copy(j).wait()
        y = nn(pm[...], xb[lax.rem(j, 4)]).astype(BF).reshape(8, 32, M)
        xp[j // 8, :, ds(lax.rem(j, 8) * 32, 32, 32), :] = y
        pl.when(j < 12)(lambda: x_copy(j + 4).start())

        @pl.when(j == 7)
        def _():
            with scope('barrier'):
                pl.semaphore_wait(barrier, len(peers))
            lq_start(KEY)
            on(outer, lb_z(2).start)
        return carry

    with scope('permute'):
        lax.fori_loop(0, 16, permute_body, None)

    for h in HEADS:
        column = 2 * (tp ^ (h // 2 * 2)) + h % 2
        for i, branches in enumerate(('0', '01', '1', '012', '12', '2', '0123', '123', '23', '3')):
            rows = [jnp.full((1, 128), bias_ref[j, column], F32) for j in map(int, branches)]
            m = functools.reduce(jnp.maximum, rows)
            beta_s[pl.ds(h * 16 + i, 1), :] = (m + jnp.log(sum(jnp.exp(r - m) for r in rows))) * math.log2(math.e)

    def signal_ready(i):
        pl.when(inner)(lambda: pl.semaphore_signal(ready.at[i], inc=1, device_id={'tp': tp ^ 1}, device_id_type=MESH))

    def wait_ready(i):
        with scope(f'ready{i}'):
            pl.when(outer)(lambda: pl.semaphore_wait(ready.at[i], 1))

    signal_ready(0)

    def group(g):
        low = g < 4
        return jnp.where(low, g & 1, 0), jnp.where(low, g // 2, g - 2)

    def head_number(h):
        return 2 * (tp ^ (h // 2 * 2)) + h % 2

    def project(heads, sigma, pair, kinds):
        for h in heads:
            t = head_number(h) + reverse(pair)
            x, swap = xp[side ^ sigma, pl.ds(2 * (t & 3), 2)].reshape(H, M), (t & 7) >> 2
            for t in kinds:
                y = nn(x, ws[t, :, part(h % 2, B)])
                for j in TWO:
                    piece = y[part(j, B)]
                    kv_s[h, 8 * sigma + 2 * pair + (j ^ swap), t] = (piece.T if t == VAL else piece).astype(BF)

    def phases_of(j):
        return [j % 2 + 2 * i for i in TWO], (j // 2) ^ side

    def rank_of(phase, h):
        rel = (phase - head_number(h)) & 7
        return (rel & 1) * 4 + ((rel >> 1) & 1) * 2 + (rel >> 2)

    def queries(heads, w, j):
        phases, half = phases_of(j)
        x = jnp.concatenate([xp[side, 2 * f + half] for f in phases])
        for h in heads:
            y = nn(x, ws[w, :, part(h % 2, B)]).astype(BF)
            for i, f in enumerate(phases):
                q_s[h, rank_of(f + 4 * half, h)] = y[part(i, B)]

    with scope('own_w'):
        for t in range(3):
            own_load(t).wait()
    own, partner = HEADS[:2], HEADS[2:]

    def mix(b, c):
        return jnp.concatenate([b, b, c, c], axis=1)

    def keys_of(ref, h, i, weights):
        parts = []
        n = 0
        for count, b in weights:
            def values(i=i + n, count=count):
                v = [ref[h, i + j, VAL] for j in range(count)]
                return v[0] if count == 1 else jnp.concatenate(v, axis=1)
            parts.append((values, count * B, b))
            n += count
        return (lambda: ref[h, i:i + n, KEY].reshape(n * B, B)), parts

    def chunk_tiles(p, j, kind):
        both_phases, half = phases_of(j)

        def put(h, phase, ot):
            k = 2 * (phase & 3) + half
            y = ot.T.astype(BF)
            for i in TWO:
                pl.when(p == i)(lambda i=i: o_at(k, i, 0, (h % 2) * B, B).__setitem__(..., y))

        def tile(h, phases, ranks, wide, narrow, s_ref, n_ref):
            def done(ot):
                for i, phase in enumerate(phases):
                    put(h, phase, ot[:, part(i, B)])
            return tile_steps(lambda: jnp.concatenate([q_s[h, r] for r in ranks]), wide, narrow, s_ref, n_ref, done)

        h = 2 * p + (j % 2) ^ 1
        rest = tile(h, both_phases, [rank_of(f + 4 * half, h) for f in both_phases], [keys_of(kv_s, h, i, [(2, None)]) for i in range(0, 8, 2)], [], t_scr, None)
        h = 2 * p + (j % 2)
        a = head_number(h)
        b0, b01, b1, b012, b12, b2, b0123, b123, b23, b3 = [beta_s[pl.ds(h * 16 + i, 1), :] for i in range(10)]
        phases = [a & 3, (a & 3) ^ 2]
        both = [keys_of(kv_s, h, i, [(2, b)]) for i, b in ((2, b01), (4, b0), (6, b0), (10, b1))]
        if kind == 0:
            both += [keys_of(kv_s, h, 0, [(1, mix(b0123, b01)), (1, mix(b012, b01))]), keys_of(kv_s, h, 8, [(1, mix(b123, b1)), (1, mix(b12, b1))])]
            first = [keys_of(kvp_s, h, i, [(1, b23), (1, b2)]) for i in (0, 2)] + [keys_of(kvr_s, h, i, [(2, b3)]) for i in (0, 2)]
        else:
            both += [keys_of(kv_s, h, 0, [(2, mix(b012, b01))]), keys_of(kv_s, h, 8, [(2, mix(b12, b1))])]
            first = [keys_of(kvp_s, h, i, [(2, b2)]) for i in (0, 2)]
        with scope(f'tile{kind}'):
            run_tiles([rest, tile(h, phases, [kind, rank_of(phases[1] + 4 * half, h)], both, first, s_scr, t_scr.at[:, pl.ds(0, B)])])

    def send_o(ks, p):
        @pl.when(outer)
        def _():
            for k in ks:
                for half in TWO:
                    o_copy(order(k), p, half).start()

    def step_body(t, carry):
        packed = functools.reduce(lambda x, i: jnp.where(t == i, TABLE[i], x), range(len(TABLE)), 0)
        code, n, event = packed % 16, packed // 16 % 16, packed // 256

        def step_o():
            with scope('own_kv'):
                project(own, *group(n), (KEY, VAL))

        def step_kv(t_):
            with scope(f'par_{t_}'):
                for i in TWO:
                    project(partner, *group(2 * n + i), (t_,))

        def step_q(heads, w):
            with scope(f'que_{w}'):
                queries(heads, w, n)

        def step_out(v, m):
            @pl.when(inner)
            def _():
                k = order(n)

                def halves():
                    for half in TWO:
                        with scope(f'wait_h{half}'):
                            arrived(ws.at[0, pl.ds(0, B), :], o_recv.at[k, half])
                        o_times(k, v, m, half * 128, 128)

                def whole():
                    with scope('wait_o'):
                        for half in TWO:
                            arrived(ws.at[0, pl.ds(0, B), :], o_recv.at[k, half])
                    with scope(f'out{v}'):
                        o_times(k, v, m)

                if m == 2:
                    pl.when(n == 0)(halves)
                    pl.when(n > 0)(whole)
                else:
                    with scope(f'out{v}'):
                        o_times(k, v, m)

        f = functools.partial
        kinds = {'-': lambda: None, 'O': step_o, 'P': f(step_q, own, QUE), 'K': f(step_kv, KEY), 'V': f(step_kv, VAL), 'Q': f(step_q, partner, KEY),
                 'A': lambda: chunk_tiles(n // 4, n % 4, 0), 'B': lambda: chunk_tiles(n // 4, n % 4, 1), 'R': f(step_out, 2, 2), 'L': f(step_out, 1, 1), 'N': f(step_out, 0, 1)}
        choose(code, [kinds[c] for c in KINDS])
        call = functools.partial

        events = {
            'free': [call(signal_ready, 1), call(on, inner, lambda: start(wo_own()))],
            'r0': [call(wait_ready, 0)],
            'r1': [call(wait_ready, 1)],
            'so': [call(kv_start, kvp_copy, own)],
            'po': [call(kv_wait, kvp_copy, own)],
            'sp': [call(kv_start, kvp_copy, partner)],
            'pp': [call(kv_wait, kvp_copy, partner)],
        }
        for t_, c in enumerate('kvq'):
            events['b' + c] = [call(lq_start, t_)]
            events['l' + c] = [call(ev_last, t_)]
            events['w' + c] = [call(ev_weights, t_)]
            for i in TWO:
                for e, f in zip('zxy', (ev_z, ev_xy, ev_y)):
                    events[f'{e}{c}{i}'] = [call(f, lq_copy, 2 * t_ + i)]
        for i, vs in enumerate(((2, 3), (1,), (0,))):
            events[f'b{i}'] = [call(lo_start, *vs)]
            for e, f in zip('zmxycwv', (call(ev_z, lo_copy), call(ev_near, lo_copy), call(ev_far, lo_copy), call(ev_y, lo_copy), ev_lb, ev_wo, ev_wo_ready)):
                events[f'{e}{i}'] = [call(on, inner, call(f, *vs))]
        events['v0'] += [call(on, inner, lambda: local(xp.at[1 - side, pl.ds(0, 2)], wo_sem.at[4]))]
        for v in range(4):
            events[f'd{v}'] = [call(on, outer, lambda v=v: lb_z(v).start())]
        for h in HEADS:
            for z in TWO:
                events[f's{h}{z}'] = [kvr_copy(h, z).start]
            events[f'f{h}'] = [call(kv_forward, [h])]
            events[f'g{h}'] = [call(kv_wait, kvf_copy, [h])]
        for k in ROWS:
            for p in TWO:
                events['op'[p] + str(k)] = [call(send_o, (k,), p)]
        def run(names):
            for name in names.split(','):
                where, _, name = name.rpartition(':')
                if where:
                    on(inner if where == 'i' else outer, *events[name])
                else:
                    for c in events[name]:
                        c()

        @pl.when(event > 0)
        def _():
            choose(event - 1, [functools.partial(run, names) for names in EVENTS])
        return carry

    lax.fori_loop(0, len(TABLE), step_body, None)

    all_sent(lq_ref, 0)
    all_sent(lo_ref.at[:, 0, 0], 2)
    all_sent(lb_ref.at[:, 0], 3)
    all_sent(kvp_s, 4)
    all_sent(kvr_s.at[:, pl.ds(0, 2)], 5)
    all_sent(kvr_s.at[:, pl.ds(0, 2)], 6)

    @pl.when(outer)
    def _():
        all_sent(xb, 7)

    @pl.when(inner)
    def _():
        all_sent(lo_ref.at[:, pl.ds(0, 7)], 1)
        with scope('y_sent'):
            all_sent(xp.at[side, :, :, pl.ds(H, 3 * H)], 8)
        local(xp.at[side, :, :, pl.ds(0, H)], sent.at[9])

    for seg in TWO:
        @pl.when(tp != 1 + seg)
        def _(seg=seg):
            with scope(f'recv{seg}'):
                arrived(out_ref.at[seg], y_recv.at[seg])


PROGRAM = (
    'O.i:zk0,i:zk1', 'O.i:bv,o:zk0', 'O.o:zk1,s00,i:xk0', 'O.o:bv,o:xk0,i:xk1,o:s01,d3', 'O.o:xk1,i:yk0,i:zv0', 'O.o:yk0,i:yk1,i:zv1,i:s01,i:bq',
    'P.o:bq,so', 'P.o:yk1,lk,o:zv0,d1,i:xv0', 'P.wk,o:zv1,i:xv1', 'K.i:zq0', 'K.o:xv0,i:zq1,f0', 'K.o:xv1,o:zq0,i:yv0,i:yv1,b0,b1,r0,po,g0,o:zq1',
    'T0.o0,o1,d0,o:yv0,o:yv1,lv,i:xq0,i:xq1', 'P.wv,z0,o:xq0,b2', 'V.o:xq1,sp,o:s10,o:s11', 'V.c0,o:s20,o:s21',
    'V.free,yq0,yq1,lq,m0,z1,o:s30,o:s31,wq', 'Q.pp,r1,x0,c1,m1,y0', 'T4.p0,p1,x1,w0,v0', 'R.y1,w1,v1,i:s10,i:s11', 'L', 'Q', 'T5.p2,p3,o:f1', 'R',
    'L', 'Q', 'Q.i:f1,o:g1,i:s20,i:s21', 'T2.i:g1,o:f2', 'T1.o2,o3,o:g2,o:f3', 'R.i:s30,i:s31', 'L.i:f2', 'R', 'L.i:g2', 'T6.p4,o4,p5,o5,o:g3', 'R',
    'T3.i:f3,z2,c2', 'L.i:g3', 'T7.p6,o6,p7,o7', 'R.m2,x2', 'L', 'R.y2', 'L.w2', '-.v2', 'N', 'N', 'N', 'R', 'L', 'N', 'N', 'N', 'N', 'N',
)
KINDS = '-OPKVQABRLN'


def tables():
    table, seen = [], {}
    names = tuple(dict.fromkeys(s.partition('.')[2] for s in PROGRAM if '.' in s))
    for s in PROGRAM:
        name, _, after = s.partition('.')
        kind, n = name[0], seen.get(name[0], 0)
        seen[kind] = n + 1
        if kind == 'T':
            n = int(name[1:])
            kind = 'AB'[n in (2, 3, 4, 5)]
        table.append(KINDS.index(kind) + 16 * n + 256 * (names.index(after) + 1 if after else 0))
    return table, names


TABLE, EVENTS = tables()


def main(bias, x, wk, wv, wq, w_out):
    anyspec = pl.BlockSpec(memory_space=pl.ANY)
    vmem = [((4, B, M), BF), ((B, B), BF), ((2, 8, B, M), BF), ((3, M, H), BF), ((4, 8, B, B), BF), ((4, 12, 2, B, B), BF), ((4, 4, 2, B, B), BF), ((4, 4, 2, B, B), BF),
            ((3072, H), F32), ((M, H), F32), ((64, 128), F32)]
    dma = [(4,), (9,), (5,), (10,), (6, 5), (4, 5), (4, 2), (3, 4), (8, 2), (2,)]
    return pl.pallas_call(
        main_kernel,
        in_specs=[pl.BlockSpec(memory_space=pltpu.SMEM)] + [anyspec] * 5,
        out_specs=[anyspec] * 4,
        out_shape=[jax.ShapeDtypeStruct(s, BF) for s in ((2, 8, B, H), (8, 6, B, B), (4, 8, 2, 64, H), (4, 2, B, H))],
        scratch_shapes=[pltpu.VMEM(*v) for v in vmem] + [pltpu.SemaphoreType.DMA(d) for d in dma] + [pltpu.SemaphoreType.REGULAR((2,))],
        compiler_params=params(collective_id=0, has_side_effects=True),
        cost_estimate=pl.CostEstimate(flops=10**11, bytes_accessed=10**8, transcendentals=0),
        name='main',
    )(bias, x, wk, wv, wq, w_out)[0]


def solution(mesh):
    def device_fn(hidden, w_query, w_key, w_value, w_out, branch_bias):
        return unpermute(main(branch_bias, hidden, w_key, w_value, w_query, w_out))

    return jax.shard_map(device_fn, mesh=mesh, in_specs=(P(('dp', 'sp'), None), P(None, 'tp'), P(None, 'tp'), P(None, 'tp'), P('tp', None), P(None, None)), out_specs=P(('dp', 'sp'), 'tp'), check_vma=False)
```

```python
import functools
import math

import jax
import jax.numpy as jnp
from jax import lax
from jax.experimental import pallas as pl
from jax.experimental.pallas import tpu as pltpu
from jax.sharding import PartitionSpec as P

MESH = pl.DeviceIdType.MESH
BF = jnp.bfloat16
F32 = jnp.float32
B, H, M = 256, 512, 2048
KAPPA = math.log2(math.e) / 16
VMEM = 66_900_000
SLOT = (0, 4, 2, 6, 1, 5, 3, 7)
KEY, VAL, QUE = range(3)
HEADS = range(4)
TWO = range(2)
ROWS = range(8)


def nn(a, b):
    return lax.dot_general(a, b, (((1,), (0,)), ((), ())), preferred_element_type=F32)


def nt(a, b):
    return lax.dot_general(a, b, (((1,), (1,)), ((), ())), preferred_element_type=F32)


def params(**kw):
    return pltpu.CompilerParams(vmem_limit_bytes=VMEM, **kw)


def ds(start, size, align=128):
    return pl.ds(pl.multiple_of(start, align), size)


def part(i, size):
    return slice(i * size, i * size + size)


def phase_matrix(transposed):
    r = lax.broadcasted_iota(jnp.int32, (B, B), int(transposed))
    p = lax.broadcasted_iota(jnp.int32, (B, B), int(not transposed))
    k = r // 32
    return (p == (r % 32) * 8 + k // 2 + 4 * (k % 2)).astype(F32).astype(BF)


def unpermute_kernel(y_ref, o_ref, y_s, o_s, load, store):
    pieces = [(s, j) for s in TWO for j in range(4)]

    def get(i):
        s, j = pieces[i]
        return pltpu.make_async_copy(y_ref.at[s, :, pl.ds(j * 64, 64)], y_s.at[i], load.at[i])

    def put(i):
        return pltpu.make_async_copy(o_s.at[i], o_ref.at[pl.ds(i * H, H)], store.at[i])

    for i in ROWS:
        get(i).start()
    pm = phase_matrix(True)
    for i in range(0, 8, 2):
        group = (i, i + 1)
        for k in group:
            get(k).wait()
        for k in group:
            for j in TWO:
                o_s[k, part(j, B), :] = nn(pm, y_s[k, :, part(j, 32), :].reshape(B, H)).astype(BF)
        for k in group:
            put(k).start()
    for i in ROWS:
        put(i).wait()


def unpermute(y):
    anyspec = pl.BlockSpec(memory_space=pl.ANY)
    return pl.pallas_call(
        unpermute_kernel,
        in_specs=[anyspec],
        out_specs=anyspec,
        out_shape=jax.ShapeDtypeStruct((2 * M, H), BF),
        scratch_shapes=[pltpu.VMEM((8, 8, 64, H), BF), pltpu.VMEM((8, H, H), BF), pltpu.SemaphoreType.DMA((8,)), pltpu.SemaphoreType.DMA((8,))],
        compiler_params=params(),
        name='unpermute',
    )(y)


def tile_steps(q, wide, narrow, s_ref, n_ref, done):
    st = {}
    logits, sums = [], []

    def add(name, x):
        st[name] = st[name] + x if name in st else x

    for groups, ref in ((wide, s_ref), (narrow, n_ref)):
        off = 0
        for keys, parts in groups:
            def qk(keys=keys, parts=parts, off=off, ref=ref):
                s = nt(keys(), q() if ref is s_ref else q()[:B])
                o = 0
                for _, n, b in parts:
                    piece = s[o:o + n]
                    ref[pl.ds(off + o, n), :] = piece
                    t = jnp.max(piece, axis=0, keepdims=True) * KAPPA
                    if b is not None:
                        t = t + fit(b, t)
                    if ref is n_ref:
                        t = jnp.concatenate([t, st['top'][:, B:]], axis=1)
                    st['top'] = jnp.maximum(st['top'], t) if 'top' in st else t
                    o += n
            logits.append(qk)
            for v, n, b in parts:
                def sv(v=v, n=n, b=b, off=off, ref=ref):
                    top = st['top'] if ref is s_ref else st['top'][:, :B]
                    e = jnp.exp2(ref[pl.ds(off, n), :] * KAPPA - (top if b is None else top - fit(b, top)))
                    name = 'w' if ref is s_ref else 'n'
                    add('l' + name, jnp.sum(e, axis=0, keepdims=True))
                    add('o' + name, nn(v(), e.astype(BF)))
                sums.append(sv)
                off += n

    def finish():
        o, l = st['ow'], st['lw']
        if narrow:
            o = jnp.concatenate([o[:, :B] + st['on'], o[:, B:]], axis=1)
            l = jnp.concatenate([l[:, :B] + st['ln'], l[:, B:]], axis=1)
        done(o / l)

    return logits, sums + [finish]


def fit(b, like):
    return b if b.shape == like.shape else jnp.concatenate([b] * (like.shape[1] // 128), axis=1)


def interleave(a, b):
    i = j = 0
    while i < len(a) or j < len(b):
        if j >= len(b) or (i < len(a) and i * len(b) <= j * len(a)):
            a[i]()
            i += 1
        else:
            b[j]()
            j += 1


def run_tiles(tiles):
    before = []
    for logits, sums in tiles:
        interleave(logits, before)
        before = sums
    interleave([], before)


def choose(x, cases):
    def among(lo, hi):
        mid = (lo + hi) // 2
        if hi - lo == 1:
            cases[lo]()
        else:
            pl.when(x < mid)(lambda: among(lo, mid))
            pl.when(x >= mid)(lambda: among(mid, hi))
    among(0, len(cases))


def on(cond, *calls):
    @pl.when(cond)
    def _():
        for c in calls:
            c()


def scope(name):
    return jax.named_scope(name)


def main_kernel(bias_ref, x_ref, wk_ref, wv_ref, wq_ref, wout_ref, out_ref, lq_ref, lo_ref, lb_ref,
                xb, pm, xp, ws, q_s, kv_s, kvp_s, kvr_s, s_scr, t_scr,
                beta_s, x_sem, w_sem, wo_sem, sent, lq_recv, lo_recv, lb_recv, kv_recv, o_recv, y_recv, ready):
    dp, tp, sp = lax.axis_index('dp'), lax.axis_index('tp'), lax.axis_index('sp')
    idx = dp * 4 + sp
    side = tp // 2
    inner = (tp == 1) | (tp == 2)
    outer = jnp.logical_not(inner)
    W = (wk_ref, wv_ref, wq_ref)
    peer_x, peer_y, peer_c = {'dp': dp ^ 1}, {'sp': sp ^ 2}, {'sp': sp ^ 1}

    def remote(src, dst, ss, rs, dev):
        return pltpu.make_async_remote_copy(src_ref=src, dst_ref=dst, send_sem=ss, recv_sem=rs, device_id=dev, device_id_type=MESH)

    def lq_copy(t, src, dst, dev):
        return remote(lq_ref.at[src, t], lq_ref.at[dst, t], sent.at[0], lq_recv.at[t, min(dst, 4)], dev)

    def lq_z(t):
        return remote(W[t // 2].at[ds(idx * B, B), pl.ds(t % 2 * B, B)], lq_ref.at[0, t], sent.at[0], lq_recv.at[t, 0], {'tp': tp ^ 2})

    def lq_start(t):
        for i in TWO:
            lq_z(2 * t + i).start()

    def lo_copy(v, src, dst, dev):
        return remote(lo_ref.at[v, src], lo_ref.at[v, dst], sent.at[1], lo_recv.at[v, min(dst, 4)], dev)

    def lo_z(v):
        dst = 2 - side
        b = (tp ^ dst) - 2
        return remote(wout_ref.at[ds(idx * 64, 64, 64), ds((dst ^ v) * H, H)], lo_ref.at[v, 0, b], sent.at[2], lo_recv.at[v, 0], {'tp': dst})

    def lb_z(v):
        return remote(wout_ref.at[ds(sp % 2 * B, B), ds((tp ^ 1 ^ v) * H, H)], lb_ref.at[v, sp % 2], sent.at[3], lb_recv.at[v, 0], {'tp': tp ^ 1})

    def lb_core(v):
        return remote(lb_ref.at[v, sp % 2], lb_ref.at[v, sp % 2], sent.at[3], lb_recv.at[v, 1], peer_c)

    def lo_start(*vs):
        for v in vs:
            lo_z(v).start()

    def arrived(ref, sem):
        remote(ref, ref, sent.at[0], sem, peer_c).wait_recv()

    def all_sent(ref, i):
        remote(ref, ref, sent.at[i], sent.at[i], peer_c).wait_send()

    def lo_zwait(v):
        arrived(lo_ref.at[v, 0], lo_recv.at[v, 0])

    def hop(copy, p, i):
        near, far, n = (peer_x, peer_y, 1) if copy is lo_copy and p == 2 else (peer_y, peer_x, 2)
        f = 3 - n
        return copy(p, *((0, n, near), (0, f, far), (0, 4, peer_c), (n, 3, far), (n, 4 + n, peer_c), (f, 4 + f, peer_c), (3, 7, peer_c))[i])

    def ev_z(copy, *ps):
        for p in ps:
            with scope(f'z_{copy.__name__}{p}'):
                lq_z(p).wait_recv() if copy is lq_copy else lo_zwait(p)
            hop(copy, p, 0).start()
        for p in ps:
            hop(copy, p, 1).start()
            hop(copy, p, 2).start()

    def ev_near(copy, *ps):
        for p in ps:
            with scope(f'n_{copy.__name__}{p}'):
                hop(copy, p, 0).wait_recv()
            hop(copy, p, 3).start()
            hop(copy, p, 4).start()

    def ev_far(copy, *ps):
        for p in ps:
            with scope(f'f_{copy.__name__}{p}'):
                hop(copy, p, 1).wait_recv()
            hop(copy, p, 5).start()

    def ev_xy(copy, *ps):
        ev_near(copy, *ps)
        ev_far(copy, *ps)

    def ev_y(copy, *ps):
        for p in ps:
            with scope(f'y_{copy.__name__}{p}'):
                hop(copy, p, 3).wait_recv()
            hop(copy, p, 6).start()
            if copy is lq_copy and p >= 2:
                start(w_load(p, SLOT[:4]))

    def ev_done(copy, *ps):
        for p in ps:
            with scope(f'c_{copy.__name__}{p}'):
                if copy is lq_copy:
                    arrived(lq_ref.at[pl.ds(4, 4), p], lq_recv.at[p, 4])
                else:
                    arrived(lo_ref.at[p, pl.ds(4, 4)], lo_recv.at[p, 4])

    def w_load(p, slots):
        return [pltpu.make_async_copy(lq_ref.at[SLOT.index(m), p], ws.at[p // 2 % 2, ds((idx ^ m) * B, B), pl.ds(p % 2 * B, B)], w_sem.at[p]) for m in slots]

    def own_load(t):
        return pltpu.make_async_copy(W[t], ws.at[t], w_sem.at[6 + t])

    def start(copies):
        for c in copies:
            c.start()

    def wait(copies):
        for c in copies:
            c.wait()

    def ev_last(t):
        pieces = [2 * t + i for i in TWO]
        ev_done(lq_copy, *pieces)
        for p in pieces:
            start(w_load(p, SLOT[4:] if t else SLOT))

    def local(ref, sem):
        pltpu.make_async_copy(ref, ref, sem).wait()

    def ev_weights(t):
        with scope(f'load{t}'):
            for i in TWO:
                local(ws.at[t % 2, :, pl.ds(i * B, B)], w_sem.at[2 * t + i])

    def ev_wo(*vs):
        ev_done(lo_copy, *vs)
        for v in vs:
            lb_core(v).wait_recv()
        start(wo_load(*vs))

    def ev_wo_ready(*vs):
        with scope(f'wo{vs[0]}'):
            for v in vs:
                local(xp.at[1 - side, pl.ds(2, 6), :, pl.ds((v ^ 2) * H, H)], wo_sem.at[v])

    def ev_lb(*vs):
        for v in vs:
            with scope(f'lb{v}'):
                lb_z(v).wait_recv()
            lb_core(v).start()

    wo = xp.at[1 - side]

    def wo_own():
        return [pltpu.make_async_copy(wout_ref.at[pl.ds(r * B, B), pl.ds(c * H, H)], xp.at[1 - side, r, :, ds((c ^ tp ^ 2) * H, H)], wo_sem.at[4])
                for r in TWO for c in range(4)]

    def wo_load(*vs):
        out = []
        for v in vs:
            cols = pl.ds((v ^ 2) * H, H)
            for s, m in enumerate(SLOT):
                row = (idx ^ m) * 64
                for b in TWO:
                    out.append(pltpu.make_async_copy(lo_ref.at[v, s, b], xp.at[1 - side, 4 + 2 * b + row // B, ds(row % B, 64, 64), cols], wo_sem.at[v]))
            for r in TWO:
                out.append(pltpu.make_async_copy(lb_ref.at[v, r], xp.at[1 - side, 2 + r, :, cols], wo_sem.at[v]))
        return out

    def kvp_copy(h, s):
        return remote(kv_s.at[h, pl.ds(8 * s, 2)], kvp_s.at[h, pl.ds(2 * s, 2)], sent.at[4], kv_recv.at[0, h], peer_c)

    def kvr_copy(h, s):
        return remote(kv_s.at[h, 8 * s], kvr_s.at[h, s], sent.at[5], kv_recv.at[1, h], peer_y)

    def kvf_copy(h, s):
        return remote(kvr_s.at[h, s], kvr_s.at[h, 2 + s], sent.at[6], kv_recv.at[2, h], peer_c)

    def kv_start(copy, heads):
        for h in heads:
            for s in TWO:
                copy(h, s).start()

    def kv_wait(copy, heads):
        with scope(f'w_{copy.__name__}{heads[0]}'):
            for h in heads:
                i = (kvp_copy, kvr_copy, kvf_copy).index(copy)
                arrived((kvp_s.at[h], kvr_s.at[h, pl.ds(0, 2)], kvr_s.at[h, pl.ds(2, 2)])[i], kv_recv.at[i, h])

    def kv_forward(heads):
        kv_wait(kvr_copy, heads)
        kv_start(kvf_copy, heads)

    def reverse(i):
        return (i % 2) * 2 + i // 2

    def order(n):
        return 2 * reverse(n % 4) + ((n // 4) ^ side)

    def o_at(k, p, theirs, col, size, row=0, rows=B):
        if p:
            return ws.at[1 + theirs, ds(k * B + row, rows), ds(col, size)]
        return xb.at[k // 2, pl.ds(row, rows), ds((k % 2) * 1024 + theirs * H + col, size)]

    def o_copy(k, p, half):
        row = half * 128
        return remote(o_at(k, p, 0, 0, H, row, 128), o_at(k, p, 1, 0, H, row, 128), sent.at[7], o_recv.at[k, half], {'tp': tp ^ 1})

    def o_times(k, v, n, row=0, rows=B):
        cols = pl.ds((v ^ 2) * H, n * H)
        y = nn(xb[k // 2, pl.ds(row, rows), ds((k % 2) * 1024, 1024)], wo[0:4, :, cols].reshape(1024, n * H))
        for i in TWO:
            y = y + nn(ws[1 + i, ds(k * B + row, rows), :], wo[part(2 + i, 2), :, cols].reshape(H, n * H))
        y = y.astype(BF)
        for i in range(n):
            y_src(k, v + i, row, rows)[...] = y[:, part(i, H)]
            y_copy(k, v + i, side, row, rows).start() if v else y_local(k).start()

    def y_src(k, v, row=0, rows=B):
        return xp.at[side, k, pl.ds(row, rows), pl.ds(v * H, H)]

    def y_copy(k, v, seg, row, rows):
        return remote(y_src(k, v, row, rows), out_ref.at[seg, k, pl.ds(row, rows)], sent.at[8], y_recv.at[seg], {'tp': tp ^ v})

    def y_local(k):
        return pltpu.make_async_copy(y_src(k, 0), out_ref.at[side, k], sent.at[9])

    def x_copy(j):
        return pltpu.make_async_copy(x_ref.at[ds(j * B, B), :], xb.at[lax.rem(j, 4)], x_sem.at[lax.rem(j, 4)])

    for j in range(4):
        x_copy(j).start()
    barrier = pltpu.get_barrier_semaphore()
    peers = [{'tp': tp ^ 1}, {'tp': tp ^ 2}, {'tp': tp ^ 3}, peer_x, peer_y, peer_c]
    for dev in peers:
        pl.semaphore_signal(barrier, inc=1, device_id=dev, device_id_type=MESH)
    for t in range(3):
        own_load(t).start()

    pm[...] = phase_matrix(False)

    def permute_body(j, carry):
        x_copy(j).wait()
        y = nn(pm[...], xb[lax.rem(j, 4)]).astype(BF).reshape(8, 32, M)
        xp[j // 8, :, ds(lax.rem(j, 8) * 32, 32, 32), :] = y
        pl.when(j < 12)(lambda: x_copy(j + 4).start())

        @pl.when(j == 7)
        def _():
            with scope('barrier'):
                pl.semaphore_wait(barrier, len(peers))
            lq_start(KEY)
            on(outer, lb_z(2).start)
        return carry

    with scope('permute'):
        lax.fori_loop(0, 16, permute_body, None)

    for h in HEADS:
        column = 2 * (tp ^ (h // 2 * 2)) + h % 2
        for i, branches in enumerate(('0', '01', '1', '012', '12', '2', '0123', '123', '23', '3')):
            rows = [jnp.full((1, 128), bias_ref[j, column], F32) for j in map(int, branches)]
            m = functools.reduce(jnp.maximum, rows)
            beta_s[pl.ds(h * 16 + i, 1), :] = (m + jnp.log(sum(jnp.exp(r - m) for r in rows))) * math.log2(math.e)

    def signal_ready(i):
        pl.when(inner)(lambda: pl.semaphore_signal(ready.at[i], inc=1, device_id={'tp': tp ^ 1}, device_id_type=MESH))

    def wait_ready(i):
        with scope(f'ready{i}'):
            pl.when(outer)(lambda: pl.semaphore_wait(ready.at[i], 1))

    signal_ready(0)

    def group(g):
        low = g < 4
        return jnp.where(low, g & 1, 0), jnp.where(low, g // 2, g - 2)

    def head_number(h):
        return 2 * (tp ^ (h // 2 * 2)) + h % 2

    def project(heads, sigma, pair, kinds):
        for h in heads:
            t = head_number(h) + reverse(pair)
            x, swap = xp[side ^ sigma, pl.ds(2 * (t & 3), 2)].reshape(H, M), (t & 7) >> 2
            for t in kinds:
                y = nn(x, ws[t, :, part(h % 2, B)])
                for j in TWO:
                    piece = y[part(j, B)]
                    kv_s[h, 8 * sigma + 2 * pair + (j ^ swap), t] = (piece.T if t == VAL else piece).astype(BF)

    def phases_of(j):
        return [j % 2 + 2 * i for i in TWO], (j // 2) ^ side

    def rank_of(phase, h):
        rel = (phase - head_number(h)) & 7
        return (rel & 1) * 4 + ((rel >> 1) & 1) * 2 + (rel >> 2)

    def queries(heads, w, j):
        phases, half = phases_of(j)
        x = jnp.concatenate([xp[side, 2 * f + half] for f in phases])
        for h in heads:
            y = nn(x, ws[w, :, part(h % 2, B)]).astype(BF)
            for i, f in enumerate(phases):
                q_s[h, rank_of(f + 4 * half, h)] = y[part(i, B)]

    with scope('own_w'):
        for t in range(3):
            own_load(t).wait()
    own, partner = HEADS[:2], HEADS[2:]

    def mix(b, c):
        return jnp.concatenate([b, b, c, c], axis=1)

    def keys_of(ref, h, i, weights):
        parts = []
        n = 0
        for count, b in weights:
            def values(i=i + n, count=count):
                v = [ref[h, i + j, VAL] for j in range(count)]
                return v[0] if count == 1 else jnp.concatenate(v, axis=1)
            parts.append((values, count * B, b))
            n += count
        return (lambda: ref[h, i:i + n, KEY].reshape(n * B, B)), parts

    def chunk_tiles(p, j, kind):
        both_phases, half = phases_of(j)

        def put(h, phase, ot):
            k = 2 * (phase & 3) + half
            y = ot.T.astype(BF)
            for i in TWO:
                pl.when(p == i)(lambda i=i: o_at(k, i, 0, (h % 2) * B, B).__setitem__(..., y))

        def tile(h, phases, ranks, wide, narrow, s_ref, n_ref):
            def done(ot):
                for i, phase in enumerate(phases):
                    put(h, phase, ot[:, part(i, B)])
            return tile_steps(lambda: jnp.concatenate([q_s[h, r] for r in ranks]), wide, narrow, s_ref, n_ref, done)

        h = 2 * p + (j % 2) ^ 1
        rest = tile(h, both_phases, [rank_of(f + 4 * half, h) for f in both_phases], [keys_of(kv_s, h, i, [(2, None)]) for i in range(0, 8, 2)], [], t_scr, None)
        h = 2 * p + (j % 2)
        a = head_number(h)
        b0, b01, b1, b012, b12, b2, b0123, b123, b23, b3 = [beta_s[pl.ds(h * 16 + i, 1), :] for i in range(10)]
        phases = [a & 3, (a & 3) ^ 2]
        both = [keys_of(kv_s, h, i, [(2, b)]) for i, b in ((2, b01), (4, b0), (6, b0), (10, b1))]
        if kind == 0:
            both += [keys_of(kv_s, h, 0, [(1, mix(b0123, b01)), (1, mix(b012, b01))]), keys_of(kv_s, h, 8, [(1, mix(b123, b1)), (1, mix(b12, b1))])]
            first = [keys_of(kvp_s, h, i, [(1, b23), (1, b2)]) for i in (0, 2)] + [keys_of(kvr_s, h, i, [(2, b3)]) for i in (0, 2)]
        else:
            both += [keys_of(kv_s, h, 0, [(2, mix(b012, b01))]), keys_of(kv_s, h, 8, [(2, mix(b12, b1))])]
            first = [keys_of(kvp_s, h, i, [(2, b2)]) for i in (0, 2)]
        with scope(f'tile{kind}'):
            run_tiles([rest, tile(h, phases, [kind, rank_of(phases[1] + 4 * half, h)], both, first, s_scr, t_scr.at[:, pl.ds(0, B)])])

    def send_o(ks, p):
        @pl.when(outer)
        def _():
            for k in ks:
                for half in TWO:
                    o_copy(order(k), p, half).start()

    def step_body(t, carry):
        packed = functools.reduce(lambda x, i: jnp.where(t == i, TABLE[i], x), range(len(TABLE)), 0)
        code, n, event = packed % 16, packed // 16 % 16, packed // 256

        def step_o():
            with scope('own_kv'):
                project(own, *group(n), (KEY, VAL))

        def step_kv(t_):
            with scope(f'par_{t_}'):
                for i in TWO:
                    project(partner, *group(2 * n + i), (t_,))

        def step_q(heads, w):
            with scope(f'que_{w}'):
                queries(heads, w, n)

        def step_out(v, m):
            @pl.when(inner)
            def _():
                k = order(n)

                def halves():
                    for half in TWO:
                        with scope(f'wait_h{half}'):
                            arrived(ws.at[0, pl.ds(0, B), :], o_recv.at[k, half])
                        o_times(k, v, m, half * 128, 128)

                def whole():
                    with scope('wait_o'):
                        for half in TWO:
                            arrived(ws.at[0, pl.ds(0, B), :], o_recv.at[k, half])
                    with scope(f'out{v}'):
                        o_times(k, v, m)

                if m == 2:
                    pl.when(n == 0)(halves)
                    pl.when(n > 0)(whole)
                else:
                    with scope(f'out{v}'):
                        o_times(k, v, m)

        f = functools.partial
        kinds = {'-': lambda: None, 'O': step_o, 'P': f(step_q, own, QUE), 'K': f(step_kv, KEY), 'V': f(step_kv, VAL), 'Q': f(step_q, partner, KEY),
                 'A': lambda: chunk_tiles(n // 4, n % 4, 0), 'B': lambda: chunk_tiles(n // 4, n % 4, 1), 'R': f(step_out, 2, 2), 'L': f(step_out, 1, 1), 'N': f(step_out, 0, 1)}
        choose(code, [kinds[c] for c in KINDS])
        call = functools.partial

        events = {
            'free': [call(signal_ready, 1), call(on, inner, lambda: start(wo_own()))],
            'r0': [call(wait_ready, 0)],
            'r1': [call(wait_ready, 1)],
            'so': [call(kv_start, kvp_copy, own)],
            'po': [call(kv_wait, kvp_copy, own)],
            'sp': [call(kv_start, kvp_copy, partner)],
            'pp': [call(kv_wait, kvp_copy, partner)],
        }
        for t_, c in enumerate('kvq'):
            events['b' + c] = [call(lq_start, t_)]
            events['l' + c] = [call(ev_last, t_)]
            events['w' + c] = [call(ev_weights, t_)]
            for i in TWO:
                for e, f in zip('zxy', (ev_z, ev_xy, ev_y)):
                    events[f'{e}{c}{i}'] = [call(f, lq_copy, 2 * t_ + i)]
        for i, vs in enumerate(((2, 3), (1,), (0,))):
            events[f'b{i}'] = [call(lo_start, *vs)]
            for e, f in zip('zmxycwv', (call(ev_z, lo_copy), call(ev_near, lo_copy), call(ev_far, lo_copy), call(ev_y, lo_copy), ev_lb, ev_wo, ev_wo_ready)):
                events[f'{e}{i}'] = [call(on, inner, call(f, *vs))]
        events['v0'] += [call(on, inner, lambda: local(xp.at[1 - side, pl.ds(0, 2)], wo_sem.at[4]))]
        for v in range(4):
            events[f'd{v}'] = [call(on, outer, lambda v=v: lb_z(v).start())]
        for h in HEADS:
            for z in TWO:
                events[f's{h}{z}'] = [kvr_copy(h, z).start]
            events[f'f{h}'] = [call(kv_forward, [h])]
            events[f'g{h}'] = [call(kv_wait, kvf_copy, [h])]
        for k in ROWS:
            for p in TWO:
                events['op'[p] + str(k)] = [call(send_o, (k,), p)]
        def run(names):
            for name in names.split(','):
                where, _, name = name.rpartition(':')
                if where:
                    on(inner if where == 'i' else outer, *events[name])
                else:
                    for c in events[name]:
                        c()

        @pl.when(event > 0)
        def _():
            choose(event - 1, [functools.partial(run, names) for names in EVENTS])
        return carry

    lax.fori_loop(0, len(TABLE), step_body, None)

    all_sent(lq_ref, 0)
    all_sent(lo_ref.at[:, 0, 0], 2)
    all_sent(lb_ref.at[:, 0], 3)
    all_sent(kvp_s, 4)
    all_sent(kvr_s.at[:, pl.ds(0, 2)], 5)
    all_sent(kvr_s.at[:, pl.ds(0, 2)], 6)

    @pl.when(outer)
    def _():
        all_sent(xb, 7)

    @pl.when(inner)
    def _():
        all_sent(lo_ref.at[:, pl.ds(0, 7)], 1)
        with scope('y_sent'):
            all_sent(xp.at[side, :, :, pl.ds(H, 3 * H)], 8)
        local(xp.at[side, :, :, pl.ds(0, H)], sent.at[9])

    for seg in TWO:
        @pl.when(tp != 1 + seg)
        def _(seg=seg):
            with scope(f'recv{seg}'):
                arrived(out_ref.at[seg], y_recv.at[seg])


PROGRAM = (
    'O.i:zk0,i:zk1', 'O.i:bv,o:zk0', 'O.o:zk1,s00,i:xk0', 'O.o:bv,o:xk0,i:xk1,o:s01,d3', 'O.o:xk1,i:yk0,i:zv0', 'O.o:yk0,i:yk1,i:zv1,i:s01,i:bq',
    'P.o:bq,so', 'P.o:yk1,lk,o:zv0,d1,i:xv0', 'P.wk,o:zv1,i:xv1', 'K.i:zq0', 'K.o:xv0,i:zq1,f0', 'K.o:xv1,o:zq0,i:yv0,i:yv1,b0,b1,r0,po,g0,o:zq1',
    'T0.o0,o1,d0,o:yv0,o:yv1,lv,i:xq0,i:xq1', 'P.wv,z0,o:xq0,b2', 'V.o:xq1,sp,o:s10,o:s11', 'V.c0,z1,o:s20,o:s21',
    'V.free,yq0,yq1,lq,m0,o:s30,o:s31,wq', 'Q.pp,r1,x0,c1', 'T4.p0,p1,m1,x1,y0,w0,v0', 'R.y1,w1,v1,i:s10,i:s11', 'L', 'Q', 'T5.p2,p3,o:f1', 'R', 'L',
    'Q', 'Q.i:f1,o:g1,i:s20,i:s21', 'T2.i:g1,o:f2', 'T1.o2,o3,o:g2,o:f3', 'R.i:s30,i:s31', 'L.i:f2', 'R', 'L.i:g2', 'T6.p4,o4,p5,o5,o:g3', 'R',
    'T3.i:f3,z2,c2', 'L.i:g3', 'T7.p6,o6,p7,o7', 'R.m2,x2', 'L', 'R.y2', 'L.w2', '-.v2', 'N', 'N', 'N', 'R', 'L', 'N', 'N', 'N', 'N', 'N',
)
KINDS = '-OPKVQABRLN'


def tables():
    table, seen = [], {}
    names = tuple(dict.fromkeys(s.partition('.')[2] for s in PROGRAM if '.' in s))
    for s in PROGRAM:
        name, _, after = s.partition('.')
        kind, n = name[0], seen.get(name[0], 0)
        seen[kind] = n + 1
        if kind == 'T':
            n = int(name[1:])
            kind = 'AB'[n in (2, 3, 4, 5)]
        table.append(KINDS.index(kind) + 16 * n + 256 * (names.index(after) + 1 if after else 0))
    return table, names


TABLE, EVENTS = tables()


def main(bias, x, wk, wv, wq, w_out):
    anyspec = pl.BlockSpec(memory_space=pl.ANY)
    vmem = [((4, B, M), BF), ((B, B), BF), ((2, 8, B, M), BF), ((3, M, H), BF), ((4, 8, B, B), BF), ((4, 12, 2, B, B), BF), ((4, 4, 2, B, B), BF), ((4, 4, 2, B, B), BF),
            ((3072, H), F32), ((M, H), F32), ((64, 128), F32)]
    dma = [(4,), (9,), (5,), (10,), (6, 5), (4, 5), (4, 2), (3, 4), (8, 2), (2,)]
    return pl.pallas_call(
        main_kernel,
        in_specs=[pl.BlockSpec(memory_space=pltpu.SMEM)] + [anyspec] * 5,
        out_specs=[anyspec] * 4,
        out_shape=[jax.ShapeDtypeStruct(s, BF) for s in ((2, 8, B, H), (8, 6, B, B), (4, 8, 2, 64, H), (4, 2, B, H))],
        scratch_shapes=[pltpu.VMEM(*v) for v in vmem] + [pltpu.SemaphoreType.DMA(d) for d in dma] + [pltpu.SemaphoreType.REGULAR((2,))],
        compiler_params=params(collective_id=0, has_side_effects=True),
        cost_estimate=pl.CostEstimate(flops=10**11, bytes_accessed=10**8, transcendentals=0),
        name='main',
    )(bias, x, wk, wv, wq, w_out)[0]


def solution(mesh):
    def device_fn(hidden, w_query, w_key, w_value, w_out, branch_bias):
        return unpermute(main(branch_bias, hidden, w_key, w_value, w_query, w_out))

    return jax.shard_map(device_fn, mesh=mesh, in_specs=(P(('dp', 'sp'), None), P(None, 'tp'), P(None, 'tp'), P(None, 'tp'), P('tp', None), P(None, None)), out_specs=P(('dp', 'sp'), 'tp'), check_vma=False)
```

```python
import functools
import math

import jax
import jax.numpy as jnp
from jax import lax
from jax.experimental import pallas as pl
from jax.experimental.pallas import tpu as pltpu
from jax.sharding import PartitionSpec as P

MESH = pl.DeviceIdType.MESH
BF = jnp.bfloat16
F32 = jnp.float32
B, H, M = 256, 512, 2048
KAPPA = math.log2(math.e) / 16
VMEM = 66_900_000
SLOT = (0, 4, 2, 6, 1, 5, 3, 7)
KEY, VAL, QUE = range(3)
HEADS = range(4)
TWO = range(2)
ROWS = range(8)


def nn(a, b):
    return lax.dot_general(a, b, (((1,), (0,)), ((), ())), preferred_element_type=F32)


def nt(a, b):
    return lax.dot_general(a, b, (((1,), (1,)), ((), ())), preferred_element_type=F32)


def params(**kw):
    return pltpu.CompilerParams(vmem_limit_bytes=VMEM, **kw)


def ds(start, size, align=128):
    return pl.ds(pl.multiple_of(start, align), size)


def part(i, size):
    return slice(i * size, i * size + size)


def phase_matrix(transposed):
    r = lax.broadcasted_iota(jnp.int32, (B, B), int(transposed))
    p = lax.broadcasted_iota(jnp.int32, (B, B), int(not transposed))
    k = r // 32
    return (p == (r % 32) * 8 + k // 2 + 4 * (k % 2)).astype(F32).astype(BF)


def unpermute_kernel(y_ref, o_ref, y_s, o_s, load, store):
    pieces = [(s, j) for s in TWO for j in range(4)]

    def get(i):
        s, j = pieces[i]
        return pltpu.make_async_copy(y_ref.at[s, :, pl.ds(j * 64, 64)], y_s.at[i], load.at[i])

    def put(i):
        return pltpu.make_async_copy(o_s.at[i], o_ref.at[pl.ds(i * H, H)], store.at[i])

    for i in ROWS:
        get(i).start()
    pm = phase_matrix(True)
    for i in range(0, 8, 2):
        group = (i, i + 1)
        for k in group:
            get(k).wait()
        for k in group:
            for j in TWO:
                o_s[k, part(j, B), :] = nn(pm, y_s[k, :, part(j, 32), :].reshape(B, H)).astype(BF)
        for k in group:
            put(k).start()
    for i in ROWS:
        put(i).wait()


def unpermute(y):
    anyspec = pl.BlockSpec(memory_space=pl.ANY)
    return pl.pallas_call(
        unpermute_kernel,
        in_specs=[anyspec],
        out_specs=anyspec,
        out_shape=jax.ShapeDtypeStruct((2 * M, H), BF),
        scratch_shapes=[pltpu.VMEM((8, 8, 64, H), BF), pltpu.VMEM((8, H, H), BF), pltpu.SemaphoreType.DMA((8,)), pltpu.SemaphoreType.DMA((8,))],
        compiler_params=params(),
        name='unpermute',
    )(y)


def tile_steps(q, wide, narrow, s_ref, n_ref, done):
    st = {}
    logits, sums = [], []

    def add(name, x):
        st[name] = st[name] + x if name in st else x

    for groups, ref in ((wide, s_ref), (narrow, n_ref)):
        off = 0
        for keys, parts in groups:
            def qk(keys=keys, parts=parts, off=off, ref=ref):
                s = nt(keys(), q() if ref is s_ref else q()[:B])
                o = 0
                for _, n, b in parts:
                    piece = s[o:o + n]
                    ref[pl.ds(off + o, n), :] = piece
                    t = jnp.max(piece, axis=0, keepdims=True) * KAPPA
                    if b is not None:
                        t = t + fit(b, t)
                    if ref is n_ref:
                        t = jnp.concatenate([t, st['top'][:, B:]], axis=1)
                    st['top'] = jnp.maximum(st['top'], t) if 'top' in st else t
                    o += n
            logits.append(qk)
            for v, n, b in parts:
                def sv(v=v, n=n, b=b, off=off, ref=ref):
                    top = st['top'] if ref is s_ref else st['top'][:, :B]
                    e = jnp.exp2(ref[pl.ds(off, n), :] * KAPPA - (top if b is None else top - fit(b, top)))
                    name = 'w' if ref is s_ref else 'n'
                    add('l' + name, jnp.sum(e, axis=0, keepdims=True))
                    add('o' + name, nn(v(), e.astype(BF)))
                sums.append(sv)
                off += n

    def finish():
        o, l = st['ow'], st['lw']
        if narrow:
            o = jnp.concatenate([o[:, :B] + st['on'], o[:, B:]], axis=1)
            l = jnp.concatenate([l[:, :B] + st['ln'], l[:, B:]], axis=1)
        done(o / l)

    return logits, sums + [finish]


def fit(b, like):
    return b if b.shape == like.shape else jnp.concatenate([b] * (like.shape[1] // 128), axis=1)


def interleave(a, b):
    i = j = 0
    while i < len(a) or j < len(b):
        if j >= len(b) or (i < len(a) and i * len(b) <= j * len(a)):
            a[i]()
            i += 1
        else:
            b[j]()
            j += 1


def run_tiles(tiles):
    before = []
    for logits, sums in tiles:
        interleave(logits, before)
        before = sums
    interleave([], before)


def choose(x, cases):
    def among(lo, hi):
        mid = (lo + hi) // 2
        if hi - lo == 1:
            cases[lo]()
        else:
            pl.when(x < mid)(lambda: among(lo, mid))
            pl.when(x >= mid)(lambda: among(mid, hi))
    among(0, len(cases))


def on(cond, *calls):
    @pl.when(cond)
    def _():
        for c in calls:
            c()


def scope(name):
    return jax.named_scope(name)


def main_kernel(bias_ref, x_ref, wk_ref, wv_ref, wq_ref, wout_ref, out_ref, lq_ref, lo_ref, lb_ref,
                xb, pm, xp, ws, q_s, kv_s, kvp_s, kvr_s, s_scr, t_scr,
                beta_s, x_sem, w_sem, wo_sem, sent, lq_recv, lo_recv, lb_recv, kv_recv, o_recv, y_recv, ready):
    dp, tp, sp = lax.axis_index('dp'), lax.axis_index('tp'), lax.axis_index('sp')
    idx = dp * 4 + sp
    side = tp // 2
    inner = (tp == 1) | (tp == 2)
    outer = jnp.logical_not(inner)
    W = (wk_ref, wv_ref, wq_ref)
    peer_x, peer_y, peer_c = {'dp': dp ^ 1}, {'sp': sp ^ 2}, {'sp': sp ^ 1}

    def remote(src, dst, ss, rs, dev):
        return pltpu.make_async_remote_copy(src_ref=src, dst_ref=dst, send_sem=ss, recv_sem=rs, device_id=dev, device_id_type=MESH)

    def lq_copy(t, src, dst, dev):
        return remote(lq_ref.at[src, t], lq_ref.at[dst, t], sent.at[0], lq_recv.at[t, min(dst, 4)], dev)

    def lq_z(t):
        return remote(W[t // 2].at[ds(idx * B, B), pl.ds(t % 2 * B, B)], lq_ref.at[0, t], sent.at[0], lq_recv.at[t, 0], {'tp': tp ^ 2})

    def lq_start(t):
        for i in TWO:
            lq_z(2 * t + i).start()

    def lo_copy(v, src, dst, dev):
        return remote(lo_ref.at[v, src], lo_ref.at[v, dst], sent.at[1], lo_recv.at[v, min(dst, 4)], dev)

    def lo_z(v):
        dst = 2 - side
        b = (tp ^ dst) - 2
        return remote(wout_ref.at[ds(idx * 64, 64, 64), ds((dst ^ v) * H, H)], lo_ref.at[v, 0, b], sent.at[2], lo_recv.at[v, 0], {'tp': dst})

    def lb_z(v):
        return remote(wout_ref.at[ds(sp % 2 * B, B), ds((tp ^ 1 ^ v) * H, H)], lb_ref.at[v, sp % 2], sent.at[3], lb_recv.at[v, 0], {'tp': tp ^ 1})

    def lb_core(v):
        return remote(lb_ref.at[v, sp % 2], lb_ref.at[v, sp % 2], sent.at[3], lb_recv.at[v, 1], peer_c)

    def lo_start(*vs):
        for v in vs:
            lo_z(v).start()

    def arrived(ref, sem):
        remote(ref, ref, sent.at[0], sem, peer_c).wait_recv()

    def all_sent(ref, i):
        remote(ref, ref, sent.at[i], sent.at[i], peer_c).wait_send()

    def lo_zwait(v):
        arrived(lo_ref.at[v, 0], lo_recv.at[v, 0])

    def hop(copy, p, i):
        near, far, n = (peer_x, peer_y, 1) if copy is lo_copy and p == 2 else (peer_y, peer_x, 2)
        f = 3 - n
        return copy(p, *((0, n, near), (0, f, far), (0, 4, peer_c), (n, 3, far), (n, 4 + n, peer_c), (f, 4 + f, peer_c), (3, 7, peer_c))[i])

    def ev_z(copy, *ps):
        for p in ps:
            with scope(f'z_{copy.__name__}{p}'):
                lq_z(p).wait_recv() if copy is lq_copy else lo_zwait(p)
            hop(copy, p, 0).start()
        for p in ps:
            hop(copy, p, 1).start()
            hop(copy, p, 2).start()

    def ev_near(copy, *ps):
        for p in ps:
            with scope(f'n_{copy.__name__}{p}'):
                hop(copy, p, 0).wait_recv()
            hop(copy, p, 3).start()
            hop(copy, p, 4).start()

    def ev_far(copy, *ps):
        for p in ps:
            with scope(f'f_{copy.__name__}{p}'):
                hop(copy, p, 1).wait_recv()
            hop(copy, p, 5).start()

    def ev_xy(copy, *ps):
        ev_near(copy, *ps)
        ev_far(copy, *ps)

    def ev_y(copy, *ps):
        for p in ps:
            with scope(f'y_{copy.__name__}{p}'):
                hop(copy, p, 3).wait_recv()
            hop(copy, p, 6).start()
            if copy is lq_copy and p >= 2:
                start(w_load(p, SLOT[:4]))

    def ev_done(copy, *ps):
        for p in ps:
            with scope(f'c_{copy.__name__}{p}'):
                if copy is lq_copy:
                    arrived(lq_ref.at[pl.ds(4, 4), p], lq_recv.at[p, 4])
                else:
                    arrived(lo_ref.at[p, pl.ds(4, 4)], lo_recv.at[p, 4])

    def w_load(p, slots):
        return [pltpu.make_async_copy(lq_ref.at[SLOT.index(m), p], ws.at[p // 2 % 2, ds((idx ^ m) * B, B), pl.ds(p % 2 * B, B)], w_sem.at[p]) for m in slots]

    def own_load(t):
        return pltpu.make_async_copy(W[t], ws.at[t], w_sem.at[6 + t])

    def start(copies):
        for c in copies:
            c.start()

    def wait(copies):
        for c in copies:
            c.wait()

    def ev_last(t):
        pieces = [2 * t + i for i in TWO]
        ev_done(lq_copy, *pieces)
        for p in pieces:
            start(w_load(p, SLOT[4:] if t else SLOT))

    def local(ref, sem):
        pltpu.make_async_copy(ref, ref, sem).wait()

    def ev_weights(t):
        with scope(f'load{t}'):
            for i in TWO:
                local(ws.at[t % 2, :, pl.ds(i * B, B)], w_sem.at[2 * t + i])

    def ev_wo(*vs):
        ev_done(lo_copy, *vs)
        for v in vs:
            lb_core(v).wait_recv()
        start(wo_load(*vs))

    def ev_wo_ready(*vs):
        with scope(f'wo{vs[0]}'):
            for v in vs:
                local(xp.at[1 - side, pl.ds(2, 6), :, pl.ds((v ^ 2) * H, H)], wo_sem.at[v])

    def ev_lb(*vs):
        for v in vs:
            with scope(f'lb{v}'):
                lb_z(v).wait_recv()
            lb_core(v).start()

    wo = xp.at[1 - side]

    def wo_own():
        return [pltpu.make_async_copy(wout_ref.at[pl.ds(r * B, B), pl.ds(c * H, H)], xp.at[1 - side, r, :, ds((c ^ tp ^ 2) * H, H)], wo_sem.at[4])
                for r in TWO for c in range(4)]

    def wo_load(*vs):
        out = []
        for v in vs:
            cols = pl.ds((v ^ 2) * H, H)
            for s, m in enumerate(SLOT):
                row = (idx ^ m) * 64
                for b in TWO:
                    out.append(pltpu.make_async_copy(lo_ref.at[v, s, b], xp.at[1 - side, 4 + 2 * b + row // B, ds(row % B, 64, 64), cols], wo_sem.at[v]))
            for r in TWO:
                out.append(pltpu.make_async_copy(lb_ref.at[v, r], xp.at[1 - side, 2 + r, :, cols], wo_sem.at[v]))
        return out

    def kvp_copy(h, s):
        return remote(kv_s.at[h, pl.ds(8 * s, 2)], kvp_s.at[h, pl.ds(2 * s, 2)], sent.at[4], kv_recv.at[0, h], peer_c)

    def kvr_copy(h, s):
        return remote(kv_s.at[h, 8 * s], kvr_s.at[h, s], sent.at[5], kv_recv.at[1, h], peer_y)

    def kvf_copy(h, s):
        return remote(kvr_s.at[h, s], kvr_s.at[h, 2 + s], sent.at[6], kv_recv.at[2, h], peer_c)

    def kv_start(copy, heads):
        for h in heads:
            for s in TWO:
                copy(h, s).start()

    def kv_wait(copy, heads):
        with scope(f'w_{copy.__name__}{heads[0]}'):
            for h in heads:
                i = (kvp_copy, kvr_copy, kvf_copy).index(copy)
                arrived((kvp_s.at[h], kvr_s.at[h, pl.ds(0, 2)], kvr_s.at[h, pl.ds(2, 2)])[i], kv_recv.at[i, h])

    def kv_forward(heads):
        kv_wait(kvr_copy, heads)
        kv_start(kvf_copy, heads)

    def reverse(i):
        return (i % 2) * 2 + i // 2

    def order(n):
        return 2 * reverse(n % 4) + ((n // 4) ^ side)

    def o_at(k, p, theirs, col, size, row=0, rows=B):
        if p:
            return ws.at[1 + theirs, ds(k * B + row, rows), ds(col, size)]
        return xb.at[k // 2, pl.ds(row, rows), ds((k % 2) * 1024 + theirs * H + col, size)]

    def o_copy(k, p, half):
        row = half * 128
        return remote(o_at(k, p, 0, 0, H, row, 128), o_at(k, p, 1, 0, H, row, 128), sent.at[7], o_recv.at[k, half], {'tp': tp ^ 1})

    def o_times(k, v, n, row=0, rows=B):
        cols = pl.ds((v ^ 2) * H, n * H)
        y = nn(xb[k // 2, pl.ds(row, rows), ds((k % 2) * 1024, 1024)], wo[0:4, :, cols].reshape(1024, n * H))
        for i in TWO:
            y = y + nn(ws[1 + i, ds(k * B + row, rows), :], wo[part(2 + i, 2), :, cols].reshape(H, n * H))
        y = y.astype(BF)
        for i in range(n):
            y_src(k, v + i, row, rows)[...] = y[:, part(i, H)]
            y_copy(k, v + i, side, row, rows).start() if v else y_local(k).start()

    def y_src(k, v, row=0, rows=B):
        return xp.at[side, k, pl.ds(row, rows), pl.ds(v * H, H)]

    def y_copy(k, v, seg, row, rows):
        return remote(y_src(k, v, row, rows), out_ref.at[seg, k, pl.ds(row, rows)], sent.at[8], y_recv.at[seg], {'tp': tp ^ v})

    def y_local(k):
        return pltpu.make_async_copy(y_src(k, 0), out_ref.at[side, k], sent.at[9])

    def x_copy(j):
        return pltpu.make_async_copy(x_ref.at[ds(j * B, B), :], xb.at[lax.rem(j, 4)], x_sem.at[lax.rem(j, 4)])

    for j in range(4):
        x_copy(j).start()
    barrier = pltpu.get_barrier_semaphore()
    peers = [{'tp': tp ^ 1}, {'tp': tp ^ 2}, {'tp': tp ^ 3}, peer_x, peer_y, peer_c]
    for dev in peers:
        pl.semaphore_signal(barrier, inc=1, device_id=dev, device_id_type=MESH)
    for t in range(3):
        own_load(t).start()

    pm[...] = phase_matrix(False)

    def permute_body(j, carry):
        x_copy(j).wait()
        y = nn(pm[...], xb[lax.rem(j, 4)]).astype(BF).reshape(8, 32, M)
        xp[j // 8, :, ds(lax.rem(j, 8) * 32, 32, 32), :] = y
        pl.when(j < 12)(lambda: x_copy(j + 4).start())

        @pl.when(j == 7)
        def _():
            with scope('barrier'):
                pl.semaphore_wait(barrier, len(peers))
            lq_start(KEY)
            on(outer, lb_z(2).start)
        return carry

    with scope('permute'):
        lax.fori_loop(0, 16, permute_body, None)

    for h in HEADS:
        column = 2 * (tp ^ (h // 2 * 2)) + h % 2
        for i, branches in enumerate(('0', '01', '1', '012', '12', '2', '0123', '123', '23', '3')):
            rows = [jnp.full((1, 128), bias_ref[j, column], F32) for j in map(int, branches)]
            m = functools.reduce(jnp.maximum, rows)
            beta_s[pl.ds(h * 16 + i, 1), :] = (m + jnp.log(sum(jnp.exp(r - m) for r in rows))) * math.log2(math.e)

    def signal_ready(i):
        pl.when(inner)(lambda: pl.semaphore_signal(ready.at[i], inc=1, device_id={'tp': tp ^ 1}, device_id_type=MESH))

    def wait_ready(i):
        with scope(f'ready{i}'):
            pl.when(outer)(lambda: pl.semaphore_wait(ready.at[i], 1))

    signal_ready(0)

    def group(g):
        low = g < 4
        return jnp.where(low, g & 1, 0), jnp.where(low, g // 2, g - 2)

    def head_number(h):
        return 2 * (tp ^ (h // 2 * 2)) + h % 2

    def project(heads, sigma, pair, kinds):
        for h in heads:
            t = head_number(h) + reverse(pair)
            x, swap = xp[side ^ sigma, pl.ds(2 * (t & 3), 2)].reshape(H, M), (t & 7) >> 2
            for t in kinds:
                y = nn(x, ws[t, :, part(h % 2, B)])
                for j in TWO:
                    piece = y[part(j, B)]
                    kv_s[h, 8 * sigma + 2 * pair + (j ^ swap), t] = (piece.T if t == VAL else piece).astype(BF)

    def phases_of(j):
        return [j % 2 + 2 * i for i in TWO], (j // 2) ^ side

    def rank_of(phase, h):
        rel = (phase - head_number(h)) & 7
        return (rel & 1) * 4 + ((rel >> 1) & 1) * 2 + (rel >> 2)

    def queries(heads, w, j):
        phases, half = phases_of(j)
        x = jnp.concatenate([xp[side, 2 * f + half] for f in phases])
        for h in heads:
            y = nn(x, ws[w, :, part(h % 2, B)]).astype(BF)
            for i, f in enumerate(phases):
                q_s[h, rank_of(f + 4 * half, h)] = y[part(i, B)]

    with scope('own_w'):
        for t in range(3):
            own_load(t).wait()
    own, partner = HEADS[:2], HEADS[2:]

    def mix(b, c):
        return jnp.concatenate([b, b, c, c], axis=1)

    def keys_of(ref, h, i, weights):
        parts = []
        n = 0
        for count, b in weights:
            def values(i=i + n, count=count):
                v = [ref[h, i + j, VAL] for j in range(count)]
                return v[0] if count == 1 else jnp.concatenate(v, axis=1)
            parts.append((values, count * B, b))
            n += count
        return (lambda: ref[h, i:i + n, KEY].reshape(n * B, B)), parts

    def chunk_tiles(p, j, kind):
        both_phases, half = phases_of(j)

        def put(h, phase, ot):
            k = 2 * (phase & 3) + half
            y = ot.T.astype(BF)
            for i in TWO:
                pl.when(p == i)(lambda i=i: o_at(k, i, 0, (h % 2) * B, B).__setitem__(..., y))

        def tile(h, phases, ranks, wide, narrow, s_ref, n_ref):
            def done(ot):
                for i, phase in enumerate(phases):
                    put(h, phase, ot[:, part(i, B)])
            return tile_steps(lambda: jnp.concatenate([q_s[h, r] for r in ranks]), wide, narrow, s_ref, n_ref, done)

        h = 2 * p + (j % 2) ^ 1
        rest = tile(h, both_phases, [rank_of(f + 4 * half, h) for f in both_phases], [keys_of(kv_s, h, i, [(2, None)]) for i in range(0, 8, 2)], [], t_scr, None)
        h = 2 * p + (j % 2)
        a = head_number(h)
        b0, b01, b1, b012, b12, b2, b0123, b123, b23, b3 = [beta_s[pl.ds(h * 16 + i, 1), :] for i in range(10)]
        phases = [a & 3, (a & 3) ^ 2]
        both = [keys_of(kv_s, h, i, [(2, b)]) for i, b in ((2, b01), (4, b0), (6, b0), (10, b1))]
        if kind == 0:
            both += [keys_of(kv_s, h, 0, [(1, mix(b0123, b01)), (1, mix(b012, b01))]), keys_of(kv_s, h, 8, [(1, mix(b123, b1)), (1, mix(b12, b1))])]
            first = [keys_of(kvp_s, h, i, [(1, b23), (1, b2)]) for i in (0, 2)] + [keys_of(kvr_s, h, i, [(2, b3)]) for i in (0, 2)]
        else:
            both += [keys_of(kv_s, h, 0, [(2, mix(b012, b01))]), keys_of(kv_s, h, 8, [(2, mix(b12, b1))])]
            first = [keys_of(kvp_s, h, i, [(2, b2)]) for i in (0, 2)]
        with scope(f'tile{kind}'):
            run_tiles([rest, tile(h, phases, [kind, rank_of(phases[1] + 4 * half, h)], both, first, s_scr, t_scr.at[:, pl.ds(0, B)])])

    def send_o(ks, p):
        @pl.when(outer)
        def _():
            for k in ks:
                for half in TWO:
                    o_copy(order(k), p, half).start()

    def step_body(t, carry):
        packed = functools.reduce(lambda x, i: jnp.where(t == i, TABLE[i], x), range(len(TABLE)), 0)
        code, n, event = packed % 16, packed // 16 % 16, packed // 256

        def step_o():
            with scope('own_kv'):
                project(own, *group(n), (KEY, VAL))

        def step_kv(t_):
            with scope(f'par_{t_}'):
                for i in TWO:
                    project(partner, *group(2 * n + i), (t_,))

        def step_q(heads, w):
            with scope(f'que_{w}'):
                queries(heads, w, n)

        def step_out(v, m):
            @pl.when(inner)
            def _():
                k = order(n)

                def halves():
                    for half in TWO:
                        with scope(f'wait_h{half}'):
                            arrived(ws.at[0, pl.ds(0, B), :], o_recv.at[k, half])
                        o_times(k, v, m, half * 128, 128)

                def whole():
                    with scope('wait_o'):
                        for half in TWO:
                            arrived(ws.at[0, pl.ds(0, B), :], o_recv.at[k, half])
                    with scope(f'out{v}'):
                        o_times(k, v, m)

                if m == 2:
                    pl.when(n == 0)(halves)
                    pl.when(n > 0)(whole)
                else:
                    with scope(f'out{v}'):
                        o_times(k, v, m)

        f = functools.partial
        kinds = {'-': lambda: None, 'O': step_o, 'P': f(step_q, own, QUE), 'K': f(step_kv, KEY), 'V': f(step_kv, VAL), 'Q': f(step_q, partner, KEY),
                 'A': lambda: chunk_tiles(n // 4, n % 4, 0), 'B': lambda: chunk_tiles(n // 4, n % 4, 1), 'R': f(step_out, 2, 2), 'L': f(step_out, 1, 1), 'N': f(step_out, 0, 1)}
        choose(code, [kinds[c] for c in KINDS])
        call = functools.partial

        events = {
            'free': [call(signal_ready, 1), call(on, inner, lambda: start(wo_own()))],
            'r0': [call(wait_ready, 0)],
            'r1': [call(wait_ready, 1)],
            'so': [call(kv_start, kvp_copy, own)],
            'po': [call(kv_wait, kvp_copy, own)],
            'sp': [call(kv_start, kvp_copy, partner)],
            'pp': [call(kv_wait, kvp_copy, partner)],
        }
        for t_, c in enumerate('kvq'):
            events['b' + c] = [call(lq_start, t_)]
            events['l' + c] = [call(ev_last, t_)]
            events['w' + c] = [call(ev_weights, t_)]
            for i in TWO:
                for e, f in zip('zxy', (ev_z, ev_xy, ev_y)):
                    events[f'{e}{c}{i}'] = [call(f, lq_copy, 2 * t_ + i)]
        for i, vs in enumerate(((2, 3), (1,), (0,))):
            events[f'b{i}'] = [call(lo_start, *vs)]
            for e, f in zip('zmxycwv', (call(ev_z, lo_copy), call(ev_near, lo_copy), call(ev_far, lo_copy), call(ev_y, lo_copy), ev_lb, ev_wo, ev_wo_ready)):
                events[f'{e}{i}'] = [call(on, inner, call(f, *vs))]
        events['v0'] += [call(on, inner, lambda: local(xp.at[1 - side, pl.ds(0, 2)], wo_sem.at[4]))]
        for v in range(4):
            events[f'd{v}'] = [call(on, outer, lambda v=v: lb_z(v).start())]
        for h in HEADS:
            for z in TWO:
                events[f's{h}{z}'] = [kvr_copy(h, z).start]
            events[f'f{h}'] = [call(kv_forward, [h])]
            events[f'g{h}'] = [call(kv_wait, kvf_copy, [h])]
        for k in ROWS:
            for p in TWO:
                events['op'[p] + str(k)] = [call(send_o, (k,), p)]
        def run(names):
            for name in names.split(','):
                where, _, name = name.rpartition(':')
                if where:
                    on(inner if where == 'i' else outer, *events[name])
                else:
                    for c in events[name]:
                        c()

        @pl.when(event > 0)
        def _():
            choose(event - 1, [functools.partial(run, names) for names in EVENTS])
        return carry

    lax.fori_loop(0, len(TABLE), step_body, None)

    all_sent(lq_ref, 0)
    all_sent(lo_ref.at[:, 0, 0], 2)
    all_sent(lb_ref.at[:, 0], 3)
    all_sent(kvp_s, 4)
    all_sent(kvr_s.at[:, pl.ds(0, 2)], 5)
    all_sent(kvr_s.at[:, pl.ds(0, 2)], 6)

    @pl.when(outer)
    def _():
        all_sent(xb, 7)

    @pl.when(inner)
    def _():
        all_sent(lo_ref.at[:, pl.ds(0, 7)], 1)
        with scope('y_sent'):
            all_sent(xp.at[side, :, :, pl.ds(H, 3 * H)], 8)
        local(xp.at[side, :, :, pl.ds(0, H)], sent.at[9])

    for seg in TWO:
        @pl.when(tp != 1 + seg)
        def _(seg=seg):
            with scope(f'recv{seg}'):
                arrived(out_ref.at[seg], y_recv.at[seg])


PROGRAM = (
    'O.i:zk0,i:zk1', 'O.i:bv,o:zk0', 'O.o:zk1,s00,i:xk0', 'O.o:bv,o:xk0,i:xk1,o:s01,d3', 'O.o:xk1,i:yk0,i:zv0', 'O.o:yk0,i:yk1,i:zv1,i:s01,i:bq',
    'P.o:bq,so', 'P.o:yk1,lk,o:zv0,d1,i:xv0', 'P.wk,o:zv1,i:xv1', 'K.i:zq0', 'K.o:xv0,i:zq1,f0', 'K.o:xv1,o:zq0,i:yv0,i:yv1,b0,b1,r0,po,g0,o:zq1',
    'T0.o0,o1,d0,o:yv0,o:yv1,lv,i:xq0,i:xq1', 'P.wv,z0,o:xq0,b2', 'V.o:xq1,sp,o:s10,o:s11', 'V.c0,z1,o:s20,o:s21',
    'V.free,yq0,yq1,lq,m0,o:s30,o:s31,wq', 'Q.pp,r1,x0,c1,i:s10,i:s11', 'T4.p0,p1,m1,x1,y0,w0,v0', 'R.y1,w1,v1,i:s20,i:s21', 'L', 'Q.f1',
    'T5.p2,p3,g1', 'R', 'L', 'T1.o2,o3,o:f2', 'R.i:s30,i:s31', 'L', 'Q.o:g2', 'Q.i:f2,o:f3', 'T2', 'R.i:g2', 'L', 'T6.p4,o4,p5,o5,o:g3',
    'R.i:f3,z2,c2', 'L', 'T3.i:g3', 'T7.p6,o6,p7,o7', 'R', 'L.m2,x2', 'R.y2', 'L.w2', '-.v2', 'N', 'N', 'N', 'R', 'L', 'N', 'N', 'N', 'N', 'N',
)
KINDS = '-OPKVQABRLN'


def tables():
    table, seen = [], {}
    names = tuple(dict.fromkeys(s.partition('.')[2] for s in PROGRAM if '.' in s))
    for s in PROGRAM:
        name, _, after = s.partition('.')
        kind, n = name[0], seen.get(name[0], 0)
        seen[kind] = n + 1
        if kind == 'T':
            n = int(name[1:])
            kind = 'AB'[n in (2, 3, 4, 5)]
        table.append(KINDS.index(kind) + 16 * n + 256 * (names.index(after) + 1 if after else 0))
    return table, names


TABLE, EVENTS = tables()


def main(bias, x, wk, wv, wq, w_out):
    anyspec = pl.BlockSpec(memory_space=pl.ANY)
    vmem = [((4, B, M), BF), ((B, B), BF), ((2, 8, B, M), BF), ((3, M, H), BF), ((4, 8, B, B), BF), ((4, 12, 2, B, B), BF), ((4, 4, 2, B, B), BF), ((4, 4, 2, B, B), BF),
            ((3072, H), F32), ((M, H), F32), ((64, 128), F32)]
    dma = [(4,), (9,), (5,), (10,), (6, 5), (4, 5), (4, 2), (3, 4), (8, 2), (2,)]
    return pl.pallas_call(
        main_kernel,
        in_specs=[pl.BlockSpec(memory_space=pltpu.SMEM)] + [anyspec] * 5,
        out_specs=[anyspec] * 4,
        out_shape=[jax.ShapeDtypeStruct(s, BF) for s in ((2, 8, B, H), (8, 6, B, B), (4, 8, 2, 64, H), (4, 2, B, H))],
        scratch_shapes=[pltpu.VMEM(*v) for v in vmem] + [pltpu.SemaphoreType.DMA(d) for d in dma] + [pltpu.SemaphoreType.REGULAR((2,))],
        compiler_params=params(collective_id=0, has_side_effects=True),
        cost_estimate=pl.CostEstimate(flops=10**11, bytes_accessed=10**8, transcendentals=0),
        name='main',
    )(bias, x, wk, wv, wq, w_out)[0]


def solution(mesh):
    def device_fn(hidden, w_query, w_key, w_value, w_out, branch_bias):
        return unpermute(main(branch_bias, hidden, w_key, w_value, w_query, w_out))

    return jax.shard_map(device_fn, mesh=mesh, in_specs=(P(('dp', 'sp'), None), P(None, 'tp'), P(None, 'tp'), P(None, 'tp'), P('tp', None), P(None, None)), out_specs=P(('dp', 'sp'), 'tp'), check_vma=False)
```

```python
import functools
import math

import jax
import jax.numpy as jnp
from jax import lax
from jax.experimental import pallas as pl
from jax.experimental.pallas import tpu as pltpu
from jax.sharding import PartitionSpec as P

MESH = pl.DeviceIdType.MESH
BF = jnp.bfloat16
F32 = jnp.float32
B, H, M = 256, 512, 2048
KAPPA = math.log2(math.e) / 16
VMEM = 66_900_000
SLOT = (0, 4, 2, 6, 1, 5, 3, 7)
KEY, VAL, QUE = range(3)
HEADS = range(4)
TWO = range(2)
ROWS = range(8)


def nn(a, b):
    return lax.dot_general(a, b, (((1,), (0,)), ((), ())), preferred_element_type=F32)


def nt(a, b):
    return lax.dot_general(a, b, (((1,), (1,)), ((), ())), preferred_element_type=F32)


def params(**kw):
    return pltpu.CompilerParams(vmem_limit_bytes=VMEM, **kw)


def ds(start, size, align=128):
    return pl.ds(pl.multiple_of(start, align), size)


def part(i, size):
    return slice(i * size, i * size + size)


def phase_matrix(transposed):
    r = lax.broadcasted_iota(jnp.int32, (B, B), int(transposed))
    p = lax.broadcasted_iota(jnp.int32, (B, B), int(not transposed))
    k = r // 32
    return (p == (r % 32) * 8 + k // 2 + 4 * (k % 2)).astype(F32).astype(BF)


def unpermute_kernel(y_ref, o_ref, y_s, o_s, load, store):
    pieces = [(s, j) for s in TWO for j in range(4)]

    def get(i):
        s, j = pieces[i]
        return pltpu.make_async_copy(y_ref.at[s, :, pl.ds(j * 64, 64)], y_s.at[i], load.at[i])

    def put(i):
        return pltpu.make_async_copy(o_s.at[i], o_ref.at[pl.ds(i * H, H)], store.at[i])

    for i in ROWS:
        get(i).start()
    pm = phase_matrix(True)
    for i in range(0, 8, 2):
        group = (i, i + 1)
        for k in group:
            get(k).wait()
        for k in group:
            for j in TWO:
                o_s[k, part(j, B), :] = nn(pm, y_s[k, :, part(j, 32), :].reshape(B, H)).astype(BF)
        for k in group:
            put(k).start()
    for i in ROWS:
        put(i).wait()


def unpermute(y):
    anyspec = pl.BlockSpec(memory_space=pl.ANY)
    return pl.pallas_call(
        unpermute_kernel,
        in_specs=[anyspec],
        out_specs=anyspec,
        out_shape=jax.ShapeDtypeStruct((2 * M, H), BF),
        scratch_shapes=[pltpu.VMEM((8, 8, 64, H), BF), pltpu.VMEM((8, H, H), BF), pltpu.SemaphoreType.DMA((8,)), pltpu.SemaphoreType.DMA((8,))],
        compiler_params=params(),
        name='unpermute',
    )(y)


def tile_steps(q, wide, narrow, s_ref, n_ref, done):
    st = {}
    logits, sums = [], []

    def add(name, x):
        st[name] = st[name] + x if name in st else x

    for groups, ref in ((wide, s_ref), (narrow, n_ref)):
        off = 0
        for keys, parts in groups:
            def qk(keys=keys, parts=parts, off=off, ref=ref):
                s = nt(keys(), q() if ref is s_ref else q()[:B])
                o = 0
                for _, n, b in parts:
                    piece = s[o:o + n]
                    ref[pl.ds(off + o, n), :] = piece
                    t = jnp.max(piece, axis=0, keepdims=True) * KAPPA
                    if b is not None:
                        t = t + fit(b, t)
                    if ref is n_ref:
                        t = jnp.concatenate([t, st['top'][:, B:]], axis=1)
                    st['top'] = jnp.maximum(st['top'], t) if 'top' in st else t
                    o += n
            logits.append(qk)
            for v, n, b in parts:
                def sv(v=v, n=n, b=b, off=off, ref=ref):
                    top = st['top'] if ref is s_ref else st['top'][:, :B]
                    e = jnp.exp2(ref[pl.ds(off, n), :] * KAPPA - (top if b is None else top - fit(b, top)))
                    name = 'w' if ref is s_ref else 'n'
                    add('l' + name, jnp.sum(e, axis=0, keepdims=True))
                    add('o' + name, nn(v(), e.astype(BF)))
                sums.append(sv)
                off += n

    def finish():
        o, l = st['ow'], st['lw']
        if narrow:
            o = jnp.concatenate([o[:, :B] + st['on'], o[:, B:]], axis=1)
            l = jnp.concatenate([l[:, :B] + st['ln'], l[:, B:]], axis=1)
        done(o / l)

    return logits, sums + [finish]


def fit(b, like):
    return b if b.shape == like.shape else jnp.concatenate([b] * (like.shape[1] // 128), axis=1)


def interleave(a, b):
    i = j = 0
    while i < len(a) or j < len(b):
        if j >= len(b) or (i < len(a) and i * len(b) <= j * len(a)):
            a[i]()
            i += 1
        else:
            b[j]()
            j += 1


def run_tiles(tiles):
    before = []
    for logits, sums in tiles:
        interleave(logits, before)
        before = sums
    interleave([], before)


def choose(x, cases):
    def among(lo, hi):
        mid = (lo + hi) // 2
        if hi - lo == 1:
            cases[lo]()
        else:
            pl.when(x < mid)(lambda: among(lo, mid))
            pl.when(x >= mid)(lambda: among(mid, hi))
    among(0, len(cases))


def on(cond, *calls):
    @pl.when(cond)
    def _():
        for c in calls:
            c()


def scope(name):
    return jax.named_scope(name)


def main_kernel(bias_ref, x_ref, wk_ref, wv_ref, wq_ref, wout_ref, out_ref, lq_ref, lo_ref, lb_ref,
                xb, pm, xp, ws, q_s, kv_s, kvp_s, kvr_s, s_scr, t_scr,
                beta_s, x_sem, w_sem, wo_sem, sent, lq_recv, lo_recv, lb_recv, kv_recv, o_recv, y_recv, ready):
    dp, tp, sp = lax.axis_index('dp'), lax.axis_index('tp'), lax.axis_index('sp')
    idx = dp * 4 + sp
    side = tp // 2
    inner = (tp == 1) | (tp == 2)
    outer = jnp.logical_not(inner)
    W = (wk_ref, wv_ref, wq_ref)
    peer_x, peer_y, peer_c = {'dp': dp ^ 1}, {'sp': sp ^ 2}, {'sp': sp ^ 1}

    def remote(src, dst, ss, rs, dev):
        return pltpu.make_async_remote_copy(src_ref=src, dst_ref=dst, send_sem=ss, recv_sem=rs, device_id=dev, device_id_type=MESH)

    def lq_copy(t, src, dst, dev):
        return remote(lq_ref.at[src, t], lq_ref.at[dst, t], sent.at[0], lq_recv.at[t, min(dst, 4)], dev)

    def lq_z(t):
        return remote(W[t // 2].at[ds(idx * B, B), pl.ds(t % 2 * B, B)], lq_ref.at[0, t], sent.at[0], lq_recv.at[t, 0], {'tp': tp ^ 2})

    def lq_start(t):
        for i in TWO:
            lq_z(2 * t + i).start()

    def lo_copy(v, src, dst, dev):
        return remote(lo_ref.at[v, src], lo_ref.at[v, dst], sent.at[1], lo_recv.at[v, min(dst, 4)], dev)

    def lo_z(v):
        dst = 2 - side
        b = (tp ^ dst) - 2
        return remote(wout_ref.at[ds(idx * 64, 64, 64), ds((dst ^ v) * H, H)], lo_ref.at[v, 0, b], sent.at[2], lo_recv.at[v, 0], {'tp': dst})

    def lb_z(v):
        return remote(wout_ref.at[ds(sp % 2 * B, B), ds((tp ^ 1 ^ v) * H, H)], lb_ref.at[v, sp % 2], sent.at[3], lb_recv.at[v, 0], {'tp': tp ^ 1})

    def lb_core(v):
        return remote(lb_ref.at[v, sp % 2], lb_ref.at[v, sp % 2], sent.at[3], lb_recv.at[v, 1], peer_c)

    def lo_start(*vs):
        for v in vs:
            lo_z(v).start()

    def arrived(ref, sem):
        remote(ref, ref, sent.at[0], sem, peer_c).wait_recv()

    def all_sent(ref, i):
        remote(ref, ref, sent.at[i], sent.at[i], peer_c).wait_send()

    def lo_zwait(v):
        arrived(lo_ref.at[v, 0], lo_recv.at[v, 0])

    def hop(copy, p, i):
        near, far, n = (peer_x, peer_y, 1) if (copy is lo_copy and p == 2) or (copy is lq_copy and p == 5) else (peer_y, peer_x, 2)
        f = 3 - n
        return copy(p, *((0, n, near), (0, f, far), (0, 4, peer_c), (n, 3, far), (n, 4 + n, peer_c), (f, 4 + f, peer_c), (3, 7, peer_c))[i])

    def ev_z(copy, *ps):
        for p in ps:
            with scope(f'z_{copy.__name__}{p}'):
                lq_z(p).wait_recv() if copy is lq_copy else lo_zwait(p)
            hop(copy, p, 0).start()
        for p in ps:
            hop(copy, p, 1).start()
            hop(copy, p, 2).start()

    def ev_near(copy, *ps):
        for p in ps:
            with scope(f'n_{copy.__name__}{p}'):
                hop(copy, p, 0).wait_recv()
            hop(copy, p, 3).start()
            hop(copy, p, 4).start()

    def ev_far(copy, *ps):
        for p in ps:
            with scope(f'f_{copy.__name__}{p}'):
                hop(copy, p, 1).wait_recv()
            hop(copy, p, 5).start()

    def ev_xy(copy, *ps):
        ev_near(copy, *ps)
        ev_far(copy, *ps)

    def ev_y(copy, *ps):
        for p in ps:
            with scope(f'y_{copy.__name__}{p}'):
                hop(copy, p, 3).wait_recv()
            hop(copy, p, 6).start()
            if copy is lq_copy and p >= 2:
                start(w_load(p, SLOT[:4]))

    def ev_done(copy, *ps):
        for p in ps:
            with scope(f'c_{copy.__name__}{p}'):
                if copy is lq_copy:
                    arrived(lq_ref.at[pl.ds(4, 4), p], lq_recv.at[p, 4])
                else:
                    arrived(lo_ref.at[p, pl.ds(4, 4)], lo_recv.at[p, 4])

    def w_load(p, slots):
        return [pltpu.make_async_copy(lq_ref.at[SLOT.index(m), p], ws.at[p // 2 % 2, ds((idx ^ m) * B, B), pl.ds(p % 2 * B, B)], w_sem.at[p]) for m in slots]

    def own_load(t):
        return pltpu.make_async_copy(W[t], ws.at[t], w_sem.at[6 + t])

    def start(copies):
        for c in copies:
            c.start()

    def wait(copies):
        for c in copies:
            c.wait()

    def ev_last(t):
        pieces = [2 * t + i for i in TWO]
        ev_done(lq_copy, *pieces)
        for p in pieces:
            start(w_load(p, SLOT[4:] if t else SLOT))

    def local(ref, sem):
        pltpu.make_async_copy(ref, ref, sem).wait()

    def ev_weights(t):
        with scope(f'load{t}'):
            for i in TWO:
                local(ws.at[t % 2, :, pl.ds(i * B, B)], w_sem.at[2 * t + i])

    def ev_wo(*vs):
        ev_done(lo_copy, *vs)
        for v in vs:
            lb_core(v).wait_recv()
        start(wo_load(*vs))

    def ev_wo_ready(*vs):
        with scope(f'wo{vs[0]}'):
            for v in vs:
                local(xp.at[1 - side, pl.ds(2, 6), :, pl.ds((v ^ 2) * H, H)], wo_sem.at[v])

    def ev_lb(*vs):
        for v in vs:
            with scope(f'lb{v}'):
                lb_z(v).wait_recv()
            lb_core(v).start()

    wo = xp.at[1 - side]

    def wo_own():
        return [pltpu.make_async_copy(wout_ref.at[pl.ds(r * B, B), pl.ds(c * H, H)], xp.at[1 - side, r, :, ds((c ^ tp ^ 2) * H, H)], wo_sem.at[4])
                for r in TWO for c in range(4)]

    def wo_load(*vs):
        out = []
        for v in vs:
            cols = pl.ds((v ^ 2) * H, H)
            for s, m in enumerate(SLOT):
                row = (idx ^ m) * 64
                for b in TWO:
                    out.append(pltpu.make_async_copy(lo_ref.at[v, s, b], xp.at[1 - side, 4 + 2 * b + row // B, ds(row % B, 64, 64), cols], wo_sem.at[v]))
            for r in TWO:
                out.append(pltpu.make_async_copy(lb_ref.at[v, r], xp.at[1 - side, 2 + r, :, cols], wo_sem.at[v]))
        return out

    def kvp_copy(h, s):
        return remote(kv_s.at[h, pl.ds(8 * s, 2)], kvp_s.at[h, pl.ds(2 * s, 2)], sent.at[4], kv_recv.at[0, h], peer_c)

    def kvr_copy(h, s):
        return remote(kv_s.at[h, 8 * s], kvr_s.at[h, s], sent.at[5], kv_recv.at[1, h], peer_y)

    def kvf_copy(h, s):
        return remote(kvr_s.at[h, s], kvr_s.at[h, 2 + s], sent.at[6], kv_recv.at[2, h], peer_c)

    def kv_start(copy, heads):
        for h in heads:
            for s in TWO:
                copy(h, s).start()

    def kv_wait(copy, heads):
        with scope(f'w_{copy.__name__}{heads[0]}'):
            for h in heads:
                i = (kvp_copy, kvr_copy, kvf_copy).index(copy)
                arrived((kvp_s.at[h], kvr_s.at[h, pl.ds(0, 2)], kvr_s.at[h, pl.ds(2, 2)])[i], kv_recv.at[i, h])

    def kv_forward(heads):
        kv_wait(kvr_copy, heads)
        kv_start(kvf_copy, heads)

    def reverse(i):
        return (i % 2) * 2 + i // 2

    def order(n):
        return 2 * reverse(n % 4) + ((n // 4) ^ side)

    def o_at(k, p, theirs, col, size, row=0, rows=B):
        if p:
            return ws.at[1 + theirs, ds(k * B + row, rows), ds(col, size)]
        return xb.at[k // 2, pl.ds(row, rows), ds((k % 2) * 1024 + theirs * H + col, size)]

    def o_copy(k, p, half):
        row = half * 128
        return remote(o_at(k, p, 0, 0, H, row, 128), o_at(k, p, 1, 0, H, row, 128), sent.at[7], o_recv.at[k, half], {'tp': tp ^ 1})

    def o_times(k, v, n, row=0, rows=B):
        cols = pl.ds((v ^ 2) * H, n * H)
        y = nn(xb[k // 2, pl.ds(row, rows), ds((k % 2) * 1024, 1024)], wo[0:4, :, cols].reshape(1024, n * H))
        for i in TWO:
            y = y + nn(ws[1 + i, ds(k * B + row, rows), :], wo[part(2 + i, 2), :, cols].reshape(H, n * H))
        y = y.astype(BF)
        for i in range(n):
            y_src(k, v + i, row, rows)[...] = y[:, part(i, H)]
            y_copy(k, v + i, side, row, rows).start() if v else y_local(k).start()

    def y_src(k, v, row=0, rows=B):
        return xp.at[side, k, pl.ds(row, rows), pl.ds(v * H, H)]

    def y_copy(k, v, seg, row, rows):
        return remote(y_src(k, v, row, rows), out_ref.at[seg, k, pl.ds(row, rows)], sent.at[8], y_recv.at[seg], {'tp': tp ^ v})

    def y_local(k):
        return pltpu.make_async_copy(y_src(k, 0), out_ref.at[side, k], sent.at[9])

    def x_copy(j):
        return pltpu.make_async_copy(x_ref.at[ds(j * B, B), :], xb.at[lax.rem(j, 4)], x_sem.at[lax.rem(j, 4)])

    for j in range(4):
        x_copy(j).start()
    barrier = pltpu.get_barrier_semaphore()
    peers = [{'tp': tp ^ 1}, {'tp': tp ^ 2}, {'tp': tp ^ 3}, peer_x, peer_y, peer_c]
    for dev in peers:
        pl.semaphore_signal(barrier, inc=1, device_id=dev, device_id_type=MESH)
    for t in range(3):
        own_load(t).start()

    pm[...] = phase_matrix(False)

    def permute_body(j, carry):
        x_copy(j).wait()
        y = nn(pm[...], xb[lax.rem(j, 4)]).astype(BF).reshape(8, 32, M)
        xp[j // 8, :, ds(lax.rem(j, 8) * 32, 32, 32), :] = y
        pl.when(j < 12)(lambda: x_copy(j + 4).start())

        @pl.when(j == 2)
        def _():
            with scope('barrier'):
                pl.semaphore_wait(barrier, len(peers))
            lq_start(KEY)
            on(outer, lb_z(2).start)
        return carry

    with scope('permute'):
        lax.fori_loop(0, 16, permute_body, None)

    for h in HEADS:
        column = 2 * (tp ^ (h // 2 * 2)) + h % 2
        for i, branches in enumerate(('0', '01', '1', '012', '12', '2', '0123', '123', '23', '3')):
            rows = [jnp.full((1, 128), bias_ref[j, column], F32) for j in map(int, branches)]
            m = functools.reduce(jnp.maximum, rows)
            beta_s[pl.ds(h * 16 + i, 1), :] = (m + jnp.log(sum(jnp.exp(r - m) for r in rows))) * math.log2(math.e)

    def signal_ready(i):
        pl.when(inner)(lambda: pl.semaphore_signal(ready.at[i], inc=1, device_id={'tp': tp ^ 1}, device_id_type=MESH))

    def wait_ready(i):
        with scope(f'ready{i}'):
            pl.when(outer)(lambda: pl.semaphore_wait(ready.at[i], 1))

    signal_ready(0)

    def group(g):
        low = g < 4
        return jnp.where(low, g & 1, 0), jnp.where(low, g // 2, g - 2)

    def head_number(h):
        return 2 * (tp ^ (h // 2 * 2)) + h % 2

    def project(heads, sigma, pair, kinds):
        for h in heads:
            t = head_number(h) + reverse(pair)
            x, swap = xp[side ^ sigma, pl.ds(2 * (t & 3), 2)].reshape(H, M), (t & 7) >> 2
            for t in kinds:
                y = nn(x, ws[t, :, part(h % 2, B)])
                for j in TWO:
                    piece = y[part(j, B)]
                    kv_s[h, 8 * sigma + 2 * pair + (j ^ swap), t] = (piece.T if t == VAL else piece).astype(BF)

    def phases_of(j):
        return [j % 2 + 2 * i for i in TWO], (j // 2) ^ side

    def rank_of(phase, h):
        rel = (phase - head_number(h)) & 7
        return (rel & 1) * 4 + ((rel >> 1) & 1) * 2 + (rel >> 2)

    def queries(heads, w, j):
        phases, half = phases_of(j)
        x = jnp.concatenate([xp[side, 2 * f + half] for f in phases])
        for h in heads:
            y = nn(x, ws[w, :, part(h % 2, B)]).astype(BF)
            for i, f in enumerate(phases):
                q_s[h, rank_of(f + 4 * half, h)] = y[part(i, B)]

    with scope('own_w'):
        for t in range(3):
            own_load(t).wait()
    own, partner = HEADS[:2], HEADS[2:]

    def mix(b, c):
        return jnp.concatenate([b, b, c, c], axis=1)

    def keys_of(ref, h, i, weights):
        parts = []
        n = 0
        for count, b in weights:
            def values(i=i + n, count=count):
                v = [ref[h, i + j, VAL] for j in range(count)]
                return v[0] if count == 1 else jnp.concatenate(v, axis=1)
            parts.append((values, count * B, b))
            n += count
        return (lambda: ref[h, i:i + n, KEY].reshape(n * B, B)), parts

    def chunk_tiles(p, j, kind):
        both_phases, half = phases_of(j)

        def put(h, phase, ot):
            k = 2 * (phase & 3) + half
            y = ot.T.astype(BF)
            for i in TWO:
                pl.when(p == i)(lambda i=i: o_at(k, i, 0, (h % 2) * B, B).__setitem__(..., y))

        def tile(h, phases, ranks, wide, narrow, s_ref, n_ref):
            def done(ot):
                for i, phase in enumerate(phases):
                    put(h, phase, ot[:, part(i, B)])
            return tile_steps(lambda: jnp.concatenate([q_s[h, r] for r in ranks]), wide, narrow, s_ref, n_ref, done)

        h = 2 * p + (j % 2) ^ 1
        rest = tile(h, both_phases, [rank_of(f + 4 * half, h) for f in both_phases], [keys_of(kv_s, h, i, [(2, None)]) for i in range(0, 8, 2)], [], t_scr, None)
        h = 2 * p + (j % 2)
        a = head_number(h)
        b0, b01, b1, b012, b12, b2, b0123, b123, b23, b3 = [beta_s[pl.ds(h * 16 + i, 1), :] for i in range(10)]
        phases = [a & 3, (a & 3) ^ 2]
        both = [keys_of(kv_s, h, i, [(2, b)]) for i, b in ((2, b01), (4, b0), (6, b0), (10, b1))]
        if kind == 0:
            both += [keys_of(kv_s, h, 0, [(1, mix(b0123, b01)), (1, mix(b012, b01))]), keys_of(kv_s, h, 8, [(1, mix(b123, b1)), (1, mix(b12, b1))])]
            first = [keys_of(kvp_s, h, i, [(1, b23), (1, b2)]) for i in (0, 2)] + [keys_of(kvr_s, h, i, [(2, b3)]) for i in (0, 2)]
        else:
            both += [keys_of(kv_s, h, 0, [(2, mix(b012, b01))]), keys_of(kv_s, h, 8, [(2, mix(b12, b1))])]
            first = [keys_of(kvp_s, h, i, [(2, b2)]) for i in (0, 2)]
        with scope(f'tile{kind}'):
            run_tiles([rest, tile(h, phases, [kind, rank_of(phases[1] + 4 * half, h)], both, first, s_scr, t_scr.at[:, pl.ds(0, B)])])

    def send_o(ks, p):
        @pl.when(outer)
        def _():
            for k in ks:
                for half in TWO:
                    o_copy(order(k), p, half).start()

    def step_body(t, carry):
        packed = functools.reduce(lambda x, i: jnp.where(t == i, TABLE[i], x), range(len(TABLE)), 0)
        code, n, event = packed % 16, packed // 16 % 16, packed // 256

        def step_o():
            with scope('own_kv'):
                project(own, *group(n), (KEY, VAL))

        def step_kv(t_):
            with scope(f'par_{t_}'):
                for i in TWO:
                    project(partner, *group(2 * n + i), (t_,))

        def step_q(heads, w):
            with scope(f'que_{w}'):
                queries(heads, w, n)

        def step_out(v, m):
            @pl.when(inner)
            def _():
                k = order(n)

                def halves():
                    for half in TWO:
                        with scope(f'wait_h{half}'):
                            arrived(ws.at[0, pl.ds(0, B), :], o_recv.at[k, half])
                        o_times(k, v, m, half * 128, 128)

                def whole():
                    with scope('wait_o'):
                        for half in TWO:
                            arrived(ws.at[0, pl.ds(0, B), :], o_recv.at[k, half])
                    with scope(f'out{v}'):
                        o_times(k, v, m)

                if m == 2:
                    pl.when(n == 0)(halves)
                    pl.when(n > 0)(whole)
                else:
                    with scope(f'out{v}'):
                        o_times(k, v, m)

        f = functools.partial
        kinds = {'-': lambda: None, 'O': step_o, 'P': f(step_q, own, QUE), 'K': f(step_kv, KEY), 'V': f(step_kv, VAL), 'Q': f(step_q, partner, KEY),
                 'A': lambda: chunk_tiles(n // 4, n % 4, 0), 'B': lambda: chunk_tiles(n // 4, n % 4, 1), 'R': f(step_out, 2, 2), 'L': f(step_out, 1, 1), 'N': f(step_out, 0, 1)}
        choose(code, [kinds[c] for c in KINDS])
        call = functools.partial

        events = {
            'free': [call(signal_ready, 1), call(on, inner, lambda: start(wo_own()))],
            'r0': [call(wait_ready, 0)],
            'r1': [call(wait_ready, 1)],
            'so': [call(kv_start, kvp_copy, own)],
            'po': [call(kv_wait, kvp_copy, own)],
            'sp': [call(kv_start, kvp_copy, partner)],
            'pp': [call(kv_wait, kvp_copy, partner)],
        }
        for t_, c in enumerate('kvq'):
            events['b' + c] = [call(lq_start, t_)]
            events['l' + c] = [call(ev_last, t_)]
            events['w' + c] = [call(ev_weights, t_)]
            events['z' + c] = [call(ev_z, lq_copy, 2 * t_, 2 * t_ + 1)]
            for i in TWO:
                for e, f in zip('zmfxy', (ev_z, ev_near, ev_far, ev_xy, ev_y)):
                    events[f'{e}{c}{i}'] = [call(f, lq_copy, 2 * t_ + i)]
        for i, vs in enumerate(((2, 3), (1,), (0,))):
            events[f'b{i}'] = [call(lo_start, *vs)]
            for e, f in zip('zmxycwv', (call(ev_z, lo_copy), call(ev_near, lo_copy), call(ev_far, lo_copy), call(ev_y, lo_copy), ev_lb, ev_wo, ev_wo_ready)):
                events[f'{e}{i}'] = [call(on, inner, call(f, *vs))]
        events['v0'] += [call(on, inner, lambda: local(xp.at[1 - side, pl.ds(0, 2)], wo_sem.at[4]))]
        for v in range(4):
            events[f'd{v}'] = [call(on, outer, lambda v=v: lb_z(v).start())]
        for h in HEADS:
            for z in TWO:
                events[f's{h}{z}'] = [kvr_copy(h, z).start]
            events[f'f{h}'] = [call(kv_forward, [h])]
            events[f'g{h}'] = [call(kv_wait, kvf_copy, [h])]
        for k in ROWS:
            for p in TWO:
                events['op'[p] + str(k)] = [call(send_o, (k,), p)]
        def run(names):
            for name in names.split(','):
                where, _, name = name.rpartition(':')
                if where:
                    on(inner if where == 'i' else outer, *events[name])
                else:
                    for c in events[name]:
                        c()

        @pl.when(event > 0)
        def _():
            choose(event - 1, [functools.partial(run, names) for names in EVENTS])
        return carry

    lax.fori_loop(0, len(TABLE), step_body, None)

    all_sent(lq_ref, 0)
    all_sent(lo_ref.at[:, 0, 0], 2)
    all_sent(lb_ref.at[:, 0], 3)
    all_sent(kvp_s, 4)
    all_sent(kvr_s.at[:, pl.ds(0, 2)], 5)
    all_sent(kvr_s.at[:, pl.ds(0, 2)], 6)

    @pl.when(outer)
    def _():
        all_sent(xb, 7)

    @pl.when(inner)
    def _():
        all_sent(lo_ref.at[:, pl.ds(0, 7)], 1)
        with scope('y_sent'):
            all_sent(xp.at[side, :, :, pl.ds(H, 3 * H)], 8)
        local(xp.at[side, :, :, pl.ds(0, H)], sent.at[9])

    for seg in TWO:
        @pl.when(tp != 1 + seg)
        def _(seg=seg):
            with scope(f'recv{seg}'):
                arrived(out_ref.at[seg], y_recv.at[seg])


PROGRAM = (
    'O.i:zk0,i:zk1', 'O.i:bv,o:zk0', 'O.o:zk1,s00,i:xk0', 'O.o:bv,o:xk0,i:xk1,o:s01,d3', 'O.o:xk1,i:yk0,i:zv0', 'O.o:yk0,i:yk1,i:zv1,i:s01,i:bq',
    'P.o:bq,so', 'P.o:yk1,lk,o:zv0,d1,i:xv0', 'P.wk,o:zv1,i:xv1', 'K', 'K.o:xv0,i:zq,f0', 'K.o:xv1,i:yv0,i:yv1,b0,b1,r0,po,g0,o:zq',
    'T0.o0,o1,d0,o:yv0,o:yv1,lv,mq0,i:mq1,i:fq0,i:fq1', 'P.wv,z0,o:mq1,b2', 'V.o:fq0,o:fq1,sp,o:s10,o:s11', 'V.c0,z1,o:s20,o:s21',
    'V.free,yq0,yq1,lq,m0,o:s30,o:s31,wq', 'Q.pp,r1,x0,c1,i:s10,i:s11', 'T4.p0,p1,m1,x1,y0,w0,v0', 'R.y1,w1,v1,i:s20,i:s21', 'L', 'Q.f1',
    'T5.p2,p3,g1', 'R', 'L', 'T1.o2,o3,o:f2', 'R.i:s30,i:s31', 'L', 'Q.o:g2', 'Q.i:f2,o:f3', 'T2', 'R.i:g2', 'L', 'T6.p4,o4,p5,o5,o:g3',
    'R.i:f3,z2,c2', 'L', 'T3.i:g3', 'T7.p6,o6,p7,o7', 'R', 'L.m2,x2', 'R.y2', 'L.w2', '-.v2', 'N', 'N', 'N', 'R', 'L', 'N', 'N', 'N', 'N', 'N',
)
KINDS = '-OPKVQABRLN'


def tables():
    table, seen = [], {}
    names = tuple(dict.fromkeys(s.partition('.')[2] for s in PROGRAM if '.' in s))
    for s in PROGRAM:
        name, _, after = s.partition('.')
        kind, n = name[0], seen.get(name[0], 0)
        seen[kind] = n + 1
        if kind == 'T':
            n = int(name[1:])
            kind = 'AB'[n in (2, 3, 4, 5)]
        table.append(KINDS.index(kind) + 16 * n + 256 * (names.index(after) + 1 if after else 0))
    return table, names


TABLE, EVENTS = tables()


def main(bias, x, wk, wv, wq, w_out):
    anyspec = pl.BlockSpec(memory_space=pl.ANY)
    vmem = [((4, B, M), BF), ((B, B), BF), ((2, 8, B, M), BF), ((3, M, H), BF), ((4, 8, B, B), BF), ((4, 12, 2, B, B), BF), ((4, 4, 2, B, B), BF), ((4, 4, 2, B, B), BF),
            ((3072, H), F32), ((M, H), F32), ((64, 128), F32)]
    dma = [(4,), (9,), (5,), (10,), (6, 5), (4, 5), (4, 2), (3, 4), (8, 2), (2,)]
    return pl.pallas_call(
        main_kernel,
        in_specs=[pl.BlockSpec(memory_space=pltpu.SMEM)] + [anyspec] * 5,
        out_specs=[anyspec] * 4,
        out_shape=[jax.ShapeDtypeStruct(s, BF) for s in ((2, 8, B, H), (8, 6, B, B), (4, 8, 2, 64, H), (4, 2, B, H))],
        scratch_shapes=[pltpu.VMEM(*v) for v in vmem] + [pltpu.SemaphoreType.DMA(d) for d in dma] + [pltpu.SemaphoreType.REGULAR((2,))],
        compiler_params=params(collective_id=0, has_side_effects=True),
        cost_estimate=pl.CostEstimate(flops=10**11, bytes_accessed=10**8, transcendentals=0),
        name='main',
    )(bias, x, wk, wv, wq, w_out)[0]


def solution(mesh):
    def device_fn(hidden, w_query, w_key, w_value, w_out, branch_bias):
        return unpermute(main(branch_bias, hidden, w_key, w_value, w_query, w_out))

    return jax.shard_map(device_fn, mesh=mesh, in_specs=(P(('dp', 'sp'), None), P(None, 'tp'), P(None, 'tp'), P(None, 'tp'), P('tp', None), P(None, None)), out_specs=P(('dp', 'sp'), 'tp'), check_vma=False)
```

```python
import functools
import math

import jax
import jax.numpy as jnp
from jax import lax
from jax.experimental import pallas as pl
from jax.experimental.pallas import tpu as pltpu
from jax.sharding import PartitionSpec as P

MESH = pl.DeviceIdType.MESH
BF = jnp.bfloat16
F32 = jnp.float32
B, H, M = 256, 512, 2048
KAPPA = math.log2(math.e) / 16
VMEM = 66_900_000
SLOT = (0, 4, 2, 6, 1, 5, 3, 7)
KEY, VAL, QUE = range(3)
HEADS = range(4)
TWO = range(2)
ROWS = range(8)


def nn(a, b):
    return lax.dot_general(a, b, (((1,), (0,)), ((), ())), preferred_element_type=F32)


def nt(a, b):
    return lax.dot_general(a, b, (((1,), (1,)), ((), ())), preferred_element_type=F32)


def params(**kw):
    return pltpu.CompilerParams(vmem_limit_bytes=VMEM, **kw)


def ds(start, size, align=128):
    return pl.ds(pl.multiple_of(start, align), size)


def part(i, size):
    return slice(i * size, i * size + size)


def phase_matrix(transposed):
    r = lax.broadcasted_iota(jnp.int32, (B, B), int(transposed))
    p = lax.broadcasted_iota(jnp.int32, (B, B), int(not transposed))
    k = r // 32
    return (p == (r % 32) * 8 + k // 2 + 4 * (k % 2)).astype(F32).astype(BF)


def unpermute_kernel(y_ref, o_ref, y_s, o_s, load, store):
    pieces = [(s, j) for s in TWO for j in range(4)]

    def get(i):
        s, j = pieces[i]
        return pltpu.make_async_copy(y_ref.at[s, :, pl.ds(j * 64, 64)], y_s.at[i], load.at[i])

    def put(i):
        return pltpu.make_async_copy(o_s.at[i], o_ref.at[pl.ds(i * H, H)], store.at[i])

    for i in ROWS:
        get(i).start()
    pm = phase_matrix(True)
    for i in range(0, 8, 2):
        group = (i, i + 1)
        for k in group:
            get(k).wait()
        for k in group:
            for j in TWO:
                o_s[k, part(j, B), :] = nn(pm, y_s[k, :, part(j, 32), :].reshape(B, H)).astype(BF)
        for k in group:
            put(k).start()
    for i in ROWS:
        put(i).wait()


def unpermute(y):
    anyspec = pl.BlockSpec(memory_space=pl.ANY)
    return pl.pallas_call(
        unpermute_kernel,
        in_specs=[anyspec],
        out_specs=anyspec,
        out_shape=jax.ShapeDtypeStruct((2 * M, H), BF),
        scratch_shapes=[pltpu.VMEM((8, 8, 64, H), BF), pltpu.VMEM((8, H, H), BF), pltpu.SemaphoreType.DMA((8,)), pltpu.SemaphoreType.DMA((8,))],
        compiler_params=params(),
        name='unpermute',
    )(y)


def tile_steps(q, wide, narrow, s_ref, n_ref, done):
    st = {}
    logits, sums = [], []

    def add(name, x):
        st[name] = st[name] + x if name in st else x

    for groups, ref in ((wide, s_ref), (narrow, n_ref)):
        off = 0
        for keys, parts in groups:
            def qk(keys=keys, parts=parts, off=off, ref=ref):
                s = nt(keys(), q() if ref is s_ref else q()[:B])
                o = 0
                for _, n, b in parts:
                    piece = s[o:o + n]
                    ref[pl.ds(off + o, n), :] = piece
                    t = jnp.max(piece, axis=0, keepdims=True) * KAPPA
                    if b is not None:
                        t = t + fit(b, t)
                    if ref is n_ref:
                        t = jnp.concatenate([t, st['top'][:, B:]], axis=1)
                    st['top'] = jnp.maximum(st['top'], t) if 'top' in st else t
                    o += n
            logits.append(qk)
            for v, n, b in parts:
                def sv(v=v, n=n, b=b, off=off, ref=ref):
                    top = st['top'] if ref is s_ref else st['top'][:, :B]
                    e = jnp.exp2(ref[pl.ds(off, n), :] * KAPPA - (top if b is None else top - fit(b, top)))
                    name = 'w' if ref is s_ref else 'n'
                    add('l' + name, jnp.sum(e, axis=0, keepdims=True))
                    add('o' + name, nn(v(), e.astype(BF)))
                sums.append(sv)
                off += n

    def finish():
        o, l = st['ow'], st['lw']
        if narrow:
            o = jnp.concatenate([o[:, :B] + st['on'], o[:, B:]], axis=1)
            l = jnp.concatenate([l[:, :B] + st['ln'], l[:, B:]], axis=1)
        done(o / l)

    return logits, sums + [finish]


def fit(b, like):
    return b if b.shape == like.shape else jnp.concatenate([b] * (like.shape[1] // 128), axis=1)


def interleave(a, b):
    i = j = 0
    while i < len(a) or j < len(b):
        if j >= len(b) or (i < len(a) and i * len(b) <= j * len(a)):
            a[i]()
            i += 1
        else:
            b[j]()
            j += 1


def run_tiles(tiles):
    before = []
    for logits, sums in tiles:
        interleave(logits, before)
        before = sums
    interleave([], before)


def choose(x, cases):
    def among(lo, hi):
        mid = (lo + hi) // 2
        if hi - lo == 1:
            cases[lo]()
        else:
            pl.when(x < mid)(lambda: among(lo, mid))
            pl.when(x >= mid)(lambda: among(mid, hi))
    among(0, len(cases))


def on(cond, *calls):
    @pl.when(cond)
    def _():
        for c in calls:
            c()


def scope(name):
    return jax.named_scope(name)


def main_kernel(bias_ref, x_ref, wk_ref, wv_ref, wq_ref, wout_ref, out_ref, lq_ref, lo_ref, lb_ref,
                xb, pm, xp, ws, q_s, kv_s, kvp_s, kvr_s, s_scr, t_scr,
                beta_s, x_sem, w_sem, wo_sem, sent, lq_recv, lo_recv, lb_recv, kv_recv, o_recv, y_recv, ready):
    dp, tp, sp = lax.axis_index('dp'), lax.axis_index('tp'), lax.axis_index('sp')
    idx = dp * 4 + sp
    side = tp // 2
    inner = (tp == 1) | (tp == 2)
    outer = jnp.logical_not(inner)
    W = (wk_ref, wv_ref, wq_ref)
    peer_x, peer_y, peer_c = {'dp': dp ^ 1}, {'sp': sp ^ 2}, {'sp': sp ^ 1}

    def remote(src, dst, ss, rs, dev):
        return pltpu.make_async_remote_copy(src_ref=src, dst_ref=dst, send_sem=ss, recv_sem=rs, device_id=dev, device_id_type=MESH)

    def lq_copy(t, src, dst, dev):
        return remote(lq_ref.at[src, t], lq_ref.at[dst, t], sent.at[0], lq_recv.at[t, min(dst, 4)], dev)

    def lq_z(t):
        return remote(W[t // 2].at[ds(idx * B, B), pl.ds(t % 2 * B, B)], lq_ref.at[0, t], sent.at[0], lq_recv.at[t, 0], {'tp': tp ^ 2})

    def lq_start(t):
        for i in TWO:
            lq_z(2 * t + i).start()

    def lo_copy(v, src, dst, dev):
        return remote(lo_ref.at[v, src], lo_ref.at[v, dst], sent.at[1], lo_recv.at[v, min(dst, 4)], dev)

    def lo_z(v):
        dst = 2 - side
        b = (tp ^ dst) - 2
        return remote(wout_ref.at[ds(idx * 64, 64, 64), ds((dst ^ v) * H, H)], lo_ref.at[v, 0, b], sent.at[2], lo_recv.at[v, 0], {'tp': dst})

    def lb_z(v):
        return remote(wout_ref.at[ds(sp % 2 * B, B), ds((tp ^ 1 ^ v) * H, H)], lb_ref.at[v, sp % 2], sent.at[3], lb_recv.at[v, 0], {'tp': tp ^ 1})

    def lb_core(v):
        return remote(lb_ref.at[v, sp % 2], lb_ref.at[v, sp % 2], sent.at[3], lb_recv.at[v, 1], peer_c)

    def lo_start(*vs):
        for v in vs:
            lo_z(v).start()

    def arrived(ref, sem):
        remote(ref, ref, sent.at[0], sem, peer_c).wait_recv()

    def all_sent(ref, i):
        remote(ref, ref, sent.at[i], sent.at[i], peer_c).wait_send()

    def lo_zwait(v):
        arrived(lo_ref.at[v, 0], lo_recv.at[v, 0])

    def hop(copy, p, i):
        near, far, n = (peer_x, peer_y, 1) if (copy is lo_copy and p == 2) or (copy is lq_copy and p == 5) else (peer_y, peer_x, 2)
        f = 3 - n
        return copy(p, *((0, n, near), (0, f, far), (0, 4, peer_c), (n, 3, far), (n, 4 + n, peer_c), (f, 4 + f, peer_c), (3, 7, peer_c))[i])

    def ev_z(copy, *ps):
        for p in ps:
            with scope(f'z_{copy.__name__}{p}'):
                lq_z(p).wait_recv() if copy is lq_copy else lo_zwait(p)
            hop(copy, p, 0).start()
        for p in ps:
            hop(copy, p, 1).start()
            hop(copy, p, 2).start()

    def ev_near(copy, *ps):
        for p in ps:
            with scope(f'n_{copy.__name__}{p}'):
                hop(copy, p, 0).wait_recv()
            hop(copy, p, 3).start()
            hop(copy, p, 4).start()

    def ev_far(copy, *ps):
        for p in ps:
            with scope(f'f_{copy.__name__}{p}'):
                hop(copy, p, 1).wait_recv()
            hop(copy, p, 5).start()

    def ev_xy(copy, *ps):
        ev_near(copy, *ps)
        ev_far(copy, *ps)

    def ev_y(copy, *ps):
        for p in ps:
            with scope(f'y_{copy.__name__}{p}'):
                hop(copy, p, 3).wait_recv()
            hop(copy, p, 6).start()
            if copy is lq_copy and p >= 2:
                start(w_load(p, SLOT[:4]))

    def ev_done(copy, *ps):
        for p in ps:
            with scope(f'c_{copy.__name__}{p}'):
                if copy is lq_copy:
                    arrived(lq_ref.at[pl.ds(4, 4), p], lq_recv.at[p, 4])
                else:
                    arrived(lo_ref.at[p, pl.ds(4, 4)], lo_recv.at[p, 4])

    def w_load(p, slots):
        return [pltpu.make_async_copy(lq_ref.at[SLOT.index(m), p], ws.at[p // 2 % 2, ds((idx ^ m) * B, B), pl.ds(p % 2 * B, B)], w_sem.at[p]) for m in slots]

    def own_load(t):
        return pltpu.make_async_copy(W[t], ws.at[t], w_sem.at[6 + t])

    def start(copies):
        for c in copies:
            c.start()

    def wait(copies):
        for c in copies:
            c.wait()

    def ev_last(t):
        pieces = [2 * t + i for i in TWO]
        ev_done(lq_copy, *pieces)
        for p in pieces:
            start(w_load(p, SLOT[4:] if t else SLOT))

    def local(ref, sem):
        pltpu.make_async_copy(ref, ref, sem).wait()

    def ev_weights(t):
        with scope(f'load{t}'):
            for i in TWO:
                local(ws.at[t % 2, :, pl.ds(i * B, B)], w_sem.at[2 * t + i])

    def ev_wo(*vs):
        ev_done(lo_copy, *vs)
        for v in vs:
            lb_core(v).wait_recv()
        start(wo_load(*vs))

    def ev_wo_ready(*vs):
        with scope(f'wo{vs[0]}'):
            for v in vs:
                local(xp.at[1 - side, pl.ds(2, 6), :, pl.ds((v ^ 2) * H, H)], wo_sem.at[v])

    def ev_lb(*vs):
        for v in vs:
            with scope(f'lb{v}'):
                lb_z(v).wait_recv()
            lb_core(v).start()

    wo = xp.at[1 - side]

    def wo_own():
        return [pltpu.make_async_copy(wout_ref.at[pl.ds(r * B, B), pl.ds(c * H, H)], xp.at[1 - side, r, :, ds((c ^ tp ^ 2) * H, H)], wo_sem.at[4])
                for r in TWO for c in range(4)]

    def wo_load(*vs):
        out = []
        for v in vs:
            cols = pl.ds((v ^ 2) * H, H)
            for s, m in enumerate(SLOT):
                row = (idx ^ m) * 64
                for b in TWO:
                    out.append(pltpu.make_async_copy(lo_ref.at[v, s, b], xp.at[1 - side, 4 + 2 * b + row // B, ds(row % B, 64, 64), cols], wo_sem.at[v]))
            for r in TWO:
                out.append(pltpu.make_async_copy(lb_ref.at[v, r], xp.at[1 - side, 2 + r, :, cols], wo_sem.at[v]))
        return out

    def kvp_copy(h, s):
        return remote(kv_s.at[h, pl.ds(8 * s, 2)], kvp_s.at[h, pl.ds(2 * s, 2)], sent.at[4], kv_recv.at[0, h], peer_c)

    def kvr_copy(h, s):
        return remote(kv_s.at[h, 8 * s], kvr_s.at[h, s], sent.at[5], kv_recv.at[1, h], peer_y)

    def kvf_copy(h, s):
        return remote(kvr_s.at[h, s], kvr_s.at[h, 2 + s], sent.at[6], kv_recv.at[2, h], peer_c)

    def kv_start(copy, heads):
        for h in heads:
            for s in TWO:
                copy(h, s).start()

    def kv_wait(copy, heads):
        with scope(f'w_{copy.__name__}{heads[0]}'):
            for h in heads:
                i = (kvp_copy, kvr_copy, kvf_copy).index(copy)
                arrived((kvp_s.at[h], kvr_s.at[h, pl.ds(0, 2)], kvr_s.at[h, pl.ds(2, 2)])[i], kv_recv.at[i, h])

    def kv_forward(heads):
        kv_wait(kvr_copy, heads)
        kv_start(kvf_copy, heads)

    def reverse(i):
        return (i % 2) * 2 + i // 2

    def order(n):
        return 2 * reverse(n % 4) + ((n // 4) ^ side)

    def o_at(k, p, theirs, col, size, row=0, rows=B):
        if p:
            return ws.at[1 + theirs, ds(k * B + row, rows), ds(col, size)]
        return xb.at[k // 2, pl.ds(row, rows), ds((k % 2) * 1024 + theirs * H + col, size)]

    def o_copy(k, p, half):
        row = half * 128
        return remote(o_at(k, p, 0, 0, H, row, 128), o_at(k, p, 1, 0, H, row, 128), sent.at[7], o_recv.at[k, half], {'tp': tp ^ 1})

    def o_times(k, v, n, row=0, rows=B):
        cols = pl.ds((v ^ 2) * H, n * H)
        y = nn(xb[k // 2, pl.ds(row, rows), ds((k % 2) * 1024, 1024)], wo[0:4, :, cols].reshape(1024, n * H))
        for i in TWO:
            y = y + nn(ws[1 + i, ds(k * B + row, rows), :], wo[part(2 + i, 2), :, cols].reshape(H, n * H))
        y = y.astype(BF)
        for i in range(n):
            y_src(k, v + i, row, rows)[...] = y[:, part(i, H)]
            y_copy(k, v + i, side, row, rows).start() if v else y_local(k).start()

    def y_src(k, v, row=0, rows=B):
        return xp.at[side, k, pl.ds(row, rows), pl.ds(v * H, H)]

    def y_copy(k, v, seg, row, rows):
        return remote(y_src(k, v, row, rows), out_ref.at[seg, k, pl.ds(row, rows)], sent.at[8], y_recv.at[seg], {'tp': tp ^ v})

    def y_local(k):
        return pltpu.make_async_copy(y_src(k, 0), out_ref.at[side, k], sent.at[9])

    def x_copy(j):
        return pltpu.make_async_copy(x_ref.at[ds(j * B, B), :], xb.at[lax.rem(j, 4)], x_sem.at[lax.rem(j, 4)])

    for j in range(4):
        x_copy(j).start()
    barrier = pltpu.get_barrier_semaphore()
    peers = [{'tp': tp ^ 1}, {'tp': tp ^ 2}, {'tp': tp ^ 3}, peer_x, peer_y, peer_c]
    for dev in peers:
        pl.semaphore_signal(barrier, inc=1, device_id=dev, device_id_type=MESH)
    for t in range(3):
        own_load(t).start()

    pm[...] = phase_matrix(False)

    def permute_body(j, carry):
        x_copy(j).wait()
        y = nn(pm[...], xb[lax.rem(j, 4)]).astype(BF).reshape(8, 32, M)
        xp[j // 8, :, ds(lax.rem(j, 8) * 32, 32, 32), :] = y
        pl.when(j < 12)(lambda: x_copy(j + 4).start())

        @pl.when(j == 2)
        def _():
            with scope('barrier'):
                pl.semaphore_wait(barrier, len(peers))
            lq_start(KEY)
            on(outer, lb_z(2).start)
        return carry

    with scope('permute'):
        lax.fori_loop(0, 16, permute_body, None)

    for h in HEADS:
        column = 2 * (tp ^ (h // 2 * 2)) + h % 2
        for i, branches in enumerate(('0', '01', '1', '012', '12', '2', '0123', '123', '23', '3')):
            rows = [jnp.full((1, 128), bias_ref[j, column], F32) for j in map(int, branches)]
            m = functools.reduce(jnp.maximum, rows)
            beta_s[pl.ds(h * 16 + i, 1), :] = (m + jnp.log(sum(jnp.exp(r - m) for r in rows))) * math.log2(math.e)

    def signal_ready(i):
        pl.when(inner)(lambda: pl.semaphore_signal(ready.at[i], inc=1, device_id={'tp': tp ^ 1}, device_id_type=MESH))

    def wait_ready(i):
        with scope(f'ready{i}'):
            pl.when(outer)(lambda: pl.semaphore_wait(ready.at[i], 1))

    signal_ready(0)

    def group(g):
        low = g < 4
        return jnp.where(low, g & 1, 0), jnp.where(low, g // 2, g - 2)

    def head_number(h):
        return 2 * (tp ^ (h // 2 * 2)) + h % 2

    def project(heads, sigma, pair, kinds):
        for h in heads:
            t = head_number(h) + reverse(pair)
            x, swap = xp[side ^ sigma, pl.ds(2 * (t & 3), 2)].reshape(H, M), (t & 7) >> 2
            for t in kinds:
                y = nn(x, ws[t, :, part(h % 2, B)])
                for j in TWO:
                    piece = y[part(j, B)]
                    kv_s[h, 8 * sigma + 2 * pair + (j ^ swap), t] = (piece.T if t == VAL else piece).astype(BF)

    def phases_of(j):
        return [j % 2 + 2 * i for i in TWO], (j // 2) ^ side

    def rank_of(phase, h):
        rel = (phase - head_number(h)) & 7
        return (rel & 1) * 4 + ((rel >> 1) & 1) * 2 + (rel >> 2)

    def queries(heads, w, j):
        phases, half = phases_of(j)
        x = jnp.concatenate([xp[side, 2 * f + half] for f in phases])
        for h in heads:
            y = nn(x, ws[w, :, part(h % 2, B)]).astype(BF)
            for i, f in enumerate(phases):
                q_s[h, rank_of(f + 4 * half, h)] = y[part(i, B)]

    with scope('own_w'):
        for t in range(3):
            own_load(t).wait()
    own, partner = HEADS[:2], HEADS[2:]

    def mix(b, c):
        return jnp.concatenate([b, b, c, c], axis=1)

    def keys_of(ref, h, i, weights):
        parts = []
        n = 0
        for count, b in weights:
            def values(i=i + n, count=count):
                v = [ref[h, i + j, VAL] for j in range(count)]
                return v[0] if count == 1 else jnp.concatenate(v, axis=1)
            parts.append((values, count * B, b))
            n += count
        return (lambda: ref[h, i:i + n, KEY].reshape(n * B, B)), parts

    def chunk_tiles(p, j, kind):
        both_phases, half = phases_of(j)

        def put(h, phase, ot):
            k = 2 * (phase & 3) + half
            y = ot.T.astype(BF)
            for i in TWO:
                pl.when(p == i)(lambda i=i: o_at(k, i, 0, (h % 2) * B, B).__setitem__(..., y))

        def tile(h, phases, ranks, wide, narrow, s_ref, n_ref):
            def done(ot):
                for i, phase in enumerate(phases):
                    put(h, phase, ot[:, part(i, B)])
            return tile_steps(lambda: jnp.concatenate([q_s[h, r] for r in ranks]), wide, narrow, s_ref, n_ref, done)

        h = 2 * p + (j % 2) ^ 1
        rest = tile(h, both_phases, [rank_of(f + 4 * half, h) for f in both_phases], [keys_of(kv_s, h, i, [(2, None)]) for i in range(0, 8, 2)], [], t_scr, None)
        h = 2 * p + (j % 2)
        a = head_number(h)
        b0, b01, b1, b012, b12, b2, b0123, b123, b23, b3 = [beta_s[pl.ds(h * 16 + i, 1), :] for i in range(10)]
        phases = [a & 3, (a & 3) ^ 2]
        both = [keys_of(kv_s, h, i, [(2, b)]) for i, b in ((2, b01), (4, b0), (6, b0), (10, b1))]
        if kind == 0:
            both += [keys_of(kv_s, h, 0, [(1, mix(b0123, b01)), (1, mix(b012, b01))]), keys_of(kv_s, h, 8, [(1, mix(b123, b1)), (1, mix(b12, b1))])]
            first = [keys_of(kvp_s, h, i, [(1, b23), (1, b2)]) for i in (0, 2)] + [keys_of(kvr_s, h, i, [(2, b3)]) for i in (0, 2)]
        else:
            both += [keys_of(kv_s, h, 0, [(2, mix(b012, b01))]), keys_of(kv_s, h, 8, [(2, mix(b12, b1))])]
            first = [keys_of(kvp_s, h, i, [(2, b2)]) for i in (0, 2)]
        with scope(f'tile{kind}'):
            run_tiles([rest, tile(h, phases, [kind, rank_of(phases[1] + 4 * half, h)], both, first, s_scr, t_scr.at[:, pl.ds(0, B)])])

    def send_o(ks, p):
        @pl.when(outer)
        def _():
            for k in ks:
                for half in TWO:
                    o_copy(order(k), p, half).start()

    def step_body(t, carry):
        packed = functools.reduce(lambda x, i: jnp.where(t == i, TABLE[i], x), range(len(TABLE)), 0)
        code, n, event = packed % 16, packed // 16 % 16, packed // 256

        def step_o():
            with scope('own_kv'):
                project(own, *group(n), (KEY, VAL))

        def step_kv(t_):
            with scope(f'par_{t_}'):
                for i in TWO:
                    project(partner, *group(2 * n + i), (t_,))

        def step_q(heads, w):
            with scope(f'que_{w}'):
                queries(heads, w, n)

        def step_out(v, m):
            @pl.when(inner)
            def _():
                k = order(n)

                def halves():
                    for half in TWO:
                        with scope(f'wait_h{half}'):
                            arrived(ws.at[0, pl.ds(0, B), :], o_recv.at[k, half])
                        o_times(k, v, m, half * 128, 128)

                def whole():
                    with scope('wait_o'):
                        for half in TWO:
                            arrived(ws.at[0, pl.ds(0, B), :], o_recv.at[k, half])
                    with scope(f'out{v}'):
                        o_times(k, v, m)

                if m == 2:
                    pl.when(n == 0)(halves)
                    pl.when(n > 0)(whole)
                else:
                    with scope(f'out{v}'):
                        o_times(k, v, m)

        f = functools.partial
        kinds = {'-': lambda: None, 'O': step_o, 'P': f(step_q, own, QUE), 'K': f(step_kv, KEY), 'V': f(step_kv, VAL), 'Q': f(step_q, partner, KEY),
                 'A': lambda: chunk_tiles(n // 4, n % 4, 0), 'B': lambda: chunk_tiles(n // 4, n % 4, 1), 'R': f(step_out, 2, 2), 'L': f(step_out, 1, 1), 'N': f(step_out, 0, 1)}
        choose(code, [kinds[c] for c in KINDS])
        call = functools.partial

        events = {
            'free': [call(signal_ready, 1), call(on, inner, lambda: start(wo_own()))],
            'r0': [call(wait_ready, 0)],
            'r1': [call(wait_ready, 1)],
            'so': [call(kv_start, kvp_copy, own)],
            'po': [call(kv_wait, kvp_copy, own)],
            'sp': [call(kv_start, kvp_copy, partner)],
            'pp': [call(kv_wait, kvp_copy, partner)],
        }
        for t_, c in enumerate('kvq'):
            events['b' + c] = [call(lq_start, t_)]
            events['l' + c] = [call(ev_last, t_)]
            events['w' + c] = [call(ev_weights, t_)]
            events['z' + c] = [call(ev_z, lq_copy, 2 * t_, 2 * t_ + 1)]
            for i in TWO:
                for e, f in zip('zmfxy', (ev_z, ev_near, ev_far, ev_xy, ev_y)):
                    events[f'{e}{c}{i}'] = [call(f, lq_copy, 2 * t_ + i)]
        for i, vs in enumerate(((2, 3), (1,), (0,))):
            events[f'b{i}'] = [call(lo_start, *vs)]
            for e, f in zip('zmxycwv', (call(ev_z, lo_copy), call(ev_near, lo_copy), call(ev_far, lo_copy), call(ev_y, lo_copy), ev_lb, ev_wo, ev_wo_ready)):
                events[f'{e}{i}'] = [call(on, inner, call(f, *vs))]
        events['v0'] += [call(on, inner, lambda: local(xp.at[1 - side, pl.ds(0, 2)], wo_sem.at[4]))]
        for v in range(4):
            events[f'd{v}'] = [call(on, outer, lambda v=v: lb_z(v).start())]
        for h in HEADS:
            for z in TWO:
                events[f's{h}{z}'] = [kvr_copy(h, z).start]
            events[f'f{h}'] = [call(kv_forward, [h])]
            events[f'g{h}'] = [call(kv_wait, kvf_copy, [h])]
        for k in ROWS:
            for p in TWO:
                events['op'[p] + str(k)] = [call(send_o, (k,), p)]
        def run(names):
            for name in names.split(','):
                where, _, name = name.rpartition(':')
                if where:
                    on(inner if where == 'i' else outer, *events[name])
                else:
                    for c in events[name]:
                        c()

        @pl.when(event > 0)
        def _():
            choose(event - 1, [functools.partial(run, names) for names in EVENTS])
        return carry

    lax.fori_loop(0, len(TABLE), step_body, None)

    all_sent(lq_ref, 0)
    all_sent(lo_ref.at[:, 0, 0], 2)
    all_sent(lb_ref.at[:, 0], 3)
    all_sent(kvp_s, 4)
    all_sent(kvr_s.at[:, pl.ds(0, 2)], 5)
    all_sent(kvr_s.at[:, pl.ds(0, 2)], 6)

    @pl.when(outer)
    def _():
        all_sent(xb, 7)

    @pl.when(inner)
    def _():
        all_sent(lo_ref.at[:, pl.ds(0, 7)], 1)
        with scope('y_sent'):
            all_sent(xp.at[side, :, :, pl.ds(H, 3 * H)], 8)
        local(xp.at[side, :, :, pl.ds(0, H)], sent.at[9])

    for seg in TWO:
        @pl.when(tp != 1 + seg)
        def _(seg=seg):
            with scope(f'recv{seg}'):
                arrived(out_ref.at[seg], y_recv.at[seg])


PROGRAM = (
    'O.i:zk0,i:zk1', 'O.i:bv,o:zk0', 'O.o:bv,o:zk1,s00,i:xk0', 'O.o:xk0,i:xk1,o:s01,d3', 'O.o:xk1,i:yk0,i:zv0', 'O.o:yk0,i:yk1,i:zv1,i:s01,i:bq',
    'P.o:bq,so', 'P.o:yk1,lk,o:zv0,d1,i:xv0', 'P.wk,o:zv1,i:xv1', 'K', 'K.o:xv0,i:zq,f0', 'K.o:xv1,i:yv0,i:yv1,b0,b1,r0,po,g0,o:zq',
    'T0.o0,o1,d0,o:yv0,o:yv1,lv,mq0,i:mq1,i:fq0,i:fq1', 'P.wv,z0,o:mq1,b2', 'V.o:fq0,o:fq1,sp,o:s10,o:s11', 'V.c0,z1,o:s20,o:s21',
    'V.free,yq0,yq1,lq,m0,o:s30,o:s31,wq', 'Q.pp,r1,x0,c1,i:s10,i:s11,y0', 'T4.p0,p1,w0,m1,x1,v0', 'R.y1,w1,v1,i:s20,i:s21', 'L', 'Q.f1', 'T5.p2,g1',
    'R', 'L', 'T1.o2,p3,o3,o:f2', 'R.i:s30,i:s31', 'L', 'Q.o:g2', 'Q.i:f2,o:f3', 'T2', 'R.i:g2', 'L', 'T6.p4,o4,p5,o5,o:g3', 'R.i:f3,z2,c2', 'L',
    'T3.i:g3', 'T7.p6,o6,p7,o7', 'R', 'L.m2,x2', 'R.y2', 'L.w2', '-.v2', 'N', 'N', 'N', 'R', 'L', 'N', 'N', 'N', 'N', 'N',
)
KINDS = '-OPKVQABRLN'


def tables():
    table, seen = [], {}
    names = tuple(dict.fromkeys(s.partition('.')[2] for s in PROGRAM if '.' in s))
    for s in PROGRAM:
        name, _, after = s.partition('.')
        kind, n = name[0], seen.get(name[0], 0)
        seen[kind] = n + 1
        if kind == 'T':
            n = int(name[1:])
            kind = 'AB'[n in (2, 3, 4, 5)]
        table.append(KINDS.index(kind) + 16 * n + 256 * (names.index(after) + 1 if after else 0))
    return table, names


TABLE, EVENTS = tables()


def main(bias, x, wk, wv, wq, w_out):
    anyspec = pl.BlockSpec(memory_space=pl.ANY)
    vmem = [((4, B, M), BF), ((B, B), BF), ((2, 8, B, M), BF), ((3, M, H), BF), ((4, 8, B, B), BF), ((4, 12, 2, B, B), BF), ((4, 4, 2, B, B), BF), ((4, 4, 2, B, B), BF),
            ((3072, H), F32), ((M, H), F32), ((64, 128), F32)]
    dma = [(4,), (9,), (5,), (10,), (6, 5), (4, 5), (4, 2), (3, 4), (8, 2), (2,)]
    return pl.pallas_call(
        main_kernel,
        in_specs=[pl.BlockSpec(memory_space=pltpu.SMEM)] + [anyspec] * 5,
        out_specs=[anyspec] * 4,
        out_shape=[jax.ShapeDtypeStruct(s, BF) for s in ((2, 8, B, H), (8, 6, B, B), (4, 8, 2, 64, H), (4, 2, B, H))],
        scratch_shapes=[pltpu.VMEM(*v) for v in vmem] + [pltpu.SemaphoreType.DMA(d) for d in dma] + [pltpu.SemaphoreType.REGULAR((2,))],
        compiler_params=params(collective_id=0, has_side_effects=True),
        cost_estimate=pl.CostEstimate(flops=10**11, bytes_accessed=10**8, transcendentals=0),
        name='main',
    )(bias, x, wk, wv, wq, w_out)[0]


def solution(mesh):
    def device_fn(hidden, w_query, w_key, w_value, w_out, branch_bias):
        return unpermute(main(branch_bias, hidden, w_key, w_value, w_query, w_out))

    return jax.shard_map(device_fn, mesh=mesh, in_specs=(P(('dp', 'sp'), None), P(None, 'tp'), P(None, 'tp'), P(None, 'tp'), P('tp', None), P(None, None)), out_specs=P(('dp', 'sp'), 'tp'), check_vma=False)
```

```python
import functools
import math

import jax
import jax.numpy as jnp
from jax import lax
from jax.experimental import pallas as pl
from jax.experimental.pallas import tpu as pltpu
from jax.sharding import PartitionSpec as P

MESH = pl.DeviceIdType.MESH
BF = jnp.bfloat16
F32 = jnp.float32
B, H, M = 256, 512, 2048
KAPPA = math.log2(math.e) / 16
VMEM = 66_900_000
SLOT = (0, 4, 2, 6, 1, 5, 3, 7)
KEY, VAL, QUE = range(3)
HEADS = range(4)
TWO = range(2)
ROWS = range(8)


def nn(a, b):
    return lax.dot_general(a, b, (((1,), (0,)), ((), ())), preferred_element_type=F32)


def nt(a, b):
    return lax.dot_general(a, b, (((1,), (1,)), ((), ())), preferred_element_type=F32)


def params(**kw):
    return pltpu.CompilerParams(vmem_limit_bytes=VMEM, **kw)


def ds(start, size, align=128):
    return pl.ds(pl.multiple_of(start, align), size)


def part(i, size):
    return slice(i * size, i * size + size)


def phase_matrix(transposed):
    r = lax.broadcasted_iota(jnp.int32, (B, B), int(transposed))
    p = lax.broadcasted_iota(jnp.int32, (B, B), int(not transposed))
    k = r // 32
    return (p == (r % 32) * 8 + k // 2 + 4 * (k % 2)).astype(F32).astype(BF)


def unpermute_kernel(y_ref, o_ref, y_s, o_s, load, store):
    pieces = [(s, j) for s in TWO for j in range(4)]

    def get(i):
        s, j = pieces[i]
        return pltpu.make_async_copy(y_ref.at[s, :, pl.ds(j * 64, 64)], y_s.at[i], load.at[i])

    def put(i):
        return pltpu.make_async_copy(o_s.at[i], o_ref.at[pl.ds(i * H, H)], store.at[i])

    for i in ROWS:
        get(i).start()
    pm = phase_matrix(True)
    for i in range(0, 8, 2):
        group = (i, i + 1)
        for k in group:
            get(k).wait()
        for k in group:
            for j in TWO:
                o_s[k, part(j, B), :] = nn(pm, y_s[k, :, part(j, 32), :].reshape(B, H)).astype(BF)
        for k in group:
            put(k).start()
    for i in ROWS:
        put(i).wait()


def unpermute(y):
    anyspec = pl.BlockSpec(memory_space=pl.ANY)
    return pl.pallas_call(
        unpermute_kernel,
        in_specs=[anyspec],
        out_specs=anyspec,
        out_shape=jax.ShapeDtypeStruct((2 * M, H), BF),
        scratch_shapes=[pltpu.VMEM((8, 8, 64, H), BF), pltpu.VMEM((8, H, H), BF), pltpu.SemaphoreType.DMA((8,)), pltpu.SemaphoreType.DMA((8,))],
        compiler_params=params(),
        name='unpermute',
    )(y)


def tile_steps(q, wide, narrow, s_ref, n_ref, done):
    st = {}
    logits, sums = [], []

    def add(name, x):
        st[name] = st[name] + x if name in st else x

    for groups, ref in ((wide, s_ref), (narrow, n_ref)):
        off = 0
        for keys, parts in groups:
            def qk(keys=keys, parts=parts, off=off, ref=ref):
                s = nt(keys(), q() if ref is s_ref else q()[:B])
                o = 0
                for _, n, b in parts:
                    piece = s[o:o + n]
                    ref[pl.ds(off + o, n), :] = piece
                    t = jnp.max(piece, axis=0, keepdims=True) * KAPPA
                    if b is not None:
                        t = t + fit(b, t)
                    if ref is n_ref:
                        t = jnp.concatenate([t, st['top'][:, B:]], axis=1)
                    st['top'] = jnp.maximum(st['top'], t) if 'top' in st else t
                    o += n
            logits.append(qk)
            for v, n, b in parts:
                def sv(v=v, n=n, b=b, off=off, ref=ref):
                    top = st['top'] if ref is s_ref else st['top'][:, :B]
                    e = jnp.exp2(ref[pl.ds(off, n), :] * KAPPA - (top if b is None else top - fit(b, top)))
                    name = 'w' if ref is s_ref else 'n'
                    add('l' + name, jnp.sum(e, axis=0, keepdims=True))
                    add('o' + name, nn(v(), e.astype(BF)))
                sums.append(sv)
                off += n

    def finish():
        o, l = st['ow'], st['lw']
        if narrow:
            o = jnp.concatenate([o[:, :B] + st['on'], o[:, B:]], axis=1)
            l = jnp.concatenate([l[:, :B] + st['ln'], l[:, B:]], axis=1)
        done(o / l)

    return logits, sums + [finish]


def fit(b, like):
    return b if b.shape == like.shape else jnp.concatenate([b] * (like.shape[1] // 128), axis=1)


def interleave(a, b):
    i = j = 0
    while i < len(a) or j < len(b):
        if j >= len(b) or (i < len(a) and i * len(b) <= j * len(a)):
            a[i]()
            i += 1
        else:
            b[j]()
            j += 1


def run_tiles(tiles):
    before = []
    for logits, sums in tiles:
        interleave(logits, before)
        before = sums
    interleave([], before)


def choose(x, cases):
    def among(lo, hi):
        mid = (lo + hi) // 2
        if hi - lo == 1:
            cases[lo]()
        else:
            pl.when(x < mid)(lambda: among(lo, mid))
            pl.when(x >= mid)(lambda: among(mid, hi))
    among(0, len(cases))


def on(cond, *calls):
    @pl.when(cond)
    def _():
        for c in calls:
            c()


def scope(name):
    return jax.named_scope(name)


def main_kernel(bias_ref, x_ref, wk_ref, wv_ref, wq_ref, wout_ref, out_ref, lq_ref, lo_ref, lb_ref,
                xb, pm, xp, ws, q_s, kv_s, kvp_s, kvr_s, s_scr, t_scr,
                beta_s, x_sem, w_sem, wo_sem, sent, lq_recv, lo_recv, lb_recv, kv_recv, o_recv, y_recv, ready):
    dp, tp, sp = lax.axis_index('dp'), lax.axis_index('tp'), lax.axis_index('sp')
    idx = dp * 4 + sp
    side = tp // 2
    inner = (tp == 1) | (tp == 2)
    outer = jnp.logical_not(inner)
    W = (wk_ref, wv_ref, wq_ref)
    peer_x, peer_y, peer_c = {'dp': dp ^ 1}, {'sp': sp ^ 2}, {'sp': sp ^ 1}

    def remote(src, dst, ss, rs, dev):
        return pltpu.make_async_remote_copy(src_ref=src, dst_ref=dst, send_sem=ss, recv_sem=rs, device_id=dev, device_id_type=MESH)

    def lq_copy(t, src, dst, dev):
        return remote(lq_ref.at[src, t], lq_ref.at[dst, t], sent.at[0], lq_recv.at[t, min(dst, 4)], dev)

    def lq_z(t):
        return remote(W[t // 2].at[ds(idx * B, B), pl.ds(t % 2 * B, B)], lq_ref.at[0, t], sent.at[0], lq_recv.at[t, 0], {'tp': tp ^ 2})

    def lq_start(t):
        for i in TWO:
            lq_z(2 * t + i).start()

    def lo_copy(v, src, dst, dev):
        return remote(lo_ref.at[v, src], lo_ref.at[v, dst], sent.at[1], lo_recv.at[v, min(dst, 4)], dev)

    def lo_z(v):
        dst = 2 - side
        b = (tp ^ dst) - 2
        return remote(wout_ref.at[ds(idx * 64, 64, 64), ds((dst ^ v) * H, H)], lo_ref.at[v, 0, b], sent.at[2], lo_recv.at[v, 0], {'tp': dst})

    def lb_z(v):
        return remote(wout_ref.at[ds(sp % 2 * B, B), ds((tp ^ 1 ^ v) * H, H)], lb_ref.at[v, sp % 2], sent.at[3], lb_recv.at[v, 0], {'tp': tp ^ 1})

    def lb_core(v):
        return remote(lb_ref.at[v, sp % 2], lb_ref.at[v, sp % 2], sent.at[3], lb_recv.at[v, 1], peer_c)

    def lo_start(*vs):
        for v in vs:
            lo_z(v).start()

    def arrived(ref, sem):
        remote(ref, ref, sent.at[0], sem, peer_c).wait_recv()

    def all_sent(ref, i):
        remote(ref, ref, sent.at[i], sent.at[i], peer_c).wait_send()

    def lo_zwait(v):
        arrived(lo_ref.at[v, 0], lo_recv.at[v, 0])

    def hop(copy, p, i):
        near, far, n = (peer_x, peer_y, 1) if (copy is lo_copy and p == 2) or (copy is lq_copy and p == 5) else (peer_y, peer_x, 2)
        f = 3 - n
        return copy(p, *((0, n, near), (0, f, far), (0, 4, peer_c), (n, 3, far), (n, 4 + n, peer_c), (f, 4 + f, peer_c), (3, 7, peer_c))[i])

    def ev_z(copy, *ps):
        for p in ps:
            with scope(f'z_{copy.__name__}{p}'):
                lq_z(p).wait_recv() if copy is lq_copy else lo_zwait(p)
            hop(copy, p, 0).start()
        for p in ps:
            hop(copy, p, 1).start()
            hop(copy, p, 2).start()

    def ev_near(copy, *ps):
        for p in ps:
            with scope(f'n_{copy.__name__}{p}'):
                hop(copy, p, 0).wait_recv()
            hop(copy, p, 3).start()
            hop(copy, p, 4).start()

    def ev_far(copy, *ps):
        for p in ps:
            with scope(f'f_{copy.__name__}{p}'):
                hop(copy, p, 1).wait_recv()
            hop(copy, p, 5).start()

    def ev_xy(copy, *ps):
        ev_near(copy, *ps)
        ev_far(copy, *ps)

    def ev_y(copy, *ps):
        for p in ps:
            with scope(f'y_{copy.__name__}{p}'):
                hop(copy, p, 3).wait_recv()
            hop(copy, p, 6).start()
            if copy is lq_copy and p >= 2:
                start(w_load(p, SLOT[:4]))

    def ev_done(copy, *ps):
        for p in ps:
            with scope(f'c_{copy.__name__}{p}'):
                if copy is lq_copy:
                    arrived(lq_ref.at[pl.ds(4, 4), p], lq_recv.at[p, 4])
                else:
                    arrived(lo_ref.at[p, pl.ds(4, 4)], lo_recv.at[p, 4])

    def w_load(p, slots):
        return [pltpu.make_async_copy(lq_ref.at[SLOT.index(m), p], ws.at[p // 2 % 2, ds((idx ^ m) * B, B), pl.ds(p % 2 * B, B)], w_sem.at[p]) for m in slots]

    def own_load(t):
        return pltpu.make_async_copy(W[t], ws.at[t], w_sem.at[6 + t])

    def start(copies):
        for c in copies:
            c.start()

    def wait(copies):
        for c in copies:
            c.wait()

    def ev_last(t):
        pieces = [2 * t + i for i in TWO]
        ev_done(lq_copy, *pieces)
        for p in pieces:
            start(w_load(p, SLOT[4:] if t else SLOT))

    def local(ref, sem):
        pltpu.make_async_copy(ref, ref, sem).wait()

    def ev_weights(t):
        with scope(f'load{t}'):
            for i in TWO:
                local(ws.at[t % 2, :, pl.ds(i * B, B)], w_sem.at[2 * t + i])

    def ev_wo(*vs):
        ev_done(lo_copy, *vs)
        for v in vs:
            lb_core(v).wait_recv()
        start(wo_load(*vs))

    def ev_wo_ready(*vs):
        with scope(f'wo{vs[0]}'):
            for v in vs:
                local(xp.at[1 - side, pl.ds(2, 6), :, pl.ds((v ^ 2) * H, H)], wo_sem.at[v])

    def ev_lb(*vs):
        for v in vs:
            with scope(f'lb{v}'):
                lb_z(v).wait_recv()
            lb_core(v).start()

    wo = xp.at[1 - side]

    def wo_own():
        return [pltpu.make_async_copy(wout_ref.at[pl.ds(r * B, B), pl.ds(c * H, H)], xp.at[1 - side, r, :, ds((c ^ tp ^ 2) * H, H)], wo_sem.at[4])
                for r in TWO for c in range(4)]

    def wo_load(*vs):
        out = []
        for v in vs:
            cols = pl.ds((v ^ 2) * H, H)
            for s, m in enumerate(SLOT):
                row = (idx ^ m) * 64
                for b in TWO:
                    out.append(pltpu.make_async_copy(lo_ref.at[v, s, b], xp.at[1 - side, 4 + 2 * b + row // B, ds(row % B, 64, 64), cols], wo_sem.at[v]))
            for r in TWO:
                out.append(pltpu.make_async_copy(lb_ref.at[v, r], xp.at[1 - side, 2 + r, :, cols], wo_sem.at[v]))
        return out

    def kvp_copy(h, s):
        return remote(kv_s.at[h, pl.ds(8 * s, 2)], kvp_s.at[h, pl.ds(2 * s, 2)], sent.at[4], kv_recv.at[0, h], peer_c)

    def kvr_copy(h, s):
        return remote(kv_s.at[h, 8 * s], kvr_s.at[h, s], sent.at[5], kv_recv.at[1, h], peer_y)

    def kvf_copy(h, s):
        return remote(kvr_s.at[h, s], kvr_s.at[h, 2 + s], sent.at[6], kv_recv.at[2, h], peer_c)

    def kv_start(copy, heads):
        for h in heads:
            for s in TWO:
                copy(h, s).start()

    def kv_wait(copy, heads):
        with scope(f'w_{copy.__name__}{heads[0]}'):
            for h in heads:
                i = (kvp_copy, kvr_copy, kvf_copy).index(copy)
                arrived((kvp_s.at[h], kvr_s.at[h, pl.ds(0, 2)], kvr_s.at[h, pl.ds(2, 2)])[i], kv_recv.at[i, h])

    def kv_forward(heads):
        kv_wait(kvr_copy, heads)
        kv_start(kvf_copy, heads)

    def reverse(i):
        return (i % 2) * 2 + i // 2

    def order(n):
        return 2 * reverse(n % 4) + ((n // 4) ^ side)

    def o_at(k, p, theirs, col, size, row=0, rows=B):
        if p:
            return ws.at[1 + theirs, ds(k * B + row, rows), ds(col, size)]
        return xb.at[k // 2, pl.ds(row, rows), ds((k % 2) * 1024 + theirs * H + col, size)]

    def o_copy(k, p, half):
        row = half * 128
        return remote(o_at(k, p, 0, 0, H, row, 128), o_at(k, p, 1, 0, H, row, 128), sent.at[7], o_recv.at[k, half], {'tp': tp ^ 1})

    def o_times(k, v, n, row=0, rows=B):
        cols = pl.ds((v ^ 2) * H, n * H)
        y = nn(xb[k // 2, pl.ds(row, rows), ds((k % 2) * 1024, 1024)], wo[0:4, :, cols].reshape(1024, n * H))
        for i in TWO:
            y = y + nn(ws[1 + i, ds(k * B + row, rows), :], wo[part(2 + i, 2), :, cols].reshape(H, n * H))
        y = y.astype(BF)
        for i in range(n):
            y_src(k, v + i, row, rows)[...] = y[:, part(i, H)]
            y_copy(k, v + i, side, row, rows).start() if v else y_local(k).start()

    def y_src(k, v, row=0, rows=B):
        return xp.at[side, k, pl.ds(row, rows), pl.ds(v * H, H)]

    def y_copy(k, v, seg, row, rows):
        return remote(y_src(k, v, row, rows), out_ref.at[seg, k, pl.ds(row, rows)], sent.at[8], y_recv.at[seg], {'tp': tp ^ v})

    def y_local(k):
        return pltpu.make_async_copy(y_src(k, 0), out_ref.at[side, k], sent.at[9])

    def x_copy(j):
        return pltpu.make_async_copy(x_ref.at[ds(j * B, B), :], xb.at[lax.rem(j, 4)], x_sem.at[lax.rem(j, 4)])

    for j in range(4):
        x_copy(j).start()
    barrier = pltpu.get_barrier_semaphore()
    peers = [{'tp': tp ^ 1}, {'tp': tp ^ 2}, {'tp': tp ^ 3}, peer_x, peer_y, peer_c]
    for dev in peers:
        pl.semaphore_signal(barrier, inc=1, device_id=dev, device_id_type=MESH)
    for t in range(3):
        own_load(t).start()

    pm[...] = phase_matrix(False)

    def permute_body(j, carry):
        x_copy(j).wait()
        y = nn(pm[...], xb[lax.rem(j, 4)]).astype(BF).reshape(8, 32, M)
        xp[j // 8, :, ds(lax.rem(j, 8) * 32, 32, 32), :] = y
        pl.when(j < 12)(lambda: x_copy(j + 4).start())

        @pl.when(j == 2)
        def _():
            with scope('barrier'):
                pl.semaphore_wait(barrier, len(peers))
            lq_start(KEY)
            on(outer, lb_z(2).start)
        return carry

    with scope('permute'):
        lax.fori_loop(0, 16, permute_body, None)

    for h in HEADS:
        column = 2 * (tp ^ (h // 2 * 2)) + h % 2
        for i, branches in enumerate(('0', '01', '1', '012', '12', '2', '0123', '123', '23', '3')):
            rows = [jnp.full((1, 128), bias_ref[j, column], F32) for j in map(int, branches)]
            m = functools.reduce(jnp.maximum, rows)
            beta_s[pl.ds(h * 16 + i, 1), :] = (m + jnp.log(sum(jnp.exp(r - m) for r in rows))) * math.log2(math.e)

    def signal_ready(i):
        pl.when(inner)(lambda: pl.semaphore_signal(ready.at[i], inc=1, device_id={'tp': tp ^ 1}, device_id_type=MESH))

    def wait_ready(i):
        with scope(f'ready{i}'):
            pl.when(outer)(lambda: pl.semaphore_wait(ready.at[i], 1))

    signal_ready(0)

    def group(g):
        low = g < 4
        return jnp.where(low, g & 1, 0), jnp.where(low, g // 2, g - 2)

    def head_number(h):
        return 2 * (tp ^ (h // 2 * 2)) + h % 2

    def project(heads, sigma, pair, kinds):
        for h in heads:
            t = head_number(h) + reverse(pair)
            x, swap = xp[side ^ sigma, pl.ds(2 * (t & 3), 2)].reshape(H, M), (t & 7) >> 2
            for t in kinds:
                y = nn(x, ws[t, :, part(h % 2, B)])
                for j in TWO:
                    piece = y[part(j, B)]
                    kv_s[h, 8 * sigma + 2 * pair + (j ^ swap), t] = (piece.T if t == VAL else piece).astype(BF)

    def phases_of(j):
        return [j % 2 + 2 * i for i in TWO], (j // 2) ^ side

    def rank_of(phase, h):
        rel = (phase - head_number(h)) & 7
        return (rel & 1) * 4 + ((rel >> 1) & 1) * 2 + (rel >> 2)

    def queries(heads, w, j):
        phases, half = phases_of(j)
        x = jnp.concatenate([xp[side, 2 * f + half] for f in phases])
        for h in heads:
            y = nn(x, ws[w, :, part(h % 2, B)]).astype(BF)
            for i, f in enumerate(phases):
                q_s[h, rank_of(f + 4 * half, h)] = y[part(i, B)]

    with scope('own_w'):
        for t in range(3):
            own_load(t).wait()
    own, partner = HEADS[:2], HEADS[2:]

    def mix(b, c):
        return jnp.concatenate([b, b, c, c], axis=1)

    def keys_of(ref, h, i, weights):
        parts = []
        n = 0
        for count, b in weights:
            def values(i=i + n, count=count):
                v = [ref[h, i + j, VAL] for j in range(count)]
                return v[0] if count == 1 else jnp.concatenate(v, axis=1)
            parts.append((values, count * B, b))
            n += count
        return (lambda: ref[h, i:i + n, KEY].reshape(n * B, B)), parts

    def chunk_tiles(p, j, kind):
        both_phases, half = phases_of(j)

        def put(h, phase, ot):
            k = 2 * (phase & 3) + half
            y = ot.T.astype(BF)
            for i in TWO:
                pl.when(p == i)(lambda i=i: o_at(k, i, 0, (h % 2) * B, B).__setitem__(..., y))

        def tile(h, phases, ranks, wide, narrow, s_ref, n_ref):
            def done(ot):
                for i, phase in enumerate(phases):
                    put(h, phase, ot[:, part(i, B)])
            return tile_steps(lambda: jnp.concatenate([q_s[h, r] for r in ranks]), wide, narrow, s_ref, n_ref, done)

        h = 2 * p + (j % 2) ^ 1
        rest = tile(h, both_phases, [rank_of(f + 4 * half, h) for f in both_phases], [keys_of(kv_s, h, i, [(2, None)]) for i in range(0, 8, 2)], [], t_scr, None)
        h = 2 * p + (j % 2)
        a = head_number(h)
        b0, b01, b1, b012, b12, b2, b0123, b123, b23, b3 = [beta_s[pl.ds(h * 16 + i, 1), :] for i in range(10)]
        phases = [a & 3, (a & 3) ^ 2]
        both = [keys_of(kv_s, h, i, [(2, b)]) for i, b in ((2, b01), (4, b0), (6, b0), (10, b1))]
        if kind == 0:
            both += [keys_of(kv_s, h, 0, [(1, mix(b0123, b01)), (1, mix(b012, b01))]), keys_of(kv_s, h, 8, [(1, mix(b123, b1)), (1, mix(b12, b1))])]
            first = [keys_of(kvp_s, h, i, [(1, b23), (1, b2)]) for i in (0, 2)] + [keys_of(kvr_s, h, i, [(2, b3)]) for i in (0, 2)]
        else:
            both += [keys_of(kv_s, h, 0, [(2, mix(b012, b01))]), keys_of(kv_s, h, 8, [(2, mix(b12, b1))])]
            first = [keys_of(kvp_s, h, i, [(2, b2)]) for i in (0, 2)]
        with scope(f'tile{kind}'):
            run_tiles([rest, tile(h, phases, [kind, rank_of(phases[1] + 4 * half, h)], both, first, s_scr, t_scr.at[:, pl.ds(0, B)])])

    def send_o(ks, p):
        @pl.when(outer)
        def _():
            for k in ks:
                for half in TWO:
                    o_copy(order(k), p, half).start()

    def step_body(t, carry):
        packed = functools.reduce(lambda x, i: jnp.where(t == i, TABLE[i], x), range(len(TABLE)), 0)
        code, n, event = packed % 16, packed // 16 % 16, packed // 256

        def step_o():
            with scope('own_kv'):
                project(own, *group(n), (KEY, VAL))

        def step_kv(t_):
            with scope(f'par_{t_}'):
                for i in TWO:
                    project(partner, *group(2 * n + i), (t_,))

        def step_q(heads, w):
            with scope(f'que_{w}'):
                queries(heads, w, n)

        def step_out(v, m):
            @pl.when(inner)
            def _():
                k = order(n)

                def halves():
                    for half in TWO:
                        with scope(f'wait_h{half}'):
                            arrived(ws.at[0, pl.ds(0, B), :], o_recv.at[k, half])
                        o_times(k, v, m, half * 128, 128)

                def whole():
                    with scope('wait_o'):
                        for half in TWO:
                            arrived(ws.at[0, pl.ds(0, B), :], o_recv.at[k, half])
                    with scope(f'out{v}'):
                        o_times(k, v, m)

                if m == 2:
                    pl.when(n == 0)(halves)
                    pl.when(n > 0)(whole)
                else:
                    with scope(f'out{v}'):
                        o_times(k, v, m)

        f = functools.partial
        kinds = {'-': lambda: None, 'O': step_o, 'P': f(step_q, own, QUE), 'K': f(step_kv, KEY), 'V': f(step_kv, VAL), 'Q': f(step_q, partner, KEY),
                 'A': lambda: chunk_tiles(n // 4, n % 4, 0), 'B': lambda: chunk_tiles(n // 4, n % 4, 1), 'R': f(step_out, 2, 2), 'L': f(step_out, 1, 1), 'N': f(step_out, 0, 1)}
        choose(code, [kinds[c] for c in KINDS])
        call = functools.partial

        events = {
            'free': [call(signal_ready, 1), call(on, inner, lambda: start(wo_own()))],
            'r0': [call(wait_ready, 0)],
            'r1': [call(wait_ready, 1)],
            'so': [call(kv_start, kvp_copy, own)],
            'po': [call(kv_wait, kvp_copy, own)],
            'sp': [call(kv_start, kvp_copy, partner)],
            'pp': [call(kv_wait, kvp_copy, partner)],
        }
        for t_, c in enumerate('kvq'):
            events['b' + c] = [call(lq_start, t_)]
            events['l' + c] = [call(ev_last, t_)]
            events['w' + c] = [call(ev_weights, t_)]
            events['z' + c] = [call(ev_z, lq_copy, 2 * t_, 2 * t_ + 1)]
            for i in TWO:
                for e, f in zip('zmfxy', (ev_z, ev_near, ev_far, ev_xy, ev_y)):
                    events[f'{e}{c}{i}'] = [call(f, lq_copy, 2 * t_ + i)]
        for i, vs in enumerate(((2, 3), (1,), (0,))):
            events[f'b{i}'] = [call(lo_start, *vs)]
            for e, f in zip('zmxycwv', (call(ev_z, lo_copy), call(ev_near, lo_copy), call(ev_far, lo_copy), call(ev_y, lo_copy), ev_lb, ev_wo, ev_wo_ready)):
                events[f'{e}{i}'] = [call(on, inner, call(f, *vs))]
        events['v0'] += [call(on, inner, lambda: local(xp.at[1 - side, pl.ds(0, 2)], wo_sem.at[4]))]
        for v in range(4):
            events[f'd{v}'] = [call(on, outer, lambda v=v: lb_z(v).start())]
        for h in HEADS:
            for z in TWO:
                events[f's{h}{z}'] = [kvr_copy(h, z).start]
            events[f'f{h}'] = [call(kv_forward, [h])]
            events[f'g{h}'] = [call(kv_wait, kvf_copy, [h])]
        for k in ROWS:
            for p in TWO:
                events['op'[p] + str(k)] = [call(send_o, (k,), p)]
        def run(names):
            for name in names.split(','):
                where, _, name = name.rpartition(':')
                if where:
                    on(inner if where == 'i' else outer, *events[name])
                else:
                    for c in events[name]:
                        c()

        @pl.when(event > 0)
        def _():
            choose(event - 1, [functools.partial(run, names) for names in EVENTS])
        return carry

    lax.fori_loop(0, len(TABLE), step_body, None)

    all_sent(lq_ref, 0)
    all_sent(lo_ref.at[:, 0, 0], 2)
    all_sent(lb_ref.at[:, 0], 3)
    all_sent(kvp_s, 4)
    all_sent(kvr_s.at[:, pl.ds(0, 2)], 5)
    all_sent(kvr_s.at[:, pl.ds(0, 2)], 6)

    @pl.when(outer)
    def _():
        all_sent(xb, 7)

    @pl.when(inner)
    def _():
        all_sent(lo_ref.at[:, pl.ds(0, 7)], 1)
        with scope('y_sent'):
            all_sent(xp.at[side, :, :, pl.ds(H, 3 * H)], 8)
        local(xp.at[side, :, :, pl.ds(0, H)], sent.at[9])

    for seg in TWO:
        @pl.when(tp != 1 + seg)
        def _(seg=seg):
            with scope(f'recv{seg}'):
                arrived(out_ref.at[seg], y_recv.at[seg])


PROGRAM = (
    'O.i:zk0,i:zk1', 'O.i:bv,o:zk0', 'O.o:bv,o:zk1,s00,i:xk0', 'O.o:xk0,i:xk1,o:s01,d3', 'O.o:xk1,i:yk0,i:zv0', 'O.o:yk0,i:yk1,i:zv1,i:s01,i:bq',
    'P.o:bq,so,o:zv0,o:yk1,lk,o:zv1,d1,i:xv0', 'P.wk,i:xv1', 'K', 'K.o:xv0,i:zq,f0', 'K.o:xv1,i:yv0,i:yv1,b0,b1,r0,po,g0,o:zq',
    'T0.o0,o1,d0,o:yv0,o:yv1,lv,mq0,i:mq1,i:fq0,i:fq1', 'P.wv,z0,o:mq1,b2', 'V.o:fq0,o:fq1,sp,o:s10,o:s11', 'V.c0,z1,o:s20,o:s21',
    'V.yq0,yq1,lq,m0,o:s30,o:s31', 'P.free,wq', 'Q.pp,r1,x0,c1,i:s10,i:s11,y0', 'T4.p0,p1,w0,m1,x1,v0', 'R.y1,w1,v1,i:s20,i:s21', 'L', 'Q.f1', 'R',
    'T5.p2,g1', 'L', 'T1.o2,p3,o3,o:f2', 'R.i:s30,i:s31', 'L', 'Q.o:g2', 'Q.i:f2,o:f3', 'T2', 'R.i:g2', 'L', 'T6.p4,o4,p5,o5,o:g3', 'R.i:f3,z2,c2',
    'L', 'T3.i:g3', 'T7.p6,o6,p7,o7', 'R', 'L.m2,x2', 'R.y2', 'L.w2', '-.v2', 'N', 'N', 'N', 'R', 'L', 'N', 'N', 'N', 'N', 'N',
)
KINDS = '-OPKVQABRLN'


def tables():
    table, seen = [], {}
    names = tuple(dict.fromkeys(s.partition('.')[2] for s in PROGRAM if '.' in s))
    for s in PROGRAM:
        name, _, after = s.partition('.')
        kind, n = name[0], seen.get(name[0], 0)
        seen[kind] = n + 1
        if kind == 'T':
            n = int(name[1:])
            kind = 'AB'[n in (2, 3, 4, 5)]
        table.append(KINDS.index(kind) + 16 * n + 256 * (names.index(after) + 1 if after else 0))
    return table, names


TABLE, EVENTS = tables()


def main(bias, x, wk, wv, wq, w_out):
    anyspec = pl.BlockSpec(memory_space=pl.ANY)
    vmem = [((4, B, M), BF), ((B, B), BF), ((2, 8, B, M), BF), ((3, M, H), BF), ((4, 8, B, B), BF), ((4, 12, 2, B, B), BF), ((4, 4, 2, B, B), BF), ((4, 4, 2, B, B), BF),
            ((3072, H), F32), ((M, H), F32), ((64, 128), F32)]
    dma = [(4,), (9,), (5,), (10,), (6, 5), (4, 5), (4, 2), (3, 4), (8, 2), (2,)]
    return pl.pallas_call(
        main_kernel,
        in_specs=[pl.BlockSpec(memory_space=pltpu.SMEM)] + [anyspec] * 5,
        out_specs=[anyspec] * 4,
        out_shape=[jax.ShapeDtypeStruct(s, BF) for s in ((2, 8, B, H), (8, 6, B, B), (4, 8, 2, 64, H), (4, 2, B, H))],
        scratch_shapes=[pltpu.VMEM(*v) for v in vmem] + [pltpu.SemaphoreType.DMA(d) for d in dma] + [pltpu.SemaphoreType.REGULAR((2,))],
        compiler_params=params(collective_id=0, has_side_effects=True),
        cost_estimate=pl.CostEstimate(flops=10**11, bytes_accessed=10**8, transcendentals=0),
        name='main',
    )(bias, x, wk, wv, wq, w_out)[0]


def solution(mesh):
    def device_fn(hidden, w_query, w_key, w_value, w_out, branch_bias):
        return unpermute(main(branch_bias, hidden, w_key, w_value, w_query, w_out))

    return jax.shard_map(device_fn, mesh=mesh, in_specs=(P(('dp', 'sp'), None), P(None, 'tp'), P(None, 'tp'), P(None, 'tp'), P('tp', None), P(None, None)), out_specs=P(('dp', 'sp'), 'tp'), check_vma=False)
```

```python
import functools
import math

import jax
import jax.numpy as jnp
from jax import lax
from jax.experimental import pallas as pl
from jax.experimental.pallas import tpu as pltpu
from jax.sharding import PartitionSpec as P

MESH = pl.DeviceIdType.MESH
BF = jnp.bfloat16
F32 = jnp.float32
B, H, M = 256, 512, 2048
KAPPA = math.log2(math.e) / 16
VMEM = 66_900_000
SLOT = (0, 4, 2, 6, 1, 5, 3, 7)
KEY, VAL, QUE = range(3)
HEADS = range(4)
TWO = range(2)
QUARTERS = range(4)
ROWS = range(8)


def nn(a, b):
    return lax.dot_general(a, b, (((1,), (0,)), ((), ())), preferred_element_type=F32)


def nt(a, b):
    return lax.dot_general(a, b, (((1,), (1,)), ((), ())), preferred_element_type=F32)


def params(**kw):
    return pltpu.CompilerParams(vmem_limit_bytes=VMEM, **kw)


def ds(start, size, align=128):
    return pl.ds(pl.multiple_of(start, align), size)


def part(i, size):
    return slice(i * size, i * size + size)


def phase_matrix(transposed):
    r = lax.broadcasted_iota(jnp.int32, (B, B), int(transposed))
    p = lax.broadcasted_iota(jnp.int32, (B, B), int(not transposed))
    k = r // 32
    return (p == (r % 32) * 8 + k // 2 + 4 * (k % 2)).astype(F32).astype(BF)


def unpermute_kernel(y_ref, o_ref, y_s, o_s, load, store):
    pieces = [(s, j) for s in TWO for j in range(4)]

    def get(i):
        s, j = pieces[i]
        return pltpu.make_async_copy(y_ref.at[s, :, pl.ds(j * 64, 64)], y_s.at[i], load.at[i])

    def put(i):
        return pltpu.make_async_copy(o_s.at[i], o_ref.at[pl.ds(i * H, H)], store.at[i])

    for i in ROWS:
        get(i).start()
    pm = phase_matrix(True)
    for i in range(0, 8, 2):
        group = (i, i + 1)
        for k in group:
            get(k).wait()
        for k in group:
            for j in TWO:
                o_s[k, part(j, B), :] = nn(pm, y_s[k, :, part(j, 32), :].reshape(B, H)).astype(BF)
        for k in group:
            put(k).start()
    for i in ROWS:
        put(i).wait()


def unpermute(y):
    anyspec = pl.BlockSpec(memory_space=pl.ANY)
    return pl.pallas_call(
        unpermute_kernel,
        in_specs=[anyspec],
        out_specs=anyspec,
        out_shape=jax.ShapeDtypeStruct((2 * M, H), BF),
        scratch_shapes=[pltpu.VMEM((8, 8, 64, H), BF), pltpu.VMEM((8, H, H), BF), pltpu.SemaphoreType.DMA((8,)), pltpu.SemaphoreType.DMA((8,))],
        compiler_params=params(),
        name='unpermute',
    )(y)


def tile_steps(q, wide, narrow, s_ref, n_ref, done):
    st = {}
    logits, sums = [], []

    def add(name, x):
        st[name] = st[name] + x if name in st else x

    for groups, ref in ((wide, s_ref), (narrow, n_ref)):
        off = 0
        for keys, parts in groups:
            def qk(keys=keys, parts=parts, off=off, ref=ref):
                s = nt(keys(), q() if ref is s_ref else q()[:B])
                o = 0
                for _, n, b in parts:
                    piece = s[o:o + n]
                    ref[pl.ds(off + o, n), :] = piece
                    t = jnp.max(piece, axis=0, keepdims=True) * KAPPA
                    if b is not None:
                        t = t + fit(b, t)
                    if ref is n_ref:
                        t = jnp.concatenate([t, st['top'][:, B:]], axis=1)
                    st['top'] = jnp.maximum(st['top'], t) if 'top' in st else t
                    o += n
            logits.append(qk)
            for v, n, b in parts:
                def sv(v=v, n=n, b=b, off=off, ref=ref):
                    top = st['top'] if ref is s_ref else st['top'][:, :B]
                    e = jnp.exp2(ref[pl.ds(off, n), :] * KAPPA - (top if b is None else top - fit(b, top)))
                    name = 'w' if ref is s_ref else 'n'
                    add('l' + name, jnp.sum(e, axis=0, keepdims=True))
                    add('o' + name, nn(v(), e.astype(BF)))
                sums.append(sv)
                off += n

    def finish():
        o, l = st['ow'], st['lw']
        if narrow:
            o = jnp.concatenate([o[:, :B] + st['on'], o[:, B:]], axis=1)
            l = jnp.concatenate([l[:, :B] + st['ln'], l[:, B:]], axis=1)
        done(o / l)

    return logits, sums + [finish]


def fit(b, like):
    return b if b.shape == like.shape else jnp.concatenate([b] * (like.shape[1] // 128), axis=1)


def interleave(a, b):
    i = j = 0
    while i < len(a) or j < len(b):
        if j >= len(b) or (i < len(a) and i * len(b) <= j * len(a)):
            a[i]()
            i += 1
        else:
            b[j]()
            j += 1


def run_tiles(tiles):
    before = []
    for logits, sums in tiles:
        interleave(logits, before)
        before = sums
    interleave([], before)


def choose(x, cases):
    def among(lo, hi):
        mid = (lo + hi) // 2
        if hi - lo == 1:
            cases[lo]()
        else:
            pl.when(x < mid)(lambda: among(lo, mid))
            pl.when(x >= mid)(lambda: among(mid, hi))
    among(0, len(cases))


def on(cond, *calls):
    @pl.when(cond)
    def _():
        for c in calls:
            c()


def scope(name):
    return jax.named_scope(name)


def main_kernel(bias_ref, x_ref, wk_ref, wv_ref, wq_ref, wout_ref, out_ref, lq_ref, lo_ref, lb_ref,
                xb, pm, xp, ws, q_s, kv_s, kvp_s, kvr_s, s_scr, t_scr,
                beta_s, x_sem, w_sem, wo_sem, sent, lq_recv, lo_recv, lb_recv, kv_recv, o_recv, y_recv, ready):
    dp, tp, sp = lax.axis_index('dp'), lax.axis_index('tp'), lax.axis_index('sp')
    idx = dp * 4 + sp
    side = tp // 2
    inner = (tp == 1) | (tp == 2)
    outer = jnp.logical_not(inner)
    W = (wk_ref, wv_ref, wq_ref)
    peer_x, peer_y, peer_c = {'dp': dp ^ 1}, {'sp': sp ^ 2}, {'sp': sp ^ 1}

    def remote(src, dst, ss, rs, dev):
        return pltpu.make_async_remote_copy(src_ref=src, dst_ref=dst, send_sem=ss, recv_sem=rs, device_id=dev, device_id_type=MESH)

    def lq_copy(t, src, dst, dev):
        return remote(lq_ref.at[src, t], lq_ref.at[dst, t], sent.at[0], lq_recv.at[t, min(dst, 4)], dev)

    def lq_z(t):
        return remote(W[t // 2].at[ds(idx * B, B), pl.ds(t % 2 * B, B)], lq_ref.at[0, t], sent.at[0], lq_recv.at[t, 0], {'tp': tp ^ 2})

    def lq_start(t):
        for i in TWO:
            lq_z(2 * t + i).start()

    def lo_copy(v, src, dst, dev):
        return remote(lo_ref.at[v, src], lo_ref.at[v, dst], sent.at[1], lo_recv.at[v, min(dst, 4)], dev)

    def lo_z(v):
        dst = 2 - side
        b = (tp ^ dst) - 2
        return remote(wout_ref.at[ds(idx * 64, 64, 64), ds((dst ^ v) * H, H)], lo_ref.at[v, 0, b], sent.at[2], lo_recv.at[v, 0], {'tp': dst})

    def lb_z(v):
        return remote(wout_ref.at[ds(sp % 2 * B, B), ds((tp ^ 1 ^ v) * H, H)], lb_ref.at[v, sp % 2], sent.at[3], lb_recv.at[v, 0], {'tp': tp ^ 1})

    def lb_core(v):
        return remote(lb_ref.at[v, sp % 2], lb_ref.at[v, sp % 2], sent.at[3], lb_recv.at[v, 1], peer_c)

    def lo_start(*vs):
        for v in vs:
            lo_z(v).start()

    def arrived(ref, sem):
        remote(ref, ref, sent.at[0], sem, peer_c).wait_recv()

    def all_sent(ref, i):
        remote(ref, ref, sent.at[i], sent.at[i], peer_c).wait_send()

    def lo_zwait(v):
        arrived(lo_ref.at[v, 0], lo_recv.at[v, 0])

    def hop(copy, p, i):
        near, far, n = (peer_x, peer_y, 1) if (copy is lo_copy and p == 2) or (copy is lq_copy and p == 5) else (peer_y, peer_x, 2)
        f = 3 - n
        return copy(p, *((0, n, near), (0, f, far), (0, 4, peer_c), (n, 3, far), (n, 4 + n, peer_c), (f, 4 + f, peer_c), (3, 7, peer_c))[i])

    def ev_z(copy, *ps):
        for p in ps:
            with scope(f'z_{copy.__name__}{p}'):
                lq_z(p).wait_recv() if copy is lq_copy else lo_zwait(p)
            hop(copy, p, 0).start()
        for p in ps:
            hop(copy, p, 1).start()
            hop(copy, p, 2).start()

    def ev_near(copy, *ps):
        for p in ps:
            with scope(f'n_{copy.__name__}{p}'):
                hop(copy, p, 0).wait_recv()
            hop(copy, p, 3).start()
            hop(copy, p, 4).start()

    def ev_far(copy, *ps):
        for p in ps:
            with scope(f'f_{copy.__name__}{p}'):
                hop(copy, p, 1).wait_recv()
            hop(copy, p, 5).start()

    def ev_xy(copy, *ps):
        ev_near(copy, *ps)
        ev_far(copy, *ps)

    def ev_y(copy, *ps):
        for p in ps:
            with scope(f'y_{copy.__name__}{p}'):
                hop(copy, p, 3).wait_recv()
            hop(copy, p, 6).start()
            if copy is lq_copy and p >= 2:
                start(w_load(p, SLOT[:4]))

    def ev_done(copy, *ps):
        for p in ps:
            with scope(f'c_{copy.__name__}{p}'):
                if copy is lq_copy:
                    arrived(lq_ref.at[pl.ds(4, 4), p], lq_recv.at[p, 4])
                else:
                    arrived(lo_ref.at[p, pl.ds(4, 4)], lo_recv.at[p, 4])

    def w_load(p, slots):
        return [pltpu.make_async_copy(lq_ref.at[SLOT.index(m), p], ws.at[p // 2 % 2, ds((idx ^ m) * B, B), pl.ds(p % 2 * B, B)], w_sem.at[p]) for m in slots]

    def own_load(t):
        return pltpu.make_async_copy(W[t], ws.at[t], w_sem.at[6 + t])

    def start(copies):
        for c in copies:
            c.start()

    def wait(copies):
        for c in copies:
            c.wait()

    def ev_last(t):
        pieces = [2 * t + i for i in TWO]
        ev_done(lq_copy, *pieces)
        for p in pieces:
            start(w_load(p, SLOT[4:] if t else SLOT))

    def local(ref, sem):
        pltpu.make_async_copy(ref, ref, sem).wait()

    def ev_weights(t):
        with scope(f'load{t}'):
            for i in TWO:
                local(ws.at[t % 2, :, pl.ds(i * B, B)], w_sem.at[2 * t + i])

    def ev_wo(*vs):
        ev_done(lo_copy, *vs)
        for v in vs:
            lb_core(v).wait_recv()
        start(wo_load(*vs))

    def ev_wo_ready(*vs):
        with scope(f'wo{vs[0]}'):
            for v in vs:
                local(xp.at[1 - side, pl.ds(2, 6), :, pl.ds((v ^ 2) * H, H)], wo_sem.at[v])

    def ev_lb(*vs):
        for v in vs:
            with scope(f'lb{v}'):
                lb_z(v).wait_recv()
            lb_core(v).start()

    wo = xp.at[1 - side]

    def wo_own():
        return [pltpu.make_async_copy(wout_ref.at[pl.ds(r * B, B), pl.ds(c * H, H)], xp.at[1 - side, r, :, ds((c ^ tp ^ 2) * H, H)], wo_sem.at[4])
                for r in TWO for c in range(4)]

    def wo_load(*vs):
        out = []
        for v in vs:
            cols = pl.ds((v ^ 2) * H, H)
            for s, m in enumerate(SLOT):
                row = (idx ^ m) * 64
                for b in TWO:
                    out.append(pltpu.make_async_copy(lo_ref.at[v, s, b], xp.at[1 - side, 4 + 2 * b + row // B, ds(row % B, 64, 64), cols], wo_sem.at[v]))
            for r in TWO:
                out.append(pltpu.make_async_copy(lb_ref.at[v, r], xp.at[1 - side, 2 + r, :, cols], wo_sem.at[v]))
        return out

    def kvp_copy(h, s):
        return remote(kv_s.at[h, pl.ds(8 * s, 2)], kvp_s.at[h, pl.ds(2 * s, 2)], sent.at[4], kv_recv.at[0, h], peer_c)

    def kvr_copy(h, s):
        return remote(kv_s.at[h, 8 * s], kvr_s.at[h, s], sent.at[5], kv_recv.at[1, h], peer_y)

    def kvf_copy(h, s):
        return remote(kvr_s.at[h, s], kvr_s.at[h, 2 + s], sent.at[6], kv_recv.at[2, h], peer_c)

    def kv_start(copy, heads):
        for h in heads:
            for s in TWO:
                copy(h, s).start()

    def kv_wait(copy, heads):
        with scope(f'w_{copy.__name__}{heads[0]}'):
            for h in heads:
                i = (kvp_copy, kvr_copy, kvf_copy).index(copy)
                arrived((kvp_s.at[h], kvr_s.at[h, pl.ds(0, 2)], kvr_s.at[h, pl.ds(2, 2)])[i], kv_recv.at[i, h])

    def kv_forward(heads):
        kv_wait(kvr_copy, heads)
        kv_start(kvf_copy, heads)

    def reverse(i):
        return (i % 2) * 2 + i // 2

    def order(n):
        return 2 * reverse(n % 4) + ((n // 4) ^ side)

    def o_at(k, p, theirs, col, size, row=0, rows=B):
        if p:
            return ws.at[1 + theirs, ds(k * B + row, rows, 64), ds(col, size)]
        return xb.at[k // 2, pl.ds(row, rows), ds((k % 2) * 1024 + theirs * H + col, size)]

    def o_copy(k, p, q):
        row = q * 64
        return remote(o_at(k, p, 0, 0, H, row, 64), o_at(k, p, 1, 0, H, row, 64), sent.at[7], o_recv.at[k, q], {'tp': tp ^ 1})

    def o_times(k, v, n, row=0, rows=B):
        cols = pl.ds((v ^ 2) * H, n * H)
        y = nn(xb[k // 2, pl.ds(row, rows), ds((k % 2) * 1024, 1024)], wo[0:4, :, cols].reshape(1024, n * H))
        for i in TWO:
            y = y + nn(ws[1 + i, ds(k * B + row, rows, 64), :], wo[part(2 + i, 2), :, cols].reshape(H, n * H))
        y = y.astype(BF)
        for i in range(n):
            y_src(k, v + i, row, rows)[...] = y[:, part(i, H)]
            y_copy(k, v + i, side, row, rows).start() if v else y_local(k).start()

    def y_src(k, v, row=0, rows=B):
        return xp.at[side, k, pl.ds(row, rows), pl.ds(v * H, H)]

    def y_copy(k, v, seg, row, rows):
        return remote(y_src(k, v, row, rows), out_ref.at[seg, k, pl.ds(row, rows)], sent.at[8], y_recv.at[seg], {'tp': tp ^ v})

    def y_local(k):
        return pltpu.make_async_copy(y_src(k, 0), out_ref.at[side, k], sent.at[9])

    def x_copy(j):
        return pltpu.make_async_copy(x_ref.at[ds(j * B, B), :], xb.at[lax.rem(j, 4)], x_sem.at[lax.rem(j, 4)])

    for j in range(4):
        x_copy(j).start()
    barrier = pltpu.get_barrier_semaphore()
    peers = [{'tp': tp ^ 1}, {'tp': tp ^ 2}, {'tp': tp ^ 3}, peer_x, peer_y, peer_c]
    for dev in peers:
        pl.semaphore_signal(barrier, inc=1, device_id=dev, device_id_type=MESH)
    for t in range(3):
        own_load(t).start()

    pm[...] = phase_matrix(False)

    def permute_body(j, carry):
        x_copy(j).wait()
        y = nn(pm[...], xb[lax.rem(j, 4)]).astype(BF).reshape(8, 32, M)
        xp[j // 8, :, ds(lax.rem(j, 8) * 32, 32, 32), :] = y
        pl.when(j < 12)(lambda: x_copy(j + 4).start())

        @pl.when(j == 2)
        def _():
            with scope('barrier'):
                pl.semaphore_wait(barrier, len(peers))
            lq_start(KEY)
            on(outer, lb_z(2).start)
        return carry

    with scope('permute'):
        lax.fori_loop(0, 16, permute_body, None)

    for h in HEADS:
        column = 2 * (tp ^ (h // 2 * 2)) + h % 2
        for i, branches in enumerate(('0', '01', '1', '012', '12', '2', '0123', '123', '23', '3')):
            rows = [jnp.full((1, 128), bias_ref[j, column], F32) for j in map(int, branches)]
            m = functools.reduce(jnp.maximum, rows)
            beta_s[pl.ds(h * 16 + i, 1), :] = (m + jnp.log(sum(jnp.exp(r - m) for r in rows))) * math.log2(math.e)

    def signal_ready(i):
        pl.when(inner)(lambda: pl.semaphore_signal(ready.at[i], inc=1, device_id={'tp': tp ^ 1}, device_id_type=MESH))

    def wait_ready(i):
        with scope(f'ready{i}'):
            pl.when(outer)(lambda: pl.semaphore_wait(ready.at[i], 1))

    signal_ready(0)

    def group(g):
        low = g < 4
        return jnp.where(low, g & 1, 0), jnp.where(low, g // 2, g - 2)

    def head_number(h):
        return 2 * (tp ^ (h // 2 * 2)) + h % 2

    def project(heads, sigma, pair, kinds):
        for h in heads:
            t = head_number(h) + reverse(pair)
            x, swap = xp[side ^ sigma, pl.ds(2 * (t & 3), 2)].reshape(H, M), (t & 7) >> 2
            for t in kinds:
                y = nn(x, ws[t, :, part(h % 2, B)])
                for j in TWO:
                    piece = y[part(j, B)]
                    kv_s[h, 8 * sigma + 2 * pair + (j ^ swap), t] = (piece.T if t == VAL else piece).astype(BF)

    def phases_of(j):
        return [j % 2 + 2 * i for i in TWO], (j // 2) ^ side

    def rank_of(phase, h):
        rel = (phase - head_number(h)) & 7
        return (rel & 1) * 4 + ((rel >> 1) & 1) * 2 + (rel >> 2)

    def queries(heads, w, j):
        phases, half = phases_of(j)
        x = jnp.concatenate([xp[side, 2 * f + half] for f in phases])
        for h in heads:
            y = nn(x, ws[w, :, part(h % 2, B)]).astype(BF)
            for i, f in enumerate(phases):
                q_s[h, rank_of(f + 4 * half, h)] = y[part(i, B)]

    with scope('own_w'):
        for t in range(3):
            own_load(t).wait()
    own, partner = HEADS[:2], HEADS[2:]

    def mix(b, c):
        return jnp.concatenate([b, b, c, c], axis=1)

    def keys_of(ref, h, i, weights):
        parts = []
        n = 0
        for count, b in weights:
            def values(i=i + n, count=count):
                v = [ref[h, i + j, VAL] for j in range(count)]
                return v[0] if count == 1 else jnp.concatenate(v, axis=1)
            parts.append((values, count * B, b))
            n += count
        return (lambda: ref[h, i:i + n, KEY].reshape(n * B, B)), parts

    def chunk_tiles(p, j, kind):
        both_phases, half = phases_of(j)

        def put(h, phase, ot):
            k = 2 * (phase & 3) + half
            y = ot.T.astype(BF)
            for i in TWO:
                pl.when(p == i)(lambda i=i: o_at(k, i, 0, (h % 2) * B, B).__setitem__(..., y))

        def tile(h, phases, ranks, wide, narrow, s_ref, n_ref):
            def done(ot):
                for i, phase in enumerate(phases):
                    put(h, phase, ot[:, part(i, B)])
            return tile_steps(lambda: jnp.concatenate([q_s[h, r] for r in ranks]), wide, narrow, s_ref, n_ref, done)

        h = 2 * p + (j % 2) ^ 1
        rest = tile(h, both_phases, [rank_of(f + 4 * half, h) for f in both_phases], [keys_of(kv_s, h, i, [(1, None)]) for i in ROWS], [], t_scr, None)
        h = 2 * p + (j % 2)
        a = head_number(h)
        b0, b01, b1, b012, b12, b2, b0123, b123, b23, b3 = [beta_s[pl.ds(h * 16 + i, 1), :] for i in range(10)]
        phases = [a & 3, (a & 3) ^ 2]
        both = [keys_of(kv_s, h, i, [(2, b)] * n) for i, b, n in ((2, b01, 1), (4, b0, 2), (10, b1, 1))]
        if kind == 0:
            both += [keys_of(kv_s, h, 0, [(1, mix(b0123, b01)), (1, mix(b012, b01))]), keys_of(kv_s, h, 8, [(1, mix(b123, b1)), (1, mix(b12, b1))])]
            first = [keys_of(kvp_s, h, i, [(1, b23), (1, b2)]) for i in (0, 2)] + [keys_of(kvr_s, h, i, [(2, b3)]) for i in (0, 2)]
        else:
            both += [keys_of(kv_s, h, 0, [(2, mix(b012, b01))]), keys_of(kv_s, h, 8, [(2, mix(b12, b1))])]
            first = [keys_of(kvp_s, h, i, [(2, b2)]) for i in (0, 2)]
        with scope(f'tile{kind}'):
            run_tiles([rest, tile(h, phases, [kind, rank_of(phases[1] + 4 * half, h)], both, first, s_scr, t_scr.at[:, pl.ds(0, B)])])

    def send_o(ks, p):
        @pl.when(outer)
        def _():
            for k in ks:
                for q in QUARTERS:
                    o_copy(order(k), p, q).start()

    def step_body(t, carry):
        packed = functools.reduce(lambda x, i: jnp.where(t == i, TABLE[i], x), range(len(TABLE)), 0)
        code, n, event = packed % 16, packed // 16 % 16, packed // 256

        def step_o():
            with scope('own_kv'):
                project(own, *group(n), (KEY, VAL))

        def step_kv(t_):
            with scope(f'par_{t_}'):
                for i in TWO:
                    project(partner, *group(2 * n + i), (t_,))

        def step_q(heads, w):
            with scope(f'que_{w}'):
                queries(heads, w, n)

        def step_out(v, m):
            @pl.when(inner)
            def _():
                k = order(n)

                def wait_for(q):
                    arrived(ws.at[0, pl.ds(0, 128), :], o_recv.at[k, q])

                def quarters():
                    for q in QUARTERS:
                        with scope(f'wait_q{q}'):
                            wait_for(q)
                        o_times(k, v, m, q * 64, 64)

                def whole():
                    with scope('wait_o'):
                        for q in QUARTERS:
                            wait_for(q)
                    with scope(f'out{v}'):
                        o_times(k, v, m)

                if m == 2:
                    pl.when(n == 0)(quarters)
                    pl.when(n > 0)(whole)
                else:
                    with scope(f'out{v}'):
                        o_times(k, v, m)

        f = functools.partial
        kinds = {'-': lambda: None, 'O': step_o, 'P': f(step_q, own, QUE), 'K': f(step_kv, KEY), 'V': f(step_kv, VAL), 'Q': f(step_q, partner, KEY),
                 'A': lambda: chunk_tiles(n // 4, n % 4, 0), 'B': lambda: chunk_tiles(n // 4, n % 4, 1), 'R': f(step_out, 2, 2), 'L': f(step_out, 1, 1), 'N': f(step_out, 0, 1)}
        choose(code, [kinds[c] for c in KINDS])
        call = functools.partial

        events = {
            'free': [call(signal_ready, 1), call(on, inner, lambda: start(wo_own()))],
            'r0': [call(wait_ready, 0)],
            'r1': [call(wait_ready, 1)],
            'ko': [call(kv_start, kvp_copy, own)],
            'po': [call(kv_wait, kvp_copy, own)],
            'kp': [call(kv_start, kvp_copy, partner)],
            'pp': [call(kv_wait, kvp_copy, partner)],
        }
        for t_, c in enumerate('kvq'):
            events['b' + c] = [call(lq_start, t_)]
            events['l' + c] = [call(ev_last, t_)]
            events['w' + c] = [call(ev_weights, t_)]
            events['z' + c] = [call(ev_z, lq_copy, 2 * t_, 2 * t_ + 1)]
            for i in TWO:
                for e, f in zip('zmfxy', (ev_z, ev_near, ev_far, ev_xy, ev_y)):
                    events[f'{e}{c}{i}'] = [call(f, lq_copy, 2 * t_ + i)]
        for i, vs in enumerate(((2, 3), (1,), (0,))):
            events[f'b{i}'] = [call(lo_start, *vs)]
            for e, f in zip('zmxycwv', (call(ev_z, lo_copy), call(ev_near, lo_copy), call(ev_far, lo_copy), call(ev_y, lo_copy), ev_lb, ev_wo, ev_wo_ready)):
                events[f'{e}{i}'] = [call(on, inner, call(f, *vs))]
        events['v0'] += [call(on, inner, lambda: local(xp.at[1 - side, pl.ds(0, 2)], wo_sem.at[4]))]
        for v in range(4):
            events[f'd{v}'] = [call(on, outer, lambda v=v: lb_z(v).start())]
        for h in HEADS:
            for z in TWO:
                events[f's{h}{z}'] = [kvr_copy(h, z).start]
            events[f'f{h}'] = [call(kv_forward, [h])]
            events[f'g{h}'] = [call(kv_wait, kvf_copy, [h])]
        for k in ROWS:
            for p in TWO:
                events['op'[p] + str(k)] = [call(send_o, (k,), p)]
        def run(names):
            for name in names.split(','):
                where, _, name = name.rpartition(':')
                if where:
                    on(inner if where == 'i' else outer, *events[name])
                else:
                    for c in events[name]:
                        c()

        @pl.when(event > 0)
        def _():
            choose(event - 1, [functools.partial(run, names) for names in EVENTS])
        return carry

    lax.fori_loop(0, len(TABLE), step_body, None)

    all_sent(lq_ref, 0)
    all_sent(lo_ref.at[:, 0, 0], 2)
    all_sent(lb_ref.at[:, 0], 3)
    all_sent(kvp_s, 4)
    all_sent(kvr_s.at[:, pl.ds(0, 2)], 5)
    all_sent(kvr_s.at[:, pl.ds(0, 2)], 6)

    @pl.when(outer)
    def _():
        all_sent(xb, 7)

    @pl.when(inner)
    def _():
        all_sent(lo_ref.at[:, pl.ds(0, 7)], 1)
        with scope('y_sent'):
            all_sent(xp.at[side, :, :, pl.ds(H, 3 * H)], 8)
        local(xp.at[side, :, :, pl.ds(0, H)], sent.at[9])

    for seg in TWO:
        @pl.when(tp != 1 + seg)
        def _(seg=seg):
            with scope(f'recv{seg}'):
                arrived(out_ref.at[seg], y_recv.at[seg])


PROGRAM = (
    'O.i:zk0,i:zk1,bv', 'O.o:zk0', 'O.o:zk1,s00,i:xk0', 'O.o:xk0,i:xk1,o:s01,d3,i:bq', 'O.o:bq,o:xk1,i:yk0,i:zv0', 'O.o:yk0,i:yk1,i:zv1,i:s01',
    'P.o:zv0,o:yk1,lk,o:zv1,d1,i:xv0', 'P.wk,i:xv1', 'K.ko', 'K.o:xv0,i:zq,f0', 'K.o:xv1,i:yv0,i:yv1,b0,b1,r0,po,g0,o:zq',
    'T0.o0,o1,d0,o:yv0,o:yv1,lv,mq0,i:mq1,i:fq0,i:fq1', 'P.wv,z0,o:mq1,b2', 'V.o:fq0,o:fq1,kp,o:s10,o:s11', 'V.c0,z1,o:s20,o:s21,yq0,yq1',
    'V.lq,m0,o:s30,o:s31', 'P.free,wq', 'Q.pp,r1,x0,c1,i:s10,i:s11,y0', 'T4.p0,p1,w0,m1,x1,v0', 'R.y1,w1,v1,i:s20,i:s21', 'L', 'Q.f1', 'R',
    'T5.p2,g1', 'L', 'T1.o2,p3,o3,o:f2', 'R.i:s30,i:s31', 'L', 'Q.o:g2', 'Q.i:f2,o:f3', 'T2', 'R.i:g2', 'L', 'T6.p4,o4,p5,o5,o:g3', 'R.i:f3,z2,c2',
    'L', 'T3.i:g3', 'T7.p6,o6,p7,o7', 'R', 'L.m2,x2', 'R.y2', 'L.w2', '-.v2', 'N', 'N', 'N', 'R', 'L', 'N', 'N', 'N', 'N', 'N',
)
KINDS = '-OPKVQABRLN'


def tables():
    table, seen = [], {}
    names = tuple(dict.fromkeys(s.partition('.')[2] for s in PROGRAM if '.' in s))
    for s in PROGRAM:
        name, _, after = s.partition('.')
        kind, n = name[0], seen.get(name[0], 0)
        seen[kind] = n + 1
        if kind == 'T':
            n = int(name[1:])
            kind = 'AB'[n in (2, 3, 4, 5)]
        table.append(KINDS.index(kind) + 16 * n + 256 * (names.index(after) + 1 if after else 0))
    return table, names


TABLE, EVENTS = tables()


def main(bias, x, wk, wv, wq, w_out):
    anyspec = pl.BlockSpec(memory_space=pl.ANY)
    vmem = [((4, B, M), BF), ((B, B), BF), ((2, 8, B, M), BF), ((3, M, H), BF), ((4, 8, B, B), BF), ((4, 12, 2, B, B), BF), ((4, 4, 2, B, B), BF), ((4, 4, 2, B, B), BF),
            ((3072, H), F32), ((M, H), F32), ((64, 128), F32)]
    dma = [(4,), (9,), (5,), (10,), (6, 5), (4, 5), (4, 2), (3, 4), (8, 4), (2,)]
    return pl.pallas_call(
        main_kernel,
        in_specs=[pl.BlockSpec(memory_space=pltpu.SMEM)] + [anyspec] * 5,
        out_specs=[anyspec] * 4,
        out_shape=[jax.ShapeDtypeStruct(s, BF) for s in ((2, 8, B, H), (8, 6, B, B), (4, 8, 2, 64, H), (4, 2, B, H))],
        scratch_shapes=[pltpu.VMEM(*v) for v in vmem] + [pltpu.SemaphoreType.DMA(d) for d in dma] + [pltpu.SemaphoreType.REGULAR((2,))],
        compiler_params=params(collective_id=0, has_side_effects=True),
        cost_estimate=pl.CostEstimate(flops=10**11, bytes_accessed=10**8, transcendentals=0),
        name='main',
    )(bias, x, wk, wv, wq, w_out)[0]


def solution(mesh):
    def device_fn(hidden, w_query, w_key, w_value, w_out, branch_bias):
        return unpermute(main(branch_bias, hidden, w_key, w_value, w_query, w_out))

    return jax.shard_map(device_fn, mesh=mesh, in_specs=(P(('dp', 'sp'), None), P(None, 'tp'), P(None, 'tp'), P(None, 'tp'), P('tp', None), P(None, None)), out_specs=P(('dp', 'sp'), 'tp'), check_vma=False)
```

```python
import functools
import math

import jax
import jax.numpy as jnp
from jax import lax
from jax.experimental import pallas as pl
from jax.experimental.pallas import tpu as pltpu
from jax.sharding import PartitionSpec as P

MESH = pl.DeviceIdType.MESH
BF = jnp.bfloat16
F32 = jnp.float32
B, H, M = 256, 512, 2048
KAPPA = math.log2(math.e) / 16
VMEM = 66_900_000
SLOT = (0, 4, 2, 6, 1, 5, 3, 7)
KEY, VAL, QUE = range(3)
HEADS = range(4)
TWO = range(2)
QUARTERS = range(4)
ROWS = range(8)


def nn(a, b):
    return lax.dot_general(a, b, (((1,), (0,)), ((), ())), preferred_element_type=F32)


def nt(a, b):
    return lax.dot_general(a, b, (((1,), (1,)), ((), ())), preferred_element_type=F32)


def params(**kw):
    return pltpu.CompilerParams(vmem_limit_bytes=VMEM, **kw)


def ds(start, size, align=128):
    return pl.ds(pl.multiple_of(start, align), size)


def part(i, size):
    return slice(i * size, i * size + size)


def phase_matrix(transposed):
    r = lax.broadcasted_iota(jnp.int32, (B, B), int(transposed))
    p = lax.broadcasted_iota(jnp.int32, (B, B), int(not transposed))
    k = r // 32
    return (p == (r % 32) * 8 + k // 2 + 4 * (k % 2)).astype(F32).astype(BF)


def unpermute_kernel(y_ref, o_ref, y_s, o_s, load, store):
    pieces = [(s, j) for s in TWO for j in range(4)]

    def get(i):
        s, j = pieces[i]
        return pltpu.make_async_copy(y_ref.at[s, :, pl.ds(j * 64, 64)], y_s.at[i], load.at[i])

    def put(i):
        return pltpu.make_async_copy(o_s.at[i], o_ref.at[pl.ds(i * H, H)], store.at[i])

    for i in ROWS:
        get(i).start()
    pm = phase_matrix(True)
    for i in range(0, 8, 2):
        group = (i, i + 1)
        for k in group:
            get(k).wait()
        for k in group:
            for j in TWO:
                o_s[k, part(j, B), :] = nn(pm, y_s[k, :, part(j, 32), :].reshape(B, H)).astype(BF)
        for k in group:
            put(k).start()
    for i in ROWS:
        put(i).wait()


def unpermute(y):
    anyspec = pl.BlockSpec(memory_space=pl.ANY)
    return pl.pallas_call(
        unpermute_kernel,
        in_specs=[anyspec],
        out_specs=anyspec,
        out_shape=jax.ShapeDtypeStruct((2 * M, H), BF),
        scratch_shapes=[pltpu.VMEM((8, 8, 64, H), BF), pltpu.VMEM((8, H, H), BF), pltpu.SemaphoreType.DMA((8,)), pltpu.SemaphoreType.DMA((8,))],
        compiler_params=params(),
        name='unpermute',
    )(y)


def tile_steps(q, wide, narrow, s_ref, n_ref, done):
    st = {}
    logits, sums = [], []

    def add(name, x):
        st[name] = st[name] + x if name in st else x

    for groups, ref in ((wide, s_ref), (narrow, n_ref)):
        off = 0
        for keys, parts in groups:
            def qk(keys=keys, parts=parts, off=off, ref=ref):
                s = nt(keys(), q() if ref is s_ref else q()[:B])
                o = 0
                for _, n, b in parts:
                    piece = s[o:o + n]
                    ref[pl.ds(off + o, n), :] = piece
                    t = jnp.max(piece, axis=0, keepdims=True) * KAPPA
                    if b is not None:
                        t = t + fit(b, t)
                    if ref is n_ref:
                        t = jnp.concatenate([t, st['top'][:, B:]], axis=1)
                    st['top'] = jnp.maximum(st['top'], t) if 'top' in st else t
                    o += n
            logits.append(qk)
            for v, n, b in parts:
                def sv(v=v, n=n, b=b, off=off, ref=ref):
                    top = st['top'] if ref is s_ref else st['top'][:, :B]
                    e = jnp.exp2(ref[pl.ds(off, n), :] * KAPPA - (top if b is None else top - fit(b, top)))
                    name = 'w' if ref is s_ref else 'n'
                    add('l' + name, jnp.sum(e, axis=0, keepdims=True))
                    add('o' + name, nn(v(), e.astype(BF)))
                sums.append(sv)
                off += n

    def finish():
        o, l = st['ow'], st['lw']
        if narrow:
            o = jnp.concatenate([o[:, :B] + st['on'], o[:, B:]], axis=1)
            l = jnp.concatenate([l[:, :B] + st['ln'], l[:, B:]], axis=1)
        done(o / l)

    return logits, sums + [finish]


def fit(b, like):
    return b if b.shape == like.shape else jnp.concatenate([b] * (like.shape[1] // 128), axis=1)


def interleave(a, b):
    i = j = 0
    while i < len(a) or j < len(b):
        if j >= len(b) or (i < len(a) and i * len(b) <= j * len(a)):
            a[i]()
            i += 1
        else:
            b[j]()
            j += 1


def run_tiles(tiles):
    before = []
    for logits, sums in tiles:
        interleave(logits, before)
        before = sums
    interleave([], before)


def choose(x, cases):
    def among(lo, hi):
        mid = (lo + hi) // 2
        if hi - lo == 1:
            cases[lo]()
        else:
            pl.when(x < mid)(lambda: among(lo, mid))
            pl.when(x >= mid)(lambda: among(mid, hi))
    among(0, len(cases))


def on(cond, *calls):
    @pl.when(cond)
    def _():
        for c in calls:
            c()


def scope(name):
    return jax.named_scope(name)


def main_kernel(bias_ref, x_ref, wk_ref, wv_ref, wq_ref, wout_ref, out_ref, lq_ref, lo_ref, lb_ref,
                xb, pm, xp, ws, q_s, kv_s, kvp_s, kvr_s, s_scr, t_scr,
                beta_s, x_sem, w_sem, wo_sem, sent, lq_recv, lo_recv, lb_recv, kv_recv, o_recv, y_recv, ready):
    dp, tp, sp = lax.axis_index('dp'), lax.axis_index('tp'), lax.axis_index('sp')
    idx = dp * 4 + sp
    side = tp // 2
    inner = (tp == 1) | (tp == 2)
    outer = jnp.logical_not(inner)
    W = (wk_ref, wv_ref, wq_ref)
    peer_x, peer_y, peer_c = {'dp': dp ^ 1}, {'sp': sp ^ 2}, {'sp': sp ^ 1}

    def remote(src, dst, ss, rs, dev):
        return pltpu.make_async_remote_copy(src_ref=src, dst_ref=dst, send_sem=ss, recv_sem=rs, device_id=dev, device_id_type=MESH)

    def lq_copy(t, src, dst, dev):
        return remote(lq_ref.at[src, t], lq_ref.at[dst, t], sent.at[0], lq_recv.at[t, min(dst, 4)], dev)

    def lq_z(t):
        return remote(W[t // 2].at[ds(idx * B, B), pl.ds(t % 2 * B, B)], lq_ref.at[0, t], sent.at[0], lq_recv.at[t, 0], {'tp': tp ^ 2})

    def lq_start(t):
        for i in TWO:
            lq_z(2 * t + i).start()

    def lo_copy(v, src, dst, dev):
        return remote(lo_ref.at[v, src], lo_ref.at[v, dst], sent.at[1], lo_recv.at[v, min(dst, 4)], dev)

    def lo_z(v):
        dst = 2 - side
        b = (tp ^ dst) - 2
        return remote(wout_ref.at[ds(idx * 64, 64, 64), ds((dst ^ v) * H, H)], lo_ref.at[v, 0, b], sent.at[2], lo_recv.at[v, 0], {'tp': dst})

    def lb_z(v):
        return remote(wout_ref.at[ds(sp % 2 * B, B), ds((tp ^ 1 ^ v) * H, H)], lb_ref.at[v, sp % 2], sent.at[3], lb_recv.at[v, 0], {'tp': tp ^ 1})

    def lb_core(v):
        return remote(lb_ref.at[v, sp % 2], lb_ref.at[v, sp % 2], sent.at[3], lb_recv.at[v, 1], peer_c)

    def lo_start(*vs):
        for v in vs:
            lo_z(v).start()

    def arrived(ref, sem):
        remote(ref, ref, sent.at[0], sem, peer_c).wait_recv()

    def all_sent(ref, i):
        remote(ref, ref, sent.at[i], sent.at[i], peer_c).wait_send()

    def lo_zwait(v):
        arrived(lo_ref.at[v, 0], lo_recv.at[v, 0])

    def hop(copy, p, i):
        near, far, n = (peer_x, peer_y, 1) if (copy is lo_copy and p == 2) or (copy is lq_copy and p == 5) else (peer_y, peer_x, 2)
        f = 3 - n
        return copy(p, *((0, n, near), (0, f, far), (0, 4, peer_c), (n, 3, far), (n, 4 + n, peer_c), (f, 4 + f, peer_c), (3, 7, peer_c))[i])

    def ev_z(copy, *ps):
        for p in ps:
            with scope(f'z_{copy.__name__}{p}'):
                lq_z(p).wait_recv() if copy is lq_copy else lo_zwait(p)
            hop(copy, p, 0).start()
        for p in ps:
            hop(copy, p, 1).start()
            hop(copy, p, 2).start()

    def ev_near(copy, *ps):
        for p in ps:
            with scope(f'n_{copy.__name__}{p}'):
                hop(copy, p, 0).wait_recv()
            hop(copy, p, 3).start()
            hop(copy, p, 4).start()

    def ev_far(copy, *ps):
        for p in ps:
            with scope(f'f_{copy.__name__}{p}'):
                hop(copy, p, 1).wait_recv()
            hop(copy, p, 5).start()

    def ev_xy(copy, *ps):
        ev_near(copy, *ps)
        ev_far(copy, *ps)

    def ev_y(copy, *ps):
        for p in ps:
            with scope(f'y_{copy.__name__}{p}'):
                hop(copy, p, 3).wait_recv()
            hop(copy, p, 6).start()
            if copy is lq_copy and p >= 2:
                start(w_load(p, SLOT[:4]))

    def ev_done(copy, *ps):
        for p in ps:
            with scope(f'c_{copy.__name__}{p}'):
                if copy is lq_copy:
                    arrived(lq_ref.at[pl.ds(4, 4), p], lq_recv.at[p, 4])
                else:
                    arrived(lo_ref.at[p, pl.ds(4, 4)], lo_recv.at[p, 4])

    def w_load(p, slots):
        return [pltpu.make_async_copy(lq_ref.at[SLOT.index(m), p], ws.at[p // 2 % 2, ds((idx ^ m) * B, B), pl.ds(p % 2 * B, B)], w_sem.at[p]) for m in slots]

    def own_load(t):
        return pltpu.make_async_copy(W[t], ws.at[t], w_sem.at[6 + t])

    def start(copies):
        for c in copies:
            c.start()

    def wait(copies):
        for c in copies:
            c.wait()

    def ev_last(t):
        pieces = [2 * t + i for i in TWO]
        ev_done(lq_copy, *pieces)
        for p in pieces:
            start(w_load(p, SLOT[4:] if t else SLOT))

    def local(ref, sem):
        pltpu.make_async_copy(ref, ref, sem).wait()

    def ev_weights(t):
        with scope(f'load{t}'):
            for i in TWO:
                local(ws.at[t % 2, :, pl.ds(i * B, B)], w_sem.at[2 * t + i])

    def ev_wo(*vs):
        ev_done(lo_copy, *vs)
        for v in vs:
            lb_core(v).wait_recv()
        start(wo_load(*vs))

    def ev_wo_ready(*vs):
        with scope(f'wo{vs[0]}'):
            for v in vs:
                local(xp.at[1 - side, pl.ds(2, 6), :, pl.ds((v ^ 2) * H, H)], wo_sem.at[v])

    def ev_lb(*vs):
        for v in vs:
            with scope(f'lb{v}'):
                lb_z(v).wait_recv()
            lb_core(v).start()

    wo = xp.at[1 - side]

    def wo_own():
        return [pltpu.make_async_copy(wout_ref.at[pl.ds(r * B, B), pl.ds(c * H, H)], xp.at[1 - side, r, :, ds((c ^ tp ^ 2) * H, H)], wo_sem.at[4])
                for r in TWO for c in range(4)]

    def wo_load(*vs):
        out = []
        for v in vs:
            cols = pl.ds((v ^ 2) * H, H)
            for s, m in enumerate(SLOT):
                row = (idx ^ m) * 64
                for b in TWO:
                    out.append(pltpu.make_async_copy(lo_ref.at[v, s, b], xp.at[1 - side, 4 + 2 * b + row // B, ds(row % B, 64, 64), cols], wo_sem.at[v]))
            for r in TWO:
                out.append(pltpu.make_async_copy(lb_ref.at[v, r], xp.at[1 - side, 2 + r, :, cols], wo_sem.at[v]))
        return out

    def kvp_copy(h, s):
        return remote(kv_s.at[h, pl.ds(8 * s, 2)], kvp_s.at[h, pl.ds(2 * s, 2)], sent.at[4], kv_recv.at[0, h], peer_c)

    def kvr_copy(h, s):
        return remote(kv_s.at[h, 8 * s], kvr_s.at[h, s], sent.at[5], kv_recv.at[1, h], peer_y)

    def kvf_copy(h, s):
        return remote(kvr_s.at[h, s], kvr_s.at[h, 2 + s], sent.at[6], kv_recv.at[2, h], peer_c)

    def kv_start(copy, heads):
        for h in heads:
            for s in TWO:
                copy(h, s).start()

    def kv_wait(copy, heads):
        with scope(f'w_{copy.__name__}{heads[0]}'):
            for h in heads:
                i = (kvp_copy, kvr_copy, kvf_copy).index(copy)
                arrived((kvp_s.at[h], kvr_s.at[h, pl.ds(0, 2)], kvr_s.at[h, pl.ds(2, 2)])[i], kv_recv.at[i, h])

    def kv_forward(heads):
        kv_wait(kvr_copy, heads)
        kv_start(kvf_copy, heads)

    def reverse(i):
        return (i % 2) * 2 + i // 2

    def order(n):
        return 2 * reverse(n % 4) + ((n // 4) ^ side)

    def o_at(k, p, theirs, col, size, row=0, rows=B):
        if p:
            return ws.at[1 + theirs, ds(k * B + row, rows, 64), ds(col, size)]
        return xb.at[k // 2, pl.ds(row, rows), ds((k % 2) * 1024 + theirs * H + col, size)]

    def o_copy(k, p, q):
        row = q * 64
        return remote(o_at(k, p, 0, 0, H, row, 64), o_at(k, p, 1, 0, H, row, 64), sent.at[7], o_recv.at[k, q], {'tp': tp ^ 1})

    def o_times(k, v, n, row=0, rows=B):
        cols = pl.ds((v ^ 2) * H, n * H)
        y = nn(xb[k // 2, pl.ds(row, rows), ds((k % 2) * 1024, 1024)], wo[0:4, :, cols].reshape(1024, n * H))
        for i in TWO:
            y = y + nn(ws[1 + i, ds(k * B + row, rows, 64), :], wo[part(2 + i, 2), :, cols].reshape(H, n * H))
        y = y.astype(BF)
        for i in range(n):
            y_src(k, v + i, row, rows)[...] = y[:, part(i, H)]
            y_copy(k, v + i, side, row, rows).start() if v else y_local(k).start()

    def y_src(k, v, row=0, rows=B):
        return xp.at[side, k, pl.ds(row, rows), pl.ds(v * H, H)]

    def y_copy(k, v, seg, row, rows):
        return remote(y_src(k, v, row, rows), out_ref.at[seg, k, pl.ds(row, rows)], sent.at[8], y_recv.at[seg], {'tp': tp ^ v})

    def y_local(k):
        return pltpu.make_async_copy(y_src(k, 0), out_ref.at[side, k], sent.at[9])

    def x_copy(j):
        return pltpu.make_async_copy(x_ref.at[ds(j * B, B), :], xb.at[lax.rem(j, 4)], x_sem.at[lax.rem(j, 4)])

    for j in range(4):
        x_copy(j).start()
    barrier = pltpu.get_barrier_semaphore()
    peers = [{'tp': tp ^ 1}, {'tp': tp ^ 2}, {'tp': tp ^ 3}, peer_x, peer_y, peer_c]
    for dev in peers:
        pl.semaphore_signal(barrier, inc=1, device_id=dev, device_id_type=MESH)
    for t in range(3):
        own_load(t).start()

    pm[...] = phase_matrix(False)

    def permute_body(j, carry):
        x_copy(j).wait()
        y = nn(pm[...], xb[lax.rem(j, 4)]).astype(BF).reshape(8, 32, M)
        xp[j // 8, :, ds(lax.rem(j, 8) * 32, 32, 32), :] = y
        pl.when(j < 12)(lambda: x_copy(j + 4).start())

        @pl.when(j == 2)
        def _():
            with scope('barrier'):
                pl.semaphore_wait(barrier, len(peers))
            lq_start(KEY)
            on(outer, lb_z(2).start)
        return carry

    with scope('permute'):
        lax.fori_loop(0, 16, permute_body, None)

    for h in HEADS:
        column = 2 * (tp ^ (h // 2 * 2)) + h % 2
        for i, branches in enumerate(('0', '01', '1', '012', '12', '2', '0123', '123', '23', '3')):
            rows = [jnp.full((1, 128), bias_ref[j, column], F32) for j in map(int, branches)]
            m = functools.reduce(jnp.maximum, rows)
            beta_s[pl.ds(h * 16 + i, 1), :] = (m + jnp.log(sum(jnp.exp(r - m) for r in rows))) * math.log2(math.e)

    def signal_ready(i):
        pl.when(inner)(lambda: pl.semaphore_signal(ready.at[i], inc=1, device_id={'tp': tp ^ 1}, device_id_type=MESH))

    def wait_ready(i):
        with scope(f'ready{i}'):
            pl.when(outer)(lambda: pl.semaphore_wait(ready.at[i], 1))

    signal_ready(0)

    def group(g):
        low = g < 4
        return jnp.where(low, g & 1, 0), jnp.where(low, g // 2, g - 2)

    def head_number(h):
        return 2 * (tp ^ (h // 2 * 2)) + h % 2

    def project(heads, sigma, pair, kinds):
        for h in heads:
            t = head_number(h) + reverse(pair)
            x, swap = xp[side ^ sigma, pl.ds(2 * (t & 3), 2)].reshape(H, M), (t & 7) >> 2
            for t in kinds:
                y = nn(x, ws[t, :, part(h % 2, B)])
                for j in TWO:
                    piece = y[part(j, B)]
                    kv_s[h, 8 * sigma + 2 * pair + (j ^ swap), t] = (piece.T if t == VAL else piece).astype(BF)

    def phases_of(j):
        return [j % 2 + 2 * i for i in TWO], (j // 2) ^ side

    def rank_of(phase, h):
        rel = (phase - head_number(h)) & 7
        return (rel & 1) * 4 + ((rel >> 1) & 1) * 2 + (rel >> 2)

    def queries(heads, w, j):
        phases, half = phases_of(j)
        x = jnp.concatenate([xp[side, 2 * f + half] for f in phases])
        for h in heads:
            y = nn(x, ws[w, :, part(h % 2, B)]).astype(BF)
            for i, f in enumerate(phases):
                q_s[h, rank_of(f + 4 * half, h)] = y[part(i, B)]

    with scope('own_w'):
        for t in range(3):
            own_load(t).wait()
    own, partner = HEADS[:2], HEADS[2:]

    def mix(b, c):
        return jnp.concatenate([b, b, c, c], axis=1)

    def keys_of(ref, h, i, weights):
        parts = []
        n = 0
        for count, b in weights:
            def values(i=i + n, count=count):
                v = [ref[h, i + j, VAL] for j in range(count)]
                return v[0] if count == 1 else jnp.concatenate(v, axis=1)
            parts.append((values, count * B, b))
            n += count
        return (lambda: ref[h, i:i + n, KEY].reshape(n * B, B)), parts

    def chunk_tiles(p, j, kind):
        both_phases, half = phases_of(j)

        def put(h, phase, ot):
            k = 2 * (phase & 3) + half
            y = ot.T.astype(BF)
            for i in TWO:
                pl.when(p == i)(lambda i=i: o_at(k, i, 0, (h % 2) * B, B).__setitem__(..., y))

        def tile(h, phases, ranks, wide, narrow, s_ref, n_ref):
            def done(ot):
                for i, phase in enumerate(phases):
                    put(h, phase, ot[:, part(i, B)])
            return tile_steps(lambda: jnp.concatenate([q_s[h, r] for r in ranks]), wide, narrow, s_ref, n_ref, done)

        h = 2 * p + (j % 2) ^ 1
        rest = tile(h, both_phases, [rank_of(f + 4 * half, h) for f in both_phases], [keys_of(kv_s, h, i, [(1, None)]) for i in ROWS], [], t_scr, None)
        h = 2 * p + (j % 2)
        a = head_number(h)
        b0, b01, b1, b012, b12, b2, b0123, b123, b23, b3 = [beta_s[pl.ds(h * 16 + i, 1), :] for i in range(10)]
        phases = [a & 3, (a & 3) ^ 2]
        both = [keys_of(kv_s, h, i, [(2, b)] * n) for i, b, n in ((2, b01, 1), (4, b0, 2), (10, b1, 1))]
        if kind == 0:
            both += [keys_of(kv_s, h, 0, [(1, mix(b0123, b01)), (1, mix(b012, b01))]), keys_of(kv_s, h, 8, [(1, mix(b123, b1)), (1, mix(b12, b1))])]
            first = [keys_of(kvp_s, h, i, [(1, b23), (1, b2)]) for i in (0, 2)] + [keys_of(kvr_s, h, i, [(2, b3)]) for i in (0, 2)]
        else:
            both += [keys_of(kv_s, h, 0, [(2, mix(b012, b01))]), keys_of(kv_s, h, 8, [(2, mix(b12, b1))])]
            first = [keys_of(kvp_s, h, i, [(2, b2)]) for i in (0, 2)]
        with scope(f'tile{kind}'):
            run_tiles([rest, tile(h, phases, [kind, rank_of(phases[1] + 4 * half, h)], both, first, s_scr, t_scr.at[:, pl.ds(0, B)])])

    def send_o(ks, p):
        @pl.when(outer)
        def _():
            for k in ks:
                for q in QUARTERS:
                    o_copy(order(k), p, q).start()

    def step_body(t, carry):
        packed = functools.reduce(lambda x, i: jnp.where(t == i, TABLE[i], x), range(len(TABLE)), 0)
        code, n, event = packed % 16, packed // 16 % 16, packed // 256

        def step_o():
            with scope('own_kv'):
                project(own, *group(n), (KEY, VAL))

        def step_kv(t_):
            with scope(f'par_{t_}'):
                for i in TWO:
                    project(partner, *group(2 * n + i), (t_,))

        def step_q(heads, w):
            with scope(f'que_{w}'):
                queries(heads, w, n)

        def step_out(v, m):
            @pl.when(inner)
            def _():
                k = order(n)

                def wait_for(q):
                    arrived(ws.at[0, pl.ds(0, 128), :], o_recv.at[k, q])

                def quarters():
                    for q in QUARTERS:
                        with scope(f'wait_q{q}'):
                            wait_for(q)
                        o_times(k, v, m, q * 64, 64)

                def whole():
                    with scope('wait_o'):
                        for q in QUARTERS:
                            wait_for(q)
                    with scope(f'out{v}'):
                        o_times(k, v, m)

                if m == 2:
                    pl.when(n == 0)(quarters)
                    pl.when(n > 0)(whole)
                else:
                    with scope(f'out{v}'):
                        o_times(k, v, m)

        f = functools.partial
        kinds = {'-': lambda: None, 'O': step_o, 'P': f(step_q, own, QUE), 'K': f(step_kv, KEY), 'V': f(step_kv, VAL), 'Q': f(step_q, partner, KEY),
                 'A': lambda: chunk_tiles(n // 4, n % 4, 0), 'B': lambda: chunk_tiles(n // 4, n % 4, 1), 'R': f(step_out, 2, 2), 'L': f(step_out, 1, 1), 'N': f(step_out, 0, 1)}
        choose(code, [kinds[c] for c in KINDS])
        call = functools.partial

        events = {
            'free': [call(signal_ready, 1), call(on, inner, lambda: start(wo_own()))],
            'r0': [call(wait_ready, 0)],
            'r1': [call(wait_ready, 1)],
            'ko': [call(kv_start, kvp_copy, own)],
            'po': [call(kv_wait, kvp_copy, own)],
            'kp': [call(kv_start, kvp_copy, partner)],
            'pp': [call(kv_wait, kvp_copy, partner)],
        }
        for t_, c in enumerate('kvq'):
            events['b' + c] = [call(lq_start, t_)]
            events['l' + c] = [call(ev_last, t_)]
            events['w' + c] = [call(ev_weights, t_)]
            events['z' + c] = [call(ev_z, lq_copy, 2 * t_, 2 * t_ + 1)]
            for i in TWO:
                for e, f in zip('zmfxy', (ev_z, ev_near, ev_far, ev_xy, ev_y)):
                    events[f'{e}{c}{i}'] = [call(f, lq_copy, 2 * t_ + i)]
        for i, vs in enumerate(((2, 3), (1,), (0,))):
            events[f'b{i}'] = [call(lo_start, *vs)]
            for e, f in zip('zmxycwv', (call(ev_z, lo_copy), call(ev_near, lo_copy), call(ev_far, lo_copy), call(ev_y, lo_copy), ev_lb, ev_wo, ev_wo_ready)):
                events[f'{e}{i}'] = [call(on, inner, call(f, *vs))]
        events['v0'] += [call(on, inner, lambda: local(xp.at[1 - side, pl.ds(0, 2)], wo_sem.at[4]))]
        for v in range(4):
            events[f'd{v}'] = [call(on, outer, lambda v=v: lb_z(v).start())]
        for h in HEADS:
            for z in TWO:
                events[f's{h}{z}'] = [kvr_copy(h, z).start]
            events[f'f{h}'] = [call(kv_forward, [h])]
            events[f'g{h}'] = [call(kv_wait, kvf_copy, [h])]
        for k in ROWS:
            for p in TWO:
                events['op'[p] + str(k)] = [call(send_o, (k,), p)]
        def run(names):
            for name in names.split(','):
                where, _, name = name.rpartition(':')
                if where:
                    on(inner if where == 'i' else outer, *events[name])
                else:
                    for c in events[name]:
                        c()

        @pl.when(event > 0)
        def _():
            choose(event - 1, [functools.partial(run, names) for names in EVENTS])
        return carry

    lax.fori_loop(0, len(TABLE), step_body, None)

    all_sent(lq_ref, 0)
    all_sent(lo_ref.at[:, 0, 0], 2)
    all_sent(lb_ref.at[:, 0], 3)
    all_sent(kvp_s, 4)
    all_sent(kvr_s.at[:, pl.ds(0, 2)], 5)
    all_sent(kvr_s.at[:, pl.ds(0, 2)], 6)

    @pl.when(outer)
    def _():
        all_sent(xb, 7)

    @pl.when(inner)
    def _():
        all_sent(lo_ref.at[:, pl.ds(0, 7)], 1)
        with scope('y_sent'):
            all_sent(xp.at[side, :, :, pl.ds(H, 3 * H)], 8)
        local(xp.at[side, :, :, pl.ds(0, H)], sent.at[9])

    for seg in TWO:
        @pl.when(tp != 1 + seg)
        def _(seg=seg):
            with scope(f'recv{seg}'):
                arrived(out_ref.at[seg], y_recv.at[seg])


PROGRAM = (
    'O.i:zk0,i:zk1,bv', 'O.o:zk0', 'O.o:zk1,s00,i:xk0', 'O.o:xk0,i:xk1,o:s01,d3,i:bq', 'O.o:bq,o:xk1,i:yk0,i:zv0', 'O.o:yk0,i:yk1,i:zv1,i:s01',
    'P.o:zv0,o:yk1,lk,o:zv1,d1,i:xv0', 'P.wk,i:xv1', 'K.ko', 'K.o:xv0,i:zq,f0', 'K.o:xv1,i:yv0,i:yv1,b0,b1,r0,po,g0,o:zq',
    'T0.o0,o1,d0,o:yv0,o:yv1,lv,mq0,i:mq1,i:fq0,i:fq1', 'P.wv,o:mq1,b2', 'V.z0,o:fq0,o:fq1,kp,o:s10,o:s11', 'V.c0,z1,o:s20,o:s21,yq0,yq1',
    'V.lq,o:s30,o:s31', 'P.free,wq,m0', 'Q.pp,r1,x0,c1,i:s10,i:s11', 'T4.p0,p1,y0,w0,m1,x1,v0', 'R.y1,w1,v1,i:s20,i:s21', 'L', 'Q.f1', 'R',
    'T5.p2,g1', 'L', 'T1.o2,p3,o3,o:f2', 'R.i:s30,i:s31', 'L', 'Q.o:g2', 'Q.i:f2,o:f3', 'T2', 'R.i:g2', 'L', 'T6.p4,o4,p5,o5,o:g3', 'R.i:f3,z2,c2',
    'L', 'T3.i:g3', 'T7.p6,o6,p7,o7', 'R', 'L.m2,x2', 'R.y2', 'L.w2', '-.v2', 'N', 'N', 'N', 'R', 'L', 'N', 'N', 'N', 'N', 'N',
)
KINDS = '-OPKVQABRLN'


def tables():
    table, seen = [], {}
    names = tuple(dict.fromkeys(s.partition('.')[2] for s in PROGRAM if '.' in s))
    for s in PROGRAM:
        name, _, after = s.partition('.')
        kind, n = name[0], seen.get(name[0], 0)
        seen[kind] = n + 1
        if kind == 'T':
            n = int(name[1:])
            kind = 'AB'[n in (2, 3, 4, 5)]
        table.append(KINDS.index(kind) + 16 * n + 256 * (names.index(after) + 1 if after else 0))
    return table, names


TABLE, EVENTS = tables()


def main(bias, x, wk, wv, wq, w_out):
    anyspec = pl.BlockSpec(memory_space=pl.ANY)
    vmem = [((4, B, M), BF), ((B, B), BF), ((2, 8, B, M), BF), ((3, M, H), BF), ((4, 8, B, B), BF), ((4, 12, 2, B, B), BF), ((4, 4, 2, B, B), BF), ((4, 4, 2, B, B), BF),
            ((3072, H), F32), ((M, H), F32), ((64, 128), F32)]
    dma = [(4,), (9,), (5,), (10,), (6, 5), (4, 5), (4, 2), (3, 4), (8, 4), (2,)]
    return pl.pallas_call(
        main_kernel,
        in_specs=[pl.BlockSpec(memory_space=pltpu.SMEM)] + [anyspec] * 5,
        out_specs=[anyspec] * 4,
        out_shape=[jax.ShapeDtypeStruct(s, BF) for s in ((2, 8, B, H), (8, 6, B, B), (4, 8, 2, 64, H), (4, 2, B, H))],
        scratch_shapes=[pltpu.VMEM(*v) for v in vmem] + [pltpu.SemaphoreType.DMA(d) for d in dma] + [pltpu.SemaphoreType.REGULAR((2,))],
        compiler_params=params(collective_id=0, has_side_effects=True),
        cost_estimate=pl.CostEstimate(flops=10**11, bytes_accessed=10**8, transcendentals=0),
        name='main',
    )(bias, x, wk, wv, wq, w_out)[0]


def solution(mesh):
    def device_fn(hidden, w_query, w_key, w_value, w_out, branch_bias):
        return unpermute(main(branch_bias, hidden, w_key, w_value, w_query, w_out))

    return jax.shard_map(device_fn, mesh=mesh, in_specs=(P(('dp', 'sp'), None), P(None, 'tp'), P(None, 'tp'), P(None, 'tp'), P('tp', None), P(None, None)), out_specs=P(('dp', 'sp'), 'tp'), check_vma=False)
```

```python
import functools
import math

import jax
import jax.numpy as jnp
from jax import lax
from jax.experimental import pallas as pl
from jax.experimental.pallas import tpu as pltpu
from jax.sharding import PartitionSpec as P

MESH = pl.DeviceIdType.MESH
BF = jnp.bfloat16
F32 = jnp.float32
B, H, M = 256, 512, 2048
KAPPA = math.log2(math.e) / 16
VMEM = 66_900_000
SLOT = (0, 4, 2, 6, 1, 5, 3, 7)
KEY, VAL, QUE = range(3)
HEADS = range(4)
TWO = range(2)
QUARTERS = range(4)
ROWS = range(8)


def nn(a, b):
    return lax.dot_general(a, b, (((1,), (0,)), ((), ())), preferred_element_type=F32)


def nt(a, b):
    return lax.dot_general(a, b, (((1,), (1,)), ((), ())), preferred_element_type=F32)


def params(**kw):
    return pltpu.CompilerParams(vmem_limit_bytes=VMEM, **kw)


def ds(start, size, align=128):
    return pl.ds(pl.multiple_of(start, align), size)


def part(i, size):
    return slice(i * size, i * size + size)


def phase_matrix(transposed):
    r = lax.broadcasted_iota(jnp.int32, (B, B), int(transposed))
    p = lax.broadcasted_iota(jnp.int32, (B, B), int(not transposed))
    k = r // 32
    return (p == (r % 32) * 8 + k // 2 + 4 * (k % 2)).astype(F32).astype(BF)


def unpermute_kernel(y_ref, o_ref, y_s, o_s, load, store):
    pieces = [(s, j) for s in TWO for j in range(4)]

    def get(i):
        s, j = pieces[i]
        return pltpu.make_async_copy(y_ref.at[s, :, pl.ds(j * 64, 64)], y_s.at[i], load.at[i])

    def put(i):
        return pltpu.make_async_copy(o_s.at[i], o_ref.at[pl.ds(i * H, H)], store.at[i])

    for i in ROWS:
        get(i).start()
    pm = phase_matrix(True)
    for i in range(0, 8, 2):
        group = (i, i + 1)
        for k in group:
            get(k).wait()
        for k in group:
            for j in TWO:
                o_s[k, part(j, B), :] = nn(pm, y_s[k, :, part(j, 32), :].reshape(B, H)).astype(BF)
        for k in group:
            put(k).start()
    for i in ROWS:
        put(i).wait()


def unpermute(y):
    anyspec = pl.BlockSpec(memory_space=pl.ANY)
    return pl.pallas_call(
        unpermute_kernel,
        in_specs=[anyspec],
        out_specs=anyspec,
        out_shape=jax.ShapeDtypeStruct((2 * M, H), BF),
        scratch_shapes=[pltpu.VMEM((8, 8, 64, H), BF), pltpu.VMEM((8, H, H), BF), pltpu.SemaphoreType.DMA((8,)), pltpu.SemaphoreType.DMA((8,))],
        compiler_params=params(),
        name='unpermute',
    )(y)


def tile_steps(q, wide, narrow, s_ref, n_ref, done):
    st = {}
    logits, sums = [], []

    def add(name, x):
        st[name] = st[name] + x if name in st else x

    for groups, ref in ((wide, s_ref), (narrow, n_ref)):
        off = 0
        for keys, parts in groups:
            def qk(keys=keys, parts=parts, off=off, ref=ref):
                s = nt(keys(), q() if ref is s_ref else q()[:B])
                o = 0
                for _, n, b in parts:
                    piece = s[o:o + n]
                    ref[pl.ds(off + o, n), :] = piece
                    t = jnp.max(piece, axis=0, keepdims=True) * KAPPA
                    if b is not None:
                        t = t + fit(b, t)
                    if ref is n_ref:
                        t = jnp.concatenate([t, st['top'][:, B:]], axis=1)
                    st['top'] = jnp.maximum(st['top'], t) if 'top' in st else t
                    o += n
            logits.append(qk)
            for v, n, b in parts:
                def sv(v=v, n=n, b=b, off=off, ref=ref):
                    top = st['top'] if ref is s_ref else st['top'][:, :B]
                    e = jnp.exp2(ref[pl.ds(off, n), :] * KAPPA - (top if b is None else top - fit(b, top)))
                    name = 'w' if ref is s_ref else 'n'
                    add('l' + name, jnp.sum(e, axis=0, keepdims=True))
                    add('o' + name, nn(v(), e.astype(BF)))
                sums.append(sv)
                off += n

    def finish():
        o, l = st['ow'], st['lw']
        if narrow:
            o = jnp.concatenate([o[:, :B] + st['on'], o[:, B:]], axis=1)
            l = jnp.concatenate([l[:, :B] + st['ln'], l[:, B:]], axis=1)
        done(o / l)

    return logits, sums + [finish]


def fit(b, like):
    return b if b.shape == like.shape else jnp.concatenate([b] * (like.shape[1] // 128), axis=1)


def interleave(a, b):
    i = j = 0
    while i < len(a) or j < len(b):
        if j >= len(b) or (i < len(a) and i * len(b) <= j * len(a)):
            a[i]()
            i += 1
        else:
            b[j]()
            j += 1


def run_tiles(tiles):
    before = []
    for logits, sums in tiles:
        interleave(logits, before)
        before = sums
    interleave([], before)


def choose(x, cases):
    def among(lo, hi):
        mid = (lo + hi) // 2
        if hi - lo == 1:
            cases[lo]()
        else:
            pl.when(x < mid)(lambda: among(lo, mid))
            pl.when(x >= mid)(lambda: among(mid, hi))
    among(0, len(cases))


def on(cond, *calls):
    @pl.when(cond)
    def _():
        for c in calls:
            c()


def scope(name):
    return jax.named_scope(name)


def main_kernel(bias_ref, x_ref, wk_ref, wv_ref, wq_ref, wout_ref, out_ref, lq_ref, lo_ref, lb_ref,
                xb, pm, xp, ws, q_s, kv_s, kvp_s, kvr_s, s_scr, t_scr,
                beta_s, x_sem, w_sem, wo_sem, sent, lq_recv, lo_recv, lb_recv, kv_recv, o_recv, y_recv, ready):
    dp, tp, sp = lax.axis_index('dp'), lax.axis_index('tp'), lax.axis_index('sp')
    idx = dp * 4 + sp
    side = tp // 2
    inner = (tp == 1) | (tp == 2)
    outer = jnp.logical_not(inner)
    W = (wk_ref, wv_ref, wq_ref)
    peer_x, peer_y, peer_c = {'dp': dp ^ 1}, {'sp': sp ^ 2}, {'sp': sp ^ 1}

    def remote(src, dst, ss, rs, dev):
        return pltpu.make_async_remote_copy(src_ref=src, dst_ref=dst, send_sem=ss, recv_sem=rs, device_id=dev, device_id_type=MESH)

    def lq_copy(t, src, dst, dev):
        return remote(lq_ref.at[src, t], lq_ref.at[dst, t], sent.at[0], lq_recv.at[t, min(dst, 4)], dev)

    def lq_z(t):
        return remote(W[t // 2].at[ds(idx * B, B), pl.ds(t % 2 * B, B)], lq_ref.at[0, t], sent.at[0], lq_recv.at[t, 0], {'tp': tp ^ 2})

    def lq_start(t):
        for i in TWO:
            lq_z(2 * t + i).start()

    def lo_copy(v, src, dst, dev):
        return remote(lo_ref.at[v, src], lo_ref.at[v, dst], sent.at[1], lo_recv.at[v, min(dst, 4)], dev)

    def lo_z(v):
        dst = 2 - side
        b = (tp ^ dst) - 2
        return remote(wout_ref.at[ds(idx * 64, 64, 64), ds((dst ^ v) * H, H)], lo_ref.at[v, 0, b], sent.at[2], lo_recv.at[v, 0], {'tp': dst})

    def lb_z(v):
        return remote(wout_ref.at[ds(sp % 2 * B, B), ds((tp ^ 1 ^ v) * H, H)], lb_ref.at[v, sp % 2], sent.at[3], lb_recv.at[v, 0], {'tp': tp ^ 1})

    def lb_core(v):
        return remote(lb_ref.at[v, sp % 2], lb_ref.at[v, sp % 2], sent.at[3], lb_recv.at[v, 1], peer_c)

    def lo_start(*vs):
        for v in vs:
            lo_z(v).start()

    def arrived(ref, sem):
        remote(ref, ref, sent.at[0], sem, peer_c).wait_recv()

    def all_sent(ref, i):
        remote(ref, ref, sent.at[i], sent.at[i], peer_c).wait_send()

    def lo_zwait(v):
        arrived(lo_ref.at[v, 0], lo_recv.at[v, 0])

    def hop(copy, p, i):
        near, far, n = (peer_x, peer_y, 1) if (copy is lo_copy and p == 2) or (copy is lq_copy and p == 5) else (peer_y, peer_x, 2)
        f = 3 - n
        return copy(p, *((0, n, near), (0, f, far), (0, 4, peer_c), (n, 3, far), (n, 4 + n, peer_c), (f, 4 + f, peer_c), (3, 7, peer_c))[i])

    def ev_z(copy, *ps):
        for p in ps:
            with scope(f'z_{copy.__name__}{p}'):
                lq_z(p).wait_recv() if copy is lq_copy else lo_zwait(p)
            hop(copy, p, 0).start()
        for p in ps:
            hop(copy, p, 1).start()
            hop(copy, p, 2).start()

    def ev_near(copy, *ps):
        for p in ps:
            with scope(f'n_{copy.__name__}{p}'):
                hop(copy, p, 0).wait_recv()
            hop(copy, p, 3).start()
            hop(copy, p, 4).start()

    def ev_far(copy, *ps):
        for p in ps:
            with scope(f'f_{copy.__name__}{p}'):
                hop(copy, p, 1).wait_recv()
            hop(copy, p, 5).start()

    def ev_xy(copy, *ps):
        ev_near(copy, *ps)
        ev_far(copy, *ps)

    def ev_y(copy, *ps):
        for p in ps:
            with scope(f'y_{copy.__name__}{p}'):
                hop(copy, p, 3).wait_recv()
            hop(copy, p, 6).start()
            if copy is lq_copy and p >= 2:
                start(w_load(p, SLOT[:4]))

    def ev_done(copy, *ps):
        for p in ps:
            with scope(f'c_{copy.__name__}{p}'):
                if copy is lq_copy:
                    arrived(lq_ref.at[pl.ds(4, 4), p], lq_recv.at[p, 4])
                else:
                    arrived(lo_ref.at[p, pl.ds(4, 4)], lo_recv.at[p, 4])

    def w_load(p, slots):
        return [pltpu.make_async_copy(lq_ref.at[SLOT.index(m), p], ws.at[p // 2 % 2, ds((idx ^ m) * B, B), pl.ds(p % 2 * B, B)], w_sem.at[p]) for m in slots]

    def own_load(t):
        return pltpu.make_async_copy(W[t], ws.at[t], w_sem.at[6 + t])

    def start(copies):
        for c in copies:
            c.start()

    def wait(copies):
        for c in copies:
            c.wait()

    def ev_last(t):
        pieces = [2 * t + i for i in TWO]
        ev_done(lq_copy, *pieces)
        for p in pieces:
            start(w_load(p, SLOT[4:] if t else SLOT))

    def local(ref, sem):
        pltpu.make_async_copy(ref, ref, sem).wait()

    def ev_weights(t):
        with scope(f'load{t}'):
            for i in TWO:
                local(ws.at[t % 2, :, pl.ds(i * B, B)], w_sem.at[2 * t + i])

    def ev_wo(*vs):
        ev_done(lo_copy, *vs)
        for v in vs:
            lb_core(v).wait_recv()
        start(wo_load(*vs))

    def ev_wo_ready(*vs):
        with scope(f'wo{vs[0]}'):
            for v in vs:
                local(xp.at[1 - side, pl.ds(2, 6), :, pl.ds((v ^ 2) * H, H)], wo_sem.at[v])

    def ev_lb(*vs):
        for v in vs:
            with scope(f'lb{v}'):
                lb_z(v).wait_recv()
            lb_core(v).start()

    wo = xp.at[1 - side]

    def wo_own():
        return [pltpu.make_async_copy(wout_ref.at[pl.ds(r * B, B), pl.ds(c * H, H)], xp.at[1 - side, r, :, ds((c ^ tp ^ 2) * H, H)], wo_sem.at[4])
                for r in TWO for c in range(4)]

    def wo_load(*vs):
        out = []
        for v in vs:
            cols = pl.ds((v ^ 2) * H, H)
            for s, m in enumerate(SLOT):
                row = (idx ^ m) * 64
                for b in TWO:
                    out.append(pltpu.make_async_copy(lo_ref.at[v, s, b], xp.at[1 - side, 4 + 2 * b + row // B, ds(row % B, 64, 64), cols], wo_sem.at[v]))
            for r in TWO:
                out.append(pltpu.make_async_copy(lb_ref.at[v, r], xp.at[1 - side, 2 + r, :, cols], wo_sem.at[v]))
        return out

    def kvp_copy(h, s):
        return remote(kv_s.at[h, pl.ds(8 * s, 2)], kvp_s.at[h, pl.ds(2 * s, 2)], sent.at[4], kv_recv.at[0, h], peer_c)

    def kvr_copy(h, s):
        return remote(kv_s.at[h, 8 * s], kvr_s.at[h, s], sent.at[5], kv_recv.at[1, h], peer_y)

    def kvf_copy(h, s):
        return remote(kvr_s.at[h, s], kvr_s.at[h, 2 + s], sent.at[6], kv_recv.at[2, h], peer_c)

    def kv_start(copy, heads):
        for h in heads:
            for s in TWO:
                copy(h, s).start()

    def kv_wait(copy, heads):
        with scope(f'w_{copy.__name__}{heads[0]}'):
            for h in heads:
                i = (kvp_copy, kvr_copy, kvf_copy).index(copy)
                arrived((kvp_s.at[h], kvr_s.at[h, pl.ds(0, 2)], kvr_s.at[h, pl.ds(2, 2)])[i], kv_recv.at[i, h])

    def kv_forward(heads):
        kv_wait(kvr_copy, heads)
        kv_start(kvf_copy, heads)

    def reverse(i):
        return (i % 2) * 2 + i // 2

    def order(n):
        return 2 * reverse(n % 4) + ((n // 4) ^ side)

    def o_at(k, p, theirs, col, size, row=0, rows=B):
        if p:
            return ws.at[1 + theirs, ds(k * B + row, rows, 64), ds(col, size)]
        return xb.at[k // 2, pl.ds(row, rows), ds((k % 2) * 1024 + theirs * H + col, size)]

    def o_copy(k, p, q):
        row = q * 64
        return remote(o_at(k, p, 0, 0, H, row, 64), o_at(k, p, 1, 0, H, row, 64), sent.at[7], o_recv.at[k, q], {'tp': tp ^ 1})

    def o_times(k, v, n, row=0, rows=B):
        cols = pl.ds((v ^ 2) * H, n * H)
        y = nn(xb[k // 2, pl.ds(row, rows), ds((k % 2) * 1024, 1024)], wo[0:4, :, cols].reshape(1024, n * H))
        for i in TWO:
            y = y + nn(ws[1 + i, ds(k * B + row, rows, 64), :], wo[part(2 + i, 2), :, cols].reshape(H, n * H))
        y = y.astype(BF)
        for i in range(n):
            y_src(k, v + i, row, rows)[...] = y[:, part(i, H)]
            y_copy(k, v + i, side, row, rows).start() if v else y_local(k).start()

    def y_src(k, v, row=0, rows=B):
        return xp.at[side, k, pl.ds(row, rows), pl.ds(v * H, H)]

    def y_copy(k, v, seg, row, rows):
        return remote(y_src(k, v, row, rows), out_ref.at[seg, k, pl.ds(row, rows)], sent.at[8], y_recv.at[seg], {'tp': tp ^ v})

    def y_local(k):
        return pltpu.make_async_copy(y_src(k, 0), out_ref.at[side, k], sent.at[9])

    def x_copy(j):
        return pltpu.make_async_copy(x_ref.at[ds(j * B, B), :], xb.at[lax.rem(j, 4)], x_sem.at[lax.rem(j, 4)])

    for j in range(4):
        x_copy(j).start()
    barrier = pltpu.get_barrier_semaphore()
    peers = [{'tp': tp ^ 1}, {'tp': tp ^ 2}, {'tp': tp ^ 3}, peer_x, peer_y, peer_c]
    for dev in peers:
        pl.semaphore_signal(barrier, inc=1, device_id=dev, device_id_type=MESH)
    for t in range(3):
        own_load(t).start()

    pm[...] = phase_matrix(False)

    def permute_body(j, carry):
        x_copy(j).wait()
        y = nn(pm[...], xb[lax.rem(j, 4)]).astype(BF).reshape(8, 32, M)
        xp[j // 8, :, ds(lax.rem(j, 8) * 32, 32, 32), :] = y
        pl.when(j < 12)(lambda: x_copy(j + 4).start())

        @pl.when(j == 2)
        def _():
            with scope('barrier'):
                pl.semaphore_wait(barrier, len(peers))
            lq_start(KEY)
            on(outer, lb_z(2).start)
        return carry

    with scope('permute'):
        lax.fori_loop(0, 16, permute_body, None)

    for h in HEADS:
        column = 2 * (tp ^ (h // 2 * 2)) + h % 2
        for i, branches in enumerate(('0', '01', '1', '012', '12', '2', '0123', '123', '23', '3')):
            rows = [jnp.full((1, 128), bias_ref[j, column], F32) for j in map(int, branches)]
            m = functools.reduce(jnp.maximum, rows)
            beta_s[pl.ds(h * 16 + i, 1), :] = (m + jnp.log(sum(jnp.exp(r - m) for r in rows))) * math.log2(math.e)

    def signal_ready(i):
        pl.when(inner)(lambda: pl.semaphore_signal(ready.at[i], inc=1, device_id={'tp': tp ^ 1}, device_id_type=MESH))

    def wait_ready(i):
        with scope(f'ready{i}'):
            pl.when(outer)(lambda: pl.semaphore_wait(ready.at[i], 1))

    signal_ready(0)

    def group(g):
        low = g < 4
        return jnp.where(low, g & 1, 0), jnp.where(low, g // 2, g - 2)

    def head_number(h):
        return 2 * (tp ^ (h // 2 * 2)) + h % 2

    def project(heads, sigma, pair, kinds):
        for h in heads:
            t = head_number(h) + reverse(pair)
            x, swap = xp[side ^ sigma, pl.ds(2 * (t & 3), 2)].reshape(H, M), (t & 7) >> 2
            for t in kinds:
                y = nn(x, ws[t, :, part(h % 2, B)])
                for j in TWO:
                    piece = y[part(j, B)]
                    kv_s[h, 8 * sigma + 2 * pair + (j ^ swap), t] = (piece.T if t == VAL else piece).astype(BF)

    def phases_of(j):
        return [j % 2 + 2 * i for i in TWO], (j // 2) ^ side

    def rank_of(phase, h):
        rel = (phase - head_number(h)) & 7
        return (rel & 1) * 4 + ((rel >> 1) & 1) * 2 + (rel >> 2)

    def queries(heads, w, j):
        phases, half = phases_of(j)
        x = jnp.concatenate([xp[side, 2 * f + half] for f in phases])
        for h in heads:
            y = nn(x, ws[w, :, part(h % 2, B)]).astype(BF)
            for i, f in enumerate(phases):
                q_s[h, rank_of(f + 4 * half, h)] = y[part(i, B)]

    with scope('own_w'):
        for t in range(3):
            own_load(t).wait()
    own, partner = HEADS[:2], HEADS[2:]

    def mix(b, c):
        return jnp.concatenate([b, b, c, c], axis=1)

    def keys_of(ref, h, i, weights):
        parts = []
        n = 0
        for count, b in weights:
            def values(i=i + n, count=count):
                v = [ref[h, i + j, VAL] for j in range(count)]
                return v[0] if count == 1 else jnp.concatenate(v, axis=1)
            parts.append((values, count * B, b))
            n += count
        return (lambda: ref[h, i:i + n, KEY].reshape(n * B, B)), parts

    def chunk_tiles(p, j, kind):
        both_phases, half = phases_of(j)

        def put(h, phase, ot):
            k = 2 * (phase & 3) + half
            y = ot.T.astype(BF)
            for i in TWO:
                pl.when(p == i)(lambda i=i: o_at(k, i, 0, (h % 2) * B, B).__setitem__(..., y))

        def tile(h, phases, ranks, wide, narrow, s_ref, n_ref):
            def done(ot):
                for i, phase in enumerate(phases):
                    put(h, phase, ot[:, part(i, B)])
            return tile_steps(lambda: jnp.concatenate([q_s[h, r] for r in ranks]), wide, narrow, s_ref, n_ref, done)

        h = 2 * p + (j % 2) ^ 1
        rest = tile(h, both_phases, [rank_of(f + 4 * half, h) for f in both_phases], [keys_of(kv_s, h, i, [(1, None)]) for i in ROWS], [], t_scr, None)
        h = 2 * p + (j % 2)
        a = head_number(h)
        b0, b01, b1, b012, b12, b2, b0123, b123, b23, b3 = [beta_s[pl.ds(h * 16 + i, 1), :] for i in range(10)]
        phases = [a & 3, (a & 3) ^ 2]
        both = [keys_of(kv_s, h, i, [(2, b)] * n) for i, b, n in ((2, b01, 1), (4, b0, 2), (10, b1, 1))]
        if kind == 0:
            both += [keys_of(kv_s, h, 0, [(1, mix(b0123, b01)), (1, mix(b012, b01))]), keys_of(kv_s, h, 8, [(1, mix(b123, b1)), (1, mix(b12, b1))])]
            first = [keys_of(kvp_s, h, i, [(1, b23), (1, b2)]) for i in (0, 2)] + [keys_of(kvr_s, h, i, [(2, b3)]) for i in (0, 2)]
        else:
            both += [keys_of(kv_s, h, 0, [(2, mix(b012, b01))]), keys_of(kv_s, h, 8, [(2, mix(b12, b1))])]
            first = [keys_of(kvp_s, h, i, [(2, b2)]) for i in (0, 2)]
        with scope(f'tile{kind}'):
            run_tiles([rest, tile(h, phases, [kind, rank_of(phases[1] + 4 * half, h)], both, first, s_scr, t_scr.at[:, pl.ds(0, B)])])

    def send_o(ks, p):
        @pl.when(outer)
        def _():
            for k in ks:
                for q in QUARTERS:
                    o_copy(order(k), p, q).start()

    def step_body(t, carry):
        packed = functools.reduce(lambda x, i: jnp.where(t == i, TABLE[i], x), range(len(TABLE)), 0)
        code, n, event = packed % 16, packed // 16 % 16, packed // 256

        def step_o():
            with scope('own_kv'):
                project(own, *group(n), (KEY, VAL))

        def step_kv(t_):
            with scope(f'par_{t_}'):
                for i in TWO:
                    project(partner, *group(2 * n + i), (t_,))

        def step_q(heads, w):
            with scope(f'que_{w}'):
                queries(heads, w, n)

        def step_out(v, m):
            @pl.when(inner)
            def _():
                k = order(n)

                def wait_for(q):
                    arrived(ws.at[0, pl.ds(0, 128), :], o_recv.at[k, q])

                def quarters():
                    for q in QUARTERS:
                        with scope(f'wait_q{q}'):
                            wait_for(q)
                        o_times(k, v, m, q * 64, 64)
                        if q == 0:
                            ev_y(lo_copy, 1)
                        if q == 2:
                            ev_wo(1)

                def whole():
                    with scope('wait_o'):
                        for q in QUARTERS:
                            wait_for(q)
                    with scope(f'out{v}'):
                        o_times(k, v, m)

                if m == 2:
                    pl.when(n == 0)(quarters)
                    pl.when(n > 0)(whole)
                else:
                    with scope(f'out{v}'):
                        o_times(k, v, m)

        f = functools.partial
        kinds = {'-': lambda: None, 'O': step_o, 'P': f(step_q, own, QUE), 'K': f(step_kv, KEY), 'V': f(step_kv, VAL), 'Q': f(step_q, partner, KEY),
                 'A': lambda: chunk_tiles(n // 4, n % 4, 0), 'B': lambda: chunk_tiles(n // 4, n % 4, 1), 'R': f(step_out, 2, 2), 'L': f(step_out, 1, 1), 'N': f(step_out, 0, 1)}
        choose(code, [kinds[c] for c in KINDS])
        call = functools.partial

        events = {
            'free': [call(signal_ready, 1), call(on, inner, lambda: start(wo_own()))],
            'r0': [call(wait_ready, 0)],
            'r1': [call(wait_ready, 1)],
            'ko': [call(kv_start, kvp_copy, own)],
            'po': [call(kv_wait, kvp_copy, own)],
            'kp': [call(kv_start, kvp_copy, partner)],
            'pp': [call(kv_wait, kvp_copy, partner)],
        }
        for t_, c in enumerate('kvq'):
            events['b' + c] = [call(lq_start, t_)]
            events['l' + c] = [call(ev_last, t_)]
            events['w' + c] = [call(ev_weights, t_)]
            events['z' + c] = [call(ev_z, lq_copy, 2 * t_, 2 * t_ + 1)]
            for i in TWO:
                for e, f in zip('zmfxy', (ev_z, ev_near, ev_far, ev_xy, ev_y)):
                    events[f'{e}{c}{i}'] = [call(f, lq_copy, 2 * t_ + i)]
        for i, vs in enumerate(((2, 3), (1,), (0,))):
            events[f'b{i}'] = [call(lo_start, *vs)]
            for e, f in zip('zmxycwv', (call(ev_z, lo_copy), call(ev_near, lo_copy), call(ev_far, lo_copy), call(ev_y, lo_copy), ev_lb, ev_wo, ev_wo_ready)):
                events[f'{e}{i}'] = [call(on, inner, call(f, *vs))]
        events['v0'] += [call(on, inner, lambda: local(xp.at[1 - side, pl.ds(0, 2)], wo_sem.at[4]))]
        for v in range(4):
            events[f'd{v}'] = [call(on, outer, lambda v=v: lb_z(v).start())]
        for h in HEADS:
            for z in TWO:
                events[f's{h}{z}'] = [kvr_copy(h, z).start]
            events[f'f{h}'] = [call(kv_forward, [h])]
            events[f'g{h}'] = [call(kv_wait, kvf_copy, [h])]
        for k in ROWS:
            for p in TWO:
                events['op'[p] + str(k)] = [call(send_o, (k,), p)]
        def run(names):
            for name in names.split(','):
                where, _, name = name.rpartition(':')
                if where:
                    on(inner if where == 'i' else outer, *events[name])
                else:
                    for c in events[name]:
                        c()

        @pl.when(event > 0)
        def _():
            choose(event - 1, [functools.partial(run, names) for names in EVENTS])
        return carry

    lax.fori_loop(0, len(TABLE), step_body, None)

    all_sent(lq_ref, 0)
    all_sent(lo_ref.at[:, 0, 0], 2)
    all_sent(lb_ref.at[:, 0], 3)
    all_sent(kvp_s, 4)
    all_sent(kvr_s.at[:, pl.ds(0, 2)], 5)
    all_sent(kvr_s.at[:, pl.ds(0, 2)], 6)

    @pl.when(outer)
    def _():
        all_sent(xb, 7)

    @pl.when(inner)
    def _():
        all_sent(lo_ref.at[:, pl.ds(0, 7)], 1)
        with scope('y_sent'):
            all_sent(xp.at[side, :, :, pl.ds(H, 3 * H)], 8)
        local(xp.at[side, :, :, pl.ds(0, H)], sent.at[9])

    for seg in TWO:
        @pl.when(tp != 1 + seg)
        def _(seg=seg):
            with scope(f'recv{seg}'):
                arrived(out_ref.at[seg], y_recv.at[seg])


PROGRAM = (
    'O.i:zk0,i:zk1,bv', 'O.o:zk0', 'O.o:zk1,s00,i:xk0', 'O.o:xk0,i:xk1,o:s01,d3,i:bq', 'O.o:bq,o:xk1,i:yk0,i:zv0', 'O.o:yk0,i:yk1,i:zv1,i:s01',
    'P.o:zv0,o:yk1,lk,o:zv1,d1,i:xv0', 'P.wk,i:xv1', 'K.ko', 'K.o:xv0,i:zq,f0', 'K.o:xv1,i:yv0,i:yv1,b0,b1,r0,po,g0,o:zq',
    'T0.o0,o1,d0,o:yv0,o:yv1,lv,mq0,i:mq1,i:fq0,i:fq1', 'P.wv,o:mq1,b2', 'V.z0,o:fq0,o:fq1,kp,o:s10,o:s11', 'V.c0,z1,o:s20,o:s21,yq0,yq1',
    'V.lq,o:s30,o:s31', 'P.free,wq,m0', 'Q.pp,r1,x0,c1,i:s10,i:s11', 'T4.p0,p1,y0,w0,m1,x1,v0', 'R.v1,i:s20,i:s21', 'L', 'Q.f1', 'R', 'L',
    'T5.p2,g1', 'T1.o2,p3,o3,o:f2', 'R.i:s30,i:s31', 'L', 'Q.o:g2', 'Q.i:f2,o:f3', 'T2', 'R.i:g2', 'L', 'T6.p4,o4,p5,o5,o:g3', 'R.i:f3,z2,c2', 'L',
    'T3.i:g3', 'T7.p6,o6,p7,o7', 'R', 'L.m2,x2', 'R.y2', 'L.w2', '-.v2', 'N', 'N', 'N', 'R', 'L', 'N', 'N', 'N', 'N', 'N',
)
KINDS = '-OPKVQABRLN'


def tables():
    table, seen = [], {}
    names = tuple(dict.fromkeys(s.partition('.')[2] for s in PROGRAM if '.' in s))
    for s in PROGRAM:
        name, _, after = s.partition('.')
        kind, n = name[0], seen.get(name[0], 0)
        seen[kind] = n + 1
        if kind == 'T':
            n = int(name[1:])
            kind = 'AB'[n in (2, 3, 4, 5)]
        table.append(KINDS.index(kind) + 16 * n + 256 * (names.index(after) + 1 if after else 0))
    return table, names


TABLE, EVENTS = tables()


def main(bias, x, wk, wv, wq, w_out):
    anyspec = pl.BlockSpec(memory_space=pl.ANY)
    vmem = [((4, B, M), BF), ((B, B), BF), ((2, 8, B, M), BF), ((3, M, H), BF), ((4, 8, B, B), BF), ((4, 12, 2, B, B), BF), ((4, 4, 2, B, B), BF), ((4, 4, 2, B, B), BF),
            ((3072, H), F32), ((M, H), F32), ((64, 128), F32)]
    dma = [(4,), (9,), (5,), (10,), (6, 5), (4, 5), (4, 2), (3, 4), (8, 4), (2,)]
    return pl.pallas_call(
        main_kernel,
        in_specs=[pl.BlockSpec(memory_space=pltpu.SMEM)] + [anyspec] * 5,
        out_specs=[anyspec] * 4,
        out_shape=[jax.ShapeDtypeStruct(s, BF) for s in ((2, 8, B, H), (8, 6, B, B), (4, 8, 2, 64, H), (4, 2, B, H))],
        scratch_shapes=[pltpu.VMEM(*v) for v in vmem] + [pltpu.SemaphoreType.DMA(d) for d in dma] + [pltpu.SemaphoreType.REGULAR((2,))],
        compiler_params=params(collective_id=0, has_side_effects=True),
        cost_estimate=pl.CostEstimate(flops=10**11, bytes_accessed=10**8, transcendentals=0),
        name='main',
    )(bias, x, wk, wv, wq, w_out)[0]


def solution(mesh):
    def device_fn(hidden, w_query, w_key, w_value, w_out, branch_bias):
        return unpermute(main(branch_bias, hidden, w_key, w_value, w_query, w_out))

    return jax.shard_map(device_fn, mesh=mesh, in_specs=(P(('dp', 'sp'), None), P(None, 'tp'), P(None, 'tp'), P(None, 'tp'), P('tp', None), P(None, None)), out_specs=P(('dp', 'sp'), 'tp'), check_vma=False)
```

```python
import functools
import math

import jax
import jax.numpy as jnp
from jax import lax
from jax.experimental import pallas as pl
from jax.experimental.pallas import tpu as pltpu
from jax.sharding import PartitionSpec as P

MESH = pl.DeviceIdType.MESH
BF = jnp.bfloat16
F32 = jnp.float32
B, H, M = 256, 512, 2048
KAPPA = math.log2(math.e) / 16
VMEM = 66_900_000
SLOT = (0, 4, 2, 6, 1, 5, 3, 7)
KEY, VAL, QUE = range(3)
HEADS = range(4)
TWO = range(2)
QUARTERS = range(4)
ROWS = range(8)


def nn(a, b):
    return lax.dot_general(a, b, (((1,), (0,)), ((), ())), preferred_element_type=F32)


def nt(a, b):
    return lax.dot_general(a, b, (((1,), (1,)), ((), ())), preferred_element_type=F32)


def params(**kw):
    return pltpu.CompilerParams(vmem_limit_bytes=VMEM, **kw)


def ds(start, size, align=128):
    return pl.ds(pl.multiple_of(start, align), size)


def part(i, size):
    return slice(i * size, i * size + size)


def phase_matrix(transposed):
    r = lax.broadcasted_iota(jnp.int32, (B, B), int(transposed))
    p = lax.broadcasted_iota(jnp.int32, (B, B), int(not transposed))
    k = r // 32
    return (p == (r % 32) * 8 + k // 2 + 4 * (k % 2)).astype(F32).astype(BF)


def unpermute_kernel(y_ref, o_ref, y_s, o_s, load, store):
    pieces = [(s, j) for s in TWO for j in range(4)]

    def get(i):
        s, j = pieces[i]
        return pltpu.make_async_copy(y_ref.at[s, :, pl.ds(j * 64, 64)], y_s.at[i], load.at[i])

    def put(i):
        return pltpu.make_async_copy(o_s.at[i], o_ref.at[pl.ds(i * H, H)], store.at[i])

    for i in ROWS:
        get(i).start()
    pm = phase_matrix(True)
    for i in range(0, 8, 2):
        group = (i, i + 1)
        for k in group:
            get(k).wait()
        for k in group:
            for j in TWO:
                o_s[k, part(j, B), :] = nn(pm, y_s[k, :, part(j, 32), :].reshape(B, H)).astype(BF)
        for k in group:
            put(k).start()
    for i in ROWS:
        put(i).wait()


def unpermute(y):
    anyspec = pl.BlockSpec(memory_space=pl.ANY)
    return pl.pallas_call(
        unpermute_kernel,
        in_specs=[anyspec],
        out_specs=anyspec,
        out_shape=jax.ShapeDtypeStruct((2 * M, H), BF),
        scratch_shapes=[pltpu.VMEM((8, 8, 64, H), BF), pltpu.VMEM((8, H, H), BF), pltpu.SemaphoreType.DMA((8,)), pltpu.SemaphoreType.DMA((8,))],
        compiler_params=params(),
        name='unpermute',
    )(y)


def tile_steps(q, wide, narrow, s_ref, n_ref, done):
    st = {}
    logits, sums = [], []

    def add(name, x):
        st[name] = st[name] + x if name in st else x

    for groups, ref in ((wide, s_ref), (narrow, n_ref)):
        off = 0
        for keys, parts in groups:
            def qk(keys=keys, parts=parts, off=off, ref=ref):
                s = nt(keys(), q() if ref is s_ref else q()[:B])
                o = 0
                for _, n, b in parts:
                    piece = s[o:o + n]
                    ref[pl.ds(off + o, n), :] = piece
                    t = jnp.max(piece, axis=0, keepdims=True) * KAPPA
                    if b is not None:
                        t = t + fit(b, t)
                    if ref is n_ref:
                        t = jnp.concatenate([t, st['top'][:, B:]], axis=1)
                    st['top'] = jnp.maximum(st['top'], t) if 'top' in st else t
                    o += n
            logits.append(qk)
            for v, n, b in parts:
                def sv(v=v, n=n, b=b, off=off, ref=ref):
                    top = st['top'] if ref is s_ref else st['top'][:, :B]
                    e = jnp.exp2(ref[pl.ds(off, n), :] * KAPPA - (top if b is None else top - fit(b, top)))
                    name = 'w' if ref is s_ref else 'n'
                    add('l' + name, jnp.sum(e, axis=0, keepdims=True))
                    add('o' + name, nn(v(), e.astype(BF)))
                sums.append(sv)
                off += n

    def finish():
        o, l = st['ow'], st['lw']
        if narrow:
            o = jnp.concatenate([o[:, :B] + st['on'], o[:, B:]], axis=1)
            l = jnp.concatenate([l[:, :B] + st['ln'], l[:, B:]], axis=1)
        done(o / l)

    return logits, sums + [finish]


def fit(b, like):
    return b if b.shape == like.shape else jnp.concatenate([b] * (like.shape[1] // 128), axis=1)


def interleave(a, b):
    i = j = 0
    while i < len(a) or j < len(b):
        if j >= len(b) or (i < len(a) and i * len(b) <= j * len(a)):
            a[i]()
            i += 1
        else:
            b[j]()
            j += 1


def run_tiles(tiles):
    before = []
    for logits, sums in tiles:
        interleave(logits, before)
        before = sums
    interleave([], before)


def choose(x, cases):
    def among(lo, hi):
        mid = (lo + hi) // 2
        if hi - lo == 1:
            cases[lo]()
        else:
            pl.when(x < mid)(lambda: among(lo, mid))
            pl.when(x >= mid)(lambda: among(mid, hi))
    among(0, len(cases))


def on(cond, *calls):
    @pl.when(cond)
    def _():
        for c in calls:
            c()


def scope(name):
    return jax.named_scope(name)


def main_kernel(bias_ref, x_ref, wk_ref, wv_ref, wq_ref, wout_ref, out_ref, lq_ref, lo_ref, lb_ref,
                xb, pm, xp, ws, q_s, kv_s, kvp_s, kvr_s, s_scr, t_scr,
                beta_s, x_sem, w_sem, wo_sem, sent, lq_recv, lo_recv, lb_recv, kv_recv, o_recv, y_recv, ready):
    dp, tp, sp = lax.axis_index('dp'), lax.axis_index('tp'), lax.axis_index('sp')
    idx = dp * 4 + sp
    side = tp // 2
    inner = (tp == 1) | (tp == 2)
    outer = jnp.logical_not(inner)
    W = (wk_ref, wv_ref, wq_ref)
    peer_x, peer_y, peer_c = {'dp': dp ^ 1}, {'sp': sp ^ 2}, {'sp': sp ^ 1}

    def remote(src, dst, ss, rs, dev):
        return pltpu.make_async_remote_copy(src_ref=src, dst_ref=dst, send_sem=ss, recv_sem=rs, device_id=dev, device_id_type=MESH)

    def lq_copy(t, src, dst, dev):
        return remote(lq_ref.at[src, t], lq_ref.at[dst, t], sent.at[0], lq_recv.at[t, min(dst, 4)], dev)

    def lq_z(t):
        return remote(W[t // 2].at[ds(idx * B, B), pl.ds(t % 2 * B, B)], lq_ref.at[0, t], sent.at[0], lq_recv.at[t, 0], {'tp': tp ^ 2})

    def lq_start(t):
        for i in TWO:
            lq_z(2 * t + i).start()

    def lo_copy(v, src, dst, dev):
        return remote(lo_ref.at[v, src], lo_ref.at[v, dst], sent.at[1], lo_recv.at[v, min(dst, 4)], dev)

    def lo_z(v):
        dst = 2 - side
        b = (tp ^ dst) - 2
        return remote(wout_ref.at[ds(idx * 64, 64, 64), ds((dst ^ v) * H, H)], lo_ref.at[v, 0, b], sent.at[2], lo_recv.at[v, 0], {'tp': dst})

    def lb_z(v):
        return remote(wout_ref.at[ds(sp % 2 * B, B), ds((tp ^ 1 ^ v) * H, H)], lb_ref.at[v, sp % 2], sent.at[3], lb_recv.at[v, 0], {'tp': tp ^ 1})

    def lb_core(v):
        return remote(lb_ref.at[v, sp % 2], lb_ref.at[v, sp % 2], sent.at[3], lb_recv.at[v, 1], peer_c)

    def lo_start(*vs):
        for v in vs:
            lo_z(v).start()

    def arrived(ref, sem):
        remote(ref, ref, sent.at[0], sem, peer_c).wait_recv()

    def all_sent(ref, i):
        remote(ref, ref, sent.at[i], sent.at[i], peer_c).wait_send()

    def lo_zwait(v):
        arrived(lo_ref.at[v, 0], lo_recv.at[v, 0])

    def hop(copy, p, i):
        near, far, n = (peer_x, peer_y, 1) if (copy is lo_copy and p == 2) or (copy is lq_copy and p in (3, 5)) else (peer_y, peer_x, 2)
        f = 3 - n
        return copy(p, *((0, n, near), (0, f, far), (0, 4, peer_c), (n, 3, far), (n, 4 + n, peer_c), (f, 4 + f, peer_c), (3, 7, peer_c))[i])

    def ev_z(copy, *ps):
        for p in ps:
            with scope(f'z_{copy.__name__}{p}'):
                lq_z(p).wait_recv() if copy is lq_copy else lo_zwait(p)
            hop(copy, p, 0).start()
        for p in ps:
            hop(copy, p, 1).start()
            hop(copy, p, 2).start()

    def ev_near(copy, *ps):
        for p in ps:
            with scope(f'n_{copy.__name__}{p}'):
                hop(copy, p, 0).wait_recv()
            hop(copy, p, 3).start()
            hop(copy, p, 4).start()

    def ev_far(copy, *ps):
        for p in ps:
            with scope(f'f_{copy.__name__}{p}'):
                hop(copy, p, 1).wait_recv()
            hop(copy, p, 5).start()

    def ev_xy(copy, *ps):
        ev_near(copy, *ps)
        ev_far(copy, *ps)

    def ev_y(copy, *ps):
        for p in ps:
            with scope(f'y_{copy.__name__}{p}'):
                hop(copy, p, 3).wait_recv()
            hop(copy, p, 6).start()
            if copy is lq_copy and p >= 2:
                start(w_load(p, SLOT[:4]))

    def ev_done(copy, *ps):
        for p in ps:
            with scope(f'c_{copy.__name__}{p}'):
                if copy is lq_copy:
                    arrived(lq_ref.at[pl.ds(4, 4), p], lq_recv.at[p, 4])
                else:
                    arrived(lo_ref.at[p, pl.ds(4, 4)], lo_recv.at[p, 4])

    def w_load(p, slots):
        return [pltpu.make_async_copy(lq_ref.at[SLOT.index(m), p], ws.at[p // 2 % 2, ds((idx ^ m) * B, B), pl.ds(p % 2 * B, B)], w_sem.at[p]) for m in slots]

    def own_load(t):
        return pltpu.make_async_copy(W[t], ws.at[t], w_sem.at[6 + t])

    def start(copies):
        for c in copies:
            c.start()

    def wait(copies):
        for c in copies:
            c.wait()

    def ev_last(t):
        pieces = [2 * t + i for i in TWO]
        ev_done(lq_copy, *pieces)
        for p in pieces:
            start(w_load(p, SLOT[4:] if t else SLOT))

    def local(ref, sem):
        pltpu.make_async_copy(ref, ref, sem).wait()

    def ev_weights(t):
        with scope(f'load{t}'):
            for i in TWO:
                local(ws.at[t % 2, :, pl.ds(i * B, B)], w_sem.at[2 * t + i])

    def ev_wo(*vs):
        ev_done(lo_copy, *vs)
        for v in vs:
            lb_core(v).wait_recv()
        start(wo_load(*vs))

    def ev_wo_ready(*vs):
        with scope(f'wo{vs[0]}'):
            for v in vs:
                local(xp.at[1 - side, pl.ds(2, 6), :, pl.ds((v ^ 2) * H, H)], wo_sem.at[v])

    def ev_lb(*vs):
        for v in vs:
            with scope(f'lb{v}'):
                lb_z(v).wait_recv()
            lb_core(v).start()

    wo = xp.at[1 - side]

    def wo_own():
        return [pltpu.make_async_copy(wout_ref.at[pl.ds(r * B, B), pl.ds(c * H, H)], xp.at[1 - side, r, :, ds((c ^ tp ^ 2) * H, H)], wo_sem.at[4])
                for r in TWO for c in range(4)]

    def wo_load(*vs):
        out = []
        for v in vs:
            cols = pl.ds((v ^ 2) * H, H)
            for s, m in enumerate(SLOT):
                row = (idx ^ m) * 64
                for b in TWO:
                    out.append(pltpu.make_async_copy(lo_ref.at[v, s, b], xp.at[1 - side, 4 + 2 * b + row // B, ds(row % B, 64, 64), cols], wo_sem.at[v]))
            for r in TWO:
                out.append(pltpu.make_async_copy(lb_ref.at[v, r], xp.at[1 - side, 2 + r, :, cols], wo_sem.at[v]))
        return out

    def kvp_copy(h, s):
        return remote(kv_s.at[h, pl.ds(8 * s, 2)], kvp_s.at[h, pl.ds(2 * s, 2)], sent.at[4], kv_recv.at[0, h], peer_c)

    def kvr_copy(h, s):
        return remote(kv_s.at[h, 8 * s], kvr_s.at[h, s], sent.at[5], kv_recv.at[1, h], peer_y)

    def kvf_copy(h, s):
        return remote(kvr_s.at[h, s], kvr_s.at[h, 2 + s], sent.at[6], kv_recv.at[2, h], peer_c)

    def kv_start(copy, heads):
        for h in heads:
            for s in TWO:
                copy(h, s).start()

    def kv_wait(copy, heads):
        with scope(f'w_{copy.__name__}{heads[0]}'):
            for h in heads:
                i = (kvp_copy, kvr_copy, kvf_copy).index(copy)
                arrived((kvp_s.at[h], kvr_s.at[h, pl.ds(0, 2)], kvr_s.at[h, pl.ds(2, 2)])[i], kv_recv.at[i, h])

    def kv_forward(heads):
        kv_wait(kvr_copy, heads)
        kv_start(kvf_copy, heads)

    def reverse(i):
        return (i % 2) * 2 + i // 2

    def order(n):
        return 2 * reverse(n % 4) + ((n // 4) ^ side)

    def o_at(k, p, theirs, col, size, row=0, rows=B):
        if p:
            return ws.at[1 + theirs, ds(k * B + row, rows, 64), ds(col, size)]
        return xb.at[k // 2, pl.ds(row, rows), ds((k % 2) * 1024 + theirs * H + col, size)]

    def o_copy(k, p, q):
        row = q * 64
        return remote(o_at(k, p, 0, 0, H, row, 64), o_at(k, p, 1, 0, H, row, 64), sent.at[7], o_recv.at[k, q], {'tp': tp ^ 1})

    def o_times(k, v, n, row=0, rows=B):
        cols = pl.ds((v ^ 2) * H, n * H)
        y = nn(xb[k // 2, pl.ds(row, rows), ds((k % 2) * 1024, 1024)], wo[0:4, :, cols].reshape(1024, n * H))
        for i in TWO:
            y = y + nn(ws[1 + i, ds(k * B + row, rows, 64), :], wo[part(2 + i, 2), :, cols].reshape(H, n * H))
        y = y.astype(BF)
        for i in range(n):
            y_src(k, v + i, row, rows)[...] = y[:, part(i, H)]
            y_copy(k, v + i, side, row, rows).start() if v else y_local(k).start()

    def y_src(k, v, row=0, rows=B):
        return xp.at[side, k, pl.ds(row, rows), pl.ds(v * H, H)]

    def y_copy(k, v, seg, row, rows):
        return remote(y_src(k, v, row, rows), out_ref.at[seg, k, pl.ds(row, rows)], sent.at[8], y_recv.at[seg], {'tp': tp ^ v})

    def y_local(k):
        return pltpu.make_async_copy(y_src(k, 0), out_ref.at[side, k], sent.at[9])

    def x_copy(j):
        return pltpu.make_async_copy(x_ref.at[ds(j * B, B), :], xb.at[lax.rem(j, 4)], x_sem.at[lax.rem(j, 4)])

    for j in range(4):
        x_copy(j).start()
    barrier = pltpu.get_barrier_semaphore()
    peers = [{'tp': tp ^ 1}, {'tp': tp ^ 2}, {'tp': tp ^ 3}, peer_x, peer_y, peer_c]
    for dev in peers:
        pl.semaphore_signal(barrier, inc=1, device_id=dev, device_id_type=MESH)
    for t in range(3):
        own_load(t).start()

    pm[...] = phase_matrix(False)

    def permute_body(j, carry):
        x_copy(j).wait()
        y = nn(pm[...], xb[lax.rem(j, 4)]).astype(BF).reshape(8, 32, M)
        xp[j // 8, :, ds(lax.rem(j, 8) * 32, 32, 32), :] = y
        pl.when(j < 12)(lambda: x_copy(j + 4).start())

        @pl.when(j == 2)
        def _():
            with scope('barrier'):
                pl.semaphore_wait(barrier, len(peers))
            lq_start(KEY)
            on(outer, lb_z(2).start)
        return carry

    with scope('permute'):
        lax.fori_loop(0, 16, permute_body, None)

    for h in HEADS:
        column = 2 * (tp ^ (h // 2 * 2)) + h % 2
        for i, branches in enumerate(('0', '01', '1', '012', '12', '2', '0123', '123', '23', '3')):
            rows = [jnp.full((1, 128), bias_ref[j, column], F32) for j in map(int, branches)]
            m = functools.reduce(jnp.maximum, rows)
            beta_s[pl.ds(h * 16 + i, 1), :] = (m + jnp.log(sum(jnp.exp(r - m) for r in rows))) * math.log2(math.e)

    def signal_ready(i):
        pl.when(inner)(lambda: pl.semaphore_signal(ready.at[i], inc=1, device_id={'tp': tp ^ 1}, device_id_type=MESH))

    def wait_ready(i):
        with scope(f'ready{i}'):
            pl.when(outer)(lambda: pl.semaphore_wait(ready.at[i], 1))

    signal_ready(0)

    def group(g):
        low = g < 4
        return jnp.where(low, g & 1, 0), jnp.where(low, g // 2, g - 2)

    def head_number(h):
        return 2 * (tp ^ (h // 2 * 2)) + h % 2

    def project(heads, sigma, pair, kinds):
        for h in heads:
            t = head_number(h) + reverse(pair)
            x, swap = xp[side ^ sigma, pl.ds(2 * (t & 3), 2)].reshape(H, M), (t & 7) >> 2
            for t in kinds:
                y = nn(x, ws[t, :, part(h % 2, B)])
                for j in TWO:
                    piece = y[part(j, B)]
                    kv_s[h, 8 * sigma + 2 * pair + (j ^ swap), t] = (piece.T if t == VAL else piece).astype(BF)

    def phases_of(j):
        return [j % 2 + 2 * i for i in TWO], (j // 2) ^ side

    def rank_of(phase, h):
        rel = (phase - head_number(h)) & 7
        return (rel & 1) * 4 + ((rel >> 1) & 1) * 2 + (rel >> 2)

    def queries(heads, w, j):
        phases, half = phases_of(j)
        x = jnp.concatenate([xp[side, 2 * f + half] for f in phases])
        for h in heads:
            y = nn(x, ws[w, :, part(h % 2, B)]).astype(BF)
            for i, f in enumerate(phases):
                q_s[h, rank_of(f + 4 * half, h)] = y[part(i, B)]

    with scope('own_w'):
        for t in range(3):
            own_load(t).wait()
    own, partner = HEADS[:2], HEADS[2:]

    def mix(b, c):
        return jnp.concatenate([b, b, c, c], axis=1)

    def keys_of(ref, h, i, weights):
        parts = []
        n = 0
        for count, b in weights:
            def values(i=i + n, count=count):
                v = [ref[h, i + j, VAL] for j in range(count)]
                return v[0] if count == 1 else jnp.concatenate(v, axis=1)
            parts.append((values, count * B, b))
            n += count
        return (lambda: ref[h, i:i + n, KEY].reshape(n * B, B)), parts

    def chunk_tiles(p, j, kind):
        both_phases, half = phases_of(j)

        def put(h, phase, ot):
            k = 2 * (phase & 3) + half
            y = ot.T.astype(BF)
            for i in TWO:
                pl.when(p == i)(lambda i=i: o_at(k, i, 0, (h % 2) * B, B).__setitem__(..., y))

        def tile(h, phases, ranks, wide, narrow, s_ref, n_ref):
            def done(ot):
                for i, phase in enumerate(phases):
                    put(h, phase, ot[:, part(i, B)])
            return tile_steps(lambda: jnp.concatenate([q_s[h, r] for r in ranks]), wide, narrow, s_ref, n_ref, done)

        h = 2 * p + (j % 2) ^ 1
        rest = tile(h, both_phases, [rank_of(f + 4 * half, h) for f in both_phases], [keys_of(kv_s, h, i, [(1, None)]) for i in ROWS], [], t_scr, None)
        h = 2 * p + (j % 2)
        a = head_number(h)
        b0, b01, b1, b012, b12, b2, b0123, b123, b23, b3 = [beta_s[pl.ds(h * 16 + i, 1), :] for i in range(10)]
        phases = [a & 3, (a & 3) ^ 2]
        both = [keys_of(kv_s, h, i, [(2, b)] * n) for i, b, n in ((2, b01, 1), (4, b0, 2), (10, b1, 1))]
        if kind == 0:
            both += [keys_of(kv_s, h, 0, [(1, mix(b0123, b01)), (1, mix(b012, b01))]), keys_of(kv_s, h, 8, [(1, mix(b123, b1)), (1, mix(b12, b1))])]
            first = [keys_of(kvp_s, h, i, [(1, b23), (1, b2)]) for i in (0, 2)] + [keys_of(kvr_s, h, i, [(2, b3)]) for i in (0, 2)]
        else:
            both += [keys_of(kv_s, h, 0, [(2, mix(b012, b01))]), keys_of(kv_s, h, 8, [(2, mix(b12, b1))])]
            first = [keys_of(kvp_s, h, i, [(2, b2)]) for i in (0, 2)]
        with scope(f'tile{kind}'):
            run_tiles([rest, tile(h, phases, [kind, rank_of(phases[1] + 4 * half, h)], both, first, s_scr, t_scr.at[:, pl.ds(0, B)])])

    def send_o(ks, p):
        @pl.when(outer)
        def _():
            for k in ks:
                for q in QUARTERS:
                    o_copy(order(k), p, q).start()

    def step_body(t, carry):
        packed = functools.reduce(lambda x, i: jnp.where(t == i, TABLE[i], x), range(len(TABLE)), 0)
        code, n, event = packed % 16, packed // 16 % 16, packed // 256

        def step_o():
            with scope('own_kv'):
                project(own, *group(n), (KEY, VAL))

        def step_kv(t_):
            with scope(f'par_{t_}'):
                for i in TWO:
                    project(partner, *group(2 * n + i), (t_,))

        def step_q(heads, w):
            with scope(f'que_{w}'):
                queries(heads, w, n)

        def step_out(v, m):
            @pl.when(inner)
            def _():
                k = order(n)

                def wait_for(q):
                    arrived(ws.at[0, pl.ds(0, 128), :], o_recv.at[k, q])

                def quarters():
                    for q in QUARTERS:
                        with scope(f'wait_q{q}'):
                            wait_for(q)
                        o_times(k, v, m, q * 64, 64)
                        if q == 0:
                            ev_y(lo_copy, 1)
                        if q == 2:
                            ev_wo(1)

                def whole():
                    with scope('wait_o'):
                        for q in QUARTERS:
                            wait_for(q)
                    with scope(f'out{v}'):
                        o_times(k, v, m)

                if m == 2:
                    pl.when(n == 0)(quarters)
                    pl.when(n > 0)(whole)
                else:
                    with scope(f'out{v}'):
                        o_times(k, v, m)

        f = functools.partial
        kinds = {'-': lambda: None, 'O': step_o, 'P': f(step_q, own, QUE), 'K': f(step_kv, KEY), 'V': f(step_kv, VAL), 'Q': f(step_q, partner, KEY),
                 'A': lambda: chunk_tiles(n // 4, n % 4, 0), 'B': lambda: chunk_tiles(n // 4, n % 4, 1), 'R': f(step_out, 2, 2), 'L': f(step_out, 1, 1), 'N': f(step_out, 0, 1)}
        choose(code, [kinds[c] for c in KINDS])
        call = functools.partial

        events = {
            'free': [call(signal_ready, 1), call(on, inner, lambda: start(wo_own()))],
            'r0': [call(wait_ready, 0)],
            'r1': [call(wait_ready, 1)],
            'ko': [call(kv_start, kvp_copy, own)],
            'po': [call(kv_wait, kvp_copy, own)],
            'kp': [call(kv_start, kvp_copy, partner)],
            'pp': [call(kv_wait, kvp_copy, partner)],
        }
        for t_, c in enumerate('kvq'):
            events['b' + c] = [call(lq_start, t_)]
            events['l' + c] = [call(ev_last, t_)]
            events['w' + c] = [call(ev_weights, t_)]
            events['z' + c] = [call(ev_z, lq_copy, 2 * t_, 2 * t_ + 1)]
            for i in TWO:
                for e, f in zip('zmfxy', (ev_z, ev_near, ev_far, ev_xy, ev_y)):
                    events[f'{e}{c}{i}'] = [call(f, lq_copy, 2 * t_ + i)]
        for i, vs in enumerate(((2, 3), (1,), (0,))):
            events[f'b{i}'] = [call(lo_start, *vs)]
            for e, f in zip('zmxycwv', (call(ev_z, lo_copy), call(ev_near, lo_copy), call(ev_far, lo_copy), call(ev_y, lo_copy), ev_lb, ev_wo, ev_wo_ready)):
                events[f'{e}{i}'] = [call(on, inner, call(f, *vs))]
        events['v0'] += [call(on, inner, lambda: local(xp.at[1 - side, pl.ds(0, 2)], wo_sem.at[4]))]
        for v in range(4):
            events[f'd{v}'] = [call(on, outer, lambda v=v: lb_z(v).start())]
        for h in HEADS:
            for z in TWO:
                events[f's{h}{z}'] = [kvr_copy(h, z).start]
            events[f'f{h}'] = [call(kv_forward, [h])]
            events[f'g{h}'] = [call(kv_wait, kvf_copy, [h])]
        for k in ROWS:
            for p in TWO:
                events['op'[p] + str(k)] = [call(send_o, (k,), p)]
        def run(names):
            for name in names.split(','):
                where, _, name = name.rpartition(':')
                if where:
                    on(inner if where == 'i' else outer, *events[name])
                else:
                    for c in events[name]:
                        c()

        @pl.when(event > 0)
        def _():
            choose(event - 1, [functools.partial(run, names) for names in EVENTS])
        return carry

    lax.fori_loop(0, len(TABLE), step_body, None)

    all_sent(lq_ref, 0)
    all_sent(lo_ref.at[:, 0, 0], 2)
    all_sent(lb_ref.at[:, 0], 3)
    all_sent(kvp_s, 4)
    all_sent(kvr_s.at[:, pl.ds(0, 2)], 5)
    all_sent(kvr_s.at[:, pl.ds(0, 2)], 6)

    @pl.when(outer)
    def _():
        all_sent(xb, 7)

    @pl.when(inner)
    def _():
        all_sent(lo_ref.at[:, pl.ds(0, 7)], 1)
        with scope('y_sent'):
            all_sent(xp.at[side, :, :, pl.ds(H, 3 * H)], 8)
        local(xp.at[side, :, :, pl.ds(0, H)], sent.at[9])

    for seg in TWO:
        @pl.when(tp != 1 + seg)
        def _(seg=seg):
            with scope(f'recv{seg}'):
                arrived(out_ref.at[seg], y_recv.at[seg])


PROGRAM = (
    'O.i:zk0,i:zk1,bv', 'O.o:zk0', 'O.o:zk1,s00,i:xk0', 'O.o:xk0,i:xk1,o:s01,d3,i:bq', 'O.o:bq,o:xk1,i:yk0,i:zv0', 'O.o:yk0,i:yk1,i:zv1,i:s01',
    'P.o:zv0,o:yk1,lk,o:zv1,d1,i:xv0', 'P.wk,i:xv1', 'K.ko', 'K.o:xv1,o:xv0,i:zq,f0', 'K.i:yv0,i:yv1,b0,b1,r0,po,g0,o:zq',
    'T0.o0,o1,d0,o:yv0,o:yv1,lv,i:mq0,i:mq1,i:fq0,i:fq1', 'P.wv,o:mq0,o:mq1,b2', 'V.z0,o:fq0,o:fq1,kp,o:s10,o:s11', 'V.c0,z1,o:s20,o:s21,yq0,yq1',
    'V.lq,o:s30,o:s31', 'P.free,wq,m0', 'Q.pp,r1,x0,c1,i:s10,i:s11', 'T4.p0,p1,y0,w0,m1,x1,v0', 'R.v1,i:s20,i:s21', 'L', 'Q.f1', 'R', 'L',
    'T5.p2,g1', 'T1.o2,p3,o3,o:f2', 'R.i:s30,i:s31', 'L', 'Q.o:g2', 'Q.i:f2,o:f3', 'T2', 'R.i:g2', 'L', 'T6.p4,o4,p5,o5,o:g3', 'R.i:f3,z2,c2', 'L',
    'T3.i:g3', 'T7.p6,o6,p7,o7', 'R', 'L.m2,x2', 'R.y2', 'L.w2', '-.v2', 'N', 'N', 'N', 'R', 'L', 'N', 'N', 'N', 'N', 'N',
)
KINDS = '-OPKVQABRLN'


def tables():
    table, seen = [], {}
    names = tuple(dict.fromkeys(s.partition('.')[2] for s in PROGRAM if '.' in s))
    for s in PROGRAM:
        name, _, after = s.partition('.')
        kind, n = name[0], seen.get(name[0], 0)
        seen[kind] = n + 1
        if kind == 'T':
            n = int(name[1:])
            kind = 'AB'[n in (2, 3, 4, 5)]
        table.append(KINDS.index(kind) + 16 * n + 256 * (names.index(after) + 1 if after else 0))
    return table, names


TABLE, EVENTS = tables()


def main(bias, x, wk, wv, wq, w_out):
    anyspec = pl.BlockSpec(memory_space=pl.ANY)
    vmem = [((4, B, M), BF), ((B, B), BF), ((2, 8, B, M), BF), ((3, M, H), BF), ((4, 8, B, B), BF), ((4, 12, 2, B, B), BF), ((4, 4, 2, B, B), BF), ((4, 4, 2, B, B), BF),
            ((3072, H), F32), ((M, H), F32), ((64, 128), F32)]
    dma = [(4,), (9,), (5,), (10,), (6, 5), (4, 5), (4, 2), (3, 4), (8, 4), (2,)]
    return pl.pallas_call(
        main_kernel,
        in_specs=[pl.BlockSpec(memory_space=pltpu.SMEM)] + [anyspec] * 5,
        out_specs=[anyspec] * 4,
        out_shape=[jax.ShapeDtypeStruct(s, BF) for s in ((2, 8, B, H), (8, 6, B, B), (4, 8, 2, 64, H), (4, 2, B, H))],
        scratch_shapes=[pltpu.VMEM(*v) for v in vmem] + [pltpu.SemaphoreType.DMA(d) for d in dma] + [pltpu.SemaphoreType.REGULAR((2,))],
        compiler_params=params(collective_id=0, has_side_effects=True),
        cost_estimate=pl.CostEstimate(flops=10**11, bytes_accessed=10**8, transcendentals=0),
        name='main',
    )(bias, x, wk, wv, wq, w_out)[0]


def solution(mesh):
    def device_fn(hidden, w_query, w_key, w_value, w_out, branch_bias):
        return unpermute(main(branch_bias, hidden, w_key, w_value, w_query, w_out))

    return jax.shard_map(device_fn, mesh=mesh, in_specs=(P(('dp', 'sp'), None), P(None, 'tp'), P(None, 'tp'), P(None, 'tp'), P('tp', None), P(None, None)), out_specs=P(('dp', 'sp'), 'tp'), check_vma=False)
```

```python
import functools
import math

import jax
import jax.numpy as jnp
from jax import lax
from jax.experimental import pallas as pl
from jax.experimental.pallas import tpu as pltpu
from jax.sharding import PartitionSpec as P

MESH = pl.DeviceIdType.MESH
BF = jnp.bfloat16
F32 = jnp.float32
B, H, M = 256, 512, 2048
KAPPA = math.log2(math.e) / 16
VMEM = 66_900_000
SLOT = (0, 4, 2, 6, 1, 5, 3, 7)
KEY, VAL, QUE = range(3)
HEADS = range(4)
TWO = range(2)
QUARTERS = range(4)
ROWS = range(8)


def nn(a, b):
    return lax.dot_general(a, b, (((1,), (0,)), ((), ())), preferred_element_type=F32)


def nt(a, b):
    return lax.dot_general(a, b, (((1,), (1,)), ((), ())), preferred_element_type=F32)


def params(**kw):
    return pltpu.CompilerParams(vmem_limit_bytes=VMEM, **kw)


def ds(start, size, align=128):
    return pl.ds(pl.multiple_of(start, align), size)


def part(i, size):
    return slice(i * size, i * size + size)


def phase_matrix(transposed):
    r = lax.broadcasted_iota(jnp.int32, (B, B), int(transposed))
    p = lax.broadcasted_iota(jnp.int32, (B, B), int(not transposed))
    k = r // 32
    return (p == (r % 32) * 8 + k // 2 + 4 * (k % 2)).astype(F32).astype(BF)


def unpermute_kernel(y_ref, o_ref, y_s, o_s, load, store):
    pieces = [(s, j) for s in TWO for j in range(4)]

    def get(i):
        s, j = pieces[i]
        return pltpu.make_async_copy(y_ref.at[s, :, pl.ds(j * 64, 64)], y_s.at[i], load.at[i])

    def put(i):
        return pltpu.make_async_copy(o_s.at[i], o_ref.at[pl.ds(i * H, H)], store.at[i])

    for i in ROWS:
        get(i).start()
    pm = phase_matrix(True)
    for first, last in ((0, 1), (1, 3), (3, 5), (5, 7), (7, 8)):
        group = range(first, last)
        for k in group:
            get(k).wait()
        for k in group:
            for j in TWO:
                o_s[k, part(j, B), :] = nn(pm, y_s[k, :, part(j, 32), :].reshape(B, H)).astype(BF)
        for k in group:
            put(k).start()
    for i in ROWS:
        put(i).wait()


def unpermute(y):
    anyspec = pl.BlockSpec(memory_space=pl.ANY)
    return pl.pallas_call(
        unpermute_kernel,
        in_specs=[anyspec],
        out_specs=anyspec,
        out_shape=jax.ShapeDtypeStruct((2 * M, H), BF),
        scratch_shapes=[pltpu.VMEM((8, 8, 64, H), BF), pltpu.VMEM((8, H, H), BF), pltpu.SemaphoreType.DMA((8,)), pltpu.SemaphoreType.DMA((8,))],
        compiler_params=params(),
        name='unpermute',
    )(y)


def tile_steps(q, wide, narrow, s_ref, n_ref, done):
    st = {}
    logits, sums = [], []

    def add(name, x):
        st[name] = st[name] + x if name in st else x

    for groups, ref in ((wide, s_ref), (narrow, n_ref)):
        off = 0
        for keys, parts in groups:
            def qk(keys=keys, parts=parts, off=off, ref=ref):
                s = nt(keys(), q() if ref is s_ref else q()[:B])
                o = 0
                for _, n, b in parts:
                    piece = s[o:o + n]
                    ref[pl.ds(off + o, n), :] = piece
                    t = jnp.max(piece, axis=0, keepdims=True) * KAPPA
                    if b is not None:
                        t = t + fit(b, t)
                    if ref is n_ref:
                        t = jnp.concatenate([t, st['top'][:, B:]], axis=1)
                    st['top'] = jnp.maximum(st['top'], t) if 'top' in st else t
                    o += n
            logits.append(qk)
            for v, n, b in parts:
                def sv(v=v, n=n, b=b, off=off, ref=ref):
                    top = st['top'] if ref is s_ref else st['top'][:, :B]
                    e = jnp.exp2(ref[pl.ds(off, n), :] * KAPPA - (top if b is None else top - fit(b, top)))
                    name = 'w' if ref is s_ref else 'n'
                    add('l' + name, jnp.sum(e, axis=0, keepdims=True))
                    add('o' + name, nn(v(), e.astype(BF)))
                sums.append(sv)
                off += n

    def finish():
        o, l = st['ow'], st['lw']
        if narrow:
            o = jnp.concatenate([o[:, :B] + st['on'], o[:, B:]], axis=1)
            l = jnp.concatenate([l[:, :B] + st['ln'], l[:, B:]], axis=1)
        done(o / l)

    return logits, sums + [finish]


def fit(b, like):
    return b if b.shape == like.shape else jnp.concatenate([b] * (like.shape[1] // 128), axis=1)


def interleave(a, b):
    i = j = 0
    while i < len(a) or j < len(b):
        if j >= len(b) or (i < len(a) and i * len(b) <= j * len(a)):
            a[i]()
            i += 1
        else:
            b[j]()
            j += 1


def run_tiles(tiles):
    before = []
    for logits, sums in tiles:
        interleave(logits, before)
        before = sums
    interleave([], before)


def choose(x, cases):
    def among(lo, hi):
        mid = (lo + hi) // 2
        if hi - lo == 1:
            cases[lo]()
        else:
            pl.when(x < mid)(lambda: among(lo, mid))
            pl.when(x >= mid)(lambda: among(mid, hi))
    among(0, len(cases))


def on(cond, *calls):
    @pl.when(cond)
    def _():
        for c in calls:
            c()


def scope(name):
    return jax.named_scope(name)


def main_kernel(bias_ref, x_ref, wk_ref, wv_ref, wq_ref, wout_ref, out_ref, lq_ref, lo_ref, lb_ref,
                xb, pm, xp, ws, q_s, kv_s, kvp_s, kvr_s, s_scr, t_scr,
                beta_s, x_sem, w_sem, wo_sem, sent, lq_recv, lo_recv, lb_recv, kv_recv, o_recv, y_recv, ready):
    dp, tp, sp = lax.axis_index('dp'), lax.axis_index('tp'), lax.axis_index('sp')
    idx = dp * 4 + sp
    side = tp // 2
    inner = (tp == 1) | (tp == 2)
    outer = jnp.logical_not(inner)
    W = (wk_ref, wv_ref, wq_ref)
    peer_x, peer_y, peer_c = {'dp': dp ^ 1}, {'sp': sp ^ 2}, {'sp': sp ^ 1}

    def remote(src, dst, ss, rs, dev):
        return pltpu.make_async_remote_copy(src_ref=src, dst_ref=dst, send_sem=ss, recv_sem=rs, device_id=dev, device_id_type=MESH)

    def lq_copy(t, src, dst, dev):
        return remote(lq_ref.at[src, t], lq_ref.at[dst, t], sent.at[0], lq_recv.at[t, min(dst, 4)], dev)

    def lq_z(t):
        return remote(W[t // 2].at[ds(idx * B, B), pl.ds(t % 2 * B, B)], lq_ref.at[0, t], sent.at[0], lq_recv.at[t, 0], {'tp': tp ^ 2})

    def lq_start(t):
        for i in TWO:
            lq_z(2 * t + i).start()

    def lo_copy(v, src, dst, dev):
        return remote(lo_ref.at[v, src], lo_ref.at[v, dst], sent.at[1], lo_recv.at[v, min(dst, 4)], dev)

    def lo_z(v):
        dst = 2 - side
        b = (tp ^ dst) - 2
        return remote(wout_ref.at[ds(idx * 64, 64, 64), ds((dst ^ v) * H, H)], lo_ref.at[v, 0, b], sent.at[2], lo_recv.at[v, 0], {'tp': dst})

    def lb_z(v):
        return remote(wout_ref.at[ds(sp % 2 * B, B), ds((tp ^ 1 ^ v) * H, H)], lb_ref.at[v, sp % 2], sent.at[3], lb_recv.at[v, 0], {'tp': tp ^ 1})

    def lb_core(v):
        return remote(lb_ref.at[v, sp % 2], lb_ref.at[v, sp % 2], sent.at[3], lb_recv.at[v, 1], peer_c)

    def lo_start(*vs):
        for v in vs:
            lo_z(v).start()

    def arrived(ref, sem):
        remote(ref, ref, sent.at[0], sem, peer_c).wait_recv()

    def all_sent(ref, i):
        remote(ref, ref, sent.at[i], sent.at[i], peer_c).wait_send()

    def lo_zwait(v):
        arrived(lo_ref.at[v, 0], lo_recv.at[v, 0])

    def hop(copy, p, i):
        near, far, n = (peer_x, peer_y, 1) if (copy is lo_copy and p == 2) or (copy is lq_copy and p == 5) else (peer_y, peer_x, 2)
        f = 3 - n
        return copy(p, *((0, n, near), (0, f, far), (0, 4, peer_c), (n, 3, far), (n, 4 + n, peer_c), (f, 4 + f, peer_c), (3, 7, peer_c))[i])

    def ev_z(copy, *ps):
        for p in ps:
            with scope(f'z_{copy.__name__}{p}'):
                lq_z(p).wait_recv() if copy is lq_copy else lo_zwait(p)
            hop(copy, p, 0).start()
        for p in ps:
            hop(copy, p, 1).start()
            hop(copy, p, 2).start()

    def ev_near(copy, *ps):
        for p in ps:
            with scope(f'n_{copy.__name__}{p}'):
                hop(copy, p, 0).wait_recv()
            hop(copy, p, 3).start()
            hop(copy, p, 4).start()

    def ev_far(copy, *ps):
        for p in ps:
            with scope(f'f_{copy.__name__}{p}'):
                hop(copy, p, 1).wait_recv()
            hop(copy, p, 5).start()

    def ev_xy(copy, *ps):
        ev_near(copy, *ps)
        ev_far(copy, *ps)

    def ev_y(copy, *ps):
        for p in ps:
            with scope(f'y_{copy.__name__}{p}'):
                hop(copy, p, 3).wait_recv()
            hop(copy, p, 6).start()
            if copy is lq_copy and p >= 2:
                start(w_load(p, SLOT[:4]))

    def ev_done(copy, *ps):
        for p in ps:
            with scope(f'c_{copy.__name__}{p}'):
                if copy is lq_copy:
                    arrived(lq_ref.at[pl.ds(4, 4), p], lq_recv.at[p, 4])
                else:
                    arrived(lo_ref.at[p, pl.ds(4, 4)], lo_recv.at[p, 4])

    def w_load(p, slots):
        return [pltpu.make_async_copy(lq_ref.at[SLOT.index(m), p], ws.at[p // 2 % 2, ds((idx ^ m) * B, B), pl.ds(p % 2 * B, B)], w_sem.at[p]) for m in slots]

    def own_load(t):
        return pltpu.make_async_copy(W[t], ws.at[t], w_sem.at[6 + t])

    def start(copies):
        for c in copies:
            c.start()

    def wait(copies):
        for c in copies:
            c.wait()

    def ev_last(t):
        pieces = [2 * t + i for i in TWO]
        ev_done(lq_copy, *pieces)
        for p in pieces:
            start(w_load(p, SLOT[4:] if t else SLOT))

    def local(ref, sem):
        pltpu.make_async_copy(ref, ref, sem).wait()

    def ev_weights(t):
        with scope(f'load{t}'):
            for i in TWO:
                local(ws.at[t % 2, :, pl.ds(i * B, B)], w_sem.at[2 * t + i])

    def ev_wo(*vs):
        ev_done(lo_copy, *vs)
        for v in vs:
            lb_core(v).wait_recv()
        start(wo_load(*vs))

    def ev_wo_ready(*vs):
        with scope(f'wo{vs[0]}'):
            for v in vs:
                local(xp.at[1 - side, pl.ds(2, 6), :, pl.ds((v ^ 2) * H, H)], wo_sem.at[v])

    def ev_lb(*vs):
        for v in vs:
            with scope(f'lb{v}'):
                lb_z(v).wait_recv()
            lb_core(v).start()

    wo = xp.at[1 - side]

    def wo_own():
        return [pltpu.make_async_copy(wout_ref.at[pl.ds(r * B, B), pl.ds(c * H, H)], xp.at[1 - side, r, :, ds((c ^ tp ^ 2) * H, H)], wo_sem.at[4])
                for r in TWO for c in range(4)]

    def wo_load(*vs):
        out = []
        for v in vs:
            cols = pl.ds((v ^ 2) * H, H)
            for s, m in enumerate(SLOT):
                row = (idx ^ m) * 64
                for b in TWO:
                    out.append(pltpu.make_async_copy(lo_ref.at[v, s, b], xp.at[1 - side, 4 + 2 * b + row // B, ds(row % B, 64, 64), cols], wo_sem.at[v]))
            for r in TWO:
                out.append(pltpu.make_async_copy(lb_ref.at[v, r], xp.at[1 - side, 2 + r, :, cols], wo_sem.at[v]))
        return out

    def kvp_copy(h, s):
        return remote(kv_s.at[h, pl.ds(8 * s, 2)], kvp_s.at[h, pl.ds(2 * s, 2)], sent.at[4], kv_recv.at[0, h], peer_c)

    def kvr_copy(h, s):
        return remote(kv_s.at[h, 8 * s], kvr_s.at[h, s], sent.at[5], kv_recv.at[1, h], peer_y)

    def kvf_copy(h, s):
        return remote(kvr_s.at[h, s], kvr_s.at[h, 2 + s], sent.at[6], kv_recv.at[2, h], peer_c)

    def kv_start(copy, heads):
        for h in heads:
            for s in TWO:
                copy(h, s).start()

    def kv_wait(copy, heads):
        with scope(f'w_{copy.__name__}{heads[0]}'):
            for h in heads:
                i = (kvp_copy, kvr_copy, kvf_copy).index(copy)
                arrived((kvp_s.at[h], kvr_s.at[h, pl.ds(0, 2)], kvr_s.at[h, pl.ds(2, 2)])[i], kv_recv.at[i, h])

    def kv_forward(heads):
        kv_wait(kvr_copy, heads)
        kv_start(kvf_copy, heads)

    def reverse(i):
        return (i % 2) * 2 + i // 2

    def order(n):
        return 2 * reverse(n % 4) + ((n // 4) ^ side)

    def o_at(k, p, theirs, col, size, row=0, rows=B):
        if p:
            return ws.at[1 + theirs, ds(k * B + row, rows, 64), ds(col, size)]
        return xb.at[k // 2, pl.ds(row, rows), ds((k % 2) * 1024 + theirs * H + col, size)]

    def o_copy(k, p, q):
        row = q * 64
        return remote(o_at(k, p, 0, 0, H, row, 64), o_at(k, p, 1, 0, H, row, 64), sent.at[7], o_recv.at[k, q], {'tp': tp ^ 1})

    def o_times(k, v, n, row=0, rows=B):
        cols = pl.ds((v ^ 2) * H, n * H)
        y = nn(xb[k // 2, pl.ds(row, rows), ds((k % 2) * 1024, 1024)], wo[0:4, :, cols].reshape(1024, n * H))
        for i in TWO:
            y = y + nn(ws[1 + i, ds(k * B + row, rows, 64), :], wo[part(2 + i, 2), :, cols].reshape(H, n * H))
        y = y.astype(BF)
        for i in range(n):
            y_src(k, v + i, row, rows)[...] = y[:, part(i, H)]
            y_copy(k, v + i, side, row, rows).start() if v else y_local(k).start()

    def y_src(k, v, row=0, rows=B):
        return xp.at[side, k, pl.ds(row, rows), pl.ds(v * H, H)]

    def y_copy(k, v, seg, row, rows):
        return remote(y_src(k, v, row, rows), out_ref.at[seg, k, pl.ds(row, rows)], sent.at[8], y_recv.at[seg], {'tp': tp ^ v})

    def y_local(k):
        return pltpu.make_async_copy(y_src(k, 0), out_ref.at[side, k], sent.at[9])

    def x_copy(j):
        return pltpu.make_async_copy(x_ref.at[ds(j * B, B), :], xb.at[lax.rem(j, 4)], x_sem.at[lax.rem(j, 4)])

    for j in range(4):
        x_copy(j).start()
    barrier = pltpu.get_barrier_semaphore()
    peers = [{'tp': tp ^ 1}, {'tp': tp ^ 2}, {'tp': tp ^ 3}, peer_x, peer_y, peer_c]
    for dev in peers:
        pl.semaphore_signal(barrier, inc=1, device_id=dev, device_id_type=MESH)
    for t in range(3):
        own_load(t).start()

    pm[...] = phase_matrix(False)

    def permute_body(j, carry):
        x_copy(j).wait()
        y = nn(pm[...], xb[lax.rem(j, 4)]).astype(BF).reshape(8, 32, M)
        xp[j // 8, :, ds(lax.rem(j, 8) * 32, 32, 32), :] = y
        pl.when(j < 12)(lambda: x_copy(j + 4).start())

        @pl.when(j == 2)
        def _():
            with scope('barrier'):
                pl.semaphore_wait(barrier, len(peers))
            lq_start(KEY)
            on(outer, lb_z(2).start)
        return carry

    with scope('permute'):
        lax.fori_loop(0, 16, permute_body, None)

    for h in HEADS:
        column = 2 * (tp ^ (h // 2 * 2)) + h % 2
        for i, branches in enumerate(('0', '01', '1', '012', '12', '2', '0123', '123', '23', '3')):
            rows = [jnp.full((1, 128), bias_ref[j, column], F32) for j in map(int, branches)]
            m = functools.reduce(jnp.maximum, rows)
            beta_s[pl.ds(h * 16 + i, 1), :] = (m + jnp.log(sum(jnp.exp(r - m) for r in rows))) * math.log2(math.e)

    def signal_ready(i):
        pl.when(inner)(lambda: pl.semaphore_signal(ready.at[i], inc=1, device_id={'tp': tp ^ 1}, device_id_type=MESH))

    def wait_ready(i):
        with scope(f'ready{i}'):
            pl.when(outer)(lambda: pl.semaphore_wait(ready.at[i], 1))

    signal_ready(0)

    def group(g):
        low = g < 4
        return jnp.where(low, g & 1, 0), jnp.where(low, g // 2, g - 2)

    def head_number(h):
        return 2 * (tp ^ (h // 2 * 2)) + h % 2

    def project(heads, sigma, pair, kinds):
        for h in heads:
            t = head_number(h) + reverse(pair)
            x, swap = xp[side ^ sigma, pl.ds(2 * (t & 3), 2)].reshape(H, M), (t & 7) >> 2
            for t in kinds:
                y = nn(x, ws[t, :, part(h % 2, B)])
                for j in TWO:
                    piece = y[part(j, B)]
                    kv_s[h, 8 * sigma + 2 * pair + (j ^ swap), t] = (piece.T if t == VAL else piece).astype(BF)

    def phases_of(j):
        return [j % 2 + 2 * i for i in TWO], (j // 2) ^ side

    def rank_of(phase, h):
        rel = (phase - head_number(h)) & 7
        return (rel & 1) * 4 + ((rel >> 1) & 1) * 2 + (rel >> 2)

    def queries(heads, w, j):
        phases, half = phases_of(j)
        x = jnp.concatenate([xp[side, 2 * f + half] for f in phases])
        for h in heads:
            y = nn(x, ws[w, :, part(h % 2, B)]).astype(BF)
            for i, f in enumerate(phases):
                q_s[h, rank_of(f + 4 * half, h)] = y[part(i, B)]

    with scope('own_w'):
        for t in range(3):
            own_load(t).wait()
    own, partner = HEADS[:2], HEADS[2:]

    def mix(b, c):
        return jnp.concatenate([b, b, c, c], axis=1)

    def keys_of(ref, h, i, weights):
        parts = []
        n = 0
        for count, b in weights:
            def values(i=i + n, count=count):
                v = [ref[h, i + j, VAL] for j in range(count)]
                return v[0] if count == 1 else jnp.concatenate(v, axis=1)
            parts.append((values, count * B, b))
            n += count
        return (lambda: ref[h, i:i + n, KEY].reshape(n * B, B)), parts

    def chunk_tiles(p, j, kind):
        both_phases, half = phases_of(j)

        def put(h, phase, ot):
            k = 2 * (phase & 3) + half
            y = ot.T.astype(BF)
            for i in TWO:
                pl.when(p == i)(lambda i=i: o_at(k, i, 0, (h % 2) * B, B).__setitem__(..., y))

        def tile(h, phases, ranks, wide, narrow, s_ref, n_ref):
            def done(ot):
                for i, phase in enumerate(phases):
                    put(h, phase, ot[:, part(i, B)])
            return tile_steps(lambda: jnp.concatenate([q_s[h, r] for r in ranks]), wide, narrow, s_ref, n_ref, done)

        h = 2 * p + (j % 2) ^ 1
        rest = tile(h, both_phases, [rank_of(f + 4 * half, h) for f in both_phases], [keys_of(kv_s, h, i, [(1, None)]) for i in ROWS], [], t_scr, None)
        h = 2 * p + (j % 2)
        a = head_number(h)
        b0, b01, b1, b012, b12, b2, b0123, b123, b23, b3 = [beta_s[pl.ds(h * 16 + i, 1), :] for i in range(10)]
        phases = [a & 3, (a & 3) ^ 2]
        both = [keys_of(kv_s, h, i, [(2, b)] * n) for i, b, n in ((2, b01, 1), (4, b0, 2), (10, b1, 1))]
        if kind == 0:
            both += [keys_of(kv_s, h, 0, [(1, mix(b0123, b01)), (1, mix(b012, b01))]), keys_of(kv_s, h, 8, [(1, mix(b123, b1)), (1, mix(b12, b1))])]
            first = [keys_of(kvp_s, h, i, [(1, b23), (1, b2)]) for i in (0, 2)] + [keys_of(kvr_s, h, i, [(2, b3)]) for i in (0, 2)]
        else:
            both += [keys_of(kv_s, h, 0, [(2, mix(b012, b01))]), keys_of(kv_s, h, 8, [(2, mix(b12, b1))])]
            first = [keys_of(kvp_s, h, i, [(2, b2)]) for i in (0, 2)]
        with scope(f'tile{kind}'):
            run_tiles([rest, tile(h, phases, [kind, rank_of(phases[1] + 4 * half, h)], both, first, s_scr, t_scr.at[:, pl.ds(0, B)])])

    def send_o(ks, p):
        @pl.when(outer)
        def _():
            for k in ks:
                for q in QUARTERS:
                    o_copy(order(k), p, q).start()

    def step_body(t, carry):
        packed = functools.reduce(lambda x, i: jnp.where(t == i, TABLE[i], x), range(len(TABLE)), 0)
        code, n, event = packed % 16, packed // 16 % 16, packed // 256

        def step_o():
            with scope('own_kv'):
                project(own, *group(n), (KEY, VAL))

        def step_kv(t_):
            with scope(f'par_{t_}'):
                for i in TWO:
                    project(partner, *group(2 * n + i), (t_,))

        def step_q(heads, w):
            with scope(f'que_{w}'):
                queries(heads, w, n)

        def step_out(v, m):
            @pl.when(inner)
            def _():
                k = order(n)

                def wait_for(q):
                    arrived(ws.at[0, pl.ds(0, 128), :], o_recv.at[k, q])

                def quarters():
                    for q in QUARTERS:
                        with scope(f'wait_q{q}'):
                            wait_for(q)
                        o_times(k, v, m, q * 64, 64)
                        if q == 0:
                            ev_y(lo_copy, 1)
                        if q == 2:
                            ev_wo(1)

                def whole():
                    with scope('wait_o'):
                        for q in QUARTERS:
                            wait_for(q)
                    with scope(f'out{v}'):
                        o_times(k, v, m)

                if m == 2:
                    pl.when(n == 0)(quarters)
                    pl.when(n > 0)(whole)
                else:
                    with scope(f'out{v}'):
                        o_times(k, v, m)

        f = functools.partial
        kinds = {'-': lambda: None, 'O': step_o, 'P': f(step_q, own, QUE), 'K': f(step_kv, KEY), 'V': f(step_kv, VAL), 'Q': f(step_q, partner, KEY),
                 'A': lambda: chunk_tiles(n // 4, n % 4, 0), 'B': lambda: chunk_tiles(n // 4, n % 4, 1), 'R': f(step_out, 2, 2), 'L': f(step_out, 1, 1), 'N': f(step_out, 0, 1)}
        choose(code, [kinds[c] for c in KINDS])
        call = functools.partial

        events = {
            'free': [call(signal_ready, 1), call(on, inner, lambda: start(wo_own()))],
            'r0': [call(wait_ready, 0)],
            'r1': [call(wait_ready, 1)],
            'ko': [call(kv_start, kvp_copy, own)],
            'po': [call(kv_wait, kvp_copy, own)],
            'kp': [call(kv_start, kvp_copy, partner)],
            'pp': [call(kv_wait, kvp_copy, partner)],
        }
        for t_, c in enumerate('kvq'):
            events['b' + c] = [call(lq_start, t_)]
            events['l' + c] = [call(ev_last, t_)]
            events['w' + c] = [call(ev_weights, t_)]
            events['z' + c] = [call(ev_z, lq_copy, 2 * t_, 2 * t_ + 1)]
            for i in TWO:
                for e, f in zip('zmfxy', (ev_z, ev_near, ev_far, ev_xy, ev_y)):
                    events[f'{e}{c}{i}'] = [call(f, lq_copy, 2 * t_ + i)]
        for i, vs in enumerate(((2, 3), (1,), (0,))):
            events[f'b{i}'] = [call(lo_start, *vs)]
            for e, f in zip('zmxycwv', (call(ev_z, lo_copy), call(ev_near, lo_copy), call(ev_far, lo_copy), call(ev_y, lo_copy), ev_lb, ev_wo, ev_wo_ready)):
                events[f'{e}{i}'] = [call(on, inner, call(f, *vs))]
        events['v0'] += [call(on, inner, lambda: local(xp.at[1 - side, pl.ds(0, 2)], wo_sem.at[4]))]
        for v in range(4):
            events[f'd{v}'] = [call(on, outer, lambda v=v: lb_z(v).start())]
        for h in HEADS:
            for z in TWO:
                events[f's{h}{z}'] = [kvr_copy(h, z).start]
            events[f'f{h}'] = [call(kv_forward, [h])]
            events[f'g{h}'] = [call(kv_wait, kvf_copy, [h])]
        for k in ROWS:
            for p in TWO:
                events['op'[p] + str(k)] = [call(send_o, (k,), p)]
        def run(names):
            for name in names.split(','):
                where, _, name = name.rpartition(':')
                if where:
                    on(inner if where == 'i' else outer, *events[name])
                else:
                    for c in events[name]:
                        c()

        @pl.when(event > 0)
        def _():
            choose(event - 1, [functools.partial(run, names) for names in EVENTS])
        return carry

    lax.fori_loop(0, len(TABLE), step_body, None)

    all_sent(lq_ref, 0)
    all_sent(lo_ref.at[:, 0, 0], 2)
    all_sent(lb_ref.at[:, 0], 3)
    all_sent(kvp_s, 4)
    all_sent(kvr_s.at[:, pl.ds(0, 2)], 5)
    all_sent(kvr_s.at[:, pl.ds(0, 2)], 6)

    @pl.when(outer)
    def _():
        all_sent(xb, 7)

    @pl.when(inner)
    def _():
        all_sent(lo_ref.at[:, pl.ds(0, 7)], 1)
        with scope('y_sent'):
            all_sent(xp.at[side, :, :, pl.ds(H, 3 * H)], 8)
        local(xp.at[side, :, :, pl.ds(0, H)], sent.at[9])

    for seg in TWO:
        @pl.when(tp != 1 + seg)
        def _(seg=seg):
            with scope(f'recv{seg}'):
                arrived(out_ref.at[seg], y_recv.at[seg])


PROGRAM = (
    'O.i:zk0,i:zk1,bv', 'O.o:zk0', 'O.o:zk1,s00,i:xk0', 'O.o:xk0,i:xk1,o:s01,d3,i:bq', 'O.o:bq,o:xk1,i:yk0,i:zv0', 'O.o:yk0,i:yk1,i:zv1,i:s01',
    'P.o:zv0,o:yk1,lk,o:zv1,d1,i:xv0', 'P.wk,i:xv1', 'K.ko', 'K.o:xv0,i:zq,f0', 'K.o:xv1,i:yv0,i:yv1,b0,b1,r0,po,g0,o:zq',
    'T0.o0,o1,d0,o:yv0,o:yv1,lv,mq0,i:mq1,i:fq0,i:fq1', 'P.wv,o:mq1,b2', 'V.z0,o:fq0,o:fq1,kp,o:s10,o:s11', 'V.c0,z1,o:s20,o:s21,yq0,yq1',
    'V.lq,o:s30,o:s31', 'P.free,wq,m0', 'Q.pp,r1,x0,c1,i:s10,i:s11', 'T4.p0,p1,y0,w0,m1,x1,v0', 'R.v1,i:s20,i:s21', 'L', 'Q.f1', 'R', 'L',
    'T5.p2,g1', 'T1.o2,p3,o3,o:f2', 'R.i:s30,i:s31', 'L', 'Q.o:g2', 'Q.i:f2,o:f3', 'T2', 'R.i:g2', 'L', 'T6.p4,o4,p5,o5,o:g3', 'R.i:f3,z2,c2', 'L',
    'T3.i:g3', 'T7.p6,o6,p7,o7', 'R', 'L.m2,x2', 'R.y2', 'L.w2', '-.v2', 'N', 'N', 'N', 'R', 'L', 'N', 'N', 'N', 'N', 'N',
)
KINDS = '-OPKVQABRLN'


def tables():
    table, seen = [], {}
    names = tuple(dict.fromkeys(s.partition('.')[2] for s in PROGRAM if '.' in s))
    for s in PROGRAM:
        name, _, after = s.partition('.')
        kind, n = name[0], seen.get(name[0], 0)
        seen[kind] = n + 1
        if kind == 'T':
            n = int(name[1:])
            kind = 'AB'[n in (2, 3, 4, 5)]
        table.append(KINDS.index(kind) + 16 * n + 256 * (names.index(after) + 1 if after else 0))
    return table, names


TABLE, EVENTS = tables()


def main(bias, x, wk, wv, wq, w_out):
    anyspec = pl.BlockSpec(memory_space=pl.ANY)
    vmem = [((4, B, M), BF), ((B, B), BF), ((2, 8, B, M), BF), ((3, M, H), BF), ((4, 8, B, B), BF), ((4, 12, 2, B, B), BF), ((4, 4, 2, B, B), BF), ((4, 4, 2, B, B), BF),
            ((3072, H), F32), ((M, H), F32), ((64, 128), F32)]
    dma = [(4,), (9,), (5,), (10,), (6, 5), (4, 5), (4, 2), (3, 4), (8, 4), (2,)]
    return pl.pallas_call(
        main_kernel,
        in_specs=[pl.BlockSpec(memory_space=pltpu.SMEM)] + [anyspec] * 5,
        out_specs=[anyspec] * 4,
        out_shape=[jax.ShapeDtypeStruct(s, BF) for s in ((2, 8, B, H), (8, 6, B, B), (4, 8, 2, 64, H), (4, 2, B, H))],
        scratch_shapes=[pltpu.VMEM(*v) for v in vmem] + [pltpu.SemaphoreType.DMA(d) for d in dma] + [pltpu.SemaphoreType.REGULAR((2,))],
        compiler_params=params(collective_id=0, has_side_effects=True),
        cost_estimate=pl.CostEstimate(flops=10**11, bytes_accessed=10**8, transcendentals=0),
        name='main',
    )(bias, x, wk, wv, wq, w_out)[0]


def solution(mesh):
    def device_fn(hidden, w_query, w_key, w_value, w_out, branch_bias):
        return unpermute(main(branch_bias, hidden, w_key, w_value, w_query, w_out))

    return jax.shard_map(device_fn, mesh=mesh, in_specs=(P(('dp', 'sp'), None), P(None, 'tp'), P(None, 'tp'), P(None, 'tp'), P('tp', None), P(None, None)), out_specs=P(('dp', 'sp'), 'tp'), check_vma=False)
```
